32 devices in a mesh: dp: 4 (over z), expert: 8 (over y, x, core).
Axes of the slice: x: 2, y: 2, z: 4, core: 2. Of those that a mesh axis runs over, the one named last changes fastest.
Arguments:
- inputs: bfloat16 [4096, 2048], P(('dp', 'expert')), may hold values from -6 to 6
- segments: int32 [32, 128], P(('dp', 'expert')), may hold values from 0 to 3, never falling along the last dimension, each value on 1 to 64 neighbouring positions
- routes: int32 [4096, 8], P(('dp', 'expert')), may hold values from 0 to 15, all different within a row; in each aligned block of 128 rows (0 to 127, 128 to 255, ...) at most 96 rows name the same one
- w_qkv: bfloat16 [2048, 3, 2048], P('dp'), may hold values from -0.125 to 0.125
- w_out: bfloat16 [2048, 2048], P('dp'), may hold values from -0.5 to 0.5
- w_router: bfloat16 [2048, 16], P('dp'), may hold values from -0.375 to 0.375
- gains: bfloat16 [2048, 4], P('dp'), may hold values from 0.5 to 1.5
- w_gate: bfloat16 [16, 2048, 1024], P('expert'), may hold values from -0.125 to 0.125
- w_up: bfloat16 [16, 2048, 1024], P('expert'), may hold values from -0.125 to 0.125
- w_down: bfloat16 [16, 1024, 2048], P('expert'), may hold values from -0.375 to 0.375
- cotangent: bfloat16 [4096, 2048], P(('dp', 'expert')), may hold values from -6 to 6
Outputs:
- output: bfloat16 [4096, 2048], P(('dp', 'expert'))
- grad_inputs: bfloat16 [4096, 2048], P(('dp', 'expert'))
- grad_w_qkv: float32 [2048, 3, 2048], P('dp')
- grad_w_out: float32 [2048, 2048], P('dp')
- grad_w_router: float32 [2048, 16], P('dp')
- grad_gains: float32 [2048, 4], P('dp')
- grad_w_gate: float32 [16, 2048, 1024], P('expert', 'dp')
- grad_w_up: float32 [16, 2048, 1024], P('expert', 'dp')
- grad_w_down: float32 [16, 1024, 2048], P('expert', 'dp')
The draws below stay inside these ranges and needn't reach their ends.
Inputs may be any that keep to these rules, and one draw needn't show every extreme that they name: `routes`: each token names 8 different experts. Within the 128 rows of one device no expert is named more than 96 times, and in every draw some device's rows name some expert exactly 96 times. `segments`: segment numbers never fall along a sequence.
All inputs are finite; a program needn't handle non-finite values.
Results may differ from the reference program's by a relative error of at most 0.018.
The reference program's roundings to bfloat16 on the way count: a program that leaves them out, or rounds other values in their place, can miss the bound.
Values may be sent and summed in bfloat16 or wider, within the bound.
A program may use at most 512 MiB of HBM per device.

```python
import math
import jax
import jax.numpy as jnp
import numpy as np
from jax import lax

D = 2048
HD = 128
FF = 1024
TOP = 8
SEQ = 128
EXPERTS = 16
TOK_DEV = 128
SEQS = 32
TOKENS = 4096
CAP = 96
DEVICES = 32


def block_levels(stream_key, extent, cuts, smallest, high):
    gain, own = 1.0, jax.random.fold_in(stream_key, 6)
    for dim, blocks in cuts:
        heights = jnp.exp(jax.random.uniform(jax.random.fold_in(own, dim), (blocks,), jnp.float32, smallest / len(cuts), high / len(cuts)))
        gain = gain * jnp.repeat(heights, extent[dim] // blocks).reshape([-1 if axis == dim else 1 for axis in range(len(extent))])
    return gain


def split_up(amount, total, most, slope):
    portions = [(1 << 20) // math.isqrt(rank ** slope) + 1 for rank in range(2, amount + 1)]
    rest, counts = total - most - (amount - 1), [1] * (amount - 1)
    while rest > 0:
        free = [i for i in range(amount - 1) if counts[i] < most]
        pool, remaining = sum([portions[i] for i in free]), rest
        for i in free:
            extra = min(most - counts[i], max(1, remaining * portions[i] // pool), rest)
            counts[i] = counts[i] + extra
            rest = rest - extra
    return np.array([most] + counts)


def ragged(own_key, amount, total, bound, lean):
    if amount == 2:
        one = jax.random.randint(own_key, (), max(1, total - bound), min(bound, total - 1) + 1)
        return jnp.stack([one, total - one])
    lengths = jnp.asarray(split_up(amount, total, bound, lean), jnp.int32)
    twos = (amount - 1) // 2
    source_of, sink = lengths[1:1 + 2 * twos:2], lengths[2:2 + 2 * twos:2]
    slack = jnp.minimum(source_of - 1, bound - sink)
    passed = jax.random.randint(jax.random.fold_in(own_key, 1), (twos,), 0, 1 << 20) % (slack + 1)
    lengths = lengths.at[1:1 + 2 * twos:2].set(source_of - passed).at[2:2 + 2 * twos:2].set(sink + passed)
    return lengths[jax.random.permutation(jax.random.fold_in(own_key, 2), amount)]


def assign_block(own_key, own, number, rows, count, top, limit, lean):
    order = jax.random.permutation(own_key, count)
    heavy_load, usual = portions_of(count, rows * top, limit, lean, True), portions_of(count, rows * top, limit, lean, False)
    places = jnp.arange(count)

    def named(tallies, turn):
        used = int((tallies > 0).sum())
        fixed = max(1, used // 4)
        shifted = fixed + (places - fixed + turn * (used - fixed)) % max(1, count - fixed)
        return jnp.zeros((count,), jnp.int32).at[order[jnp.where(places < fixed, places, shifted)]].set(jnp.asarray(tallies, jnp.int32))

    tallies = jnp.where(number % 4 == 0, named(heavy_load, number // 4), named(usual, number - number // 4 - 1))
    mixed = jax.random.permutation(jax.random.fold_in(own, 3), count)
    source_of, taker = mixed[0:count // 2 * 2:2], mixed[1:count // 2 * 2:2]
    slack = jnp.minimum(tallies[source_of] - 1, limit - tallies[taker]) // 2
    slack = jnp.where((source_of == order[0]) | (taker == order[0]) | (tallies[taker] == 0), 0, jnp.maximum(slack, 0))
    shifted = jax.random.randint(jax.random.fold_in(own, 4), (count // 2,), 0, 1 << 20) % (slack + 1)
    tallies = tallies.at[source_of].add(-shifted).at[taker].add(shifted)
    members = jnp.searchsorted(jnp.cumsum(tallies), jnp.arange(rows * top), side="right").astype(jnp.int32)
    grid = members.reshape(top, rows).T
    grid = grid[jax.random.permutation(jax.random.fold_in(own, 1), rows)]
    turn = jax.random.randint(jax.random.fold_in(own, 2), (rows, 1), 0, top)
    return jnp.take_along_axis(grid, (jnp.arange(top)[None, :] + turn) % top, axis=1)


def portions_of(count, total, bound, skew, full):
    weights = [(1 << 20) // math.isqrt(grade ** skew) + 1 for grade in range(1, count + 1)]
    largest = bound if full else min(bound, max(-(-total // count), total * weights[0] // sum(weights)))
    least = 1 if total - largest >= count - 1 else 0
    counts, surplus = [largest] + [least] * (count - 1), total - largest - least * (count - 1)
    while surplus > 0:
        movable = [i for i in range(1, count) if counts[i] < largest] or [i for i in range(1, count) if counts[i] < bound]
        pool, budget = sum([weights[i] for i in movable]), surplus
        for i in movable:
            more = min(bound - counts[i], max(1, budget * weights[i] // pool), surplus)
            counts[i] = counts[i] + more
            surplus = surplus - more
    return np.array(counts)


def bell_draw(rng, dims, scale, most, pieces=(), held_as=jnp.bfloat16):
    gain = block_levels(rng, dims, pieces, -0.22, 0.18) if pieces else 1.0
    values = jax.random.normal(rng, dims, jnp.float32) * scale * gain
    return jnp.minimum(jnp.maximum(values, -most), most).astype(held_as)


def setup_inputs(seed: int = 0) -> dict:
    key_of = jax.random.split(jax.random.key(seed), 12)
    inputs = bell_draw(key_of[0], (TOKENS, D), 1.0, 6.0, ((0, 32),))
    segments = jax.vmap(lambda own: jnp.searchsorted(jnp.cumsum(ragged(own, 4, SEQ, SEQ // 2, 1)), jnp.arange(SEQ), side="right"))(jax.random.split(key_of[1], SEQS)).reshape((SEQS, SEQ)).astype(jnp.int32)
    routes_keys = jax.random.split(jax.random.fold_in(key_of[2], 1), TOKENS // TOK_DEV)
    routes_turns = jax.random.permutation(jax.random.fold_in(key_of[2], 3), TOKENS // TOK_DEV)
    routes = jax.vmap(lambda own, number: assign_block(jax.random.fold_in(key_of[2], 2), own, number, TOK_DEV, EXPERTS, TOP, CAP, 2))(routes_keys, routes_turns).reshape((TOKENS, TOP))
    w_qkv = bell_draw(key_of[3], (D, 3, D), D ** -0.5, 0.125, ((0, 4),))
    w_out = bell_draw(key_of[4], (D, D), (D // 16) ** -0.5, 0.5, ((0, 4),))
    w_router = bell_draw(key_of[5], (D, EXPERTS), (D // 9) ** -0.5, 0.375, ((0, 4),))
    gains = jnp.clip(1.0 + 0.1 * jax.random.normal(key_of[6], (D, 4), jnp.float32), 0.5, 1.5).astype(jnp.bfloat16)
    w_gate = bell_draw(key_of[7], (EXPERTS, D, FF), D ** -0.5, 0.125, ((0, 8),))
    w_up = bell_draw(key_of[8], (EXPERTS, D, FF), D ** -0.5, 0.125, ((0, 8),))
    w_down = bell_draw(key_of[9], (EXPERTS, FF, D), (FF // 4) ** -0.5, 0.375, ((0, 8),))
    cotangent = bell_draw(key_of[10], (TOKENS, D), 1.0, 6.0, ((0, 32),))
    return {"inputs": inputs, "segments": segments, "routes": routes, "w_qkv": w_qkv, "w_out": w_out, "w_router": w_router, "gains": gains, "w_gate": w_gate, "w_up": w_up, "w_down": w_down, "cotangent": cotangent}


eps_norm = 1e-05
rope_base = 10000.0
masked_score = -1e+30

def rms_forward(values, gain_col):
    inv_rms = lax.rsqrt(lax.optimization_barrier(jnp.mean(values * values, axis=-1, keepdims=True)) + eps_norm)
    return (values * inv_rms * gain_col, inv_rms)

def rms_backward(values, inv_rms, gain_col, grad_out):
    normed = values * inv_rms
    grad_gain = lax.optimization_barrier(jnp.sum(grad_out * normed, axis=0))
    scaled = grad_out * gain_col
    grad_values = inv_rms * (scaled - normed * lax.optimization_barrier(jnp.mean(scaled * normed, axis=-1, keepdims=True)))
    return (grad_values, grad_gain)

def rope_tables(length, head_width):
    half_width = head_width // 2
    freqs = jnp.exp(-jnp.log(rope_base) * (2.0 * jnp.arange(half_width, dtype=jnp.float32) / head_width))
    angles = jnp.arange(length, dtype=jnp.float32)[:, None] * freqs[None, :]
    return (jnp.cos(angles)[:, None, :], jnp.sin(angles)[:, None, :])

def rotate(values, cos_tab, sin_tab):
    half_width = values.shape[-1] // 2
    first_half = values[..., :half_width]
    second_half = values[..., half_width:]
    return jnp.concatenate([first_half * cos_tab - second_half * sin_tab, second_half * cos_tab + first_half * sin_tab], axis=-1)

def rotate_back(values, cos_tab, sin_tab):
    half_width = values.shape[-1] // 2
    first_half = values[..., :half_width]
    second_half = values[..., half_width:]
    return jnp.concatenate([first_half * cos_tab + second_half * sin_tab, second_half * cos_tab - first_half * sin_tab], axis=-1)

def attend_scores(query_rot, key_rot, seg_ids):
    places = jnp.arange(seg_ids.shape[0], dtype=jnp.int32)
    allowed = (places[:, None] >= places[None, :]) & (seg_ids[:, None] == seg_ids[None, :])
    scores = jnp.einsum('qhd,khd->hqk', query_rot.astype(jnp.float32), key_rot.astype(jnp.float32))
    scores = scores * query_rot.shape[-1] ** (-0.5)
    return jnp.where(allowed[None], scores, masked_score)

def attend_forward(query_rot, key_rot, value_bf, seg_ids):
    scores = attend_scores(query_rot, key_rot, seg_ids)
    row_max = lax.optimization_barrier(jnp.max(scores, axis=-1, keepdims=True))
    log_total = row_max + jnp.log(lax.optimization_barrier(jnp.sum(jnp.exp(scores - row_max), axis=-1, keepdims=True)))
    weights_bf = jnp.exp(scores - log_total).astype(jnp.bfloat16)
    mixed_heads = jnp.einsum('hqk,khd->qhd', weights_bf.astype(jnp.float32), value_bf.astype(jnp.float32))
    return (mixed_heads.astype(jnp.bfloat16), log_total)

def attend_backward(query_rot, key_rot, value_bf, seg_ids, log_total, grad_heads):
    scores = attend_scores(query_rot, key_rot, seg_ids)
    probs_full = jnp.exp(scores - log_total)
    probs_bf = probs_full.astype(jnp.bfloat16)
    grad_value = jnp.einsum('hqk,qhd->khd', probs_bf.astype(jnp.float32), grad_heads.astype(jnp.float32)).astype(jnp.bfloat16)
    grad_probs = jnp.einsum('qhd,khd->hqk', grad_heads.astype(jnp.float32), value_bf.astype(jnp.float32))
    delta_rows = lax.optimization_barrier(jnp.sum(probs_full * grad_probs, axis=-1, keepdims=True))
    grad_scores = (probs_full * (grad_probs - delta_rows) * query_rot.shape[-1] ** (-0.5)).astype(jnp.bfloat16)
    grad_query = jnp.einsum('hqk,khd->qhd', grad_scores.astype(jnp.float32), key_rot.astype(jnp.float32))
    grad_key = jnp.einsum('hqk,qhd->khd', grad_scores.astype(jnp.float32), query_rot.astype(jnp.float32))
    return (grad_query, grad_key, grad_value)

def mixer_forward(inputs, seg_all, qkv_mat, out_mat, gain_mat):
    count, model_width = inputs.shape
    num_seqs, length = seg_all.shape
    head_count = model_width // HD
    shape_heads = (num_seqs, length, head_count, HD)
    inputs_f = inputs.astype(jnp.float32)
    normed_one, scale_one = rms_forward(inputs_f, gain_mat[:, 0])
    normed_one = normed_one.astype(jnp.bfloat16)
    projected = jnp.dot(normed_one, qkv_mat.reshape(model_width, 3 * model_width), preferred_element_type=jnp.float32)
    query_raw = projected[:, :model_width]
    key_raw = projected[:, model_width:2 * model_width]
    value_raw = projected[:, 2 * model_width:]
    query_norm, query_scale = rms_forward(query_raw, gain_mat[:, 1])
    key_norm, key_scale = rms_forward(key_raw, gain_mat[:, 2])
    cos_tab, sin_tab = rope_tables(length, HD)
    query_rot = rotate(query_norm.reshape(shape_heads), cos_tab, sin_tab).astype(jnp.bfloat16)
    key_rot = rotate(key_norm.reshape(shape_heads), cos_tab, sin_tab).astype(jnp.bfloat16)
    value_bf = value_raw.astype(jnp.bfloat16).reshape(shape_heads)
    mixed_heads, log_total = jax.vmap(attend_forward)(query_rot, key_rot, value_bf, seg_all)
    attn_flat = mixed_heads.reshape(count, model_width)
    after_attn = inputs_f + jnp.dot(attn_flat, out_mat, preferred_element_type=jnp.float32)
    saved = (inputs_f, scale_one, normed_one, query_raw, query_scale, key_raw, key_scale, query_rot, key_rot, value_bf, attn_flat, log_total)
    return (after_attn, saved)

def mixer_backward(saved, seg_all, qkv_mat, out_mat, gain_mat, grad_mid):
    inputs_f, scale_one, normed_one, query_raw, query_scale, key_raw, key_scale, query_rot, key_rot, value_bf, attn_flat, log_total = saved
    count, model_width = inputs_f.shape
    num_seqs, length = seg_all.shape
    head_count = model_width // HD
    shape_heads = (num_seqs, length, head_count, HD)
    grad_mid_bf = grad_mid.astype(jnp.bfloat16)
    grad_out_mat = jnp.dot(attn_flat.T, grad_mid_bf, preferred_element_type=jnp.float32)
    grad_heads = jnp.dot(grad_mid_bf, out_mat.T, preferred_element_type=jnp.float32).astype(jnp.bfloat16).reshape(shape_heads)
    grad_query, grad_key, grad_value = jax.vmap(attend_backward)(query_rot, key_rot, value_bf, seg_all, log_total, grad_heads)
    cos_tab, sin_tab = rope_tables(length, HD)
    grad_qnorm = rotate_back(grad_query, cos_tab, sin_tab).reshape(count, model_width)
    grad_knorm = rotate_back(grad_key, cos_tab, sin_tab).reshape(count, model_width)
    grad_qraw, gain_query = rms_backward(query_raw, query_scale, gain_mat[:, 1], grad_qnorm)
    grad_kraw, gain_key = rms_backward(key_raw, key_scale, gain_mat[:, 2], grad_knorm)
    grad_proj = jnp.concatenate([grad_qraw.astype(jnp.bfloat16), grad_kraw.astype(jnp.bfloat16), grad_value.reshape(count, model_width)], axis=1)
    grad_qkv_mat = jnp.dot(normed_one.T, grad_proj, preferred_element_type=jnp.float32).reshape(model_width, 3, model_width)
    grad_normed = jnp.dot(grad_proj, qkv_mat.reshape(model_width, 3 * model_width).T, preferred_element_type=jnp.float32)
    grad_front, gain_attn = rms_backward(inputs_f, scale_one, gain_mat[:, 0], grad_normed)
    return (grad_mid + grad_front, grad_qkv_mat, grad_out_mat, gain_attn, gain_query, gain_key)

def router_forward(after_attn, router_mat, gain_mat, route_ids):
    normed_two, scale_two = rms_forward(after_attn, gain_mat[:, 3])
    normed_two = normed_two.astype(jnp.bfloat16)
    logits = jnp.dot(normed_two, router_mat, preferred_element_type=jnp.float32)
    probs = jax.nn.softmax(logits, axis=-1)
    expert_ids = jnp.arange(router_mat.shape[1], dtype=jnp.int32)
    picks = (route_ids[:, :, None] == expert_ids[None, None, :]).astype(jnp.float32)
    gate_vals = lax.optimization_barrier(jnp.sum(picks * probs[:, None, :], axis=-1))
    return (normed_two, scale_two, probs, picks, gate_vals)

def router_backward(after_attn, scale_two, normed_two, probs, picks, grad_gates, router_mat, gain_mat, grad_from_experts):
    grad_probs = lax.optimization_barrier(jnp.sum(picks * grad_gates[:, :, None], axis=1))
    grad_logits = probs * (grad_probs - lax.optimization_barrier(jnp.sum(probs * grad_probs, axis=-1, keepdims=True)))
    grad_logits = grad_logits.astype(jnp.bfloat16)
    grad_router_mat = jnp.dot(normed_two.T, grad_logits, preferred_element_type=jnp.float32)
    grad_normed = grad_from_experts + jnp.dot(grad_logits, router_mat.T, preferred_element_type=jnp.float32)
    grad_mid, gain_ffn = rms_backward(after_attn, scale_two, gain_mat[:, 3], grad_normed)
    return (grad_mid, grad_router_mat, gain_ffn)

def slot_positions(flat_routes, expert_count):
    marks = (flat_routes[:, None] == jnp.arange(expert_count, dtype=jnp.int32)[None, :]).astype(jnp.int32)
    return lax.optimization_barrier(jnp.sum(marks * jnp.cumsum(marks, axis=0), axis=1)) - 1

def reference(inputs, segments, routes, w_qkv, w_out, w_router, gains, w_gate, w_up, w_down, cotangent):
    gain_mat = gains.astype(jnp.float32)
    after_attn, saved = mixer_forward(inputs, segments, w_qkv, w_out, gain_mat)
    normed_two, scale_two, probs, picks, gate_vals = router_forward(after_attn, w_router, gain_mat, routes)
    grad_top = cotangent.astype(jnp.float32)
    pair_count = TOK_DEV * TOP
    blocks = routes.reshape(DEVICES, pair_count)
    places = jax.vmap(lambda block_routes: slot_positions(block_routes, EXPERTS))(blocks)
    wide_slots = DEVICES * CAP
    sources = jnp.arange(DEVICES, dtype=jnp.int32)[:, None]
    targets = blocks * wide_slots + sources * CAP + places
    row_ids = jnp.arange(TOKENS * TOP, dtype=jnp.int32)
    table = jnp.full((EXPERTS * wide_slots,), TOKENS * TOP, dtype=jnp.int32)
    table = table.at[targets.reshape(-1)].set(row_ids).reshape(EXPERTS, wide_slots)
    model_width = inputs.shape[1]
    normed_pad = jnp.concatenate([normed_two, jnp.zeros((1, model_width), jnp.bfloat16)], axis=0)
    grad_pad = jnp.concatenate([grad_top, jnp.zeros((1, model_width), jnp.float32)], axis=0)
    gate_pad = jnp.concatenate([gate_vals.reshape(-1), jnp.zeros((1,), jnp.float32)], axis=0)

    def expert_step(carry, xs_tuple):
        mixed_acc, back_acc = carry
        gate_mat, up_mat, down_mat, slot_rows = xs_tuple
        token_ids = slot_rows // TOP
        rows_in = normed_pad[token_ids]
        gate_pre = jnp.dot(rows_in, gate_mat, preferred_element_type=jnp.float32)
        up_pre = jnp.dot(rows_in, up_mat, preferred_element_type=jnp.float32)
        sig_gate = jax.nn.sigmoid(gate_pre)
        silu_gate = gate_pre * sig_gate
        act_bf = (silu_gate * up_pre).astype(jnp.bfloat16)
        out_bf = jnp.dot(act_bf, down_mat, preferred_element_type=jnp.float32).astype(jnp.bfloat16)
        out_f = out_bf.astype(jnp.float32)
        slot_gates = gate_pad[slot_rows]
        mixed_acc = mixed_acc.at[token_ids].add(slot_gates[:, None] * out_f)
        grad_rows = grad_pad[token_ids]
        grad_gate_rows = lax.optimization_barrier(jnp.sum(grad_rows * out_f, axis=-1))
        grad_out_bf = (slot_gates[:, None] * grad_rows).astype(jnp.bfloat16)
        grad_act = jnp.dot(grad_out_bf, down_mat.T, preferred_element_type=jnp.float32)
        grad_gate_bf = (grad_act * up_pre * (sig_gate * (1.0 + gate_pre * (1.0 - sig_gate)))).astype(jnp.bfloat16)
        grad_up_bf = (grad_act * silu_gate).astype(jnp.bfloat16)
        grad_down_mat = jnp.dot(act_bf.T, grad_out_bf, preferred_element_type=jnp.float32)
        grad_gate_mat = jnp.dot(rows_in.T, grad_gate_bf, preferred_element_type=jnp.float32)
        grad_up_mat = jnp.dot(rows_in.T, grad_up_bf, preferred_element_type=jnp.float32)
        grad_rows_in = jnp.dot(grad_gate_bf, gate_mat.T, preferred_element_type=jnp.float32) + jnp.dot(grad_up_bf, up_mat.T, preferred_element_type=jnp.float32)
        back_acc = back_acc.at[token_ids].add(grad_rows_in.astype(jnp.bfloat16).astype(jnp.float32))
        return ((mixed_acc, back_acc), (grad_gate_mat, grad_up_mat, grad_down_mat, grad_gate_rows))
    start = (jnp.zeros((TOKENS + 1, model_width), jnp.float32), jnp.zeros((TOKENS + 1, model_width), jnp.float32))
    (mixed_acc, back_acc), (grad_w_gate, grad_w_up, grad_w_down, gate_rows_all) = lax.scan(expert_step, start, (w_gate, w_up, w_down, table))
    output = (after_attn + mixed_acc[:TOKENS]).astype(jnp.bfloat16)
    grad_gates = jnp.zeros((TOKENS * TOP + 1,), jnp.float32).at[table.reshape(-1)].set(gate_rows_all.reshape(-1))
    grad_gates = grad_gates[:TOKENS * TOP].reshape(TOKENS, TOP)
    grad_ffn, grad_w_router, gain_ffn = router_backward(after_attn, scale_two, normed_two, probs, picks, grad_gates, w_router, gain_mat, back_acc[:TOKENS])
    grad_mid = grad_top + grad_ffn
    grad_all, grad_w_qkv, grad_w_out, gain_attn, gain_query, gain_key = mixer_backward(saved, segments, w_qkv, w_out, gain_mat, grad_mid)
    grad_gains = jnp.stack([gain_attn, gain_query, gain_key, gain_ffn], axis=1)
    return (output, grad_all.astype(jnp.bfloat16), grad_w_qkv, grad_w_out, grad_w_router, grad_gains, grad_w_gate, grad_w_up, grad_w_down)
```

```python
import functools

import jax
import jax.numpy as jnp
from jax import lax
from jax.experimental import pallas as pl
from jax.experimental.pallas import tpu as pltpu
from jax.sharding import PartitionSpec as P

HD = 128
EPS = 1e-05
ROPE_BASE = 10000.0
MASKED = -1e30
BF = jnp.bfloat16
F32 = jnp.float32


def dot(a, b, dims):
    return lax.dot_general(a, b, (dims, ((), ())), preferred_element_type=F32)


NN = ((1,), (0,))
NT = ((1,), (1,))
TN = ((0,), (0,))


def rms_scale(values):
    return lax.rsqrt(jnp.mean(values * values, axis=-1, keepdims=True) + EPS)


def rms_backward(values, inv_rms, gain_col, grad_out):
    normed = values * inv_rms
    grad_gain = jnp.sum(grad_out * normed, axis=0)
    scaled = grad_out * gain_col
    grad_values = inv_rms * (scaled - normed * jnp.mean(scaled * normed, axis=-1, keepdims=True))
    return (grad_values, grad_gain)


def rope_tables(length):
    half = HD // 2
    freqs = jnp.exp(-jnp.log(ROPE_BASE) * (2.0 * jnp.arange(half, dtype=F32) / HD))
    angles = jnp.arange(length, dtype=F32)[:, None] * freqs[None, :]
    return (jnp.cos(angles)[:, None, :], jnp.sin(angles)[:, None, :])


def rotate(values, cos_tab, sin_tab):
    first, second = jnp.split(values, 2, axis=-1)
    return jnp.concatenate(
        [first * cos_tab - second * sin_tab, second * cos_tab + first * sin_tab], axis=-1
    )


def attend_scores(query_rot, key_rot, seg_ids):
    places = jnp.arange(seg_ids.shape[0], dtype=jnp.int32)
    allowed = (places[:, None] >= places[None, :]) & (seg_ids[:, None] == seg_ids[None, :])
    scores = jnp.einsum("qhd,khd->hqk", query_rot, key_rot, preferred_element_type=F32)
    scores = scores * query_rot.shape[-1] ** (-0.5)
    return jnp.where(allowed[None], scores, MASKED)


def attend_forward(query_rot, key_rot, value_bf, seg_ids):
    scores = attend_scores(query_rot, key_rot, seg_ids)
    row_max = jnp.max(scores, axis=-1, keepdims=True)
    log_total = row_max + jnp.log(jnp.sum(jnp.exp(scores - row_max), axis=-1, keepdims=True))
    weights_bf = jnp.exp(scores - log_total).astype(BF)
    mixed = jnp.einsum("hqk,khd->qhd", weights_bf, value_bf, preferred_element_type=F32)
    return (mixed.astype(BF), log_total)


def attend_backward(query_rot, key_rot, value_bf, seg_ids, log_total, grad_heads):
    scores = attend_scores(query_rot, key_rot, seg_ids)
    probs = jnp.exp(scores - log_total)
    grad_value = jnp.einsum(
        "hqk,qhd->khd", probs.astype(BF), grad_heads, preferred_element_type=F32
    ).astype(BF)
    grad_probs = jnp.einsum("qhd,khd->hqk", grad_heads, value_bf, preferred_element_type=F32)
    delta = jnp.sum(probs * grad_probs, axis=-1, keepdims=True)
    grad_scores = (probs * (grad_probs - delta) * query_rot.shape[-1] ** (-0.5)).astype(BF)
    grad_query = jnp.einsum("hqk,khd->qhd", grad_scores, key_rot, preferred_element_type=F32)
    grad_key = jnp.einsum("hqk,qhd->khd", grad_scores, query_rot, preferred_element_type=F32)
    return (grad_query, grad_key, grad_value)


def moe_kernel(
    fl, h_ref, g_ref, gate_ref, win_ref, wdt_ref, wd_ref, wint_ref,
    mix_ref, gh_ref, gg_ref, dwin_ref, dwd_ref, acc_in, acc_d,
):
    step = pl.program_id(0)
    h = h_ref[...]
    g = g_ref[...]
    gates = gate_ref[...]
    pre = dot(h, win_ref[...], NN)
    graw = dot(g, wdt_ref[...], NN)
    scaled_act, grad_gate, grad_up, gg = [], [], [], []
    for i in range(2):
        u = pre[:, i * fl : (i + 1) * fl]
        w = pre[:, (2 + i) * fl : (3 + i) * fl]
        gr = graw[:, i * fl : (i + 1) * fl]
        gate = gates[:, i : i + 1]
        sig = 1.0 / (1.0 + jnp.exp(-u))
        silu = u * sig
        act = silu * w
        gg.append(jnp.sum(act.astype(BF).astype(F32) * gr, axis=-1, keepdims=True))
        scaled_act.append((gate * act).astype(BF))
        gact = gate * gr
        grad_gate.append((gact * w * (sig * (1.0 + u * (1.0 - sig)))).astype(BF))
        grad_up.append((gact * silu).astype(BF))
    a = jnp.concatenate(scaled_act, axis=1)
    gin = jnp.concatenate(grad_gate + grad_up, axis=1)
    mix_ref[...] = dot(a, wd_ref[...], NN).astype(BF)
    gh_ref[...] = dot(gin, wint_ref[...], NN).astype(BF)
    gg_ref[...] = jnp.concatenate(gg, axis=1)

    @pl.when(step == 0)
    def _():
        acc_in[...] = jnp.zeros_like(acc_in)
        acc_d[...] = jnp.zeros_like(acc_d)

    acc_in[...] += dot(h, gin, TN)
    acc_d[...] += dot(a, g, TN)

    @pl.when(step == pl.num_programs(0) - 1)
    def _():
        dwin_ref[...] = acc_in[...].astype(BF)
        dwd_ref[...] = acc_d[...]


def moe(h_all, g_all, gates2, w_in, wd_t, wd, w_in_t, tile):
    count, width = h_all.shape
    hid4 = w_in.shape[1]
    hid2 = wd.shape[0]
    fl = hid2 // 2
    rows = lambda n: pl.BlockSpec((tile, n), lambda i: (i, 0))
    whole = lambda s: pl.BlockSpec(s, lambda i: (0, 0), pipeline_mode=pl.Buffered(1))
    return pl.pallas_call(
        functools.partial(moe_kernel, fl),
        grid=(count // tile,),
        in_specs=[
            rows(width), rows(width), rows(2),
            whole(w_in.shape), whole(wd_t.shape), whole(wd.shape), whole(w_in_t.shape),
        ],
        out_specs=[
            rows(width), rows(width), rows(2), whole((width, hid4)), whole((hid2, width)),
        ],
        out_shape=[
            jax.ShapeDtypeStruct((count, width), BF),
            jax.ShapeDtypeStruct((count, width), BF),
            jax.ShapeDtypeStruct((count, 2), F32),
            jax.ShapeDtypeStruct((width, hid4), BF),
            jax.ShapeDtypeStruct((hid2, width), F32),
        ],
        scratch_shapes=[pltpu.VMEM((width, hid4), F32), pltpu.VMEM((hid2, width), F32)],
        compiler_params=pltpu.CompilerParams(vmem_limit_bytes=66_000_000),
        cost_estimate=pl.CostEstimate(
            flops=2 * count * width * hid2 * 9,
            bytes_accessed=8 * count * width + 24 * hid4 * width,
            transcendentals=count * hid2,
        ),
        name="moe",
    )(h_all, g_all, gates2, w_in, wd_t, wd, w_in_t)


def body(inputs, segments, routes, w_qkv, w_out, w_router, gains, w_gate, w_up, w_down, cotangent):
    z = lax.axis_index("dp")
    e = lax.axis_index("expert")
    nz = lax.axis_size("dp")
    ne = lax.axis_size("expert")
    count, width = inputs.shape
    num_seqs, length = segments.shape
    heads = width // HD // ne
    hw = heads * HD
    expert_count = w_router.shape[1]
    per_dev = w_gate.shape[0]
    hidden = w_gate.shape[2]
    fl = hidden // nz
    both = ("dp", "expert")

    qkv_cols = lax.dynamic_slice_in_dim(w_qkv, e * hw, hw, axis=2)
    wq = lax.all_gather(qkv_cols, "dp", axis=0, tiled=True).reshape(width, 3 * hw)
    out_cols = lax.dynamic_slice_in_dim(w_out, e * hw, hw, axis=1)
    out_cols = lax.all_gather(out_cols, "dp", axis=0, tiled=True)
    wo = lax.all_to_all(
        out_cols.reshape(ne, hw, hw), "expert", split_axis=0, concat_axis=0, tiled=True
    )
    wo = wo.transpose(1, 0, 2).reshape(hw, width)
    small = lax.all_gather(
        jnp.concatenate([gains, w_router], axis=1), "dp", axis=0, tiled=True
    )
    gain_mat = small[:, :4].astype(F32)
    router = small[:, 4:]
    my_gains = lax.dynamic_slice_in_dim(gain_mat, e * hw, hw, axis=0)

    g_all = lax.all_gather(cotangent, both, axis=0, tiled=True)
    inputs_f = inputs.astype(F32)
    scale_one = rms_scale(inputs_f)
    h1 = (inputs_f * scale_one * gain_mat[:, 0]).astype(BF)
    h1_all = lax.all_gather(h1, "expert", axis=0, tiled=True)
    seg_all = lax.all_gather(segments, "expert", axis=0, tiled=True)
    plane = h1_all.shape[0]
    shape_heads = (ne * num_seqs, length, heads, HD)

    proj = dot(h1_all, wq, NN)
    q, k, v = proj[:, :hw], proj[:, hw : 2 * hw], proj[:, 2 * hw :]
    sums = jnp.stack([jnp.sum(q * q, axis=-1), jnp.sum(k * k, axis=-1)])
    scales = lax.rsqrt(lax.psum(sums, "expert") / width + EPS)
    aq, ak = scales[0][:, None], scales[1][:, None]
    cos_tab, sin_tab = rope_tables(length)
    rq = rotate((q * aq * my_gains[:, 1]).reshape(shape_heads), cos_tab, sin_tab).astype(BF)
    rk = rotate((k * ak * my_gains[:, 2]).reshape(shape_heads), cos_tab, sin_tab).astype(BF)
    vb = v.astype(BF).reshape(shape_heads)
    o, lse = jax.vmap(attend_forward)(rq, rk, vb, seg_all)
    o = o.reshape(plane, hw)
    x1_part = dot(o, wo, NN).astype(BF)
    x1 = inputs_f + lax.psum_scatter(
        x1_part, "expert", scatter_dimension=0, tiled=True
    ).astype(F32)

    a2 = rms_scale(x1)
    h2 = (x1 * a2 * gain_mat[:, 3]).astype(BF)
    probs = jax.nn.softmax(dot(h2, router, NN), axis=-1)
    picks = jnp.sum(
        (routes[:, :, None] == jnp.arange(expert_count, dtype=jnp.int32)).astype(F32), axis=1
    )
    gates = picks * probs

    h2_all = lax.all_gather(h2, both, axis=0, tiled=True)
    gates_all = lax.all_gather(gates, both, axis=0, tiled=True)
    gates2 = lax.dynamic_slice_in_dim(gates_all, e * per_dev, per_dev, axis=1)
    wg = lax.dynamic_slice_in_dim(w_gate, z * fl, fl, axis=2)
    wu = lax.dynamic_slice_in_dim(w_up, z * fl, fl, axis=2)
    wd = lax.dynamic_slice_in_dim(w_down, z * fl, fl, axis=1)
    w_in_t = jnp.concatenate(
        [wg.transpose(0, 2, 1), wu.transpose(0, 2, 1)], axis=0
    ).reshape(2 * per_dev * fl, width)
    w_in = jnp.concatenate([wg[0], wg[1], wu[0], wu[1]], axis=1)
    wd = wd.reshape(per_dev * fl, width)
    mix, gh, gg, dwin, dwd = moe(h2_all, g_all, gates2, w_in, wd.T, wd, w_in_t, 512)

    gg_full = lax.dynamic_update_slice_in_dim(
        jnp.zeros((gg.shape[0], expert_count), F32), gg, e * per_dev, axis=1
    )
    grad_gates = lax.psum_scatter(gg_full, both, scatter_dimension=0, tiled=True)

    def scatter_tokens(part):
        part = part.reshape(nz, ne, count, width).transpose(1, 0, 2, 3).reshape(-1, width)
        part = lax.psum_scatter(part, "expert", scatter_dimension=0, tiled=True)
        return lax.psum_scatter(part, "dp", scatter_dimension=0, tiled=True).astype(F32)

    grad_from_experts = scatter_tokens(gh)
    mixed = scatter_tokens(mix)
    output = (x1 + mixed).astype(BF)

    dwin = lax.all_to_all(
        dwin.reshape(nz, width // nz, 2 * per_dev * fl), "dp", split_axis=0, concat_axis=0, tiled=True
    )
    dwin = dwin.reshape(nz, width // nz, 2, per_dev, fl).transpose(2, 3, 1, 0, 4)
    dwin = dwin.reshape(2, per_dev, width // nz, hidden).astype(F32)
    grad_w_down = dwd.reshape(per_dev, fl, width)

    grad_top = cotangent.astype(F32)
    grad_probs = picks * grad_gates
    glog = (probs * (grad_probs - jnp.sum(probs * grad_probs, axis=-1, keepdims=True))).astype(BF)
    local_router = dot(h2, glog, TN)
    gh2 = grad_from_experts + dot(glog, router, NT)
    grad_ffn, gain_ffn = rms_backward(x1, a2, gain_mat[:, 3], gh2)
    gx1 = grad_top + grad_ffn
    gab = gx1.astype(BF)

    gab_all = lax.all_gather(gab, "expert", axis=0, tiled=True)
    go = dot(gab_all, wo, NT).astype(BF).reshape(shape_heads)
    grad_q, grad_k, gv = jax.vmap(attend_backward)(rq, rk, vb, seg_all, lse, go)
    gqn = rotate(grad_q, cos_tab, -sin_tab).reshape(plane, hw)
    gkn = rotate(grad_k, cos_tab, -sin_tab).reshape(plane, hw)
    nq, nk = q * aq, k * ak
    sq, sk = gqn * my_gains[:, 1], gkn * my_gains[:, 2]
    sums = jnp.stack([jnp.sum(sq * nq, axis=-1), jnp.sum(sk * nk, axis=-1)])
    means = lax.psum(sums, "expert") / width
    gq = (aq * (sq - nq * means[0][:, None])).astype(BF)
    gk = (ak * (sk - nk * means[1][:, None])).astype(BF)
    gproj = jnp.concatenate([gq, gk, gv.reshape(plane, hw)], axis=1)
    gain_q, gain_k = jnp.sum(gqn * nq, axis=0), jnp.sum(gkn * nk, axis=0)

    gh1_part = dot(gproj, wq, NT).astype(BF)
    gh1 = lax.psum_scatter(gh1_part, "expert", scatter_dimension=0, tiled=True).astype(F32)
    grad_front, gain_attn = rms_backward(inputs_f, scale_one, gain_mat[:, 0], gh1)
    grad_inputs = (gx1 + grad_front).astype(BF)

    part_qkv = dot(h1_all, gproj, TN).astype(BF)
    part_out = dot(o, gab_all, TN).astype(BF)
    part_out = lax.all_to_all(
        part_out.reshape(hw, ne, hw).transpose(1, 0, 2),
        "expert", split_axis=0, concat_axis=0, tiled=True,
    ).reshape(width, hw)
    parts = jnp.concatenate([part_qkv, part_out], axis=1)
    mine = lax.psum_scatter(parts, "dp", scatter_dimension=0, tiled=True)
    wide = lax.all_gather(mine, "expert", axis=0)
    wide = wide.reshape(ne, width // nz, 4, hw).transpose(1, 2, 0, 3)
    wide = wide.reshape(width // nz, 4, width).astype(F32)
    grad_w_qkv, grad_w_out = wide[:, :3], wide[:, 3]

    place = lambda part: lax.dynamic_update_slice_in_dim(
        jnp.zeros((width,), F32), part, e * hw, axis=0
    )
    tiny = jnp.concatenate(
        [
            local_router,
            jnp.stack([gain_attn, place(gain_q), place(gain_k), gain_ffn], axis=1),
        ],
        axis=1,
    )
    tiny = lax.psum(tiny, both)
    tiny = lax.dynamic_slice_in_dim(tiny, z * (width // nz), width // nz, axis=0)
    grad_w_router, grad_gains = tiny[:, :expert_count], tiny[:, expert_count:]
    return (
        output,
        grad_inputs,
        grad_w_qkv,
        grad_w_out,
        grad_w_router,
        grad_gains,
        dwin[0],
        dwin[1],
        grad_w_down,
    )


def solution(mesh):
    tokens = P(("dp", "expert"), None)
    rows = P("dp", None)
    rows3 = P("dp", None, None)
    owned = P("expert", None, None)
    return jax.shard_map(
        body,
        mesh=mesh,
        in_specs=(tokens, tokens, tokens, rows3, rows, rows, rows, owned, owned, owned, tokens),
        out_specs=(tokens, tokens, rows3, rows, rows, rows)
        + (P("expert", "dp", None),) * 3,
        check_vma=False,
    )
```

```python
import functools

import jax
import jax.numpy as jnp
from jax import lax
from jax.experimental import pallas as pl
from jax.experimental.pallas import tpu as pltpu
from jax.sharding import PartitionSpec as P

HD = 128
EPS = 1e-05
ROPE_BASE = 10000.0
MASKED = -1e30
BF = jnp.bfloat16
F32 = jnp.float32


def dot(a, b, dims):
    return lax.dot_general(a, b, (dims, ((), ())), preferred_element_type=F32)


NN = ((1,), (0,))
NT = ((1,), (1,))
TN = ((0,), (0,))


def rms_scale(values):
    return lax.rsqrt(jnp.mean(values * values, axis=-1, keepdims=True) + EPS)


def rms_backward(values, inv_rms, gain_col, grad_out):
    normed = values * inv_rms
    grad_gain = jnp.sum(grad_out * normed, axis=0)
    scaled = grad_out * gain_col
    grad_values = inv_rms * (scaled - normed * jnp.mean(scaled * normed, axis=-1, keepdims=True))
    return (grad_values, grad_gain)


def rope_tables(length):
    half = HD // 2
    freqs = jnp.exp(-jnp.log(ROPE_BASE) * (2.0 * jnp.arange(half, dtype=F32) / HD))
    angles = jnp.arange(length, dtype=F32)[:, None] * freqs[None, :]
    return (jnp.cos(angles)[:, None, :], jnp.sin(angles)[:, None, :])


def rotate(values, cos_tab, sin_tab):
    first, second = jnp.split(values, 2, axis=-1)
    return jnp.concatenate(
        [first * cos_tab - second * sin_tab, second * cos_tab + first * sin_tab], axis=-1
    )


def attend_scores(query_rot, key_rot, seg_ids):
    places = jnp.arange(seg_ids.shape[0], dtype=jnp.int32)
    allowed = (places[:, None] >= places[None, :]) & (seg_ids[:, None] == seg_ids[None, :])
    scores = jnp.einsum("qhd,khd->hqk", query_rot, key_rot, preferred_element_type=F32)
    scores = scores * query_rot.shape[-1] ** (-0.5)
    return jnp.where(allowed[None], scores, MASKED)


def attend_forward(query_rot, key_rot, value_bf, seg_ids):
    scores = attend_scores(query_rot, key_rot, seg_ids)
    row_max = jnp.max(scores, axis=-1, keepdims=True)
    log_total = row_max + jnp.log(jnp.sum(jnp.exp(scores - row_max), axis=-1, keepdims=True))
    weights_bf = jnp.exp(scores - log_total).astype(BF)
    mixed = jnp.einsum("hqk,khd->qhd", weights_bf, value_bf, preferred_element_type=F32)
    return (mixed.astype(BF), log_total)


def attend_backward(query_rot, key_rot, value_bf, seg_ids, log_total, grad_heads):
    scores = attend_scores(query_rot, key_rot, seg_ids)
    probs = jnp.exp(scores - log_total)
    grad_value = jnp.einsum(
        "hqk,qhd->khd", probs.astype(BF), grad_heads, preferred_element_type=F32
    ).astype(BF)
    grad_probs = jnp.einsum("qhd,khd->hqk", grad_heads, value_bf, preferred_element_type=F32)
    delta = jnp.sum(probs * grad_probs, axis=-1, keepdims=True)
    grad_scores = (probs * (grad_probs - delta) * query_rot.shape[-1] ** (-0.5)).astype(BF)
    grad_query = jnp.einsum("hqk,khd->qhd", grad_scores, key_rot, preferred_element_type=F32)
    grad_key = jnp.einsum("hqk,qhd->khd", grad_scores, query_rot, preferred_element_type=F32)
    return (grad_query, grad_key, grad_value)


MESH = pl.DeviceIdType.MESH
ANY = pl.BlockSpec(memory_space=pl.ANY)
VMEM = pl.BlockSpec(memory_space=pltpu.VMEM)
DMA = pltpu.SemaphoreType.DMA


def flip(index, bit):
    return index + bit * (1 - 2 * ((index // bit) % 2))


def flips(index, bits):
    out = [index]
    for bit in bits:
        out = out + [flip(i, bit) for i in out]
    return out


def bit_orders(ne):
    bits = [1 << b for b in range(ne.bit_length() - 1)]
    return [bits[:1] + bits[1:], bits[:1] + bits[1:][::-1]]


def nearest(z, r, nz):
    low = jnp.minimum(z, nz - 1 - z)
    near = z - (r + 1) // 2 if r % 2 else z + r // 2
    far = jnp.where(2 * z < nz, z + (r - low), z - (r - low))
    return jnp.where(r <= 2 * low, near, far)


def remote(src, dst, send, recv, peer):
    return pltpu.make_async_remote_copy(
        src_ref=src, dst_ref=dst, send_sem=send, recv_sem=recv, device_id=peer, device_id_type=MESH
    )


def for_others(nz, ne, z, e, act):
    def step(i, carry):
        flat = lax.rem(z * ne + e + i, nz * ne)
        act(flat // ne, lax.rem(flat, ne), flat)
        return carry

    lax.fori_loop(1, nz * ne, step, 0)


def meet_all(nz, ne, z, e):
    sem = pltpu.get_barrier_semaphore()

    def greet(zz, ee, flat):
        pl.semaphore_signal(sem, inc=1, device_id=(zz, ee), device_id_type=MESH)

    for_others(nz, ne, z, e, greet)
    pl.semaphore_wait(sem, nz * ne - 1)


def meet_column_and_plane(nz, ne, z, e, spread):
    sem = pltpu.get_barrier_semaphore()
    peers = [(z, flip(e, 1 << b)) for b in range(ne.bit_length() - 1)]
    if spread:
        peers += [(lax.rem(z + r, nz), e) for r in range(1, nz)]
    for peer in peers:
        pl.semaphore_signal(sem, inc=1, device_id=peer, device_id_type=MESH)
    pl.semaphore_wait(sem, len(peers))


class PlaneGather:
    def __init__(self, nz, ne, z, e, spread, x_ref, out_ref, zsend, zrecv, send, recv, local):
        self.nz, self.ne, self.z, self.e, self.spread = nz, ne, z, e, spread
        self.x, self.out = x_ref, out_ref
        self.zsend, self.zrecv, self.send, self.recv = zsend, zrecv, send, recv
        self.rounds = nz if spread else 1
        self.half = x_ref.shape[0] // 2
        self.orders = [o[1:] + o[:1] for o in bit_orders(ne)]
        self.planes = [z if spread else 0] + [nearest(z, r, nz) for r in range(1, self.rounds)]
        self.pending, self.arrivals = [], {}
        own = self.slot(0, e)
        keep = pltpu.make_async_copy(x_ref, out_ref.at[own], local)
        keep.start()
        self.pending.append(keep.wait)

    @staticmethod
    def scratch(nz, ne, spread):
        rounds = nz if spread else 1
        return [DMA((nz,)), DMA((nz,)), DMA((rounds, 2, ne - 1)), DMA((rounds, 2, ne - 1)), DMA]

    def slot(self, r, ee):
        return self.planes[r] * self.ne + ee

    def spread_own(self):
        for r in range(1, self.rounds):
            to = self.planes[r]
            copy = remote(
                self.x, self.out.at[self.slot(0, self.e)],
                self.zsend.at[r], self.zrecv.at[self.z], (to, self.e),
            )
            copy.start()
            self.pending.append(copy.wait_send)

    def forward(self, r, s, stage, subset):
        order = self.orders[s]
        rows = pl.ds(s * self.half, self.half)
        peer_e = flip(self.e, order[stage])
        n = (1 << stage) - 1 + subset
        block = self.slot(r, flips(self.e, order[:stage])[subset])
        dst = self.out.at[block, rows]
        src = self.x.at[rows] if r == 0 and subset == 0 else dst
        sems = self.send.at[r, s, n], self.recv.at[r, s, n]
        copy = remote(src, dst, *sems, (self.z, peer_e))
        copy.start()
        self.pending.append(copy.wait_send)
        got = self.out.at[self.slot(r, flips(peer_e, order[:stage])[subset]), rows]
        self.arrivals[(r, s, stage, subset)] = remote(got, got, *sems, (self.z, peer_e)).wait_recv

    def start_round(self, r):
        if r > 0:
            here = self.out.at[self.slot(r, self.e)]
            remote(
                here, here, self.zsend.at[r], self.zrecv.at[self.planes[r]], (self.planes[r], self.e)
            ).wait_recv()
        for stage in range(len(self.orders[0])):
            for s in range(2):
                self.forward(r, s, stage, 0)

    def finish_round(self, r, last=False):
        stages = len(self.orders[0])
        for stage in range(stages):
            for subset in range(1 << stage):
                for s in range(2):
                    self.arrivals.pop((r, s, stage, subset))()
                    for later in range(stage + 1, stages):
                        self.forward(r, s, later, subset + (1 << stage))

    def finish(self):
        for wait in self.pending:
            wait()


def gather_kernel(nz, ne, spread, small, *refs):
    z, e = lax.axis_index("dp"), lax.axis_index("expert")
    if small:
        x_ref, small_ref, out_ref, small_out, *sems, small_send, small_recv = refs
        meet_all(nz, ne, z, e)
    else:
        x_ref, out_ref, *sems = refs
        meet_column_and_plane(nz, ne, z, e, spread)
    net = PlaneGather(nz, ne, z, e, spread, x_ref, out_ref, *sems)
    net.spread_own()
    net.start_round(0)
    if small:
        me = z * ne + e
        small_out[me] = small_ref[...]

        def give(zz, ee, flat):
            remote(small_ref, small_out.at[me], small_send, small_recv, (zz, ee)).start()

        for_others(nz, ne, z, e, give)
    for r in range(1, net.rounds):
        net.start_round(r)
        net.finish_round(r - 1)
    net.finish_round(net.rounds - 1)
    net.finish()
    if small:
        most = small_out.at[pl.ds(0, nz * ne - 1)]
        everyone = remote(most, most, small_send, small_recv, (z, flip(e, 1)))
        everyone.wait_send()
        everyone.wait_recv()


def gather_tokens(x, nz, ne, spread, cid, small=None):
    rounds = nz if spread else 1
    out = [jax.ShapeDtypeStruct((rounds * ne, *x.shape), x.dtype)]
    scratch = PlaneGather.scratch(nz, ne, spread)
    args = [x]
    if small is not None:
        out.append(jax.ShapeDtypeStruct((nz * ne, *small.shape), small.dtype))
        scratch += [DMA, DMA]
        args.append(small)
    return pl.pallas_call(
        functools.partial(gather_kernel, nz, ne, spread, small is not None),
        out_shape=out,
        in_specs=[VMEM] * len(args),
        out_specs=[ANY, VMEM][: len(args)],
        scratch_shapes=scratch,
        compiler_params=pltpu.CompilerParams(collective_id=cid, has_side_effects=True),
        name="gather_tokens",
    )(*args)


def add_rows(dst, src, tile=16):
    def step(i, carry):
        rows = pl.ds(pl.multiple_of(i * tile, tile), tile)
        dst[rows, :] = (dst[rows, :].astype(F32) + src[rows, :].astype(F32)).astype(dst.dtype)
        return carry

    lax.fori_loop(0, dst.shape[0] // tile, step, 0)


def scatter_kernel(nz, ne, spread, small, *refs):
    z, e = lax.axis_index("dp"), lax.axis_index("expert")
    if small:
        x_ref, small_ref, out_ref, small_out, *rest, small_send, small_recv = refs
        meet_all(nz, ne, z, e)
        me = z * ne + e
        small_out[me] = small_ref[me]

        def give(zz, ee, flat):
            remote(small_ref.at[flat], small_out.at[me], small_send, small_recv, (zz, ee)).start()

        for_others(nz, ne, z, e, give)
    else:
        x_ref, out_ref, *rest = refs
        meet_column_and_plane(nz, ne, z, e, spread)
    acc, got, zgot, loads, send, recv, zsend, zrecv = rest
    rounds = nz if spread else 1
    stages = ne.bit_length() - 1
    half = out_ref.shape[0] // 2
    orders = bit_orders(ne)
    pending, arrivals, zwait = [], {}, {}
    ranks = list(range(1, rounds)) + [0]
    first = [0] * (stages + 1)
    for j in range(stages):
        first[j + 1] = first[j] + (ne >> (j + 1))

    def plane_of(r):
        return lax.rem(z + r, nz) * ne if spread else 0

    def push(r, s, j):
        order = orders[s]
        peer = (z, flip(e, order[j]))
        rest = ne >> (j + 1)
        for i in range(rest):
            n = first[j] + i
            if j == 0:
                block = flips(peer[1], order[:0:-1])[i]
                src = x_ref.at[plane_of(r) + block, pl.ds(s * half, half)]
            else:
                src = acc.at[r, s, rest + i]
            copy = remote(src, got.at[r, s, n], send.at[r, s, n], recv.at[r, s, n], peer)
            copy.start()
            pending.append(copy.wait_send)
            arrivals.setdefault((r, s, j), []).append((copy.wait_recv, i, n))

    for r in ranks:
        for s in range(2):
            push(r, s, 0)
            for i, block in enumerate(flips(e, orders[s][:0:-1])):
                copy = pltpu.make_async_copy(
                    x_ref.at[plane_of(r) + block, pl.ds(s * half, half)],
                    acc.at[r, s, i],
                    loads.at[r, s, i],
                )
                copy.start()
                arrivals.setdefault((r, s, -1), []).append(copy.wait)
    for t in range(rounds + stages):
        for place, r in enumerate(ranks):
            j = t - place
            if not 0 <= j < stages:
                continue
            for s in range(2):
                if j == 0:
                    for wait in arrivals.pop((r, s, -1)):
                        wait()
                for wait, i, n in arrivals.pop((r, s, j)):
                    wait()
                    add_rows(acc.at[r, s, i], got.at[r, s, n])
                if j + 1 < stages:
                    push(r, s, j + 1)
                elif r > 0:
                    copy = remote(
                        acc.at[r, s, 0], zgot.at[r, s], zsend.at[r, s], zrecv.at[r, s],
                        (lax.rem(z + r, nz), e),
                    )
                    copy.start()
                    pending.append(copy.wait_send)
                    zwait[(r, s)] = copy.wait_recv
    for s in range(2):
        for r in range(1, rounds):
            zwait[(r, s)]()

        def step(i, carry):
            rows = pl.ds(pl.multiple_of(i * 16, 16), 16)
            total = acc[0, s, 0, rows, :].astype(F32)
            for r in range(1, rounds):
                total = total + zgot[r, s, rows, :].astype(F32)
            out_ref[pl.ds(pl.multiple_of(s * half + i * 16, 16), 16), :] = total.astype(out_ref.dtype)
            return carry

        lax.fori_loop(0, half // 16, step, 0)
    for wait in pending:
        wait()
    if small:
        most = small_out.at[pl.ds(0, nz * ne - 1)]
        everyone = remote(most, most, small_send, small_recv, (z, flip(e, 1)))
        everyone.wait_send()
        everyone.wait_recv()


def scatter_tokens(parts, nz, ne, spread, cid, small=None):
    rounds = nz if spread else 1
    _, count, width = parts.shape
    half = count // 2
    held = (2 * rounds * (ne // 2 + ne - 1) + 2 * nz) * half * width * 2
    if held > 56_000_000:
        left = scatter_tokens(parts[..., : width // 2], nz, ne, spread, cid, small)
        right = scatter_tokens(parts[..., width // 2 :], nz, ne, spread, cid + 16)
        return [jnp.concatenate([left[0], right[0]], axis=1), *left[1:]]
    out = [jax.ShapeDtypeStruct((count, width), F32)]
    args = [parts]
    scratch = [
        pltpu.VMEM((rounds, 2, ne // 2, half, width), BF),
        pltpu.VMEM((rounds, 2, ne - 1, half, width), BF),
        pltpu.VMEM((nz, 2, half, width), BF),
        DMA((rounds, 2, ne // 2)),
        DMA((rounds, 2, ne - 1)),
        DMA((rounds, 2, ne - 1)),
        DMA((nz, 2)),
        DMA((nz, 2)),
    ]
    if small is not None:
        out.append(jax.ShapeDtypeStruct(small.shape, small.dtype))
        args.append(small)
        scratch += [DMA, DMA]
    return pl.pallas_call(
        functools.partial(scatter_kernel, nz, ne, spread, small is not None),
        out_shape=out,
        in_specs=[ANY, VMEM][: len(args)],
        out_specs=[VMEM, VMEM][: len(args)],
        scratch_shapes=scratch,
        compiler_params=pltpu.CompilerParams(
            collective_id=cid, has_side_effects=True, vmem_limit_bytes=64_000_000
        ),
        name="scatter_tokens",
    )(*args)


def start_kernel(
    nz, ne, x_ref, wqkv_ref, wout_ref, small_ref, seg_ref,
    out_ref, wq_ref, wo_ref, small_out, seg_out,
    wbuf, pbuf, zsend, zrecv, send, recv, local,
    up_send, up_recv, dn_send, dn_recv, wload, wkeep, pload, psend, precv, pkeep,
    small_send, small_recv, seg_send, seg_recv,
):
    z, e = lax.axis_index("dp"), lax.axis_index("expert")
    kinds, depth, hw = wbuf.shape
    per = ne // nz
    loads = [
        pltpu.make_async_copy(wqkv_ref.at[j, :, pl.ds(e * hw, hw)], wbuf.at[j], wload.at[j])
        for j in range(kinds)
    ]
    for copy in loads:
        copy.start()
    pieces = [
        pltpu.make_async_copy(
            wout_ref.at[pl.ds(i * hw, hw), pl.ds(e * hw, hw)], pbuf.at[i], pload.at[i]
        )
        for i in range(per)
    ]
    for copy in pieces:
        copy.start()
    meet_all(nz, ne, z, e)

    def rows_of(zz):
        return pl.ds(pl.multiple_of(zz * depth, depth), depth)

    def hop(j, zz, dist, up):
        send, recv = (up_send, up_recv) if up else (dn_send, dn_recv)
        here = wq_ref.at[j, rows_of(zz)]
        src = wbuf.at[j] if dist == 1 else here
        to = z + 1 if up else z - 1
        return remote(src, here, send.at[dist, j], recv.at[dist, j], (to, e))

    keeps = []
    for j in range(kinds):
        loads[j].wait()

        @pl.when(z + 1 < nz)
        def _():
            hop(j, z, 1, True).start()

        @pl.when(z > 0)
        def _():
            hop(j, z, 1, False).start()

        keep = pltpu.make_async_copy(wbuf.at[j], wq_ref.at[j, rows_of(z)], wkeep.at[j])
        keep.start()
        keeps.append(keep)

    def wait_all(ref, send, recv, count):
        most = ref.at[pl.ds(0, count)]
        both = remote(most, most, send, recv, (z, flip(e, 1)))
        both.wait_send()
        both.wait_recv()

    small_out[z] = small_ref[...]
    for r in range(1, nz):
        remote(
            small_ref, small_out.at[z], small_send, small_recv, (lax.rem(z + r, nz), e)
        ).start()
    seg_out[e] = seg_ref[...]
    for r in range(1, ne):
        remote(seg_ref, seg_out.at[e], seg_send, seg_recv, (z, lax.rem(e + r, ne))).start()
    net = PlaneGather(nz, ne, z, e, False, x_ref, out_ref, zsend, zrecv, send, recv, local)
    net.start_round(0)

    columns = pl.ds(e * hw, hw)
    for i in range(per):
        pieces[i].wait()
    for r in range(nz):
        for i in range(per):
            to = (lax.rem(z + r, nz), z * per + i)
            give = remote(pbuf.at[i], wo_ref.at[:, columns], psend.at[r, i], precv, to)
            if r > 0:
                give.start()
            else:
                own = pltpu.make_async_copy(pbuf.at[i], wo_ref.at[:, columns], pkeep)

                @pl.when(to[1] == e)
                def _():
                    own.start()

                @pl.when(to[1] != e)
                def _():
                    give.start()
    net.finish_round(0)
    for dist in range(1, nz):
        for j in range(kinds):

            @pl.when(z - dist >= 0)
            def _():
                got = wq_ref.at[j, rows_of(z - dist)]
                remote(got, got, up_send.at[dist, j], up_recv.at[dist, j], (z, e)).wait_recv()

                @pl.when(z + 1 < nz)
                def _():
                    if dist + 1 < nz:
                        hop(j, z - dist, dist + 1, True).start()

            @pl.when(z + dist < nz)
            def _():
                got = wq_ref.at[j, rows_of(z + dist)]
                remote(got, got, dn_send.at[dist, j], dn_recv.at[dist, j], (z, e)).wait_recv()

                @pl.when(z > 0)
                def _():
                    if dist + 1 < nz:
                        hop(j, z + dist, dist + 1, False).start()

    net.finish()
    for keep in keeps:
        keep.wait()
    for dist in range(1, nz):
        for j in range(kinds):

            @pl.when((z - dist + 1 >= 0) & (z + 1 < nz))
            def _():
                hop(j, z - dist + 1, dist, True).wait_send()

            @pl.when((z + dist - 1 < nz) & (z > 0))
            def _():
                hop(j, z + dist - 1, dist, False).wait_send()

    for r in range(nz):
        for i in range(per):
            to = (lax.rem(z + r, nz), z * per + i)
            give = remote(pbuf.at[i], wo_ref.at[:, columns], psend.at[r, i], precv, to)
            if r > 0:
                give.wait_send()
            else:
                own = pltpu.make_async_copy(pbuf.at[i], wo_ref.at[:, columns], pkeep)

                @pl.when(to[1] == e)
                def _():
                    own.wait()

                @pl.when(to[1] != e)
                def _():
                    give.wait_send()

    def wait_pieces(count):
        most = wo_ref.at[:, pl.ds(0, count * hw)]
        remote(most, most, psend.at[0, 0], precv, (z, e)).wait_recv()

    @pl.when(z == e // per)
    def _():
        wait_pieces(ne - 1)

    @pl.when(z != e // per)
    def _():
        wait_pieces(ne)

    wait_all(small_out, small_send, small_recv, nz - 1)
    wait_all(seg_out, seg_send, seg_recv, ne - 1)


def start_gather(x, w_qkv, w_out, small, seg, nz, ne, hw, cid):
    kinds, depth, width = w_qkv.shape
    per = ne // nz
    return pl.pallas_call(
        functools.partial(start_kernel, nz, ne),
        out_shape=[
            jax.ShapeDtypeStruct((ne, *x.shape), x.dtype),
            jax.ShapeDtypeStruct((kinds, nz * depth, hw), BF),
            jax.ShapeDtypeStruct((hw, width), BF),
            jax.ShapeDtypeStruct((nz, *small.shape), small.dtype),
            jax.ShapeDtypeStruct((ne, *seg.shape), seg.dtype),
        ],
        in_specs=[VMEM, ANY, ANY, VMEM, VMEM],
        out_specs=[ANY, ANY, ANY, VMEM, VMEM],
        scratch_shapes=[
            pltpu.VMEM((kinds, depth, hw), BF),
            pltpu.VMEM((per, hw, hw), BF),
            *PlaneGather.scratch(nz, ne, False),
            DMA((nz, kinds)), DMA((nz, kinds)), DMA((nz, kinds)), DMA((nz, kinds)),
            DMA((kinds,)), DMA((kinds,)), DMA((per,)), DMA((nz, per)), DMA, DMA,
            DMA, DMA, DMA, DMA,
        ],
        compiler_params=pltpu.CompilerParams(collective_id=cid, has_side_effects=True),
        name="start_gather",
    )(x, w_qkv, w_out, small, seg)


def lay_kernel(kinds, hw, x_ref, *outs):
    for k in range(kinds):
        piece = x_ref[0, :, k * hw : (k + 1) * hw].astype(F32)
        if k < kinds - 1:
            outs[0][k] = piece
        else:
            outs[1][...] = piece


def lay_mixer(wide, kinds, hw):
    ne, rows, _ = wide.shape
    return pl.pallas_call(
        functools.partial(lay_kernel, kinds, hw),
        grid=(ne,),
        in_specs=[pl.BlockSpec((1, rows, kinds * hw), lambda i: (i, 0, 0))],
        out_specs=[
            pl.BlockSpec((kinds - 1, rows, hw), lambda i: (0, 0, i)),
            pl.BlockSpec((rows, hw), lambda i: (0, i)),
        ],
        out_shape=[
            jax.ShapeDtypeStruct((kinds - 1, rows, ne * hw), F32),
            jax.ShapeDtypeStruct((rows, ne * hw), F32),
        ],
        name="lay_mixer",
    )(wide)


def lay_experts_kernel(per_dev, fl, x_ref, gate_ref, up_ref):
    for i in range(per_dev):
        gate_ref[i] = x_ref[0, :, i * fl : (i + 1) * fl].astype(F32)
        up_ref[i] = x_ref[0, :, (per_dev + i) * fl : (per_dev + i + 1) * fl].astype(F32)


def lay_experts(wide, per_dev, fl):
    nz, rows, _ = wide.shape
    out = jax.ShapeDtypeStruct((per_dev, rows, nz * fl), F32)
    spec = pl.BlockSpec((per_dev, rows, fl), lambda i: (0, 0, i))
    return pl.pallas_call(
        functools.partial(lay_experts_kernel, per_dev, fl),
        grid=(nz,),
        in_specs=[pl.BlockSpec((1, rows, 2 * per_dev * fl), lambda i: (i, 0, 0))],
        out_specs=[spec, spec],
        out_shape=[out, out],
        name="lay_experts",
    )(wide)


def moe_kernel(
    fl, h_ref, g_ref, gate_ref, win_ref, wdt_ref, wd_ref, wint_ref,
    mix_ref, gh_ref, gg_ref, dwin_ref, dwd_ref, acc_in, acc_d,
):
    step = pl.program_id(0)
    tile, width = h_ref.shape
    per_dev = gate_ref.shape[1]
    h = h_ref[...]
    g = g_ref[...]
    gates = gate_ref[...]
    pre = dot(h, win_ref[...], NN)
    graw = dot(g, wdt_ref[...], NN)
    scaled_act, grad_gate, grad_up = [], [], []
    lanes = lax.broadcasted_iota(jnp.int32, (tile, 128), 1)
    gg = jnp.zeros((tile, 128), F32)
    for i in range(per_dev):
        u = pre[:, i * fl : (i + 1) * fl]
        w = pre[:, (per_dev + i) * fl : (per_dev + 1 + i) * fl]
        gr = graw[:, i * fl : (i + 1) * fl]
        gate = gates[:, i : i + 1]
        sig = 1.0 / (1.0 + jnp.exp(-u))
        silu = u * sig
        act = silu * w
        total = jnp.sum(act.astype(BF).astype(F32) * gr, axis=-1, keepdims=True)
        gg = jnp.where(lanes == i, total, gg)
        scaled_act.append((gate * act).astype(BF))
        gact = gate * gr
        grad_gate.append((gact * w * (sig * (1.0 + u * (1.0 - sig)))).astype(BF))
        grad_up.append((gact * silu).astype(BF))
    a = jnp.concatenate(scaled_act, axis=1)
    gin = jnp.concatenate(grad_gate + grad_up, axis=1)
    blocks, rows = mix_ref.shape[0], mix_ref.shape[2]
    mix_ref[...] = dot(a, wd_ref[...], NN).astype(BF).reshape(blocks, 1, rows, width)
    gh_ref[...] = dot(gin, wint_ref[...], NN).astype(BF)
    turned = gg.T[:8]
    for i in range(blocks):
        gg_ref[i] = turned[:, i * rows : (i + 1) * rows]

    @pl.when(step == 0)
    def _():
        acc_in[...] = jnp.zeros_like(acc_in)
        acc_d[...] = jnp.zeros_like(acc_d)

    acc_in[...] += dot(h, gin, TN)
    acc_d[...] += dot(a, g, TN)

    @pl.when(step == pl.num_programs(0) - 1)
    def _():
        dwin_ref[...] = acc_in[...].astype(BF)
        dwd_ref[...] = acc_d[...]


def moe(h_all, g_all, gates2, w_in, wd_t, wd, w_in_t, nz, ne, rows_dev, blocks):
    count, width = h_all.shape
    hid4 = w_in.shape[1]
    hid2 = wd.shape[0]
    per_dev = gates2.shape[1]
    fl = hid2 // per_dev
    tile = blocks * rows_dev
    turns = ne // blocks
    rows = lambda n: pl.BlockSpec((tile, n), lambda i: (i, 0))
    whole = lambda s: pl.BlockSpec(s, lambda i: (0, 0), pipeline_mode=pl.Buffered(1))
    return pl.pallas_call(
        functools.partial(moe_kernel, fl),
        grid=(count // tile,),
        in_specs=[
            rows(width), rows(width), rows(per_dev),
            whole(w_in.shape), whole(wd_t.shape), whole(wd.shape), whole(w_in_t.shape),
        ],
        out_specs=[
            pl.BlockSpec((blocks, 1, rows_dev, width), lambda i: (i % turns, i // turns, 0, 0)),
            rows(width),
            pl.BlockSpec((blocks, 8, rows_dev), lambda i: (i, 0, 0)),
            whole((width, hid4)), whole((hid2, width)),
        ],
        out_shape=[
            jax.ShapeDtypeStruct((ne, nz, rows_dev, width), BF),
            jax.ShapeDtypeStruct((count, width), BF),
            jax.ShapeDtypeStruct((nz * ne, 8, rows_dev), F32),
            jax.ShapeDtypeStruct((width, hid4), BF),
            jax.ShapeDtypeStruct((hid2, width), F32),
        ],
        scratch_shapes=[pltpu.VMEM((width, hid4), F32), pltpu.VMEM((hid2, width), F32)],
        compiler_params=pltpu.CompilerParams(vmem_limit_bytes=66_000_000),
        cost_estimate=pl.CostEstimate(
            flops=2 * count * width * hid2 * 9,
            bytes_accessed=8 * count * width + 24 * hid4 * width,
            transcendentals=count * hid2,
        ),
        name="moe",
    )(h_all, g_all, gates2, w_in, wd_t, wd, w_in_t)


def body(inputs, segments, routes, w_qkv, w_out, w_router, gains, w_gate, w_up, w_down, cotangent):
    z = lax.axis_index("dp")
    e = lax.axis_index("expert")
    nz = lax.axis_size("dp")
    ne = lax.axis_size("expert")
    count, width = inputs.shape
    num_seqs, length = segments.shape
    heads = width // HD // ne
    hw = heads * HD
    expert_count = w_router.shape[1]
    per_dev = w_gate.shape[0]
    hidden = w_gate.shape[2]
    fl = hidden // nz
    both = ("dp", "expert")

    pad = -(expert_count + 4) % 16
    small = jnp.concatenate(
        [w_router.T, gains.T, jnp.zeros((pad, gains.shape[0]), BF)], axis=0
    )
    seg8 = jnp.broadcast_to(segments[:, None, :], (num_seqs, 8, length)).reshape(-1, length)
    in_all, wq, wo, small, seg_all = start_gather(
        inputs, w_qkv.transpose(1, 0, 2), w_out, small, seg8, nz, ne, hw, 0
    )
    small = small.transpose(1, 0, 2).reshape(-1, width)
    router_t = small[:expert_count]
    gain_mat = small[expert_count : expert_count + 4].astype(F32)
    my_gains = lax.dynamic_slice_in_dim(gain_mat, e * hw, hw, axis=1)
    seg_all = seg_all.reshape(ne * num_seqs, 8, length)[:, 0]

    cot, _ = lax.optimization_barrier((cotangent, small))
    g_all = lax.all_gather(cot, both, axis=0, tiled=True)
    in_all = in_all.reshape(ne * count, width).astype(F32)
    h1_all = (in_all * rms_scale(in_all) * gain_mat[0]).astype(BF)
    inputs_f = inputs.astype(F32)
    scale_one = rms_scale(inputs_f)
    plane = h1_all.shape[0]
    shape_heads = (ne * num_seqs, length, heads, HD)

    q, k, v = [dot(h1_all, wq[j], NN) for j in range(3)]
    sums = jnp.stack([jnp.sum(q * q, axis=-1), jnp.sum(k * k, axis=-1)])
    scales = lax.rsqrt(lax.psum(sums, "expert") / width + EPS)
    aq, ak = scales[0][:, None], scales[1][:, None]
    cos_tab, sin_tab = rope_tables(length)
    rq = rotate((q * aq * my_gains[1]).reshape(shape_heads), cos_tab, sin_tab).astype(BF)
    rk = rotate((k * ak * my_gains[2]).reshape(shape_heads), cos_tab, sin_tab).astype(BF)
    vb = v.astype(BF).reshape(shape_heads)
    o, lse = jax.vmap(attend_forward)(rq, rk, vb, seg_all)
    o = o.reshape(plane, hw)
    x1_part = dot(o, wo, NN).astype(BF)
    (x1_sum,) = scatter_tokens(x1_part.reshape(ne, count, width), nz, ne, False, 1)
    x1 = inputs_f + x1_sum

    a2 = rms_scale(x1)
    h2 = (x1 * a2 * gain_mat[3]).astype(BF)
    probs = jax.nn.softmax(dot(h2, router_t, NT), axis=-1)
    picks = jnp.sum(
        (routes[:, :, None] == jnp.arange(expert_count, dtype=jnp.int32)).astype(F32), axis=1
    )
    gates = picks * probs

    h2_all, gates_all = gather_tokens(h2, nz, ne, True, 2, small=gates.T)
    h2_all = h2_all.reshape(-1, width)
    gates2 = lax.dynamic_slice_in_dim(gates_all, e * per_dev, per_dev, axis=1)
    gates2 = gates2.transpose(0, 2, 1).reshape(-1, per_dev)
    wg = lax.dynamic_slice_in_dim(w_gate, z * fl, fl, axis=2)
    wu = lax.dynamic_slice_in_dim(w_up, z * fl, fl, axis=2)
    wd = lax.dynamic_slice_in_dim(w_down, z * fl, fl, axis=1)
    w_in_t = jnp.concatenate(
        [wg.transpose(0, 2, 1), wu.transpose(0, 2, 1)], axis=0
    ).reshape(2 * per_dev * fl, width)
    w_in = jnp.concatenate([wg[0], wg[1], wu[0], wu[1]], axis=1)
    wd = wd.reshape(per_dev * fl, width)
    mix, gh, gg, dwin, dwd = moe(
        h2_all, g_all, gates2, w_in, wd.T, wd, w_in_t, nz, ne, count, min(4, ne)
    )
    grad_from_experts, gg = scatter_tokens(
        gh.reshape(nz * ne, count, width), nz, ne, True, 3, small=gg
    )
    grad_gates = jnp.sum(gg.reshape(nz, ne, 8, count), axis=0)[:, :per_dev]
    grad_gates = grad_gates.reshape(expert_count, count).T

    mix = lax.psum_scatter(mix.reshape(-1, width), "expert", scatter_dimension=0, tiled=True)
    mix = lax.psum_scatter(mix, "dp", scatter_dimension=0, tiled=True)
    output = (x1 + mix.astype(F32)).astype(BF)

    dwin = lax.all_to_all(
        dwin.reshape(nz, width // nz, 2 * per_dev * fl), "dp", split_axis=0, concat_axis=0, tiled=True
    )
    grad_w_gate, grad_w_up = lay_experts(dwin, per_dev, fl)
    grad_w_down = dwd.reshape(per_dev, fl, width)

    grad_top = cotangent.astype(F32)
    grad_probs = picks * grad_gates
    glog = (probs * (grad_probs - jnp.sum(probs * grad_probs, axis=-1, keepdims=True))).astype(BF)
    local_router = dot(h2, glog, TN)
    gh2 = grad_from_experts + dot(glog, router_t, NN)
    grad_ffn, gain_ffn = rms_backward(x1, a2, gain_mat[3], gh2)
    gx1 = grad_top + grad_ffn
    gab = gx1.astype(BF)

    gab_all = gather_tokens(gab, nz, ne, False, 4)[0].reshape(-1, width)
    go = dot(gab_all, wo, NT).astype(BF).reshape(shape_heads)
    grad_q, grad_k, gv = jax.vmap(attend_backward)(rq, rk, vb, seg_all, lse, go)
    gqn = rotate(grad_q, cos_tab, -sin_tab).reshape(plane, hw)
    gkn = rotate(grad_k, cos_tab, -sin_tab).reshape(plane, hw)
    nq, nk = q * aq, k * ak
    sq, sk = gqn * my_gains[1], gkn * my_gains[2]
    sums = jnp.stack([jnp.sum(sq * nq, axis=-1), jnp.sum(sk * nk, axis=-1)])
    means = lax.psum(sums, "expert") / width
    gq = (aq * (sq - nq * means[0][:, None])).astype(BF)
    gk = (ak * (sk - nk * means[1][:, None])).astype(BF)
    gproj = [gq, gk, gv.reshape(plane, hw)]
    gain_q, gain_k = jnp.sum(gqn * nq, axis=0), jnp.sum(gkn * nk, axis=0)

    gh1_part = sum(dot(part, wq[j], NT) for j, part in enumerate(gproj)).astype(BF)
    (gh1,) = scatter_tokens(gh1_part.reshape(ne, count, width), nz, ne, False, 5)
    grad_front, gain_attn = rms_backward(inputs_f, scale_one, gain_mat[0], gh1)
    grad_inputs = (gx1 + grad_front).astype(BF)

    part_out = dot(o, gab_all, TN).astype(BF)
    part_out = lax.all_to_all(
        part_out.reshape(hw, ne, hw).transpose(1, 0, 2),
        "expert", split_axis=0, concat_axis=0, tiled=True,
    ).reshape(width, hw)
    parts = [dot(h1_all, part, TN).astype(BF) for part in gproj] + [part_out]
    mine = lax.psum_scatter(
        jnp.concatenate(parts, axis=1), "dp", scatter_dimension=0, tiled=True
    )
    wide = gather_tokens(mine, nz, ne, False, 6)[0]
    grad_w_qkv, grad_w_out = lay_mixer(wide, 4, hw)
    grad_w_qkv = grad_w_qkv.transpose(1, 0, 2)

    place = lambda part: lax.dynamic_update_slice_in_dim(
        jnp.zeros((width,), F32), part, e * hw, axis=0
    )
    tiny = jnp.concatenate(
        [
            local_router,
            jnp.stack([gain_attn, place(gain_q), place(gain_k), gain_ffn], axis=1),
        ],
        axis=1,
    )
    tiny = lax.psum(tiny, both)
    tiny = lax.dynamic_slice_in_dim(tiny, z * (width // nz), width // nz, axis=0)
    grad_w_router, grad_gains = tiny[:, :expert_count], tiny[:, expert_count:]
    return (
        output,
        grad_inputs,
        grad_w_qkv,
        grad_w_out,
        grad_w_router,
        grad_gains,
        grad_w_gate,
        grad_w_up,
        grad_w_down,
    )


def solution(mesh):
    tokens = P(("dp", "expert"), None)
    rows = P("dp", None)
    rows3 = P("dp", None, None)
    owned = P("expert", None, None)
    return jax.shard_map(
        body,
        mesh=mesh,
        in_specs=(tokens, tokens, tokens, rows3, rows, rows, rows, owned, owned, owned, tokens),
        out_specs=(tokens, tokens, rows3, rows, rows, rows)
        + (P("expert", "dp", None),) * 3,
        check_vma=False,
    )
```

```python
import functools

import jax
import jax.numpy as jnp
from jax import lax
from jax.experimental import pallas as pl
from jax.experimental.pallas import tpu as pltpu
from jax.sharding import PartitionSpec as P


HD = 128
EPS = 1e-05
ROPE_BASE = 10000.0
MASKED = -1e30
BF = jnp.bfloat16
F32 = jnp.float32


def dot(a, b, dims):
    return lax.dot_general(a, b, (dims, ((), ())), preferred_element_type=F32)


NN = ((1,), (0,))
NT = ((1,), (1,))
TN = ((0,), (0,))


def rms_scale(values):
    return lax.rsqrt(jnp.mean(values * values, axis=-1, keepdims=True) + EPS)


def rms_backward(values, inv_rms, gain_col, grad_out):
    normed = values * inv_rms
    grad_gain = jnp.sum(grad_out * normed, axis=0)
    scaled = grad_out * gain_col
    grad_values = inv_rms * (scaled - normed * jnp.mean(scaled * normed, axis=-1, keepdims=True))
    return (grad_values, grad_gain)


def rope_tables(length):
    half = HD // 2
    freqs = jnp.exp(-jnp.log(ROPE_BASE) * (2.0 * jnp.arange(half, dtype=F32) / HD))
    angles = jnp.arange(length, dtype=F32)[:, None] * freqs[None, :]
    return (jnp.cos(angles)[:, None, :], jnp.sin(angles)[:, None, :])


def rotate(values, cos_tab, sin_tab):
    first, second = jnp.split(values, 2, axis=-1)
    return jnp.concatenate(
        [first * cos_tab - second * sin_tab, second * cos_tab + first * sin_tab], axis=-1
    )


def attend_scores(query_rot, key_rot, seg_ids):
    places = jnp.arange(seg_ids.shape[0], dtype=jnp.int32)
    allowed = (places[:, None] >= places[None, :]) & (seg_ids[:, None] == seg_ids[None, :])
    scores = jnp.einsum("qhd,khd->hqk", query_rot, key_rot, preferred_element_type=F32)
    scores = scores * query_rot.shape[-1] ** (-0.5)
    return jnp.where(allowed[None], scores, MASKED)


def attend_forward(query_rot, key_rot, value_bf, seg_ids):
    scores = attend_scores(query_rot, key_rot, seg_ids)
    row_max = jnp.max(scores, axis=-1, keepdims=True)
    log_total = row_max + jnp.log(jnp.sum(jnp.exp(scores - row_max), axis=-1, keepdims=True))
    weights_bf = jnp.exp(scores - log_total).astype(BF)
    mixed = jnp.einsum("hqk,khd->qhd", weights_bf, value_bf, preferred_element_type=F32)
    return (mixed.astype(BF), log_total)


def attend_backward(query_rot, key_rot, value_bf, seg_ids, log_total, grad_heads):
    scores = attend_scores(query_rot, key_rot, seg_ids)
    probs = jnp.exp(scores - log_total)
    grad_value = jnp.einsum(
        "hqk,qhd->khd", probs.astype(BF), grad_heads, preferred_element_type=F32
    ).astype(BF)
    grad_probs = jnp.einsum("qhd,khd->hqk", grad_heads, value_bf, preferred_element_type=F32)
    delta = jnp.sum(probs * grad_probs, axis=-1, keepdims=True)
    grad_scores = (probs * (grad_probs - delta) * query_rot.shape[-1] ** (-0.5)).astype(BF)
    grad_query = jnp.einsum("hqk,khd->qhd", grad_scores, key_rot, preferred_element_type=F32)
    grad_key = jnp.einsum("hqk,qhd->khd", grad_scores, query_rot, preferred_element_type=F32)
    return (grad_query, grad_key, grad_value)


MESH = pl.DeviceIdType.MESH
ANY = pl.BlockSpec(memory_space=pl.ANY)
VMEM = pl.BlockSpec(memory_space=pltpu.VMEM)
DMA = pltpu.SemaphoreType.DMA


def flip(index, bit):
    return index + bit * (1 - 2 * ((index // bit) % 2))


def flips(index, bits):
    out = [index]
    for bit in bits:
        out = out + [flip(i, bit) for i in out]
    return out


def bit_orders(ne):
    bits = [1 << b for b in range(ne.bit_length() - 1)]
    return [bits[:1] + bits[1:], bits[:1] + bits[1:][::-1]]


def nearest(z, r, nz):
    low = jnp.minimum(z, nz - 1 - z)
    near = z - (r + 1) // 2 if r % 2 else z + r // 2
    far = jnp.where(2 * z < nz, z + (r - low), z - (r - low))
    return jnp.where(r <= 2 * low, near, far)


def remote(src, dst, send, recv, peer):
    return pltpu.make_async_remote_copy(
        src_ref=src, dst_ref=dst, send_sem=send, recv_sem=recv, device_id=peer, device_id_type=MESH
    )


def for_others(nz, ne, z, e, act):
    def step(i, carry):
        flat = lax.rem(z * ne + e + i, nz * ne)
        act(flat // ne, lax.rem(flat, ne), flat)
        return carry

    lax.fori_loop(1, nz * ne, step, 0)


def meet_all(nz, ne, z, e):
    sem = pltpu.get_barrier_semaphore()

    def greet(zz, ee, flat):
        pl.semaphore_signal(sem, inc=1, device_id=(zz, ee), device_id_type=MESH)

    for_others(nz, ne, z, e, greet)
    pl.semaphore_wait(sem, nz * ne - 1)


def meet_column_and_plane(nz, ne, z, e, spread):
    sem = pltpu.get_barrier_semaphore()
    peers = [(z, flip(e, 1 << b)) for b in range(ne.bit_length() - 1)]
    if spread:
        peers += [(lax.rem(z + r, nz), e) for r in range(1, nz)]
    for peer in peers:
        pl.semaphore_signal(sem, inc=1, device_id=peer, device_id_type=MESH)
    pl.semaphore_wait(sem, len(peers))


class PlaneGather:
    def __init__(self, nz, ne, z, e, spread, x_ref, out_ref, zsend, zrecv, send, recv, local):
        self.nz, self.ne, self.z, self.e, self.spread = nz, ne, z, e, spread
        self.x, self.out = x_ref, out_ref
        self.zsend, self.zrecv, self.send, self.recv = zsend, zrecv, send, recv
        self.rounds = nz if spread else 1
        self.half = x_ref.shape[0] // 2
        self.orders = [o[1:] + o[:1] for o in bit_orders(ne)]
        self.planes = [z if spread else 0] + [nearest(z, r, nz) for r in range(1, self.rounds)]
        self.pending, self.arrivals = [], {}
        own = self.slot(0, e)
        keep = pltpu.make_async_copy(x_ref, out_ref.at[own], local)
        keep.start()
        self.pending.append(keep.wait)

    @staticmethod
    def scratch(nz, ne, spread):
        rounds = nz if spread else 1
        return [DMA((nz,)), DMA((nz,)), DMA((rounds, 2, ne - 1)), DMA((rounds, 2, ne - 1)), DMA]

    def slot(self, r, ee):
        return self.planes[r] * self.ne + ee

    def spread_own(self):
        for r in range(1, self.rounds):
            to = self.planes[r]
            copy = remote(
                self.x, self.out.at[self.slot(0, self.e)],
                self.zsend.at[r], self.zrecv.at[self.z], (to, self.e),
            )
            copy.start()
            self.pending.append(copy.wait_send)

    def forward(self, r, s, stage, subset):
        order = self.orders[s]
        rows = pl.ds(s * self.half, self.half)
        peer_e = flip(self.e, order[stage])
        n = (1 << stage) - 1 + subset
        block = self.slot(r, flips(self.e, order[:stage])[subset])
        dst = self.out.at[block, rows]
        src = self.x.at[rows] if r == 0 and subset == 0 else dst
        sems = self.send.at[r, s, n], self.recv.at[r, s, n]
        copy = remote(src, dst, *sems, (self.z, peer_e))
        copy.start()
        self.pending.append(copy.wait_send)
        got = self.out.at[self.slot(r, flips(peer_e, order[:stage])[subset]), rows]
        self.arrivals[(r, s, stage, subset)] = remote(got, got, *sems, (self.z, peer_e)).wait_recv

    def start_round(self, r):
        if r > 0:
            here = self.out.at[self.slot(r, self.e)]
            remote(
                here, here, self.zsend.at[r], self.zrecv.at[self.planes[r]], (self.planes[r], self.e)
            ).wait_recv()
        for stage in range(len(self.orders[0])):
            for s in range(2):
                self.forward(r, s, stage, 0)

    def finish_round(self, r):
        stages = len(self.orders[0])
        for stage in range(stages):
            for subset in range(1 << stage):
                for s in range(2):
                    self.arrivals.pop((r, s, stage, subset))()
                    for later in range(stage + 1, stages):
                        self.forward(r, s, later, subset + (1 << stage))

    def finish(self):
        for wait in self.pending:
            wait()


def gather_kernel(nz, ne, spread, x_ref, out_ref, *sems):
    z, e = lax.axis_index("dp"), lax.axis_index("expert")
    meet_column_and_plane(nz, ne, z, e, spread)
    net = PlaneGather(nz, ne, z, e, spread, x_ref, out_ref, *sems)
    net.spread_own()
    net.start_round(0)
    for r in range(1, net.rounds):
        net.start_round(r)
        net.finish_round(r - 1)
    net.finish_round(net.rounds - 1)
    net.finish()


def gather_tokens(x, nz, ne, spread, cid):
    rounds = nz if spread else 1
    return pl.pallas_call(
        functools.partial(gather_kernel, nz, ne, spread),
        out_shape=jax.ShapeDtypeStruct((rounds * ne, *x.shape), x.dtype),
        in_specs=[VMEM],
        out_specs=ANY,
        scratch_shapes=PlaneGather.scratch(nz, ne, spread),
        compiler_params=pltpu.CompilerParams(collective_id=cid, has_side_effects=True),
        name="gather_tokens",
    )(x)


def add_rows(dst, src, tile=16):
    def step(i, carry):
        rows = pl.ds(pl.multiple_of(i * tile, tile), tile)
        dst[rows, :] = (dst[rows, :].astype(F32) + src[rows, :].astype(F32)).astype(dst.dtype)
        return carry

    lax.fori_loop(0, dst.shape[0] // tile, step, 0)


def scatter_kernel(nz, ne, spread, x_ref, *refs):
    out_ref, acc, got, zgot, loads, send, recv, zsend, zrecv = refs[-9:]
    z, e = lax.axis_index("dp"), lax.axis_index("expert")
    meet_column_and_plane(nz, ne, z, e, spread)
    rounds = nz if spread else 1
    stages = ne.bit_length() - 1
    half = out_ref.shape[0] // 2
    orders = bit_orders(ne)
    pending, arrivals, zwait = [], {}, {}
    ranks = list(range(1, rounds)) + [0]
    first = [0] * (stages + 1)
    for j in range(stages):
        first[j + 1] = first[j] + (ne >> (j + 1))

    def plane_of(r):
        return lax.rem(z + r, nz) * ne if spread else 0

    def push(r, s, j):
        order = orders[s]
        peer = (z, flip(e, order[j]))
        rest = ne >> (j + 1)
        for i in range(rest):
            n = first[j] + i
            if j == 0:
                block = flips(peer[1], order[:0:-1])[i]
                src = x_ref.at[plane_of(r) + block, pl.ds(s * half, half)]
            else:
                src = acc.at[r, s, rest + i]
            copy = remote(src, got.at[r, s, n], send.at[r, s, n], recv.at[r, s, n], peer)
            copy.start()
            pending.append(copy.wait_send)
            arrivals.setdefault((r, s, j), []).append((copy.wait_recv, i, n))

    for r in ranks:
        for s in range(2):
            push(r, s, 0)
            for i, block in enumerate(flips(e, orders[s][:0:-1])):
                copy = pltpu.make_async_copy(
                    x_ref.at[plane_of(r) + block, pl.ds(s * half, half)],
                    acc.at[r, s, i],
                    loads.at[r, s, i],
                )
                copy.start()
                arrivals.setdefault((r, s, -1), []).append(copy.wait)
    for t in range(rounds + stages):
        for place, r in enumerate(ranks):
            j = t - place
            if not 0 <= j < stages:
                continue
            for s in range(2):
                if j == 0:
                    for wait in arrivals.pop((r, s, -1)):
                        wait()
                for wait, i, n in arrivals.pop((r, s, j)):
                    wait()
                    add_rows(acc.at[r, s, i], got.at[r, s, n])
                if j + 1 < stages:
                    push(r, s, j + 1)
                elif r > 0:
                    copy = remote(
                        acc.at[r, s, 0], zgot.at[r, s], zsend.at[r, s], zrecv.at[r, s],
                        (lax.rem(z + r, nz), e),
                    )
                    copy.start()
                    pending.append(copy.wait_send)
                    zwait[(r, s)] = copy.wait_recv
    for s in range(2):
        for r in range(1, rounds):
            zwait[(r, s)]()

        def step(i, carry):
            rows = pl.ds(pl.multiple_of(i * 16, 16), 16)
            total = acc[0, s, 0, rows, :].astype(F32)
            for r in range(1, rounds):
                total = total + zgot[r, s, rows, :].astype(F32)
            out_ref[pl.ds(pl.multiple_of(s * half + i * 16, 16), 16), :] = total.astype(out_ref.dtype)
            return carry

        lax.fori_loop(0, half // 16, step, 0)
    for wait in pending:
        wait()


def scatter_tokens(parts, nz, ne, spread, cid, after=None):
    rounds = nz if spread else 1
    _, count, width = parts.shape
    half = count // 2
    held = (2 * rounds * (ne // 2 + ne - 1) + 2 * nz) * half * width * 2
    if held > 56_000_000:
        cut = width // 256 * 128
        left = scatter_tokens(parts[..., :cut], nz, ne, spread, cid, after)
        right = scatter_tokens(parts[..., cut:], nz, ne, spread, cid + 16)
        return [jnp.concatenate([left[0], right[0]], axis=1), *left[1:]]
    more = [] if after is None else [after]
    return pl.pallas_call(
        functools.partial(scatter_kernel, nz, ne, spread),
        out_shape=[jax.ShapeDtypeStruct(m.shape, m.dtype) for m in more]
        + [jax.ShapeDtypeStruct((count, width), F32)],
        in_specs=[ANY] * (1 + len(more)),
        out_specs=[ANY] * len(more) + [VMEM],
        scratch_shapes=[
            pltpu.VMEM((rounds, 2, ne // 2, half, width), BF),
            pltpu.VMEM((rounds, 2, ne - 1, half, width), BF),
            pltpu.VMEM((nz, 2, half, width), BF),
            DMA((rounds, 2, ne // 2)),
            DMA((rounds, 2, ne - 1)),
            DMA((rounds, 2, ne - 1)),
            DMA((nz, 2)),
            DMA((nz, 2)),
        ],
        input_output_aliases={1: 0} if more else {},
        compiler_params=pltpu.CompilerParams(
            collective_id=cid, has_side_effects=True, vmem_limit_bytes=64_000_000
        ),
        name="scatter_tokens",
    )(parts, *more)[::-1]


def reduce_kernel(nz, ne, x_ref, out_ref, got, total, far, send1, recv1, send2, recv2):
    z, e = lax.axis_index("dp"), lax.axis_index("expert")
    per = ne // nz
    meet_all(nz, ne, z, e)
    first = []
    for r in range(1, ne):
        to = lax.rem(e + r, ne)
        copy = remote(x_ref.at[to], got.at[r], send1.at[r], recv1.at[r], (z, to))
        copy.start()
        first.append(copy)
    acc = x_ref[e]
    for r, copy in enumerate(first):
        copy.wait_recv()
        acc = acc + got[r + 1]
    total[...] = acc
    home, place = e // per, lax.rem(e, per)
    for r in range(ne):
        to = lax.rem(e + r, ne)
        copy = remote(total, far.at[z, place], send2.at[r], recv2, (home, to))
        if r > 0:
            copy.start()
        else:

            @pl.when(home != z)
            def _():
                copy.start()

            @pl.when(home == z)
            def _():
                far[z, place] = total[...]

    for copy in first:
        copy.wait_send()
    for r in range(ne):
        copy = remote(total, far.at[z, place], send2.at[r], recv2, (home, e))
        if r > 0:
            copy.wait_send()
        else:

            @pl.when(home != z)
            def _():
                copy.wait_send()

    def arrive(count):
        flat = got.at[pl.ds(0, count)]
        remote(flat, flat, send2.at[0], recv2, (z, e)).wait_recv()

    @pl.when(home == z)
    def _():
        arrive(nz * per - 1)

    @pl.when(home != z)
    def _():
        arrive(nz * per)

    for i in range(per):
        out_ref[i] = sum(far[k, i] for k in range(nz))


def reduce_columns(x, nz, ne, cid):
    rows, width = x.shape
    per = ne // nz
    x = x.reshape(rows, ne, width // ne).transpose(1, 0, 2)
    out = pl.pallas_call(
        functools.partial(reduce_kernel, nz, ne),
        out_shape=jax.ShapeDtypeStruct((per, rows, width // ne), F32),
        in_specs=[VMEM],
        out_specs=VMEM,
        scratch_shapes=[
            pltpu.VMEM((ne, rows, width // ne), F32),
            pltpu.VMEM((rows, width // ne), F32),
            pltpu.VMEM((nz, per, rows, width // ne), F32),
            DMA((ne,)), DMA((ne,)), DMA((ne,)), DMA,
        ],
        compiler_params=pltpu.CompilerParams(collective_id=cid, has_side_effects=True),
        name="reduce_columns",
    )(x)
    return out.transpose(1, 0, 2).reshape(rows, per * (width // ne))


def start_kernel(
    nz, ne, x_ref, wqkv_ref, wout_ref, small_ref, seg_ref, _,
    out_ref, wq_ref, wo_ref, small_out, seg_out, _2,
    wbuf, pbuf, zsend, zrecv, send, recv, local,
    up_send, up_recv, dn_send, dn_recv, wload, wkeep, pload, psend, precv, pkeep,
    small_send, small_recv, seg_send, seg_recv,
):
    z, e = lax.axis_index("dp"), lax.axis_index("expert")
    kinds, depth, hw = wbuf.shape
    per = ne // nz
    loads = [
        pltpu.make_async_copy(wqkv_ref.at[j, :, pl.ds(e * hw, hw)], wbuf.at[j], wload.at[j])
        for j in range(kinds)
    ]
    for copy in loads:
        copy.start()
    pieces = [
        pltpu.make_async_copy(
            wout_ref.at[pl.ds(i * hw, hw), pl.ds(e * hw, hw)], pbuf.at[i], pload.at[i]
        )
        for i in range(per)
    ]
    for copy in pieces:
        copy.start()
    meet_all(nz, ne, z, e)

    def rows_of(zz):
        return pl.ds(pl.multiple_of(zz * depth, depth), depth)

    def hop(j, zz, dist, up):
        send, recv = (up_send, up_recv) if up else (dn_send, dn_recv)
        here = wq_ref.at[j, rows_of(zz)]
        src = wbuf.at[j] if dist == 1 else here
        to = z + 1 if up else z - 1
        return remote(src, here, send.at[dist, j], recv.at[dist, j], (to, e))

    keeps = []
    for j in range(kinds):
        loads[j].wait()

        @pl.when(z + 1 < nz)
        def _():
            hop(j, z, 1, True).start()

        @pl.when(z > 0)
        def _():
            hop(j, z, 1, False).start()

        keep = pltpu.make_async_copy(wbuf.at[j], wq_ref.at[j, rows_of(z)], wkeep.at[j])
        keep.start()
        keeps.append(keep)

    def wait_all(ref, send, recv, count):
        most = ref.at[pl.ds(0, count)]
        both = remote(most, most, send, recv, (z, flip(e, 1)))
        both.wait_send()
        both.wait_recv()

    small_out[z] = small_ref[...]
    for r in range(1, nz):
        remote(
            small_ref, small_out.at[z], small_send, small_recv, (lax.rem(z + r, nz), e)
        ).start()
    seg_out[e] = seg_ref[...]
    for r in range(1, ne):
        remote(seg_ref, seg_out.at[e], seg_send, seg_recv, (z, lax.rem(e + r, ne))).start()
    net = PlaneGather(nz, ne, z, e, False, x_ref, out_ref, zsend, zrecv, send, recv, local)
    net.start_round(0)

    columns = pl.ds(e * hw, hw)
    for i in range(per):
        pieces[i].wait()
    for r in range(nz):
        for i in range(per):
            to = (lax.rem(z + r, nz), z * per + i)
            give = remote(pbuf.at[i], wo_ref.at[:, columns], psend.at[r, i], precv, to)
            if r > 0:
                give.start()
            else:
                own = pltpu.make_async_copy(pbuf.at[i], wo_ref.at[:, columns], pkeep)

                @pl.when(to[1] == e)
                def _():
                    own.start()

                @pl.when(to[1] != e)
                def _():
                    give.start()
    net.finish_round(0)
    for dist in range(1, nz):
        for j in range(kinds):

            @pl.when(z - dist >= 0)
            def _():
                got = wq_ref.at[j, rows_of(z - dist)]
                remote(got, got, up_send.at[dist, j], up_recv.at[dist, j], (z, e)).wait_recv()

                @pl.when(z + 1 < nz)
                def _():
                    if dist + 1 < nz:
                        hop(j, z - dist, dist + 1, True).start()

            @pl.when(z + dist < nz)
            def _():
                got = wq_ref.at[j, rows_of(z + dist)]
                remote(got, got, dn_send.at[dist, j], dn_recv.at[dist, j], (z, e)).wait_recv()

                @pl.when(z > 0)
                def _():
                    if dist + 1 < nz:
                        hop(j, z + dist, dist + 1, False).start()

    net.finish()
    for keep in keeps:
        keep.wait()
    for dist in range(1, nz):
        for j in range(kinds):

            @pl.when((z - dist + 1 >= 0) & (z + 1 < nz))
            def _():
                hop(j, z - dist + 1, dist, True).wait_send()

            @pl.when((z + dist - 1 < nz) & (z > 0))
            def _():
                hop(j, z + dist - 1, dist, False).wait_send()

    for r in range(nz):
        for i in range(per):
            to = (lax.rem(z + r, nz), z * per + i)
            give = remote(pbuf.at[i], wo_ref.at[:, columns], psend.at[r, i], precv, to)
            if r > 0:
                give.wait_send()
            else:
                own = pltpu.make_async_copy(pbuf.at[i], wo_ref.at[:, columns], pkeep)

                @pl.when(to[1] == e)
                def _():
                    own.wait()

                @pl.when(to[1] != e)
                def _():
                    give.wait_send()

    def wait_pieces(count):
        most = wo_ref.at[:, pl.ds(0, count * hw)]
        remote(most, most, psend.at[0, 0], precv, (z, e)).wait_recv()

    @pl.when(z == e // per)
    def _():
        wait_pieces(ne - 1)

    @pl.when(z != e // per)
    def _():
        wait_pieces(ne)

    wait_all(small_out, small_send, small_recv, nz - 1)
    wait_all(seg_out, seg_send, seg_recv, ne - 1)


def start_gather(x, w_qkv, w_out, small, seg, after, nz, ne, hw, cid):
    kinds, depth, width = w_qkv.shape
    per = ne // nz
    return pl.pallas_call(
        functools.partial(start_kernel, nz, ne),
        out_shape=[
            jax.ShapeDtypeStruct((ne, *x.shape), x.dtype),
            jax.ShapeDtypeStruct((kinds, nz * depth, hw), BF),
            jax.ShapeDtypeStruct((hw, width), BF),
            jax.ShapeDtypeStruct((nz, *small.shape), small.dtype),
            jax.ShapeDtypeStruct((ne, *seg.shape), seg.dtype),
            jax.ShapeDtypeStruct(after.shape, after.dtype),
        ],
        in_specs=[VMEM, ANY, ANY, VMEM, VMEM, ANY],
        out_specs=[ANY, ANY, ANY, VMEM, VMEM, ANY],
        input_output_aliases={5: 5},
        scratch_shapes=[
            pltpu.VMEM((kinds, depth, hw), BF),
            pltpu.VMEM((per, hw, hw), BF),
            *PlaneGather.scratch(nz, ne, False),
            DMA((nz, kinds)), DMA((nz, kinds)), DMA((nz, kinds)), DMA((nz, kinds)),
            DMA((kinds,)), DMA((kinds,)), DMA((per,)), DMA((nz, per)), DMA, DMA,
            DMA, DMA, DMA, DMA,
        ],
        compiler_params=pltpu.CompilerParams(collective_id=cid, has_side_effects=True),
        name="start_gather",
    )(x, w_qkv, w_out, small, seg, after)


def swap_kernel(ne, x_ref, out_ref, send, recv):
    z, e = lax.axis_index("dp"), lax.axis_index("expert")
    hw = x_ref.shape[0]
    sem = pltpu.get_barrier_semaphore()
    for r in range(1, ne):
        to = (z, lax.rem(e + r, ne))
        pl.semaphore_signal(sem, inc=1, device_id=to, device_id_type=MESH)
    pl.semaphore_wait(sem, ne - 1)
    mine = pl.ds(pl.multiple_of(e * hw, hw), hw)
    copies = []
    for r in range(1, ne):
        to = lax.rem(e + r, ne)
        src = x_ref.at[:, pl.ds(pl.multiple_of(to * hw, hw), hw)]
        copy = remote(src, out_ref.at[mine, :], send.at[r], recv.at[r], (z, to))
        copy.start()
        copies.append(copy)
    out_ref[mine, :] = x_ref[:, mine]
    for copy in copies:
        copy.wait_send()
        copy.wait_recv()


def swap_in_plane(x, ne, cid):
    hw, width = x.shape
    return pl.pallas_call(
        functools.partial(swap_kernel, ne),
        out_shape=jax.ShapeDtypeStruct((width, hw), x.dtype),
        in_specs=[VMEM],
        out_specs=VMEM,
        scratch_shapes=[DMA((ne,)), DMA((ne,))],
        compiler_params=pltpu.CompilerParams(collective_id=cid, has_side_effects=True),
        name="swap_in_plane",
    )(x)


def lay_kernel(kinds, hw, x_ref, *outs):
    for k in range(kinds):
        piece = x_ref[0, :, k * hw : (k + 1) * hw].astype(F32)
        if k < kinds - 1:
            outs[0][k] = piece
        else:
            outs[1][...] = piece


def lay_mixer(wide, kinds, hw):
    ne, rows, _ = wide.shape
    return pl.pallas_call(
        functools.partial(lay_kernel, kinds, hw),
        grid=(ne,),
        in_specs=[pl.BlockSpec((1, rows, kinds * hw), lambda i: (i, 0, 0))],
        out_specs=[
            pl.BlockSpec((kinds - 1, rows, hw), lambda i: (0, 0, i)),
            pl.BlockSpec((rows, hw), lambda i: (0, i)),
        ],
        out_shape=[
            jax.ShapeDtypeStruct((kinds - 1, rows, ne * hw), F32),
            jax.ShapeDtypeStruct((rows, ne * hw), F32),
        ],
        name="lay_mixer",
    )(wide)


def lay_experts_kernel(per_dev, fl, x_ref, gate_ref, up_ref):
    for i in range(per_dev):
        gate_ref[i] = x_ref[0, :, i * fl : (i + 1) * fl].astype(F32)
        up_ref[i] = x_ref[0, :, (per_dev + i) * fl : (per_dev + i + 1) * fl].astype(F32)


def lay_experts(wide, per_dev, fl):
    nz, rows, _ = wide.shape
    out = jax.ShapeDtypeStruct((per_dev, rows, nz * fl), F32)
    spec = pl.BlockSpec((per_dev, rows, fl), lambda i: (0, 0, i))
    return pl.pallas_call(
        functools.partial(lay_experts_kernel, per_dev, fl),
        grid=(nz,),
        in_specs=[pl.BlockSpec((1, rows, 2 * per_dev * fl), lambda i: (i, 0, 0))],
        out_specs=[spec, spec],
        out_shape=[out, out],
        name="lay_experts",
    )(wide)


def moe_kernel(
    fl, h_ref, g_ref, win_ref, wdt_ref, wd_ref, wint_ref,
    mix_ref, gh_ref, dwin_ref, dwd_ref, acc_in, acc_d,
):
    step = pl.program_id(0)
    tile, width = g_ref.shape
    per_dev = wd_ref.shape[0] // fl
    e = lax.axis_index("expert")
    h = h_ref[:, :width]
    g = g_ref[...]
    extra = h_ref[:, width:].astype(F32)
    pre = dot(h, win_ref[...], NN)
    graw = dot(g, wdt_ref[...], NN)
    scaled_act, grad_gate, grad_up = [], [], []
    lanes = lax.broadcasted_iota(jnp.int32, (tile, 128), 1)
    gg = jnp.zeros((tile, 128), F32)
    split = 64
    for i in range(per_dev):
        u = pre[:, i * fl : (i + 1) * fl]
        w = pre[:, (per_dev + i) * fl : (per_dev + 1 + i) * fl]
        gr = graw[:, i * fl : (i + 1) * fl]
        mine = e * per_dev + i
        picked = (lanes == mine) | (lanes == mine + split)
        gate = jnp.sum(jnp.where(picked, extra, 0.0), axis=-1, keepdims=True)
        sig = 1.0 / (1.0 + jnp.exp(-u))
        silu = u * sig
        act = silu * w
        total = jnp.sum(act.astype(BF).astype(F32) * gr, axis=-1, keepdims=True)
        rounded = total.astype(BF).astype(F32)
        gg = jnp.where(lanes == mine, rounded, gg)
        gg = jnp.where(lanes == mine + split, total - rounded, gg)
        scaled_act.append((gate * act).astype(BF))
        gact = gate * gr
        grad_gate.append((gact * w * (sig * (1.0 + u * (1.0 - sig)))).astype(BF))
        grad_up.append((gact * silu).astype(BF))
    a = jnp.concatenate(scaled_act, axis=1)
    gin = jnp.concatenate(grad_gate + grad_up, axis=1)
    blocks, rows = mix_ref.shape[0], mix_ref.shape[2]
    mix_ref[...] = dot(a, wd_ref[...], NN).astype(BF).reshape(blocks, 1, rows, width)
    gh_ref[:, :width] = dot(gin, wint_ref[...], NN).astype(BF)
    gh_ref[:, width:] = gg.astype(BF)

    @pl.when(step == 0)
    def _():
        acc_in[...] = jnp.zeros_like(acc_in)
        acc_d[...] = jnp.zeros_like(acc_d)

    acc_in[...] += dot(h, gin, TN)
    acc_d[...] += dot(a, g, TN)

    @pl.when(step == pl.num_programs(0) - 1)
    def _():
        dwin_ref[...] = acc_in[...].astype(BF)
        dwd_ref[...] = acc_d[...]


def moe(h_all, g_all, w_in, wd_t, wd, w_in_t, per_dev, nz, ne, rows_dev, blocks):
    count, width = g_all.shape
    wide = h_all.shape[1]
    hid4 = w_in.shape[1]
    hid2 = wd.shape[0]
    fl = hid2 // per_dev
    tile = blocks * rows_dev
    turns = ne // blocks
    rows = lambda n: pl.BlockSpec((tile, n), lambda i: (i, 0))
    whole = lambda s: pl.BlockSpec(s, lambda i: (0, 0), pipeline_mode=pl.Buffered(1))
    return pl.pallas_call(
        functools.partial(moe_kernel, fl),
        grid=(count // tile,),
        in_specs=[
            rows(wide), rows(width),
            whole(w_in.shape), whole(wd_t.shape), whole(wd.shape), whole(w_in_t.shape),
        ],
        out_specs=[
            pl.BlockSpec((blocks, 1, rows_dev, width), lambda i: (i % turns, i // turns, 0, 0)),
            rows(wide),
            whole((width, hid4)), whole((hid2, width)),
        ],
        out_shape=[
            jax.ShapeDtypeStruct((ne, nz, rows_dev, width), BF),
            jax.ShapeDtypeStruct((count, wide), BF),
            jax.ShapeDtypeStruct((width, hid4), BF),
            jax.ShapeDtypeStruct((hid2, width), F32),
        ],
        scratch_shapes=[pltpu.VMEM((width, hid4), F32), pltpu.VMEM((hid2, width), F32)],
        compiler_params=pltpu.CompilerParams(vmem_limit_bytes=66_000_000),
        cost_estimate=pl.CostEstimate(
            flops=2 * count * width * hid2 * 9,
            bytes_accessed=8 * count * width + 24 * hid4 * width,
            transcendentals=count * hid2,
        ),
        name="moe",
    )(h_all, g_all, w_in, wd_t, wd, w_in_t)


def body(inputs, segments, routes, w_qkv, w_out, w_router, gains, w_gate, w_up, w_down, cotangent):
    z = lax.axis_index("dp")
    e = lax.axis_index("expert")
    nz = lax.axis_size("dp")
    ne = lax.axis_size("expert")
    count, width = inputs.shape
    num_seqs, length = segments.shape
    heads = width // HD // ne
    hw = heads * HD
    expert_count = w_router.shape[1]
    per_dev = w_gate.shape[0]
    hidden = w_gate.shape[2]
    fl = hidden // nz
    both = ("dp", "expert")

    pad = -(expert_count + 4) % 16
    small = jnp.concatenate(
        [w_router.T, gains.T, jnp.zeros((pad, gains.shape[0]), BF)], axis=0
    )
    seg8 = jnp.broadcast_to(segments[:, None, :], (num_seqs, 8, length)).reshape(-1, length)
    in_all, wq, wo, small, seg_all, cot = start_gather(
        inputs, w_qkv.transpose(1, 0, 2), w_out, small, seg8, cotangent, nz, ne, hw, 0
    )
    small = small.transpose(1, 0, 2).reshape(-1, width)
    router_t = small[:expert_count]
    gain_mat = small[expert_count : expert_count + 4].astype(F32)
    my_gains = lax.dynamic_slice_in_dim(gain_mat, e * hw, hw, axis=1)
    seg_all = seg_all.reshape(ne * num_seqs, 8, length)[:, 0]

    g_all = lax.all_gather(cot, both, axis=0, tiled=True)
    in_all = in_all.reshape(ne * count, width).astype(F32)
    h1_all = (in_all * rms_scale(in_all) * gain_mat[0]).astype(BF)
    inputs_f = inputs.astype(F32)
    scale_one = rms_scale(inputs_f)
    plane = h1_all.shape[0]
    shape_heads = (ne * num_seqs, length, heads, HD)

    q, k, v = [dot(h1_all, wq[j], NN) for j in range(3)]
    sums = jnp.stack([jnp.sum(q * q, axis=-1), jnp.sum(k * k, axis=-1)])
    scales = lax.rsqrt(lax.psum(sums, "expert") / width + EPS)
    aq, ak = scales[0][:, None], scales[1][:, None]
    cos_tab, sin_tab = rope_tables(length)
    rq = rotate((q * aq * my_gains[1]).reshape(shape_heads), cos_tab, sin_tab).astype(BF)
    rk = rotate((k * ak * my_gains[2]).reshape(shape_heads), cos_tab, sin_tab).astype(BF)
    vb = v.astype(BF).reshape(shape_heads)
    o, lse = jax.vmap(attend_forward)(rq, rk, vb, seg_all)
    o = o.reshape(plane, hw)
    x1_part = dot(o, wo, NN).astype(BF)
    (x1_sum,) = scatter_tokens(x1_part.reshape(ne, count, width), nz, ne, False, 1)
    x1 = inputs_f + x1_sum

    a2 = rms_scale(x1)
    h2 = (x1 * a2 * gain_mat[3]).astype(BF)
    probs = jax.nn.softmax(dot(h2, router_t, NT), axis=-1)
    picks = jnp.sum(
        (routes[:, :, None] == jnp.arange(expert_count, dtype=jnp.int32)).astype(F32), axis=1
    )
    gates = picks * probs

    split = 64
    high = gates.astype(BF)
    low = (gates - high.astype(F32)).astype(BF)
    blank = jnp.zeros((count, split - expert_count), BF)
    h2_all = gather_tokens(
        jnp.concatenate([h2, high, blank, low, blank], axis=1), nz, ne, True, 2
    ).reshape(-1, width + 2 * split)
    wg = lax.dynamic_slice_in_dim(w_gate, z * fl, fl, axis=2)
    wu = lax.dynamic_slice_in_dim(w_up, z * fl, fl, axis=2)
    wd = lax.dynamic_slice_in_dim(w_down, z * fl, fl, axis=1)
    w_in_t = jnp.concatenate(
        [wg.transpose(0, 2, 1), wu.transpose(0, 2, 1)], axis=0
    ).reshape(2 * per_dev * fl, width)
    w_in = jnp.concatenate([wg[0], wg[1], wu[0], wu[1]], axis=1)
    wd = wd.reshape(per_dev * fl, width)
    mix, gh, dwin, dwd = moe(
        h2_all, g_all, w_in, wd.T, wd, w_in_t, per_dev, nz, ne, count, min(4, ne)
    )
    gh_sum, mix = scatter_tokens(
        gh.reshape(nz * ne, count, width + 2 * split), nz, ne, True, 3,
        after=mix.reshape(-1, width),
    )
    grad_from_experts = gh_sum[:, :width]
    grad_gates = (
        gh_sum[:, width : width + expert_count]
        + gh_sum[:, width + split : width + split + expert_count]
    )

    mix = lax.psum_scatter(mix, "expert", scatter_dimension=0, tiled=True)
    mix = lax.psum_scatter(mix, "dp", scatter_dimension=0, tiled=True)
    output = (x1 + mix.astype(F32)).astype(BF)

    dwin = lax.all_to_all(
        dwin.reshape(nz, width // nz, 2 * per_dev * fl),
        "dp", split_axis=0, concat_axis=0, tiled=True,
    )
    grad_w_gate, grad_w_up = lay_experts(dwin, per_dev, fl)
    grad_w_down = dwd.reshape(per_dev, fl, width)

    grad_top = cotangent.astype(F32)
    grad_probs = picks * grad_gates
    glog = (probs * (grad_probs - jnp.sum(probs * grad_probs, axis=-1, keepdims=True))).astype(BF)
    local_router = dot(glog, h2, TN)
    gh2 = grad_from_experts + dot(glog, router_t, NN)
    grad_ffn, gain_ffn = rms_backward(x1, a2, gain_mat[3], gh2)
    gx1 = grad_top + grad_ffn
    gab = gx1.astype(BF)

    gab_all = gather_tokens(gab, nz, ne, False, 4).reshape(-1, width)
    go = dot(gab_all, wo, NT).astype(BF).reshape(shape_heads)
    grad_q, grad_k, gv = jax.vmap(attend_backward)(rq, rk, vb, seg_all, lse, go)
    gqn = rotate(grad_q, cos_tab, -sin_tab).reshape(plane, hw)
    gkn = rotate(grad_k, cos_tab, -sin_tab).reshape(plane, hw)
    nq, nk = q * aq, k * ak
    sq, sk = gqn * my_gains[1], gkn * my_gains[2]
    sums = jnp.stack([jnp.sum(sq * nq, axis=-1), jnp.sum(sk * nk, axis=-1)])
    means = lax.psum(sums, "expert") / width
    gq = (aq * (sq - nq * means[0][:, None])).astype(BF)
    gk = (ak * (sk - nk * means[1][:, None])).astype(BF)
    gproj = [gq, gk, gv.reshape(plane, hw)]
    gain_q, gain_k = jnp.sum(gqn * nq, axis=0), jnp.sum(gkn * nk, axis=0)

    gh1_part = sum(dot(part, wq[j], NT) for j, part in enumerate(gproj)).astype(BF)
    (gh1,) = scatter_tokens(gh1_part.reshape(ne, count, width), nz, ne, False, 5)
    grad_front, gain_attn = rms_backward(inputs_f, scale_one, gain_mat[0], gh1)
    grad_inputs = (gx1 + grad_front).astype(BF)

    part_out = dot(o, gab_all, TN).astype(BF)
    part_out = swap_in_plane(part_out, ne, 8)
    parts = [dot(h1_all, part, TN).astype(BF) for part in gproj] + [part_out]
    mine = lax.psum_scatter(
        jnp.concatenate(parts, axis=1), "dp", scatter_dimension=0, tiled=True
    )
    wide = gather_tokens(mine, nz, ne, False, 6)
    grad_w_qkv, grad_w_out = lay_mixer(wide, 4, hw)
    grad_w_qkv = grad_w_qkv.transpose(1, 0, 2)

    place = lambda part: lax.dynamic_update_slice_in_dim(
        jnp.zeros((1, width), F32), part[None], e * hw, axis=1
    )
    tiny = jnp.concatenate(
        [
            local_router, gain_attn[None], place(gain_q), place(gain_k), gain_ffn[None],
            jnp.zeros((-(expert_count + 4) % 8, width), F32),
        ],
        axis=0,
    )
    tiny = reduce_columns(tiny, nz, ne, 7)
    grad_w_router = tiny[:expert_count].T
    grad_gains = tiny[expert_count : expert_count + 4].T
    return (
        output,
        grad_inputs,
        grad_w_qkv,
        grad_w_out,
        grad_w_router,
        grad_gains,
        grad_w_gate,
        grad_w_up,
        grad_w_down,
    )


def solution(mesh):
    tokens = P(("dp", "expert"), None)
    rows = P("dp", None)
    rows3 = P("dp", None, None)
    owned = P("expert", None, None)
    return jax.shard_map(
        body,
        mesh=mesh,
        in_specs=(tokens, tokens, tokens, rows3, rows, rows, rows, owned, owned, owned, tokens),
        out_specs=(tokens, tokens, rows3, rows, rows, rows)
        + (P("expert", "dp", None),) * 3,
        check_vma=False,
    )
```

```python
import functools

import jax
import jax.numpy as jnp
from jax import lax
from jax.experimental import pallas as pl
from jax.experimental.pallas import tpu as pltpu
from jax.sharding import PartitionSpec as P


HD = 128
EPS = 1e-05
ROPE_BASE = 10000.0
MASKED = -1e30
BF = jnp.bfloat16
F32 = jnp.float32


def dot(a, b, dims):
    return lax.dot_general(a, b, (dims, ((), ())), preferred_element_type=F32)


NN = ((1,), (0,))
NT = ((1,), (1,))
TN = ((0,), (0,))


def rms_scale(values):
    return lax.rsqrt(jnp.mean(values * values, axis=-1, keepdims=True) + EPS)


def rms_backward(values, inv_rms, gain_col, grad_out):
    normed = values * inv_rms
    grad_gain = jnp.sum(grad_out * normed, axis=0)
    scaled = grad_out * gain_col
    grad_values = inv_rms * (scaled - normed * jnp.mean(scaled * normed, axis=-1, keepdims=True))
    return (grad_values, grad_gain)


def rope_tables(length):
    half = HD // 2
    freqs = jnp.exp(-jnp.log(ROPE_BASE) * (2.0 * jnp.arange(half, dtype=F32) / HD))
    angles = jnp.arange(length, dtype=F32)[:, None] * freqs[None, :]
    return (jnp.cos(angles)[:, None, :], jnp.sin(angles)[:, None, :])


def rotate(values, cos_tab, sin_tab):
    first, second = jnp.split(values, 2, axis=-1)
    return jnp.concatenate(
        [first * cos_tab - second * sin_tab, second * cos_tab + first * sin_tab], axis=-1
    )


def attend_scores(query_rot, key_rot, seg_ids):
    places = jnp.arange(seg_ids.shape[0], dtype=jnp.int32)
    allowed = (places[:, None] >= places[None, :]) & (seg_ids[:, None] == seg_ids[None, :])
    scores = jnp.einsum("qhd,khd->hqk", query_rot, key_rot, preferred_element_type=F32)
    scores = scores * query_rot.shape[-1] ** (-0.5)
    return jnp.where(allowed[None], scores, MASKED)


def attend_forward(query_rot, key_rot, value_bf, seg_ids):
    scores = attend_scores(query_rot, key_rot, seg_ids)
    row_max = jnp.max(scores, axis=-1, keepdims=True)
    log_total = row_max + jnp.log(jnp.sum(jnp.exp(scores - row_max), axis=-1, keepdims=True))
    weights_bf = jnp.exp(scores - log_total).astype(BF)
    mixed = jnp.einsum("hqk,khd->qhd", weights_bf, value_bf, preferred_element_type=F32)
    return (mixed.astype(BF), log_total)


def attend_backward(query_rot, key_rot, value_bf, seg_ids, log_total, grad_heads):
    scores = attend_scores(query_rot, key_rot, seg_ids)
    probs = jnp.exp(scores - log_total)
    grad_value = jnp.einsum(
        "hqk,qhd->khd", probs.astype(BF), grad_heads, preferred_element_type=F32
    ).astype(BF)
    grad_probs = jnp.einsum("qhd,khd->hqk", grad_heads, value_bf, preferred_element_type=F32)
    delta = jnp.sum(probs * grad_probs, axis=-1, keepdims=True)
    grad_scores = (probs * (grad_probs - delta) * query_rot.shape[-1] ** (-0.5)).astype(BF)
    grad_query = jnp.einsum("hqk,khd->qhd", grad_scores, key_rot, preferred_element_type=F32)
    grad_key = jnp.einsum("hqk,qhd->khd", grad_scores, query_rot, preferred_element_type=F32)
    return (grad_query, grad_key, grad_value)


MESH = pl.DeviceIdType.MESH
ANY = pl.BlockSpec(memory_space=pl.ANY)
VMEM = pl.BlockSpec(memory_space=pltpu.VMEM)
DMA = pltpu.SemaphoreType.DMA


def flip(index, bit):
    return index + bit * (1 - 2 * ((index // bit) % 2))


def flips(index, bits):
    out = [index]
    for bit in bits:
        out = out + [flip(i, bit) for i in out]
    return out


def bit_orders(ne):
    bits = [1 << b for b in range(ne.bit_length() - 1)]
    return [bits[:1] + bits[1:], bits[:1] + bits[1:][::-1]]


def nearest(z, r, nz):
    low = jnp.minimum(z, nz - 1 - z)
    near = z - (r + 1) // 2 if r % 2 else z + r // 2
    far = jnp.where(2 * z < nz, z + (r - low), z - (r - low))
    return jnp.where(r <= 2 * low, near, far)


def remote(src, dst, send, recv, peer):
    return pltpu.make_async_remote_copy(
        src_ref=src, dst_ref=dst, send_sem=send, recv_sem=recv, device_id=peer, device_id_type=MESH
    )


def for_others(nz, ne, z, e, act):
    def step(i, carry):
        flat = lax.rem(z * ne + e + i, nz * ne)
        act(flat // ne, lax.rem(flat, ne), flat)
        return carry

    lax.fori_loop(1, nz * ne, step, 0)


def meet_all(nz, ne, z, e):
    sem = pltpu.get_barrier_semaphore()

    def greet(zz, ee, flat):
        pl.semaphore_signal(sem, inc=1, device_id=(zz, ee), device_id_type=MESH)

    for_others(nz, ne, z, e, greet)
    pl.semaphore_wait(sem, nz * ne - 1)


def meet_column_and_plane(nz, ne, z, e, spread):
    sem = pltpu.get_barrier_semaphore()
    peers = [(z, flip(e, 1 << b)) for b in range(ne.bit_length() - 1)]
    if spread:
        peers += [(lax.rem(z + r, nz), e) for r in range(1, nz)]
    for peer in peers:
        pl.semaphore_signal(sem, inc=1, device_id=peer, device_id_type=MESH)
    pl.semaphore_wait(sem, len(peers))


class PlaneGather:
    def __init__(self, nz, ne, z, e, spread, x_ref, out_ref, zsend, zrecv, send, recv, local):
        self.nz, self.ne, self.z, self.e, self.spread = nz, ne, z, e, spread
        self.x, self.out = x_ref, out_ref
        self.zsend, self.zrecv, self.send, self.recv = zsend, zrecv, send, recv
        self.rounds = nz if spread else 1
        self.half = x_ref.shape[0] // 2
        self.orders = [o[1:] + o[:1] for o in bit_orders(ne)]
        self.planes = [z if spread else 0] + [nearest(z, r, nz) for r in range(1, self.rounds)]
        self.pending, self.arrivals = [], {}
        own = self.slot(0, e)
        keep = pltpu.make_async_copy(x_ref, out_ref.at[own], local)
        keep.start()
        self.pending.append(keep.wait)

    @staticmethod
    def scratch(nz, ne, spread):
        rounds = nz if spread else 1
        return [DMA((nz,)), DMA((nz,)), DMA((rounds, 2, ne - 1)), DMA((rounds, 2, ne - 1)), DMA]

    def slot(self, r, ee):
        return self.planes[r] * self.ne + ee

    def spread_own(self):
        for r in range(1, self.rounds):
            to = self.planes[r]
            copy = remote(
                self.x, self.out.at[self.slot(0, self.e)],
                self.zsend.at[r], self.zrecv.at[self.z], (to, self.e),
            )
            copy.start()
            self.pending.append(copy.wait_send)

    def forward(self, r, s, stage, subset):
        order = self.orders[s]
        rows = pl.ds(s * self.half, self.half)
        peer_e = flip(self.e, order[stage])
        n = (1 << stage) - 1 + subset
        block = self.slot(r, flips(self.e, order[:stage])[subset])
        dst = self.out.at[block, rows]
        src = self.x.at[rows] if r == 0 and subset == 0 else dst
        sems = self.send.at[r, s, n], self.recv.at[r, s, n]
        copy = remote(src, dst, *sems, (self.z, peer_e))
        copy.start()
        self.pending.append(copy.wait_send)
        got = self.out.at[self.slot(r, flips(peer_e, order[:stage])[subset]), rows]
        self.arrivals[(r, s, stage, subset)] = remote(got, got, *sems, (self.z, peer_e)).wait_recv

    def start_round(self, r):
        if r > 0:
            here = self.out.at[self.slot(r, self.e)]
            remote(
                here, here, self.zsend.at[r], self.zrecv.at[self.planes[r]], (self.planes[r], self.e)
            ).wait_recv()
        for stage in range(len(self.orders[0])):
            for s in range(2):
                self.forward(r, s, stage, 0)

    def finish_round(self, r):
        stages = len(self.orders[0])
        for stage in range(stages):
            for subset in range(1 << stage):
                for s in range(2):
                    self.arrivals.pop((r, s, stage, subset))()
                    for later in range(stage + 1, stages):
                        self.forward(r, s, later, subset + (1 << stage))

    def finish(self):
        for wait in self.pending:
            wait()


def gather_kernel(nz, ne, spread, x_ref, out_ref, *sems):
    z, e = lax.axis_index("dp"), lax.axis_index("expert")
    meet_column_and_plane(nz, ne, z, e, spread)
    net = PlaneGather(nz, ne, z, e, spread, x_ref, out_ref, *sems)
    net.spread_own()
    net.start_round(0)
    for r in range(1, net.rounds):
        net.start_round(r)
        net.finish_round(r - 1)
    net.finish_round(net.rounds - 1)
    net.finish()


def gather_tokens(x, nz, ne, spread, cid):
    rounds = nz if spread else 1
    return pl.pallas_call(
        functools.partial(gather_kernel, nz, ne, spread),
        out_shape=jax.ShapeDtypeStruct((rounds * ne, *x.shape), x.dtype),
        in_specs=[VMEM],
        out_specs=ANY,
        scratch_shapes=PlaneGather.scratch(nz, ne, spread),
        compiler_params=pltpu.CompilerParams(collective_id=cid, has_side_effects=True),
        name="gather_tokens",
    )(x)


def add_rows(dst, src, tile=16):
    def step(i, carry):
        rows = pl.ds(pl.multiple_of(i * tile, tile), tile)
        dst[rows, :] = (dst[rows, :].astype(F32) + src[rows, :].astype(F32)).astype(dst.dtype)
        return carry

    lax.fori_loop(0, dst.shape[0] // tile, step, 0)


def scatter_kernel(nz, ne, spread, x_ref, *refs):
    out_ref, acc, got, zgot, loads, send, recv, zsend, zrecv = refs[-9:]
    z, e = lax.axis_index("dp"), lax.axis_index("expert")
    meet_column_and_plane(nz, ne, z, e, spread)
    rounds = nz if spread else 1
    stages = ne.bit_length() - 1
    half = out_ref.shape[0] // 2
    orders = bit_orders(ne)
    pending, arrivals, zwait = [], {}, {}
    ranks = list(range(1, rounds)) + [0]
    first = [0] * (stages + 1)
    for j in range(stages):
        first[j + 1] = first[j] + (ne >> (j + 1))

    def plane_of(r):
        return lax.rem(z + r, nz) * ne if spread else 0

    def push(r, s, j):
        order = orders[s]
        peer = (z, flip(e, order[j]))
        rest = ne >> (j + 1)
        for i in range(rest):
            n = first[j] + i
            if j == 0:
                block = flips(peer[1], order[:0:-1])[i]
                src = x_ref.at[plane_of(r) + block, pl.ds(s * half, half)]
            else:
                src = acc.at[r, s, rest + i]
            copy = remote(src, got.at[r, s, n], send.at[r, s, n], recv.at[r, s, n], peer)
            copy.start()
            pending.append(copy.wait_send)
            arrivals.setdefault((r, s, j), []).append((copy.wait_recv, i, n))

    for r in ranks:
        for s in range(2):
            push(r, s, 0)
            for i, block in enumerate(flips(e, orders[s][:0:-1])):
                copy = pltpu.make_async_copy(
                    x_ref.at[plane_of(r) + block, pl.ds(s * half, half)],
                    acc.at[r, s, i],
                    loads.at[r, s, i],
                )
                copy.start()
                arrivals.setdefault((r, s, -1), []).append(copy.wait)
    for t in range(rounds + stages):
        for place, r in enumerate(ranks):
            j = t - place
            if not 0 <= j < stages:
                continue
            for s in range(2):
                if j == 0:
                    for wait in arrivals.pop((r, s, -1)):
                        wait()
                for wait, i, n in arrivals.pop((r, s, j)):
                    wait()
                    add_rows(acc.at[r, s, i], got.at[r, s, n])
                if j + 1 < stages:
                    push(r, s, j + 1)
                elif r > 0:
                    copy = remote(
                        acc.at[r, s, 0], zgot.at[r, s], zsend.at[r, s], zrecv.at[r, s],
                        (lax.rem(z + r, nz), e),
                    )
                    copy.start()
                    pending.append(copy.wait_send)
                    zwait[(r, s)] = copy.wait_recv
    for s in range(2):
        for r in range(1, rounds):
            zwait[(r, s)]()

        def step(i, carry):
            rows = pl.ds(pl.multiple_of(i * 16, 16), 16)
            total = acc[0, s, 0, rows, :].astype(F32)
            for r in range(1, rounds):
                total = total + zgot[r, s, rows, :].astype(F32)
            out_ref[pl.ds(pl.multiple_of(s * half + i * 16, 16), 16), :] = total.astype(out_ref.dtype)
            return carry

        lax.fori_loop(0, half // 16, step, 0)
    for wait in pending:
        wait()


def scatter_tokens(parts, nz, ne, spread, cid, after=None):
    rounds = nz if spread else 1
    _, count, width = parts.shape
    half = count // 2
    held = (2 * rounds * (ne // 2 + ne - 1) + 2 * nz) * half * width * 2
    if held > 56_000_000:
        cut = width // 256 * 128
        left = scatter_tokens(parts[..., :cut], nz, ne, spread, cid, after)
        right = scatter_tokens(parts[..., cut:], nz, ne, spread, cid + 16)
        return [jnp.concatenate([left[0], right[0]], axis=1), *left[1:]]
    more = [] if after is None else [after]
    return pl.pallas_call(
        functools.partial(scatter_kernel, nz, ne, spread),
        out_shape=[jax.ShapeDtypeStruct(m.shape, m.dtype) for m in more]
        + [jax.ShapeDtypeStruct((count, width), F32)],
        in_specs=[ANY] * (1 + len(more)),
        out_specs=[ANY] * len(more) + [VMEM],
        scratch_shapes=[
            pltpu.VMEM((rounds, 2, ne // 2, half, width), BF),
            pltpu.VMEM((rounds, 2, ne - 1, half, width), BF),
            pltpu.VMEM((nz, 2, half, width), BF),
            DMA((rounds, 2, ne // 2)),
            DMA((rounds, 2, ne - 1)),
            DMA((rounds, 2, ne - 1)),
            DMA((nz, 2)),
            DMA((nz, 2)),
        ],
        input_output_aliases={1: 0} if more else {},
        compiler_params=pltpu.CompilerParams(
            collective_id=cid, has_side_effects=True, vmem_limit_bytes=64_000_000
        ),
        name="scatter_tokens",
    )(parts, *more)[::-1]


def reduce_kernel(nz, ne, x_ref, out_ref, got, total, far, send1, recv1, send2, recv2):
    z, e = lax.axis_index("dp"), lax.axis_index("expert")
    per = ne // nz
    meet_all(nz, ne, z, e)
    first = []
    for r in range(1, ne):
        to = lax.rem(e + r, ne)
        copy = remote(x_ref.at[to], got.at[r], send1.at[r], recv1.at[r], (z, to))
        copy.start()
        first.append(copy)
    acc = x_ref[e]
    for r, copy in enumerate(first):
        copy.wait_recv()
        acc = acc + got[r + 1]
    total[...] = acc
    home, place = e // per, lax.rem(e, per)
    for r in range(ne):
        to = lax.rem(e + r, ne)
        copy = remote(total, far.at[z, place], send2.at[r], recv2, (home, to))
        if r > 0:
            copy.start()
        else:

            @pl.when(home != z)
            def _():
                copy.start()

            @pl.when(home == z)
            def _():
                far[z, place] = total[...]

    for copy in first:
        copy.wait_send()
    for r in range(ne):
        copy = remote(total, far.at[z, place], send2.at[r], recv2, (home, e))
        if r > 0:
            copy.wait_send()
        else:

            @pl.when(home != z)
            def _():
                copy.wait_send()

    def arrive(count):
        flat = got.at[pl.ds(0, count)]
        remote(flat, flat, send2.at[0], recv2, (z, e)).wait_recv()

    @pl.when(home == z)
    def _():
        arrive(nz * per - 1)

    @pl.when(home != z)
    def _():
        arrive(nz * per)

    for i in range(per):
        out_ref[i] = sum(far[k, i] for k in range(nz))


def reduce_columns(x, nz, ne, cid):
    rows, width = x.shape
    per = ne // nz
    x = x.reshape(rows, ne, width // ne).transpose(1, 0, 2)
    out = pl.pallas_call(
        functools.partial(reduce_kernel, nz, ne),
        out_shape=jax.ShapeDtypeStruct((per, rows, width // ne), F32),
        in_specs=[VMEM],
        out_specs=VMEM,
        scratch_shapes=[
            pltpu.VMEM((ne, rows, width // ne), F32),
            pltpu.VMEM((rows, width // ne), F32),
            pltpu.VMEM((nz, per, rows, width // ne), F32),
            DMA((ne,)), DMA((ne,)), DMA((ne,)), DMA,
        ],
        compiler_params=pltpu.CompilerParams(collective_id=cid, has_side_effects=True),
        name="reduce_columns",
    )(x)
    return out.transpose(1, 0, 2).reshape(rows, per * (width // ne))


def start_kernel(
    nz, ne, x_ref, wqkv_ref, wout_ref, small_ref, seg_ref, _,
    out_ref, wq_ref, wo_ref, small_out, seg_out, _2,
    wbuf, pbuf, zsend, zrecv, send, recv, local,
    up_send, up_recv, dn_send, dn_recv, wload, wkeep, pload, psend, precv, pkeep,
    small_send, small_recv, seg_send, seg_recv,
):
    z, e = lax.axis_index("dp"), lax.axis_index("expert")
    kinds, depth, hw = wbuf.shape
    per = ne // nz
    loads = [
        pltpu.make_async_copy(wqkv_ref.at[j, :, pl.ds(e * hw, hw)], wbuf.at[j], wload.at[j])
        for j in range(kinds)
    ]
    for copy in loads:
        copy.start()
    pieces = [
        pltpu.make_async_copy(
            wout_ref.at[pl.ds(i * hw, hw), pl.ds(e * hw, hw)], pbuf.at[i], pload.at[i]
        )
        for i in range(per)
    ]
    for copy in pieces:
        copy.start()
    meet_all(nz, ne, z, e)

    def rows_of(zz):
        return pl.ds(pl.multiple_of(zz * depth, depth), depth)

    def hop(j, zz, dist, up):
        send, recv = (up_send, up_recv) if up else (dn_send, dn_recv)
        here = wq_ref.at[j, rows_of(zz)]
        src = wbuf.at[j] if dist == 1 else here
        to = z + 1 if up else z - 1
        return remote(src, here, send.at[dist, j], recv.at[dist, j], (to, e))

    keeps = []
    for j in range(kinds):
        loads[j].wait()

        @pl.when(z + 1 < nz)
        def _():
            hop(j, z, 1, True).start()

        @pl.when(z > 0)
        def _():
            hop(j, z, 1, False).start()

        keep = pltpu.make_async_copy(wbuf.at[j], wq_ref.at[j, rows_of(z)], wkeep.at[j])
        keep.start()
        keeps.append(keep)

    def wait_all(ref, send, recv, count):
        most = ref.at[pl.ds(0, count)]
        both = remote(most, most, send, recv, (z, flip(e, 1)))
        both.wait_send()
        both.wait_recv()

    small_out[z] = small_ref[...]
    for r in range(1, nz):
        remote(
            small_ref, small_out.at[z], small_send, small_recv, (lax.rem(z + r, nz), e)
        ).start()
    seg_out[e] = seg_ref[...]
    for r in range(1, ne):
        remote(seg_ref, seg_out.at[e], seg_send, seg_recv, (z, lax.rem(e + r, ne))).start()
    net = PlaneGather(nz, ne, z, e, False, x_ref, out_ref, zsend, zrecv, send, recv, local)
    net.start_round(0)

    columns = pl.ds(e * hw, hw)
    for i in range(per):
        pieces[i].wait()
    for r in range(nz):
        for i in range(per):
            to = (lax.rem(z + r, nz), z * per + i)
            give = remote(pbuf.at[i], wo_ref.at[:, columns], psend.at[r, i], precv, to)
            if r > 0:
                give.start()
            else:
                own = pltpu.make_async_copy(pbuf.at[i], wo_ref.at[:, columns], pkeep)

                @pl.when(to[1] == e)
                def _():
                    own.start()

                @pl.when(to[1] != e)
                def _():
                    give.start()
    net.finish_round(0)
    for dist in range(1, nz):
        for j in range(kinds):

            @pl.when(z - dist >= 0)
            def _():
                got = wq_ref.at[j, rows_of(z - dist)]
                remote(got, got, up_send.at[dist, j], up_recv.at[dist, j], (z, e)).wait_recv()

                @pl.when(z + 1 < nz)
                def _():
                    if dist + 1 < nz:
                        hop(j, z - dist, dist + 1, True).start()

            @pl.when(z + dist < nz)
            def _():
                got = wq_ref.at[j, rows_of(z + dist)]
                remote(got, got, dn_send.at[dist, j], dn_recv.at[dist, j], (z, e)).wait_recv()

                @pl.when(z > 0)
                def _():
                    if dist + 1 < nz:
                        hop(j, z + dist, dist + 1, False).start()

    net.finish()
    for keep in keeps:
        keep.wait()
    for dist in range(1, nz):
        for j in range(kinds):

            @pl.when((z - dist + 1 >= 0) & (z + 1 < nz))
            def _():
                hop(j, z - dist + 1, dist, True).wait_send()

            @pl.when((z + dist - 1 < nz) & (z > 0))
            def _():
                hop(j, z + dist - 1, dist, False).wait_send()

    for r in range(nz):
        for i in range(per):
            to = (lax.rem(z + r, nz), z * per + i)
            give = remote(pbuf.at[i], wo_ref.at[:, columns], psend.at[r, i], precv, to)
            if r > 0:
                give.wait_send()
            else:
                own = pltpu.make_async_copy(pbuf.at[i], wo_ref.at[:, columns], pkeep)

                @pl.when(to[1] == e)
                def _():
                    own.wait()

                @pl.when(to[1] != e)
                def _():
                    give.wait_send()

    def wait_pieces(count):
        most = wo_ref.at[:, pl.ds(0, count * hw)]
        remote(most, most, psend.at[0, 0], precv, (z, e)).wait_recv()

    @pl.when(z == e // per)
    def _():
        wait_pieces(ne - 1)

    @pl.when(z != e // per)
    def _():
        wait_pieces(ne)

    wait_all(small_out, small_send, small_recv, nz - 1)
    wait_all(seg_out, seg_send, seg_recv, ne - 1)


def start_gather(x, w_qkv, w_out, small, seg, after, nz, ne, hw, cid):
    kinds, depth, width = w_qkv.shape
    per = ne // nz
    return pl.pallas_call(
        functools.partial(start_kernel, nz, ne),
        out_shape=[
            jax.ShapeDtypeStruct((ne, *x.shape), x.dtype),
            jax.ShapeDtypeStruct((kinds, nz * depth, hw), BF),
            jax.ShapeDtypeStruct((hw, width), BF),
            jax.ShapeDtypeStruct((nz, *small.shape), small.dtype),
            jax.ShapeDtypeStruct((ne, *seg.shape), seg.dtype),
            jax.ShapeDtypeStruct(after.shape, after.dtype),
        ],
        in_specs=[VMEM, ANY, ANY, VMEM, VMEM, ANY],
        out_specs=[ANY, ANY, ANY, VMEM, VMEM, ANY],
        input_output_aliases={5: 5},
        scratch_shapes=[
            pltpu.VMEM((kinds, depth, hw), BF),
            pltpu.VMEM((per, hw, hw), BF),
            *PlaneGather.scratch(nz, ne, False),
            DMA((nz, kinds)), DMA((nz, kinds)), DMA((nz, kinds)), DMA((nz, kinds)),
            DMA((kinds,)), DMA((kinds,)), DMA((per,)), DMA((nz, per)), DMA, DMA,
            DMA, DMA, DMA, DMA,
        ],
        compiler_params=pltpu.CompilerParams(collective_id=cid, has_side_effects=True),
        name="start_gather",
    )(x, w_qkv, w_out, small, seg, after)


def swap_kernel(ne, x_ref, out_ref, send, recv):
    z, e = lax.axis_index("dp"), lax.axis_index("expert")
    hw = x_ref.shape[0]
    sem = pltpu.get_barrier_semaphore()
    for r in range(1, ne):
        to = (z, lax.rem(e + r, ne))
        pl.semaphore_signal(sem, inc=1, device_id=to, device_id_type=MESH)
    pl.semaphore_wait(sem, ne - 1)
    mine = pl.ds(pl.multiple_of(e * hw, hw), hw)
    copies = []
    for r in range(1, ne):
        to = lax.rem(e + r, ne)
        src = x_ref.at[:, pl.ds(pl.multiple_of(to * hw, hw), hw)]
        copy = remote(src, out_ref.at[mine, :], send.at[r], recv.at[r], (z, to))
        copy.start()
        copies.append(copy)
    out_ref[mine, :] = x_ref[:, mine]
    for copy in copies:
        copy.wait_send()
        copy.wait_recv()


def swap_in_plane(x, ne, cid):
    hw, width = x.shape
    return pl.pallas_call(
        functools.partial(swap_kernel, ne),
        out_shape=jax.ShapeDtypeStruct((width, hw), x.dtype),
        in_specs=[VMEM],
        out_specs=VMEM,
        scratch_shapes=[DMA((ne,)), DMA((ne,))],
        compiler_params=pltpu.CompilerParams(collective_id=cid, has_side_effects=True),
        name="swap_in_plane",
    )(x)


def lay_kernel(kinds, hw, x_ref, *outs):
    for k in range(kinds):
        piece = x_ref[0, :, k * hw : (k + 1) * hw].astype(F32)
        if k < kinds - 1:
            outs[0][k] = piece
        else:
            outs[1][...] = piece


def lay_mixer(wide, kinds, hw):
    ne, rows, _ = wide.shape
    return pl.pallas_call(
        functools.partial(lay_kernel, kinds, hw),
        grid=(ne,),
        in_specs=[pl.BlockSpec((1, rows, kinds * hw), lambda i: (i, 0, 0))],
        out_specs=[
            pl.BlockSpec((kinds - 1, rows, hw), lambda i: (0, 0, i)),
            pl.BlockSpec((rows, hw), lambda i: (0, i)),
        ],
        out_shape=[
            jax.ShapeDtypeStruct((kinds - 1, rows, ne * hw), F32),
            jax.ShapeDtypeStruct((rows, ne * hw), F32),
        ],
        name="lay_mixer",
    )(wide)


def lay_experts_kernel(per_dev, fl, x_ref, gate_ref, up_ref):
    for i in range(per_dev):
        gate_ref[i] = x_ref[0, :, i * fl : (i + 1) * fl].astype(F32)
        up_ref[i] = x_ref[0, :, (per_dev + i) * fl : (per_dev + i + 1) * fl].astype(F32)


def lay_experts(wide, per_dev, fl):
    nz, rows, _ = wide.shape
    out = jax.ShapeDtypeStruct((per_dev, rows, nz * fl), F32)
    spec = pl.BlockSpec((per_dev, rows, fl), lambda i: (0, 0, i))
    return pl.pallas_call(
        functools.partial(lay_experts_kernel, per_dev, fl),
        grid=(nz,),
        in_specs=[pl.BlockSpec((1, rows, 2 * per_dev * fl), lambda i: (i, 0, 0))],
        out_specs=[spec, spec],
        out_shape=[out, out],
        name="lay_experts",
    )(wide)


def moe_kernel(
    fl, h_ref, g_ref, win_ref, wd_ref,
    mix_ref, gh_ref, dwin_ref, dwd_ref, acc_in, acc_d,
):
    step = pl.program_id(0)
    tile, width = g_ref.shape
    per_dev = wd_ref.shape[0] // fl
    e = lax.axis_index("expert")
    h = h_ref[:, :width]
    g = g_ref[...]
    extra = h_ref[:, width:].astype(F32)
    pre = dot(h, win_ref[...], NN)
    graw = dot(g, wd_ref[...], NT)
    scaled_act, grad_gate, grad_up = [], [], []
    lanes = lax.broadcasted_iota(jnp.int32, (tile, 128), 1)
    gg = jnp.zeros((tile, 128), F32)
    split = 64
    for i in range(per_dev):
        u = pre[:, i * fl : (i + 1) * fl]
        w = pre[:, (per_dev + i) * fl : (per_dev + 1 + i) * fl]
        gr = graw[:, i * fl : (i + 1) * fl]
        mine = e * per_dev + i
        picked = (lanes == mine) | (lanes == mine + split)
        gate = jnp.sum(jnp.where(picked, extra, 0.0), axis=-1, keepdims=True)
        sig = 1.0 / (1.0 + jnp.exp(-u))
        silu = u * sig
        act = silu * w
        total = jnp.sum(act.astype(BF).astype(F32) * gr, axis=-1, keepdims=True)
        rounded = total.astype(BF).astype(F32)
        gg = jnp.where(lanes == mine, rounded, gg)
        gg = jnp.where(lanes == mine + split, total - rounded, gg)
        scaled_act.append((gate * act).astype(BF))
        gact = gate * gr
        grad_gate.append((gact * w * (sig * (1.0 + u * (1.0 - sig)))).astype(BF))
        grad_up.append((gact * silu).astype(BF))
    a = jnp.concatenate(scaled_act, axis=1)
    gin = jnp.concatenate(grad_gate + grad_up, axis=1)
    blocks, rows = mix_ref.shape[0], mix_ref.shape[2]
    mix_ref[...] = dot(a, wd_ref[...], NN).astype(BF).reshape(blocks, 1, rows, width)
    gh_ref[:, :width] = dot(gin, win_ref[...], NT).astype(BF)
    gh_ref[:, width:] = gg.astype(BF)

    @pl.when(step == 0)
    def _():
        acc_in[...] = jnp.zeros_like(acc_in)
        acc_d[...] = jnp.zeros_like(acc_d)

    acc_in[...] += dot(h, gin, TN)
    acc_d[...] += dot(a, g, TN)

    @pl.when(step == pl.num_programs(0) - 1)
    def _():
        dwin_ref[...] = acc_in[...].astype(BF)
        dwd_ref[...] = acc_d[...]


def moe(h_all, g_all, w_in, wd, per_dev, nz, ne, rows_dev, blocks):
    count, width = g_all.shape
    wide = h_all.shape[1]
    hid4 = w_in.shape[1]
    hid2 = wd.shape[0]
    fl = hid2 // per_dev
    tile = blocks * rows_dev
    turns = ne // blocks
    rows = lambda n: pl.BlockSpec((tile, n), lambda i: (i, 0))
    whole = lambda s: pl.BlockSpec(s, lambda i: (0, 0), pipeline_mode=pl.Buffered(1))
    return pl.pallas_call(
        functools.partial(moe_kernel, fl),
        grid=(count // tile,),
        in_specs=[
            rows(wide), rows(width),
            whole(w_in.shape), whole(wd.shape),
        ],
        out_specs=[
            pl.BlockSpec((blocks, 1, rows_dev, width), lambda i: (i % turns, i // turns, 0, 0)),
            rows(wide),
            whole((width, hid4)), whole((hid2, width)),
        ],
        out_shape=[
            jax.ShapeDtypeStruct((ne, nz, rows_dev, width), BF),
            jax.ShapeDtypeStruct((count, wide), BF),
            jax.ShapeDtypeStruct((width, hid4), BF),
            jax.ShapeDtypeStruct((hid2, width), F32),
        ],
        scratch_shapes=[pltpu.VMEM((width, hid4), F32), pltpu.VMEM((hid2, width), F32)],
        compiler_params=pltpu.CompilerParams(vmem_limit_bytes=66_000_000),
        cost_estimate=pl.CostEstimate(
            flops=2 * count * width * hid2 * 9,
            bytes_accessed=8 * count * width + 24 * hid4 * width,
            transcendentals=count * hid2,
        ),
        name="moe",
    )(h_all, g_all, w_in, wd)


def moe_net_kernel(
    nz, ne, per_dev, slots, h_ref, g_ref, wg_ref, wu_ref, wd_ref,
    hall_ref, mix_ref, gh_ref, dwin_ref, dwd_ref,
    win, wd, acc_in, acc_d, htile, gtile, mixbuf, qbuf, cgot, acc, got, zgot, dbuf,
    wload, tload, mixsem, keep, flush, zsend, zrecv, send, recv,
    csend, crecv, credit, rsend, rrecv, ysend, yrecv,
):
    z, e = lax.axis_index("dp"), lax.axis_index("expert")
    rows, width = g_ref.shape[1], g_ref.shape[2]
    half = rows // 2
    fl = wd.shape[0] // per_dev
    upper = [2 << b for b in range(ne.bit_length() - 2)]
    stages = len(upper)
    pairs = ne // 2
    steps = nz * pairs
    gather_orders = [upper + [1], upper[::-1] + [1]]
    sum_orders = [[1] + upper, [1] + upper[::-1]]
    at = [e]
    for bit in [1] + upper:
        at = at + [flip(i, bit) for i in at]
    partner = (z, at[1])

    def plane(r):
        low = jnp.minimum(z, nz - 1 - z)
        near = jnp.where(lax.rem(r, 2) == 1, z - (r + 1) // 2, z + r // 2)
        far = jnp.where(2 * z < nz, z + (r - low), z - (r - low))
        return jnp.where(r <= 2 * low, near, far)

    planes = [z] + [nearest(z, r, nz) for r in range(1, nz)]

    def part(s):
        return pl.ds(s * half, half)

    def subset_mask(order, subset):
        return sum(bit for b, bit in enumerate(order) if subset >> b & 1)

    def pass_on(r, s, stage, subset, own=False):
        order = gather_orders[s]
        dst = hall_ref.at[plane(r) * ne + at[subset_mask(order, subset)], part(s)]
        n = (1 << stage) - 1 + subset
        src = h_ref.at[part(s)] if own else dst
        return remote(src, dst, send.at[r, s, n], recv.at[r, s, n], (z, at[order[stage]]))

    def take(r, s, stage, subset):
        order = gather_orders[s]
        mask = subset_mask(order, subset) | order[stage]
        n = (1 << stage) - 1 + subset
        here = hall_ref.at[plane(r) * ne + at[mask], part(s)]
        remote(here, here, send.at[r, s, n], recv.at[r, s, n], partner).wait_recv()
        for later in range(stage + 1, stages + 1):
            pass_on(r, s, later, subset + (1 << stage)).start()

    def start_round(r):
        if r > 0:
            here = hall_ref.at[planes[r] * ne + e]
            remote(here, here, zsend.at[r], zrecv.at[planes[r]], partner).wait_recv()
        for stage in range(stages + 1):
            for s in range(2):
                pass_on(r, s, stage, 0, own=r == 0).start()

    def take_pair(r, i):
        if i == 1:
            for stage in range(stages):
                for s in range(2):
                    take(r, s, stage, 0)
        mask = 2 * i
        for s in range(2):
            order = gather_orders[s]
            places = [b for b in range(stages) if order[b] & mask]
            if len(places) > 1:
                take(r, s, places[-1], sum(1 << b for b in places[:-1]))
        for s in range(2):
            order = gather_orders[s]
            take(r, s, stages, sum(1 << b for b in range(stages) if order[b] & mask))

    def blocks_of(k):
        r, i = k // pairs, lax.rem(k, pairs)
        home = plane(r)
        lane = e
        for b, bit in enumerate(upper):
            lane = lane + lax.rem(i // (1 << b), 2) * (at[bit] - e)
        return home, lane, lane + (at[1] - e)

    def loads(k):
        home, one, two = blocks_of(k)
        p = lax.rem(k, 2)
        out = []
        for j, lane in enumerate((one, two)):
            to = pl.ds(j * rows, rows)
            block = home * ne + lane
            out.append(pltpu.make_async_copy(hall_ref.at[block], htile.at[p, to], tload.at[p, 2 * j]))
            out.append(
                pltpu.make_async_copy(g_ref.at[block], gtile.at[p, to], tload.at[p, 2 * j + 1])
            )
        return out

    def mix_out(k):
        home, one, two = blocks_of(k)
        p = lax.rem(k, 2)
        return [
            pltpu.make_async_copy(
                mixbuf.at[p, pl.ds(j * rows, rows)], mix_ref.at[lane, home], mixsem.at[p, j]
            )
            for j, lane in enumerate((one, two))
        ]

    def to_partner(k):
        return remote(
            qbuf.at[lax.rem(k, 2)], cgot.at[lax.rem(k, slots)],
            csend.at[lax.rem(k, 2)], crecv.at[lax.rem(k, slots)], partner,
        )

    def place_of(t, keep_index):
        return (1 << stages) - (1 << (stages - t + 1)) + keep_index

    def push(r, s, t, keep_index):
        order = sum_orders[s]
        mask = order[t] | subset_mask(order[t + 1 :], keep_index)
        n = place_of(t, keep_index)
        return remote(
            acc.at[r, mask // 2, part(s)], got.at[r, s, n],
            rsend.at[r, s, n], rrecv.at[r, s, n], (z, at[order[t]]),
        )

    def merge(k):
        slot = lax.rem(k, slots)
        remote(cgot.at[slot], cgot.at[slot], csend.at[0], crecv.at[slot], partner).wait_recv()
        r, i = k // pairs, lax.rem(k, pairs)
        add_rows(acc.at[r, i], cgot.at[slot])

        @pl.when(k + slots < steps)
        def _():
            pl.semaphore_signal(credit, inc=1, device_id=partner, device_id_type=MESH)

        for j in range(1, pairs):

            @pl.when(i == j)
            def _():
                for s in range(2):
                    order = sum_orders[s]
                    if order[1] & (2 * j):
                        rest = [b for b, bit in enumerate(order[2:]) if bit & (2 * j)]
                        push(r, s, 1, sum(1 << b for b in rest)).start()

    def home_copy(r, s):
        return remote(
            acc.at[r, 0, part(s)], zgot.at[z, part(s)], ysend.at[r, s], yrecv.at[z, s],
            (plane(r), e),
        )

    def settle(r, t):
        for s in range(2):
            order = sum_orders[s]
            for index in range(1 << (stages - t)):
                copy = push(r, s, t, index)
                copy.wait_recv()
                mask = subset_mask(order[t + 1 :], index)
                add_rows(acc.at[r, mask // 2, part(s)], got.at[r, s, place_of(t, index)])
            if t < stages:
                for index in range(1 << (stages - t - 1)):
                    push(r, s, t + 1, index).start()
            else:

                @pl.when(r > 0)
                def _():
                    home_copy(r, s).start()

    weights = []
    for i in range(per_dev):
        cols = pl.ds(z * fl, fl)
        weights += [
            (wg_ref.at[i, :, cols], win.at[:, pl.ds(i * fl, fl)]),
            (wu_ref.at[i, :, cols], win.at[:, pl.ds((per_dev + i) * fl, fl)]),
            (wd_ref.at[i, cols, :], wd.at[pl.ds(i * fl, fl), :]),
        ]
    weights = [
        pltpu.make_async_copy(src, dst, wload.at[j]) for j, (src, dst) in enumerate(weights)
    ]
    for copy in weights:
        copy.start()
    meet_column_and_plane(nz, ne, z, e, True)
    own = pltpu.make_async_copy(h_ref, hall_ref.at[z * ne + e], keep)
    own.start()
    for r in range(1, nz):
        remote(
            h_ref, hall_ref.at[z * ne + e], zsend.at[r], zrecv.at[z], (planes[r], e)
        ).start()
    start_round(0)
    acc_in[...] = jnp.zeros_like(acc_in)
    acc_d[...] = jnp.zeros_like(acc_d)
    take_pair(0, 0)
    own.wait()
    for copy in loads(0):
        copy.start()
    for copy in weights:
        copy.wait()

    tile = 2 * rows
    lanes = lax.broadcasted_iota(jnp.int32, (tile, 128), 1)
    split = 64

    def step(k, carry):
        p = lax.rem(k, 2)
        r, i = k // pairs, lax.rem(k, pairs)
        for copy in loads(k):
            copy.wait()
        pre = dot(htile[p, :, :width], win[...], NN)
        graw = dot(gtile[p], wd[...], NT)
        extra = htile[p, :, width:].astype(F32)
        scaled_act, grad_gate, grad_up = [], [], []
        gg = jnp.zeros((tile, 128), F32)
        for j in range(per_dev):
            u = pre[:, j * fl : (j + 1) * fl]
            w = pre[:, (per_dev + j) * fl : (per_dev + 1 + j) * fl]
            gr = graw[:, j * fl : (j + 1) * fl]
            mine = e * per_dev + j
            picked = (lanes == mine) | (lanes == mine + split)
            gate = jnp.sum(jnp.where(picked, extra, 0.0), axis=-1, keepdims=True)
            sig = 1.0 / (1.0 + jnp.exp(-u))
            silu = u * sig
            act = silu * w
            total = jnp.sum(act.astype(BF).astype(F32) * gr, axis=-1, keepdims=True)
            rounded = total.astype(BF).astype(F32)
            gg = jnp.where(lanes == mine, rounded, gg)
            gg = jnp.where(lanes == mine + split, total - rounded, gg)
            scaled_act.append((gate * act).astype(BF))
            gact = gate * gr
            grad_gate.append((gact * w * (sig * (1.0 + u * (1.0 - sig)))).astype(BF))
            grad_up.append((gact * silu).astype(BF))
        a = jnp.concatenate(scaled_act, axis=1)
        gin = jnp.concatenate(grad_gate + grad_up, axis=1)

        for r1 in range(1, nz):

            @pl.when(k == (r1 - 1) * (pairs - 1) + 1)
            def _():
                start_round(r1)

        @pl.when(k + 1 < steps)
        def _():
            ahead = k + 1
            for j in range(pairs):

                @pl.when(lax.rem(ahead, pairs) == j)
                def _():
                    take_pair(ahead // pairs, j)

            for copy in loads(ahead):
                copy.start()

        @pl.when(k >= 2)
        def _():
            for copy in mix_out(k - 2):
                copy.wait()
            to_partner(k - 2).wait_send()

        mixbuf[p] = dot(a, wd[...], NN).astype(BF)
        for copy in mix_out(k):
            copy.start()
        back = dot(gin, win[...], NT).astype(BF)
        gg = gg.astype(BF)
        acc[r, i, :, :width] = back[:rows]
        acc[r, i, :, width:] = gg[:rows]
        qbuf[p, :, :width] = back[rows:]
        qbuf[p, :, width:] = gg[rows:]
        acc_in[...] += dot(htile[p, :, :width], gin, TN)
        acc_d[...] += dot(a, gtile[p], TN)

        @pl.when(k >= slots)
        def _():
            pl.semaphore_wait(credit, 1)

        to_partner(k).start()

        @pl.when(k >= 1)
        def _():
            merge(k - 1)

        for t in range(1, stages + 1):
            late = k - pairs - 2 * t

            @pl.when((late >= 0) & (lax.rem(late + pairs, pairs) == 0))
            def _():
                settle(late // pairs, t)

        return carry

    lax.fori_loop(0, steps, step, 0)
    merge(steps - 1)
    final = pltpu.make_async_copy(acc_d, dwd_ref, flush.at[0])
    final.start()
    left = sorted(
        (r * pairs + pairs + 2 * t, r, t)
        for r in range(nz)
        for t in range(1, stages + 1)
        if r * pairs + pairs + 2 * t >= steps
    )
    chunk = dbuf.shape[1]

    def flush_chunk(c):
        return pltpu.make_async_copy(
            dbuf.at[c % 2], dwin_ref.at[pl.ds(c * chunk, chunk)], flush.at[1 + c % 2]
        )

    chunks = acc_in.shape[0] // chunk
    for c in range(chunks):
        if c >= 2:
            flush_chunk(c - 2).wait()
        dbuf[c % 2] = acc_in[pl.ds(c * chunk, chunk), :].astype(BF)
        flush_chunk(c).start()
    for _, r, t in left:
        settle(jnp.int32(r), t)
    for s in range(2):
        for r in range(1, nz):
            here = zgot.at[planes[r], part(s)]
            remote(here, here, ysend.at[r, s], yrecv.at[planes[r], s], partner).wait_recv()

        def total_rows(n, carry):
            span = pl.ds(pl.multiple_of(s * half + n * 16, 16), 16)
            total = acc[0, 0, span, :].astype(F32)
            for r in range(1, nz):
                total = total + zgot[planes[r], span, :].astype(F32)
            gh_ref[span, :] = total
            return carry

        lax.fori_loop(0, half // 16, total_rows, 0)
    final.wait()
    for c in range(max(chunks - 2, 0), chunks):
        flush_chunk(c).wait()
    for k in range(max(steps - 2, 0), steps):
        for copy in mix_out(jnp.int32(k)):
            copy.wait()
        to_partner(jnp.int32(k)).wait_send()
    for r in range(nz):
        if r > 0:
            remote(
                h_ref, hall_ref.at[z * ne + e], zsend.at[r], zrecv.at[z], (planes[r], e)
            ).wait_send()
        for s in range(2):
            for stage in range(stages + 1):
                for subset in range(1 << stage):
                    pass_on(r, s, stage, subset, own=r == 0 and subset == 0).wait_send()
            for t in range(1, stages + 1):
                for index in range(1 << (stages - t)):
                    push(r, s, t, index).wait_send()
            if r > 0:
                home_copy(jnp.int32(r), s).wait_send()


def moe_net_scratch(nz, ne, per_dev, rows, width, wide, fl):
    pairs = ne // 2
    slots = 4
    stages = ne.bit_length() - 2
    vmem = [
        ((width, 2 * per_dev * fl), BF),
        ((per_dev * fl, width), BF),
        ((width, 2 * per_dev * fl), F32),
        ((per_dev * fl, width), F32),
        ((2, 2 * rows, wide), BF),
        ((2, 2 * rows, width), BF),
        ((2, 2 * rows, width), BF),
        ((2, rows, wide), BF),
        ((slots, rows, wide), BF),
        ((nz, pairs, rows, wide), BF),
        ((nz, 2, max(pairs - 1, 1), rows // 2, wide), BF),
        ((nz, rows, wide), BF),
        ((2, width // 8, 2 * per_dev * fl), BF),
    ]
    size = sum(functools.reduce(lambda a, b: a * b, s) * (2 if d == BF else 4) for s, d in vmem)
    sems = [
        DMA((3 * per_dev,)), DMA((2, 4)), DMA((2, 2)), DMA, DMA((3,)),
        DMA((nz,)), DMA((nz,)), DMA((nz, 2, ne - 1)), DMA((nz, 2, ne - 1)),
        DMA((2,)), DMA((slots,)), pltpu.SemaphoreType.REGULAR,
        DMA((nz, 2, max(pairs - 1, 1))), DMA((nz, 2, max(pairs - 1, 1))),
        DMA((nz, 2)), DMA((nz, 2)),
    ]
    fits = size <= 54_000_000 and stages >= 1 and nz > 1 and nz * pairs > slots
    return fits, slots, [pltpu.VMEM(*v) for v in vmem] + sems


def moe_net(h, g_all, w_gate, w_up, w_down, nz, ne, fl, slots, scratch, cid):
    rows, wide = h.shape
    per_dev, width, _ = w_gate.shape
    return pl.pallas_call(
        functools.partial(moe_net_kernel, nz, ne, per_dev, slots),
        out_shape=[
            jax.ShapeDtypeStruct((nz * ne, rows, wide), BF),
            jax.ShapeDtypeStruct((ne, nz, rows, width), BF),
            jax.ShapeDtypeStruct((rows, wide), F32),
            jax.ShapeDtypeStruct((width, 2 * per_dev * fl), BF),
            jax.ShapeDtypeStruct((per_dev * fl, width), F32),
        ],
        in_specs=[VMEM, ANY, ANY, ANY, ANY],
        out_specs=[ANY, ANY, VMEM, ANY, ANY],
        scratch_shapes=scratch,
        compiler_params=pltpu.CompilerParams(
            collective_id=cid, has_side_effects=True, vmem_limit_bytes=66_500_000
        ),
        name="moe_net",
    )(h, g_all.reshape(nz * ne, rows, width), w_gate, w_up, w_down)


def body(inputs, segments, routes, w_qkv, w_out, w_router, gains, w_gate, w_up, w_down, cotangent):
    z = lax.axis_index("dp")
    e = lax.axis_index("expert")
    nz = lax.axis_size("dp")
    ne = lax.axis_size("expert")
    count, width = inputs.shape
    num_seqs, length = segments.shape
    heads = width // HD // ne
    hw = heads * HD
    expert_count = w_router.shape[1]
    per_dev = w_gate.shape[0]
    hidden = w_gate.shape[2]
    fl = hidden // nz
    both = ("dp", "expert")

    pad = -(expert_count + 4) % 16
    small = jnp.concatenate(
        [w_router.T, gains.T, jnp.zeros((pad, gains.shape[0]), BF)], axis=0
    )
    seg8 = jnp.broadcast_to(segments[:, None, :], (num_seqs, 8, length)).reshape(-1, length)
    in_all, wq, wo, small, seg_all, cot = start_gather(
        inputs, w_qkv.transpose(1, 0, 2), w_out, small, seg8, cotangent, nz, ne, hw, 0
    )
    small = small.transpose(1, 0, 2).reshape(-1, width)
    router_t = small[:expert_count]
    gain_mat = small[expert_count : expert_count + 4].astype(F32)
    my_gains = lax.dynamic_slice_in_dim(gain_mat, e * hw, hw, axis=1)
    seg_all = seg_all.reshape(ne * num_seqs, 8, length)[:, 0]

    g_all = lax.all_gather(cot, both, axis=0, tiled=True)
    in_all = in_all.reshape(ne * count, width).astype(F32)
    h1_all = (in_all * rms_scale(in_all) * gain_mat[0]).astype(BF)
    inputs_f = inputs.astype(F32)
    scale_one = rms_scale(inputs_f)
    plane = h1_all.shape[0]
    shape_heads = (ne * num_seqs, length, heads, HD)

    q, k, v = [dot(h1_all, wq[j], NN) for j in range(3)]
    sums = jnp.stack([jnp.sum(q * q, axis=-1), jnp.sum(k * k, axis=-1)])
    scales = lax.rsqrt(lax.psum(sums, "expert") / width + EPS)
    aq, ak = scales[0][:, None], scales[1][:, None]
    cos_tab, sin_tab = rope_tables(length)
    rq = rotate((q * aq * my_gains[1]).reshape(shape_heads), cos_tab, sin_tab).astype(BF)
    rk = rotate((k * ak * my_gains[2]).reshape(shape_heads), cos_tab, sin_tab).astype(BF)
    vb = v.astype(BF).reshape(shape_heads)
    o, lse = jax.vmap(attend_forward)(rq, rk, vb, seg_all)
    o = o.reshape(plane, hw)
    x1_part = dot(o, wo, NN).astype(BF)
    (x1_sum,) = scatter_tokens(x1_part.reshape(ne, count, width), nz, ne, False, 1)
    x1 = inputs_f + x1_sum

    a2 = rms_scale(x1)
    h2 = (x1 * a2 * gain_mat[3]).astype(BF)
    probs = jax.nn.softmax(dot(h2, router_t, NT), axis=-1)
    picks = jnp.sum(
        (routes[:, :, None] == jnp.arange(expert_count, dtype=jnp.int32)).astype(F32), axis=1
    )
    gates = picks * probs

    split = 64
    high = gates.astype(BF)
    low = (gates - high.astype(F32)).astype(BF)
    blank = jnp.zeros((count, split - expert_count), BF)
    h2_wide = jnp.concatenate([h2, high, blank, low, blank], axis=1)
    wide = width + 2 * split
    fits, slots, scratch = moe_net_scratch(nz, ne, per_dev, count, width, wide, fl)
    if fits:
        _, mix, gh_sum, dwin, dwd = moe_net(
            h2_wide, g_all, w_gate, w_up, w_down, nz, ne, fl, slots, scratch, 2
        )
        mix = mix.reshape(-1, width)
    else:
        h2_all = gather_tokens(h2_wide, nz, ne, True, 2).reshape(-1, wide)
        wg = lax.dynamic_slice_in_dim(w_gate, z * fl, fl, axis=2)
        wu = lax.dynamic_slice_in_dim(w_up, z * fl, fl, axis=2)
        wd = lax.dynamic_slice_in_dim(w_down, z * fl, fl, axis=1).reshape(per_dev * fl, width)
        w_in = jnp.concatenate([*wg, *wu], axis=1)
        mix, gh, dwin, dwd = moe(
            h2_all, g_all, w_in, wd, per_dev, nz, ne, count, min(4, ne)
        )
        gh_sum, mix = scatter_tokens(
            gh.reshape(nz * ne, count, wide), nz, ne, True, 3, after=mix.reshape(-1, width)
        )
    grad_from_experts = gh_sum[:, :width]
    grad_gates = (
        gh_sum[:, width : width + expert_count]
        + gh_sum[:, width + split : width + split + expert_count]
    )

    mix = lax.psum_scatter(mix, "expert", scatter_dimension=0, tiled=True)
    mix = lax.psum_scatter(mix, "dp", scatter_dimension=0, tiled=True)
    output = (x1 + mix.astype(F32)).astype(BF)

    dwin = lax.all_to_all(
        dwin.reshape(nz, width // nz, 2 * per_dev * fl),
        "dp", split_axis=0, concat_axis=0, tiled=True,
    )
    grad_w_gate, grad_w_up = lay_experts(dwin, per_dev, fl)
    grad_w_down = dwd.reshape(per_dev, fl, width)

    grad_top = cotangent.astype(F32)
    grad_probs = picks * grad_gates
    glog = (probs * (grad_probs - jnp.sum(probs * grad_probs, axis=-1, keepdims=True))).astype(BF)
    local_router = dot(glog, h2, TN)
    gh2 = grad_from_experts + dot(glog, router_t, NN)
    grad_ffn, gain_ffn = rms_backward(x1, a2, gain_mat[3], gh2)
    gx1 = grad_top + grad_ffn
    gab = gx1.astype(BF)

    gab_all = gather_tokens(gab, nz, ne, False, 4).reshape(-1, width)
    go = dot(gab_all, wo, NT).astype(BF).reshape(shape_heads)
    grad_q, grad_k, gv = jax.vmap(attend_backward)(rq, rk, vb, seg_all, lse, go)
    gqn = rotate(grad_q, cos_tab, -sin_tab).reshape(plane, hw)
    gkn = rotate(grad_k, cos_tab, -sin_tab).reshape(plane, hw)
    nq, nk = q * aq, k * ak
    sq, sk = gqn * my_gains[1], gkn * my_gains[2]
    sums = jnp.stack([jnp.sum(sq * nq, axis=-1), jnp.sum(sk * nk, axis=-1)])
    means = lax.psum(sums, "expert") / width
    gq = (aq * (sq - nq * means[0][:, None])).astype(BF)
    gk = (ak * (sk - nk * means[1][:, None])).astype(BF)
    gproj = [gq, gk, gv.reshape(plane, hw)]
    gain_q, gain_k = jnp.sum(gqn * nq, axis=0), jnp.sum(gkn * nk, axis=0)

    gh1_part = sum(dot(part, wq[j], NT) for j, part in enumerate(gproj)).astype(BF)
    (gh1,) = scatter_tokens(gh1_part.reshape(ne, count, width), nz, ne, False, 5)
    grad_front, gain_attn = rms_backward(inputs_f, scale_one, gain_mat[0], gh1)
    grad_inputs = (gx1 + grad_front).astype(BF)

    part_out = dot(o, gab_all, TN).astype(BF)
    part_out = swap_in_plane(part_out, ne, 8)
    parts = [dot(h1_all, part, TN).astype(BF) for part in gproj] + [part_out]
    mine = lax.psum_scatter(
        jnp.concatenate(parts, axis=1), "dp", scatter_dimension=0, tiled=True
    )
    wide = gather_tokens(mine, nz, ne, False, 6)
    grad_w_qkv, grad_w_out = lay_mixer(wide, 4, hw)
    grad_w_qkv = grad_w_qkv.transpose(1, 0, 2)

    place = lambda part: lax.dynamic_update_slice_in_dim(
        jnp.zeros((1, width), F32), part[None], e * hw, axis=1
    )
    tiny = jnp.concatenate(
        [
            local_router, gain_attn[None], place(gain_q), place(gain_k), gain_ffn[None],
            jnp.zeros((-(expert_count + 4) % 8, width), F32),
        ],
        axis=0,
    )
    tiny = reduce_columns(tiny, nz, ne, 7)
    grad_w_router = tiny[:expert_count].T
    grad_gains = tiny[expert_count : expert_count + 4].T
    return (
        output,
        grad_inputs,
        grad_w_qkv,
        grad_w_out,
        grad_w_router,
        grad_gains,
        grad_w_gate,
        grad_w_up,
        grad_w_down,
    )


def solution(mesh):
    tokens = P(("dp", "expert"), None)
    rows = P("dp", None)
    rows3 = P("dp", None, None)
    owned = P("expert", None, None)
    return jax.shard_map(
        body,
        mesh=mesh,
        in_specs=(tokens, tokens, tokens, rows3, rows, rows, rows, owned, owned, owned, tokens),
        out_specs=(tokens, tokens, rows3, rows, rows, rows)
        + (P("expert", "dp", None),) * 3,
        check_vma=False,
    )
```

```python
import functools

import jax
import jax.numpy as jnp
from jax import lax
from jax.experimental import pallas as pl
from jax.experimental.pallas import tpu as pltpu
from jax.sharding import PartitionSpec as P


HD = 128
EPS = 1e-05
ROPE_BASE = 10000.0
MASKED = -1e30
BF = jnp.bfloat16
F32 = jnp.float32


def dot(a, b, dims):
    return lax.dot_general(a, b, (dims, ((), ())), preferred_element_type=F32)


NN = ((1,), (0,))
NT = ((1,), (1,))
TN = ((0,), (0,))


def rms_scale(values):
    return lax.rsqrt(jnp.mean(values * values, axis=-1, keepdims=True) + EPS)


def rms_backward(values, inv_rms, gain_col, grad_out):
    normed = values * inv_rms
    grad_gain = jnp.sum(grad_out * normed, axis=0)
    scaled = grad_out * gain_col
    grad_values = inv_rms * (scaled - normed * jnp.mean(scaled * normed, axis=-1, keepdims=True))
    return (grad_values, grad_gain)


MESH = pl.DeviceIdType.MESH
ANY = pl.BlockSpec(memory_space=pl.ANY)
VMEM = pl.BlockSpec(memory_space=pltpu.VMEM)
DMA = pltpu.SemaphoreType.DMA


def flip(index, bit):
    return index + bit * (1 - 2 * ((index // bit) % 2))


def flips(index, bits):
    out = [index]
    for bit in bits:
        out = out + [flip(i, bit) for i in out]
    return out


def bit_orders(ne):
    bits = [1 << b for b in range(ne.bit_length() - 1)]
    return [bits[:1] + bits[1:], bits[:1] + bits[1:][::-1]]


def nearest(z, r, nz):
    low = jnp.minimum(z, nz - 1 - z)
    near = z - (r + 1) // 2 if r % 2 else z + r // 2
    far = jnp.where(2 * z < nz, z + (r - low), z - (r - low))
    return jnp.where(r <= 2 * low, near, far)


def remote(src, dst, send, recv, peer):
    return pltpu.make_async_remote_copy(
        src_ref=src, dst_ref=dst, send_sem=send, recv_sem=recv, device_id=peer, device_id_type=MESH
    )


def for_others(nz, ne, z, e, act):
    def step(i, carry):
        flat = lax.rem(z * ne + e + i, nz * ne)
        act(flat // ne, lax.rem(flat, ne), flat)
        return carry

    lax.fori_loop(1, nz * ne, step, 0)


def meet_all(nz, ne, z, e):
    sem = pltpu.get_barrier_semaphore()

    def greet(zz, ee, flat):
        pl.semaphore_signal(sem, inc=1, device_id=(zz, ee), device_id_type=MESH)

    for_others(nz, ne, z, e, greet)
    pl.semaphore_wait(sem, nz * ne - 1)


def meet_column_and_plane(nz, ne, z, e, spread):
    sem = pltpu.get_barrier_semaphore()
    peers = [(z, flip(e, 1 << b)) for b in range(ne.bit_length() - 1)]
    if spread:
        peers += [(lax.rem(z + r, nz), e) for r in range(1, nz)]
    for peer in peers:
        pl.semaphore_signal(sem, inc=1, device_id=peer, device_id_type=MESH)
    pl.semaphore_wait(sem, len(peers))


class PlaneGather:
    def __init__(self, nz, ne, z, e, spread, x_ref, out_ref, zsend, zrecv, send, recv, local):
        self.nz, self.ne, self.z, self.e, self.spread = nz, ne, z, e, spread
        self.x, self.out = x_ref, out_ref
        self.zsend, self.zrecv, self.send, self.recv = zsend, zrecv, send, recv
        self.rounds = nz if spread else 1
        self.half = x_ref.shape[0] // 2
        self.orders = [o[1:] + o[:1] for o in bit_orders(ne)]
        self.planes = [z if spread else 0] + [nearest(z, r, nz) for r in range(1, self.rounds)]
        self.pending, self.arrivals = [], {}
        own = self.slot(0, e)
        keep = pltpu.make_async_copy(x_ref, out_ref.at[own], local)
        keep.start()
        self.pending.append(keep.wait)

    @staticmethod
    def scratch(nz, ne, spread):
        rounds = nz if spread else 1
        return [DMA((nz,)), DMA((nz,)), DMA((rounds, 2, ne - 1)), DMA((rounds, 2, ne - 1)), DMA]

    def slot(self, r, ee):
        return self.planes[r] * self.ne + ee

    def spread_own(self):
        for r in range(1, self.rounds):
            to = self.planes[r]
            copy = remote(
                self.x, self.out.at[self.slot(0, self.e)],
                self.zsend.at[r], self.zrecv.at[self.z], (to, self.e),
            )
            copy.start()
            self.pending.append(copy.wait_send)

    def forward(self, r, s, stage, subset):
        order = self.orders[s]
        rows = pl.ds(s * self.half, self.half)
        peer_e = flip(self.e, order[stage])
        n = (1 << stage) - 1 + subset
        block = self.slot(r, flips(self.e, order[:stage])[subset])
        dst = self.out.at[block, rows]
        src = self.x.at[rows] if r == 0 and subset == 0 else dst
        sems = self.send.at[r, s, n], self.recv.at[r, s, n]
        copy = remote(src, dst, *sems, (self.z, peer_e))
        copy.start()
        self.pending.append(copy.wait_send)
        got = self.out.at[self.slot(r, flips(peer_e, order[:stage])[subset]), rows]
        self.arrivals[(r, s, stage, subset)] = remote(got, got, *sems, (self.z, peer_e)).wait_recv

    def start_round(self, r):
        if r > 0:
            here = self.out.at[self.slot(r, self.e)]
            remote(
                here, here, self.zsend.at[r], self.zrecv.at[self.planes[r]], (self.planes[r], self.e)
            ).wait_recv()
        for stage in range(len(self.orders[0])):
            for s in range(2):
                self.forward(r, s, stage, 0)

    def finish_round(self, r):
        stages = len(self.orders[0])
        for stage in range(stages):
            for subset in range(1 << stage):
                for s in range(2):
                    self.arrivals.pop((r, s, stage, subset))()
                    for later in range(stage + 1, stages):
                        self.forward(r, s, later, subset + (1 << stage))

    def finish(self):
        for wait in self.pending:
            wait()


def gather_kernel(nz, ne, spread, x_ref, out_ref, *sems):
    z, e = lax.axis_index("dp"), lax.axis_index("expert")
    meet_column_and_plane(nz, ne, z, e, spread)
    net = PlaneGather(nz, ne, z, e, spread, x_ref, out_ref, *sems)
    net.spread_own()
    net.start_round(0)
    for r in range(1, net.rounds):
        net.start_round(r)
        net.finish_round(r - 1)
    net.finish_round(net.rounds - 1)
    net.finish()


def gather_tokens(x, nz, ne, spread, cid):
    rounds = nz if spread else 1
    return pl.pallas_call(
        functools.partial(gather_kernel, nz, ne, spread),
        out_shape=jax.ShapeDtypeStruct((rounds * ne, *x.shape), x.dtype),
        in_specs=[VMEM],
        out_specs=ANY,
        scratch_shapes=PlaneGather.scratch(nz, ne, spread),
        compiler_params=pltpu.CompilerParams(collective_id=cid, has_side_effects=True),
        name="gather_tokens",
    )(x)


def add_rows(dst, src, tile=16):
    def step(i, carry):
        rows = pl.ds(pl.multiple_of(i * tile, tile), tile)
        dst[rows, :] = (dst[rows, :].astype(F32) + src[rows, :].astype(F32)).astype(dst.dtype)
        return carry

    lax.fori_loop(0, dst.shape[0] // tile, step, 0)


def scatter_kernel(nz, ne, spread, x_ref, *refs):
    out_ref, acc, got, zgot, loads, send, recv, zsend, zrecv = refs[-9:]
    z, e = lax.axis_index("dp"), lax.axis_index("expert")
    meet_column_and_plane(nz, ne, z, e, spread)
    rounds = nz if spread else 1
    stages = ne.bit_length() - 1
    half = out_ref.shape[0] // 2
    orders = bit_orders(ne)
    pending, arrivals, zwait = [], {}, {}
    ranks = list(range(1, rounds)) + [0]
    first = [0] * (stages + 1)
    for j in range(stages):
        first[j + 1] = first[j] + (ne >> (j + 1))

    def plane_of(r):
        return lax.rem(z + r, nz) * ne if spread else 0

    def push(r, s, j):
        order = orders[s]
        peer = (z, flip(e, order[j]))
        rest = ne >> (j + 1)
        for i in range(rest):
            n = first[j] + i
            if j == 0:
                block = flips(peer[1], order[:0:-1])[i]
                src = x_ref.at[plane_of(r) + block, pl.ds(s * half, half)]
            else:
                src = acc.at[r, s, rest + i]
            copy = remote(src, got.at[r, s, n], send.at[r, s, n], recv.at[r, s, n], peer)
            copy.start()
            pending.append(copy.wait_send)
            arrivals.setdefault((r, s, j), []).append((copy.wait_recv, i, n))

    for r in ranks:
        for s in range(2):
            push(r, s, 0)
            for i, block in enumerate(flips(e, orders[s][:0:-1])):
                copy = pltpu.make_async_copy(
                    x_ref.at[plane_of(r) + block, pl.ds(s * half, half)],
                    acc.at[r, s, i],
                    loads.at[r, s, i],
                )
                copy.start()
                arrivals.setdefault((r, s, -1), []).append(copy.wait)
    for t in range(rounds + stages):
        for place, r in enumerate(ranks):
            j = t - place
            if not 0 <= j < stages:
                continue
            for s in range(2):
                if j == 0:
                    for wait in arrivals.pop((r, s, -1)):
                        wait()
                for wait, i, n in arrivals.pop((r, s, j)):
                    wait()
                    add_rows(acc.at[r, s, i], got.at[r, s, n])
                if j + 1 < stages:
                    push(r, s, j + 1)
                elif r > 0:
                    copy = remote(
                        acc.at[r, s, 0], zgot.at[r, s], zsend.at[r, s], zrecv.at[r, s],
                        (lax.rem(z + r, nz), e),
                    )
                    copy.start()
                    pending.append(copy.wait_send)
                    zwait[(r, s)] = copy.wait_recv
    for s in range(2):
        for r in range(1, rounds):
            zwait[(r, s)]()

        def step(i, carry):
            rows = pl.ds(pl.multiple_of(i * 16, 16), 16)
            total = acc[0, s, 0, rows, :].astype(F32)
            for r in range(1, rounds):
                total = total + zgot[r, s, rows, :].astype(F32)
            out_ref[pl.ds(pl.multiple_of(s * half + i * 16, 16), 16), :] = total.astype(out_ref.dtype)
            return carry

        lax.fori_loop(0, half // 16, step, 0)
    for wait in pending:
        wait()


def scatter_tokens(parts, nz, ne, spread, cid, after=None):
    rounds = nz if spread else 1
    _, count, width = parts.shape
    half = count // 2
    held = (2 * rounds * (ne // 2 + ne - 1) + 2 * nz) * half * width * 2
    if held > 56_000_000:
        cut = width // 256 * 128
        left = scatter_tokens(parts[..., :cut], nz, ne, spread, cid, after)
        right = scatter_tokens(parts[..., cut:], nz, ne, spread, cid + 16)
        return [jnp.concatenate([left[0], right[0]], axis=1), *left[1:]]
    more = [] if after is None else [after]
    return pl.pallas_call(
        functools.partial(scatter_kernel, nz, ne, spread),
        out_shape=[jax.ShapeDtypeStruct(m.shape, m.dtype) for m in more]
        + [jax.ShapeDtypeStruct((count, width), F32)],
        in_specs=[ANY] * (1 + len(more)),
        out_specs=[ANY] * len(more) + [VMEM],
        scratch_shapes=[
            pltpu.VMEM((rounds, 2, ne // 2, half, width), BF),
            pltpu.VMEM((rounds, 2, ne - 1, half, width), BF),
            pltpu.VMEM((nz, 2, half, width), BF),
            DMA((rounds, 2, ne // 2)),
            DMA((rounds, 2, ne - 1)),
            DMA((rounds, 2, ne - 1)),
            DMA((nz, 2)),
            DMA((nz, 2)),
        ],
        input_output_aliases={1: 0} if more else {},
        compiler_params=pltpu.CompilerParams(
            collective_id=cid, has_side_effects=True, vmem_limit_bytes=64_000_000
        ),
        name="scatter_tokens",
    )(parts, *more)[::-1]


def reduce_kernel(nz, ne, x_ref, out_ref, got, total, far, send1, recv1, send2, recv2):
    z, e = lax.axis_index("dp"), lax.axis_index("expert")
    per = ne // nz
    meet_all(nz, ne, z, e)
    first = []
    for r in range(1, ne):
        to = lax.rem(e + r, ne)
        copy = remote(x_ref.at[to], got.at[r], send1.at[r], recv1.at[r], (z, to))
        copy.start()
        first.append(copy)
    acc = x_ref[e]
    for r, copy in enumerate(first):
        copy.wait_recv()
        acc = acc + got[r + 1]
    total[...] = acc
    home, place = e // per, lax.rem(e, per)
    for r in range(ne):
        to = lax.rem(e + r, ne)
        copy = remote(total, far.at[z, place], send2.at[r], recv2, (home, to))
        if r > 0:
            copy.start()
        else:

            @pl.when(home != z)
            def _():
                copy.start()

            @pl.when(home == z)
            def _():
                far[z, place] = total[...]

    for copy in first:
        copy.wait_send()
    for r in range(ne):
        copy = remote(total, far.at[z, place], send2.at[r], recv2, (home, e))
        if r > 0:
            copy.wait_send()
        else:

            @pl.when(home != z)
            def _():
                copy.wait_send()

    def arrive(count):
        flat = got.at[pl.ds(0, count)]
        remote(flat, flat, send2.at[0], recv2, (z, e)).wait_recv()

    @pl.when(home == z)
    def _():
        arrive(nz * per - 1)

    @pl.when(home != z)
    def _():
        arrive(nz * per)

    for i in range(per):
        out_ref[i] = sum(far[k, i] for k in range(nz))


def reduce_columns(x, nz, ne, cid):
    rows, width = x.shape
    per = ne // nz
    x = x.reshape(rows, ne, width // ne).transpose(1, 0, 2)
    out = pl.pallas_call(
        functools.partial(reduce_kernel, nz, ne),
        out_shape=jax.ShapeDtypeStruct((per, rows, width // ne), F32),
        in_specs=[VMEM],
        out_specs=VMEM,
        scratch_shapes=[
            pltpu.VMEM((ne, rows, width // ne), F32),
            pltpu.VMEM((rows, width // ne), F32),
            pltpu.VMEM((nz, per, rows, width // ne), F32),
            DMA((ne,)), DMA((ne,)), DMA((ne,)), DMA,
        ],
        compiler_params=pltpu.CompilerParams(collective_id=cid, has_side_effects=True),
        name="reduce_columns",
    )(x)
    return out.transpose(1, 0, 2).reshape(rows, per * (width // ne))


def start_kernel(
    nz, ne, x_ref, wqkv_ref, wout_ref, small_ref, seg_ref, _,
    out_ref, wq_ref, wo_ref, small_out, seg_out, _2,
    wbuf, pbuf, zsend, zrecv, send, recv, local,
    up_send, up_recv, dn_send, dn_recv, wload, wkeep, pload, psend, precv, pkeep,
    small_send, small_recv, seg_send, seg_recv,
):
    z, e = lax.axis_index("dp"), lax.axis_index("expert")
    kinds, depth, hw = wbuf.shape
    per = ne // nz
    loads = [
        pltpu.make_async_copy(wqkv_ref.at[j, :, pl.ds(e * hw, hw)], wbuf.at[j], wload.at[j])
        for j in range(kinds)
    ]
    for copy in loads:
        copy.start()
    pieces = [
        pltpu.make_async_copy(
            wout_ref.at[pl.ds(i * hw, hw), pl.ds(e * hw, hw)], pbuf.at[i], pload.at[i]
        )
        for i in range(per)
    ]
    for copy in pieces:
        copy.start()
    meet_all(nz, ne, z, e)

    def rows_of(zz):
        return pl.ds(pl.multiple_of(zz * depth, depth), depth)

    def hop(j, zz, dist, up):
        send, recv = (up_send, up_recv) if up else (dn_send, dn_recv)
        here = wq_ref.at[j, rows_of(zz)]
        src = wbuf.at[j] if dist == 1 else here
        to = z + 1 if up else z - 1
        return remote(src, here, send.at[dist, j], recv.at[dist, j], (to, e))

    keeps = []
    for j in range(kinds):
        loads[j].wait()

        @pl.when(z + 1 < nz)
        def _():
            hop(j, z, 1, True).start()

        @pl.when(z > 0)
        def _():
            hop(j, z, 1, False).start()

        keep = pltpu.make_async_copy(wbuf.at[j], wq_ref.at[j, rows_of(z)], wkeep.at[j])
        keep.start()
        keeps.append(keep)

    def wait_all(ref, send, recv, count):
        most = ref.at[pl.ds(0, count)]
        both = remote(most, most, send, recv, (z, flip(e, 1)))
        both.wait_send()
        both.wait_recv()

    small_out[z] = small_ref[...]
    for r in range(1, nz):
        remote(
            small_ref, small_out.at[z], small_send, small_recv, (lax.rem(z + r, nz), e)
        ).start()
    seg_out[e] = seg_ref[...]
    for r in range(1, ne):
        remote(seg_ref, seg_out.at[e], seg_send, seg_recv, (z, lax.rem(e + r, ne))).start()
    net = PlaneGather(nz, ne, z, e, False, x_ref, out_ref, zsend, zrecv, send, recv, local)
    net.start_round(0)

    columns = pl.ds(e * hw, hw)
    for i in range(per):
        pieces[i].wait()
    for r in range(nz):
        for i in range(per):
            to = (lax.rem(z + r, nz), z * per + i)
            give = remote(pbuf.at[i], wo_ref.at[:, columns], psend.at[r, i], precv, to)
            if r > 0:
                give.start()
            else:
                own = pltpu.make_async_copy(pbuf.at[i], wo_ref.at[:, columns], pkeep)

                @pl.when(to[1] == e)
                def _():
                    own.start()

                @pl.when(to[1] != e)
                def _():
                    give.start()
    net.finish_round(0)
    for dist in range(1, nz):
        for j in range(kinds):

            @pl.when(z - dist >= 0)
            def _():
                got = wq_ref.at[j, rows_of(z - dist)]
                remote(got, got, up_send.at[dist, j], up_recv.at[dist, j], (z, e)).wait_recv()

                @pl.when(z + 1 < nz)
                def _():
                    if dist + 1 < nz:
                        hop(j, z - dist, dist + 1, True).start()

            @pl.when(z + dist < nz)
            def _():
                got = wq_ref.at[j, rows_of(z + dist)]
                remote(got, got, dn_send.at[dist, j], dn_recv.at[dist, j], (z, e)).wait_recv()

                @pl.when(z > 0)
                def _():
                    if dist + 1 < nz:
                        hop(j, z + dist, dist + 1, False).start()

    net.finish()
    for keep in keeps:
        keep.wait()
    for dist in range(1, nz):
        for j in range(kinds):

            @pl.when((z - dist + 1 >= 0) & (z + 1 < nz))
            def _():
                hop(j, z - dist + 1, dist, True).wait_send()

            @pl.when((z + dist - 1 < nz) & (z > 0))
            def _():
                hop(j, z + dist - 1, dist, False).wait_send()

    for r in range(nz):
        for i in range(per):
            to = (lax.rem(z + r, nz), z * per + i)
            give = remote(pbuf.at[i], wo_ref.at[:, columns], psend.at[r, i], precv, to)
            if r > 0:
                give.wait_send()
            else:
                own = pltpu.make_async_copy(pbuf.at[i], wo_ref.at[:, columns], pkeep)

                @pl.when(to[1] == e)
                def _():
                    own.wait()

                @pl.when(to[1] != e)
                def _():
                    give.wait_send()

    def wait_pieces(count):
        most = wo_ref.at[:, pl.ds(0, count * hw)]
        remote(most, most, psend.at[0, 0], precv, (z, e)).wait_recv()

    @pl.when(z == e // per)
    def _():
        wait_pieces(ne - 1)

    @pl.when(z != e // per)
    def _():
        wait_pieces(ne)

    wait_all(small_out, small_send, small_recv, nz - 1)
    wait_all(seg_out, seg_send, seg_recv, ne - 1)


def start_gather(x, w_qkv, w_out, small, seg, after, nz, ne, hw, cid):
    kinds, depth, width = w_qkv.shape
    per = ne // nz
    return pl.pallas_call(
        functools.partial(start_kernel, nz, ne),
        out_shape=[
            jax.ShapeDtypeStruct((ne, *x.shape), x.dtype),
            jax.ShapeDtypeStruct((kinds, nz * depth, hw), BF),
            jax.ShapeDtypeStruct((hw, width), BF),
            jax.ShapeDtypeStruct((nz, *small.shape), small.dtype),
            jax.ShapeDtypeStruct((ne, *seg.shape), seg.dtype),
            jax.ShapeDtypeStruct(after.shape, after.dtype),
        ],
        in_specs=[VMEM, ANY, ANY, VMEM, VMEM, ANY],
        out_specs=[ANY, ANY, ANY, VMEM, VMEM, ANY],
        input_output_aliases={5: 5},
        scratch_shapes=[
            pltpu.VMEM((kinds, depth, hw), BF),
            pltpu.VMEM((per, hw, hw), BF),
            *PlaneGather.scratch(nz, ne, False),
            DMA((nz, kinds)), DMA((nz, kinds)), DMA((nz, kinds)), DMA((nz, kinds)),
            DMA((kinds,)), DMA((kinds,)), DMA((per,)), DMA((nz, per)), DMA, DMA,
            DMA, DMA, DMA, DMA,
        ],
        compiler_params=pltpu.CompilerParams(collective_id=cid, has_side_effects=True),
        name="start_gather",
    )(x, w_qkv, w_out, small, seg, after)


def rope_lanes(length):
    half = HD // 2
    freqs = jnp.exp(-jnp.log(ROPE_BASE) * (2.0 * jnp.arange(half, dtype=F32) / HD))
    angles = jnp.arange(length, dtype=F32)[:, None] * freqs[None, :]
    cos, sin = jnp.cos(angles), jnp.sin(angles)
    return jnp.concatenate([cos, cos], axis=1), jnp.concatenate([-sin, sin], axis=1)


def turn(x, cos, sin):
    return x * cos + pltpu.roll(x, HD // 2, 1) * sin


def meet_plane(ne, z, e):
    sem = pltpu.get_barrier_semaphore()
    for r in range(1, ne):
        pl.semaphore_signal(
            sem, inc=1, device_id=(z, lax.rem(e + r, ne)), device_id_type=MESH
        )
    pl.semaphore_wait(sem, ne - 1)


def plane_totals(ne, z, e, mine, theirs, send, recv):
    copies = []
    for r in range(1, ne):
        to = (z, lax.rem(e + r, ne))
        copy = remote(mine, theirs.at[r], send.at[r], recv.at[r], to)
        copy.start()
        copies.append(copy)
    total = mine[...]
    for r, copy in enumerate(copies):
        copy.wait_recv()
        total = total + theirs[r + 1]
    for copy in copies:
        copy.wait_send()
    return total


def store_columns(sums, first, columns):
    rows = columns[0].shape[0]
    lanes = lax.broadcasted_iota(jnp.int32, (rows, 128), 1)
    wide = jnp.zeros((rows, 128), F32)
    for j, column in enumerate(columns):
        wide = jnp.where(lanes == j, column, wide)
    sums[:, pl.ds(first, rows)] = wide.T[:8]


def as_columns(total, out):
    rows = total.shape[1]
    for first in range(0, rows, 128):
        chunk = total[:, first : first + 128]
        out[first : first + 128, :] = jnp.concatenate([chunk] * 16, axis=0).T


def allowed_pairs(seg_ref, n):
    length = seg_ref.shape[2]
    keys = jnp.broadcast_to(seg_ref[n, :1].astype(F32), (length, length))
    i = lax.broadcasted_iota(jnp.int32, (length, length), 0)
    j = lax.broadcasted_iota(jnp.int32, (length, length), 1)
    return (i >= j) & (keys == keys.T)


def attend(rq, rk, allowed):
    scores = jnp.where(allowed, dot(rq, rk, NT) * HD ** (-0.5), MASKED)
    top = jnp.max(scores, axis=-1, keepdims=True)
    lse = top + jnp.log(jnp.sum(jnp.exp(scores - top), axis=-1, keepdims=True))
    return jnp.exp(scores - lse)


def attn_fwd_kernel(
    ne, x_ref, wq_ref, wo_ref, gain_ref, mine_ref, seg_ref, cos_ref, sin_ref,
    h1_ref, q_ref, k_ref, rq_ref, rk_ref, v_ref, o_ref, scale_ref, x1_ref,
    sums, theirs, send, recv,
):
    z, e = lax.axis_index("dp"), lax.axis_index("expert")
    width = x_ref.shape[2]
    count, hw = q_ref.shape
    length = seg_ref.shape[2]
    rows_dev = x_ref.shape[1]
    tile = min(512, count)
    meet_plane(ne, z, e)

    def normed(b, carry):
        x = x_ref[b].astype(F32)
        h1 = x * rms_scale(x) * gain_ref[:1]
        h1_ref[pl.ds(pl.multiple_of(b * rows_dev, rows_dev), rows_dev), :] = h1.astype(BF)
        return carry

    lax.fori_loop(0, ne, normed, 0)
    for first in range(0, count, tile):
        rows = slice(first, first + tile)
        h1 = h1_ref[rows, :]
        q, k = dot(h1, wq_ref[0], NN), dot(h1, wq_ref[1], NN)
        q_ref[rows, :] = q
        k_ref[rows, :] = k
        v_ref[rows, :] = dot(h1, wq_ref[2], NN).astype(BF)
        store_columns(
            sums, first, [jnp.sum(t * t, axis=-1, keepdims=True) for t in (q, k)]
        )
    total = plane_totals(ne, z, e, sums, theirs, send, recv)
    as_columns(lax.rsqrt(total / width + EPS), scale_ref)
    cos, sin = cos_ref[...], sin_ref[...]

    def sequence(n, carry):
        rows = pl.ds(pl.multiple_of(n * length, length), length)
        allowed = allowed_pairs(seg_ref, n)
        aq, ak = scale_ref[rows, 0:1], scale_ref[rows, 1:2]
        for c in range(0, hw, HD):
            cols = slice(c, c + HD)
            rq = turn(q_ref[rows, cols] * aq * mine_ref[1:2, cols], cos, sin).astype(BF)
            rk = turn(k_ref[rows, cols] * ak * mine_ref[2:3, cols], cos, sin).astype(BF)
            rq_ref[rows, cols] = rq
            rk_ref[rows, cols] = rk
            probs = attend(rq, rk, allowed).astype(BF)
            o_ref[rows, cols] = dot(probs, v_ref[rows, cols], NN).astype(BF)
        return carry

    lax.fori_loop(0, count // length, sequence, 0)
    for first in range(0, count, tile):
        x1 = dot(o_ref[first : first + tile, :], wo_ref[...], NN).astype(BF)
        blocks = tile // rows_dev
        x1_ref[first // rows_dev : first // rows_dev + blocks] = x1.reshape(
            blocks, rows_dev, width
        )


def attn_fwd(in_all, wq, wo, gain_mat, my_gains, seg, tables, cid):
    ne, rows_dev, width = in_all.shape
    count, hw = ne * rows_dev, wo.shape[0]
    return pl.pallas_call(
        functools.partial(attn_fwd_kernel, ne),
        out_shape=[
            jax.ShapeDtypeStruct((count, width), BF),
            jax.ShapeDtypeStruct((count, hw), F32),
            jax.ShapeDtypeStruct((count, hw), F32),
            jax.ShapeDtypeStruct((count, hw), BF),
            jax.ShapeDtypeStruct((count, hw), BF),
            jax.ShapeDtypeStruct((count, hw), BF),
            jax.ShapeDtypeStruct((count, hw), BF),
            jax.ShapeDtypeStruct((count, 128), F32),
            jax.ShapeDtypeStruct((ne, rows_dev, width), BF),
        ],
        in_specs=[VMEM] * 8,
        out_specs=[VMEM] * 9,
        scratch_shapes=[
            pltpu.VMEM((8, count), F32), pltpu.VMEM((ne, 8, count), F32), DMA((ne,)), DMA((ne,)),
        ],
        compiler_params=pltpu.CompilerParams(
            collective_id=cid, has_side_effects=True, vmem_limit_bytes=60_000_000
        ),
        name="attn_fwd",
    )(in_all, wq, wo, gain_mat, my_gains, seg, *tables)


def attn_bwd_kernel(
    ne, gab_ref, wq_ref, wo_ref, mine_ref, seg_ref, cos_ref, sin_ref,
    h1_ref, q_ref, k_ref, rq_ref, rk_ref, v_ref, o_ref, scale_ref,
    gh1_ref, parts_ref, gain_ref,
    pout, go_ref, gqn_ref, gkn_ref, gp_ref, sums, theirs, means, send, recv, psend, precv,
):
    z, e = lax.axis_index("dp"), lax.axis_index("expert")
    count, hw = q_ref.shape
    width = gab_ref.shape[2]
    rows_dev = gab_ref.shape[1]
    length = seg_ref.shape[2]
    tile = min(512, count)
    blocks = tile // rows_dev
    meet_plane(ne, z, e)

    gab = lambda first: gab_ref[first // rows_dev : first // rows_dev + blocks].reshape(tile, width)
    part = dot(o_ref[:tile, :], gab(0), TN)
    for first in range(tile, count, tile):
        part = part + dot(o_ref[first : first + tile, :], gab(first), TN)
    pout[...] = part.astype(BF)
    for first in range(0, count, tile):
        go_ref[first : first + tile, :] = dot(gab(first), wo_ref[...], NT).astype(BF)
    my_rows = pl.ds(pl.multiple_of(e * hw, hw), hw)
    last = pl.ds(3 * hw, hw)
    gives = []
    for r in range(1, ne):
        to = lax.rem(e + r, ne)
        give = remote(
            pout.at[:, pl.ds(pl.multiple_of(to * hw, hw), hw)], parts_ref.at[my_rows, last],
            psend.at[r], precv.at[r], (z, to),
        )
        give.start()
        gives.append(give)
    parts_ref[my_rows, last] = pout[:, my_rows]

    cos, sin = cos_ref[...], -sin_ref[...]
    gain_ref[...] = jnp.zeros_like(gain_ref)

    def sequence(n, carry):
        start = pl.multiple_of(n * length, length)
        rows = pl.ds(start, length)
        allowed = allowed_pairs(seg_ref, n)
        aq, ak = scale_ref[rows, 0:1], scale_ref[rows, 1:2]
        sum_q = jnp.zeros((length, 1), F32)
        sum_k = jnp.zeros((length, 1), F32)
        for c in range(0, hw, HD):
            cols = slice(c, c + HD)
            rq, rk, go = rq_ref[rows, cols], rk_ref[rows, cols], go_ref[rows, cols]
            probs = attend(rq, rk, allowed)
            gv = dot(probs.astype(BF), go, TN).astype(BF)
            gp_ref[rows, slice(2 * hw + c, 2 * hw + c + HD)] = gv
            grad = dot(go, v_ref[rows, cols], NT)
            delta = jnp.sum(probs * grad, axis=-1, keepdims=True)
            gs = (probs * (grad - delta) * HD ** (-0.5)).astype(BF)
            gqn = turn(dot(gs, rk, NN), cos, sin)
            gkn = turn(dot(gs, rq, TN), cos, sin)
            gqn_ref[rows, cols] = gqn
            gkn_ref[rows, cols] = gkn
            tq = gqn * (q_ref[rows, cols] * aq)
            tk = gkn * (k_ref[rows, cols] * ak)
            gain_ref[0:1, cols] += jnp.sum(tq, axis=0, keepdims=True)
            gain_ref[1:2, cols] += jnp.sum(tk, axis=0, keepdims=True)
            sum_q = sum_q + jnp.sum(tq * mine_ref[1:2, cols], axis=-1, keepdims=True)
            sum_k = sum_k + jnp.sum(tk * mine_ref[2:3, cols], axis=-1, keepdims=True)
        store_columns(sums, start, [sum_q, sum_k])
        return carry

    lax.fori_loop(0, count // length, sequence, 0)
    total = plane_totals(ne, z, e, sums, theirs, send, recv)
    as_columns(total / width, means)
    for first in range(0, count, tile):
        rows = slice(first, first + tile)
        aq, ak = scale_ref[rows, 0:1], scale_ref[rows, 1:2]
        mq, mk = means[rows, 0:1], means[rows, 1:2]
        gq = aq * (gqn_ref[rows, :] * mine_ref[1:2] - q_ref[rows, :] * aq * mq)
        gk = ak * (gkn_ref[rows, :] * mine_ref[2:3] - k_ref[rows, :] * ak * mk)
        gp_ref[rows, :hw] = gq.astype(BF)
        gp_ref[rows, hw : 2 * hw] = gk.astype(BF)
    for first in range(0, width, tile):
        rows = slice(first, first + tile)
        parts_ref[rows, : 3 * hw] = dot(h1_ref[:, rows], gp_ref[...], TN).astype(BF)
    for first in range(0, count, tile):
        rows = slice(first, first + tile)
        gh1 = dot(gp_ref[rows, :hw], wq_ref[0], NT)
        for j in range(1, 3):
            gh1 = gh1 + dot(gp_ref[rows, j * hw : (j + 1) * hw], wq_ref[j], NT)
        gh1_ref[first // rows_dev : first // rows_dev + blocks] = gh1.astype(BF).reshape(
            blocks, rows_dev, width
        )
    for give in gives:
        give.wait_send()
        give.wait_recv()


def attn_bwd(gab, wq, wo, my_gains, seg, tables, saved, cid):
    ne, rows_dev, width = gab.shape
    count, hw = ne * rows_dev, wo.shape[0]
    return pl.pallas_call(
        functools.partial(attn_bwd_kernel, ne),
        out_shape=[
            jax.ShapeDtypeStruct((ne, rows_dev, width), BF),
            jax.ShapeDtypeStruct((width, 4 * hw), BF),
            jax.ShapeDtypeStruct((8, hw), F32),
        ],
        in_specs=[VMEM] * 15,
        out_specs=[VMEM] * 3,
        scratch_shapes=[
            pltpu.VMEM((hw, width), BF),
            pltpu.VMEM((count, hw), BF),
            pltpu.VMEM((count, hw), F32),
            pltpu.VMEM((count, hw), F32),
            pltpu.VMEM((count, 3 * hw), BF),
            pltpu.VMEM((8, count), F32),
            pltpu.VMEM((ne, 8, count), F32),
            pltpu.VMEM((count, 128), F32),
            DMA((ne,)), DMA((ne,)), DMA((ne,)), DMA((ne,)),
        ],
        compiler_params=pltpu.CompilerParams(
            collective_id=cid, has_side_effects=True, vmem_limit_bytes=64_000_000
        ),
        name="attn_bwd",
    )(gab, wq, wo, my_gains, seg, *tables, *saved)


def lay_kernel(kinds, hw, x_ref, *outs):
    for k in range(kinds):
        piece = x_ref[0, :, k * hw : (k + 1) * hw].astype(F32)
        if k < kinds - 1:
            outs[0][k] = piece
        else:
            outs[1][...] = piece


def lay_mixer(wide, kinds, hw):
    ne, rows, _ = wide.shape
    return pl.pallas_call(
        functools.partial(lay_kernel, kinds, hw),
        grid=(ne,),
        in_specs=[pl.BlockSpec((1, rows, kinds * hw), lambda i: (i, 0, 0))],
        out_specs=[
            pl.BlockSpec((kinds - 1, rows, hw), lambda i: (0, 0, i)),
            pl.BlockSpec((rows, hw), lambda i: (0, i)),
        ],
        out_shape=[
            jax.ShapeDtypeStruct((kinds - 1, rows, ne * hw), F32),
            jax.ShapeDtypeStruct((rows, ne * hw), F32),
        ],
        name="lay_mixer",
    )(wide)


def lay_experts_kernel(per_dev, fl, x_ref, gate_ref, up_ref):
    for i in range(per_dev):
        gate_ref[i] = x_ref[0, :, i * fl : (i + 1) * fl].astype(F32)
        up_ref[i] = x_ref[0, :, (per_dev + i) * fl : (per_dev + i + 1) * fl].astype(F32)


def lay_experts(wide, per_dev, fl):
    nz, rows, _ = wide.shape
    out = jax.ShapeDtypeStruct((per_dev, rows, nz * fl), F32)
    spec = pl.BlockSpec((per_dev, rows, fl), lambda i: (0, 0, i))
    return pl.pallas_call(
        functools.partial(lay_experts_kernel, per_dev, fl),
        grid=(nz,),
        in_specs=[pl.BlockSpec((1, rows, 2 * per_dev * fl), lambda i: (i, 0, 0))],
        out_specs=[spec, spec],
        out_shape=[out, out],
        name="lay_experts",
    )(wide)


def moe_kernel(
    fl, h_ref, g_ref, win_ref, wd_ref,
    mix_ref, gh_ref, dwin_ref, dwd_ref, acc_in, acc_d,
):
    step = pl.program_id(0)
    tile, width = g_ref.shape
    per_dev = wd_ref.shape[0] // fl
    e = lax.axis_index("expert")
    h = h_ref[:, :width]
    g = g_ref[...]
    extra = h_ref[:, width:].astype(F32)
    pre = dot(h, win_ref[...], NN)
    graw = dot(g, wd_ref[...], NT)
    scaled_act, grad_gate, grad_up = [], [], []
    lanes = lax.broadcasted_iota(jnp.int32, (tile, 128), 1)
    gg = jnp.zeros((tile, 128), F32)
    split = 64
    for i in range(per_dev):
        u = pre[:, i * fl : (i + 1) * fl]
        w = pre[:, (per_dev + i) * fl : (per_dev + 1 + i) * fl]
        gr = graw[:, i * fl : (i + 1) * fl]
        mine = e * per_dev + i
        picked = (lanes == mine) | (lanes == mine + split)
        gate = jnp.sum(jnp.where(picked, extra, 0.0), axis=-1, keepdims=True)
        sig = 1.0 / (1.0 + jnp.exp(-u))
        silu = u * sig
        act = silu * w
        total = jnp.sum(act.astype(BF).astype(F32) * gr, axis=-1, keepdims=True)
        rounded = total.astype(BF).astype(F32)
        gg = jnp.where(lanes == mine, rounded, gg)
        gg = jnp.where(lanes == mine + split, total - rounded, gg)
        scaled_act.append((gate * act).astype(BF))
        gact = gate * gr
        grad_gate.append((gact * w * (sig * (1.0 + u * (1.0 - sig)))).astype(BF))
        grad_up.append((gact * silu).astype(BF))
    a = jnp.concatenate(scaled_act, axis=1)
    gin = jnp.concatenate(grad_gate + grad_up, axis=1)
    blocks, rows = mix_ref.shape[0], mix_ref.shape[2]
    mix_ref[...] = dot(a, wd_ref[...], NN).astype(BF).reshape(blocks, 1, rows, width)
    gh_ref[:, :width] = dot(gin, win_ref[...], NT).astype(BF)
    gh_ref[:, width:] = gg.astype(BF)

    @pl.when(step == 0)
    def _():
        acc_in[...] = jnp.zeros_like(acc_in)
        acc_d[...] = jnp.zeros_like(acc_d)

    acc_in[...] += dot(h, gin, TN)
    acc_d[...] += dot(a, g, TN)

    @pl.when(step == pl.num_programs(0) - 1)
    def _():
        dwin_ref[...] = acc_in[...].astype(BF)
        dwd_ref[...] = acc_d[...]


def moe(h_all, g_all, w_in, wd, per_dev, nz, ne, rows_dev, blocks):
    count, width = g_all.shape
    wide = h_all.shape[1]
    hid4 = w_in.shape[1]
    hid2 = wd.shape[0]
    fl = hid2 // per_dev
    tile = blocks * rows_dev
    turns = ne // blocks
    rows = lambda n: pl.BlockSpec((tile, n), lambda i: (i, 0))
    whole = lambda s: pl.BlockSpec(s, lambda i: (0, 0), pipeline_mode=pl.Buffered(1))
    return pl.pallas_call(
        functools.partial(moe_kernel, fl),
        grid=(count // tile,),
        in_specs=[
            rows(wide), rows(width),
            whole(w_in.shape), whole(wd.shape),
        ],
        out_specs=[
            pl.BlockSpec((blocks, 1, rows_dev, width), lambda i: (i % turns, i // turns, 0, 0)),
            rows(wide),
            whole((width, hid4)), whole((hid2, width)),
        ],
        out_shape=[
            jax.ShapeDtypeStruct((ne, nz, rows_dev, width), BF),
            jax.ShapeDtypeStruct((count, wide), BF),
            jax.ShapeDtypeStruct((width, hid4), BF),
            jax.ShapeDtypeStruct((hid2, width), F32),
        ],
        scratch_shapes=[pltpu.VMEM((width, hid4), F32), pltpu.VMEM((hid2, width), F32)],
        compiler_params=pltpu.CompilerParams(vmem_limit_bytes=66_000_000),
        cost_estimate=pl.CostEstimate(
            flops=2 * count * width * hid2 * 9,
            bytes_accessed=8 * count * width + 24 * hid4 * width,
            transcendentals=count * hid2,
        ),
        name="moe",
    )(h_all, g_all, w_in, wd)


def moe_net_kernel(
    nz, ne, per_dev, slots, h_ref, g_ref, wg_ref, wu_ref, wd_ref,
    hall_ref, mix_ref, gh_ref, dwin_ref, dwd_ref,
    win, wd, acc_in, acc_d, htile, gtile, mixbuf, qbuf, cgot, acc, got, zgot, dbuf,
    wload, tload, mixsem, keep, flush, zsend, zrecv, send, recv,
    csend, crecv, credit, rsend, rrecv, ysend, yrecv,
):
    z, e = lax.axis_index("dp"), lax.axis_index("expert")
    rows, width = g_ref.shape[1], g_ref.shape[2]
    half = rows // 2
    fl = wd.shape[0] // per_dev
    upper = [2 << b for b in range(ne.bit_length() - 2)]
    stages = len(upper)
    pairs = ne // 2
    steps = nz * pairs
    gather_orders = [upper + [1], upper[::-1] + [1]]
    sum_orders = [[1] + upper, [1] + upper[::-1]]
    at = [e]
    for bit in [1] + upper:
        at = at + [flip(i, bit) for i in at]
    partner = (z, at[1])

    def plane(r):
        low = jnp.minimum(z, nz - 1 - z)
        near = jnp.where(lax.rem(r, 2) == 1, z - (r + 1) // 2, z + r // 2)
        far = jnp.where(2 * z < nz, z + (r - low), z - (r - low))
        return jnp.where(r <= 2 * low, near, far)

    planes = [z] + [nearest(z, r, nz) for r in range(1, nz)]

    def part(s):
        return pl.ds(s * half, half)

    def subset_mask(order, subset):
        return sum(bit for b, bit in enumerate(order) if subset >> b & 1)

    def pass_on(r, s, stage, subset, own=False):
        order = gather_orders[s]
        dst = hall_ref.at[plane(r) * ne + at[subset_mask(order, subset)], part(s)]
        n = (1 << stage) - 1 + subset
        src = h_ref.at[part(s)] if own else dst
        return remote(src, dst, send.at[r, s, n], recv.at[r, s, n], (z, at[order[stage]]))

    def take(r, s, stage, subset):
        order = gather_orders[s]
        mask = subset_mask(order, subset) | order[stage]
        n = (1 << stage) - 1 + subset
        here = hall_ref.at[plane(r) * ne + at[mask], part(s)]
        remote(here, here, send.at[r, s, n], recv.at[r, s, n], partner).wait_recv()
        for later in range(stage + 1, stages + 1):
            pass_on(r, s, later, subset + (1 << stage)).start()

    def start_round(r):
        if r > 0:
            here = hall_ref.at[planes[r] * ne + e]
            remote(here, here, zsend.at[r], zrecv.at[planes[r]], partner).wait_recv()
        for stage in range(stages + 1):
            for s in range(2):
                pass_on(r, s, stage, 0, own=r == 0).start()

    def take_pair(r, i):
        if i == 1:
            for stage in range(stages):
                for s in range(2):
                    take(r, s, stage, 0)
        mask = 2 * i
        for s in range(2):
            order = gather_orders[s]
            places = [b for b in range(stages) if order[b] & mask]
            if len(places) > 1:
                take(r, s, places[-1], sum(1 << b for b in places[:-1]))
        for s in range(2):
            order = gather_orders[s]
            take(r, s, stages, sum(1 << b for b in range(stages) if order[b] & mask))

    def blocks_of(k):
        r, i = k // pairs, lax.rem(k, pairs)
        home = plane(r)
        lane = e
        for b, bit in enumerate(upper):
            lane = lane + lax.rem(i // (1 << b), 2) * (at[bit] - e)
        return home, lane, lane + (at[1] - e)

    def loads(k):
        home, one, two = blocks_of(k)
        p = lax.rem(k, 2)
        out = []
        for j, lane in enumerate((one, two)):
            to = pl.ds(j * rows, rows)
            block = home * ne + lane
            out.append(pltpu.make_async_copy(hall_ref.at[block], htile.at[p, to], tload.at[p, 2 * j]))
            out.append(
                pltpu.make_async_copy(g_ref.at[block], gtile.at[p, to], tload.at[p, 2 * j + 1])
            )
        return out

    def mix_out(k):
        home, one, two = blocks_of(k)
        p = lax.rem(k, 2)
        return [
            pltpu.make_async_copy(
                mixbuf.at[p, pl.ds(j * rows, rows)], mix_ref.at[lane, home], mixsem.at[p, j]
            )
            for j, lane in enumerate((one, two))
        ]

    def to_partner(k):
        return remote(
            qbuf.at[lax.rem(k, 2)], cgot.at[lax.rem(k, slots)],
            csend.at[lax.rem(k, 2)], crecv.at[lax.rem(k, slots)], partner,
        )

    def place_of(t, keep_index):
        return (1 << stages) - (1 << (stages - t + 1)) + keep_index

    def push(r, s, t, keep_index):
        order = sum_orders[s]
        mask = order[t] | subset_mask(order[t + 1 :], keep_index)
        n = place_of(t, keep_index)
        return remote(
            acc.at[r, mask // 2, part(s)], got.at[r, s, n],
            rsend.at[r, s, n], rrecv.at[r, s, n], (z, at[order[t]]),
        )

    def merge(k):
        slot = lax.rem(k, slots)
        remote(cgot.at[slot], cgot.at[slot], csend.at[0], crecv.at[slot], partner).wait_recv()
        r, i = k // pairs, lax.rem(k, pairs)
        add_rows(acc.at[r, i], cgot.at[slot])

        @pl.when(k + slots < steps)
        def _():
            pl.semaphore_signal(credit, inc=1, device_id=partner, device_id_type=MESH)

        for j in range(1, pairs):

            @pl.when(i == j)
            def _():
                for s in range(2):
                    order = sum_orders[s]
                    if order[1] & (2 * j):
                        rest = [b for b, bit in enumerate(order[2:]) if bit & (2 * j)]
                        push(r, s, 1, sum(1 << b for b in rest)).start()

    def home_copy(r, s):
        return remote(
            acc.at[r, 0, part(s)], zgot.at[z, part(s)], ysend.at[r, s], yrecv.at[z, s],
            (plane(r), e),
        )

    def settle(r, t):
        for s in range(2):
            order = sum_orders[s]
            for index in range(1 << (stages - t)):
                copy = push(r, s, t, index)
                copy.wait_recv()
                mask = subset_mask(order[t + 1 :], index)
                add_rows(acc.at[r, mask // 2, part(s)], got.at[r, s, place_of(t, index)])
            if t < stages:
                for index in range(1 << (stages - t - 1)):
                    push(r, s, t + 1, index).start()
            else:

                @pl.when(r > 0)
                def _():
                    home_copy(r, s).start()

    weights = []
    for i in range(per_dev):
        cols = pl.ds(z * fl, fl)
        weights += [
            (wg_ref.at[i, :, cols], win.at[:, pl.ds(i * fl, fl)]),
            (wu_ref.at[i, :, cols], win.at[:, pl.ds((per_dev + i) * fl, fl)]),
            (wd_ref.at[i, cols, :], wd.at[pl.ds(i * fl, fl), :]),
        ]
    weights = [
        pltpu.make_async_copy(src, dst, wload.at[j]) for j, (src, dst) in enumerate(weights)
    ]
    for copy in weights:
        copy.start()
    meet_column_and_plane(nz, ne, z, e, True)
    own = pltpu.make_async_copy(h_ref, hall_ref.at[z * ne + e], keep)
    own.start()
    for r in range(1, nz):
        remote(
            h_ref, hall_ref.at[z * ne + e], zsend.at[r], zrecv.at[z], (planes[r], e)
        ).start()
    start_round(0)
    acc_in[...] = jnp.zeros_like(acc_in)
    acc_d[...] = jnp.zeros_like(acc_d)
    take_pair(0, 0)
    own.wait()
    for copy in loads(0):
        copy.start()
    for copy in weights:
        copy.wait()

    tile = 2 * rows
    lanes = lax.broadcasted_iota(jnp.int32, (tile, 128), 1)
    split = 64

    def step(k, carry):
        p = lax.rem(k, 2)
        r, i = k // pairs, lax.rem(k, pairs)
        for copy in loads(k):
            copy.wait()
        pre = dot(htile[p, :, :width], win[...], NN)
        graw = dot(gtile[p], wd[...], NT)
        extra = htile[p, :, width:].astype(F32)
        scaled_act, grad_gate, grad_up = [], [], []
        gg = jnp.zeros((tile, 128), F32)
        for j in range(per_dev):
            u = pre[:, j * fl : (j + 1) * fl]
            w = pre[:, (per_dev + j) * fl : (per_dev + 1 + j) * fl]
            gr = graw[:, j * fl : (j + 1) * fl]
            mine = e * per_dev + j
            picked = (lanes == mine) | (lanes == mine + split)
            gate = jnp.sum(jnp.where(picked, extra, 0.0), axis=-1, keepdims=True)
            sig = 1.0 / (1.0 + jnp.exp(-u))
            silu = u * sig
            act = silu * w
            total = jnp.sum(act.astype(BF).astype(F32) * gr, axis=-1, keepdims=True)
            rounded = total.astype(BF).astype(F32)
            gg = jnp.where(lanes == mine, rounded, gg)
            gg = jnp.where(lanes == mine + split, total - rounded, gg)
            scaled_act.append((gate * act).astype(BF))
            gact = gate * gr
            grad_gate.append((gact * w * (sig * (1.0 + u * (1.0 - sig)))).astype(BF))
            grad_up.append((gact * silu).astype(BF))
        a = jnp.concatenate(scaled_act, axis=1)
        gin = jnp.concatenate(grad_gate + grad_up, axis=1)

        for r1 in range(1, nz):

            @pl.when(k == (r1 - 1) * (pairs - 1) + 1)
            def _():
                start_round(r1)

        @pl.when(k + 1 < steps)
        def _():
            ahead = k + 1
            for j in range(pairs):

                @pl.when(lax.rem(ahead, pairs) == j)
                def _():
                    take_pair(ahead // pairs, j)

            for copy in loads(ahead):
                copy.start()

        @pl.when(k >= 2)
        def _():
            for copy in mix_out(k - 2):
                copy.wait()
            to_partner(k - 2).wait_send()

        mixbuf[p] = dot(a, wd[...], NN).astype(BF)
        for copy in mix_out(k):
            copy.start()
        back = dot(gin, win[...], NT).astype(BF)
        gg = gg.astype(BF)
        acc[r, i, :, :width] = back[:rows]
        acc[r, i, :, width:] = gg[:rows]
        qbuf[p, :, :width] = back[rows:]
        qbuf[p, :, width:] = gg[rows:]
        acc_in[...] += dot(htile[p, :, :width], gin, TN)
        acc_d[...] += dot(a, gtile[p], TN)

        @pl.when(k >= slots)
        def _():
            pl.semaphore_wait(credit, 1)

        to_partner(k).start()

        @pl.when(k >= 1)
        def _():
            merge(k - 1)

        for t in range(1, stages + 1):
            late = k - pairs - 2 * t

            @pl.when((late >= 0) & (lax.rem(late + pairs, pairs) == 0))
            def _():
                settle(late // pairs, t)

        return carry

    lax.fori_loop(0, steps, step, 0)
    merge(steps - 1)
    final = pltpu.make_async_copy(acc_d, dwd_ref, flush.at[0])
    final.start()
    left = sorted(
        (r * pairs + pairs + 2 * t, r, t)
        for r in range(nz)
        for t in range(1, stages + 1)
        if r * pairs + pairs + 2 * t >= steps
    )
    chunk = dbuf.shape[1]

    def flush_chunk(c):
        return pltpu.make_async_copy(
            dbuf.at[c % 2], dwin_ref.at[pl.ds(c * chunk, chunk)], flush.at[1 + c % 2]
        )

    chunks = acc_in.shape[0] // chunk
    for c in range(chunks):
        if c >= 2:
            flush_chunk(c - 2).wait()
        dbuf[c % 2] = acc_in[pl.ds(c * chunk, chunk), :].astype(BF)
        flush_chunk(c).start()
    for _, r, t in left:
        settle(jnp.int32(r), t)
    for s in range(2):
        for r in range(1, nz):
            here = zgot.at[planes[r], part(s)]
            remote(here, here, ysend.at[r, s], yrecv.at[planes[r], s], partner).wait_recv()

        def total_rows(n, carry):
            span = pl.ds(pl.multiple_of(s * half + n * 16, 16), 16)
            total = acc[0, 0, span, :].astype(F32)
            for r in range(1, nz):
                total = total + zgot[planes[r], span, :].astype(F32)
            gh_ref[span, :] = total
            return carry

        lax.fori_loop(0, half // 16, total_rows, 0)
    final.wait()
    for c in range(max(chunks - 2, 0), chunks):
        flush_chunk(c).wait()
    for k in range(max(steps - 2, 0), steps):
        for copy in mix_out(jnp.int32(k)):
            copy.wait()
        to_partner(jnp.int32(k)).wait_send()
    for r in range(nz):
        if r > 0:
            remote(
                h_ref, hall_ref.at[z * ne + e], zsend.at[r], zrecv.at[z], (planes[r], e)
            ).wait_send()
        for s in range(2):
            for stage in range(stages + 1):
                for subset in range(1 << stage):
                    pass_on(r, s, stage, subset, own=r == 0 and subset == 0).wait_send()
            for t in range(1, stages + 1):
                for index in range(1 << (stages - t)):
                    push(r, s, t, index).wait_send()
            if r > 0:
                home_copy(jnp.int32(r), s).wait_send()


def moe_net_scratch(nz, ne, per_dev, rows, width, wide, fl):
    pairs = ne // 2
    slots = 4
    stages = ne.bit_length() - 2
    vmem = [
        ((width, 2 * per_dev * fl), BF),
        ((per_dev * fl, width), BF),
        ((width, 2 * per_dev * fl), F32),
        ((per_dev * fl, width), F32),
        ((2, 2 * rows, wide), BF),
        ((2, 2 * rows, width), BF),
        ((2, 2 * rows, width), BF),
        ((2, rows, wide), BF),
        ((slots, rows, wide), BF),
        ((nz, pairs, rows, wide), BF),
        ((nz, 2, max(pairs - 1, 1), rows // 2, wide), BF),
        ((nz, rows, wide), BF),
        ((2, width // 8, 2 * per_dev * fl), BF),
    ]
    size = sum(functools.reduce(lambda a, b: a * b, s) * (2 if d == BF else 4) for s, d in vmem)
    sems = [
        DMA((3 * per_dev,)), DMA((2, 4)), DMA((2, 2)), DMA, DMA((3,)),
        DMA((nz,)), DMA((nz,)), DMA((nz, 2, ne - 1)), DMA((nz, 2, ne - 1)),
        DMA((2,)), DMA((slots,)), pltpu.SemaphoreType.REGULAR,
        DMA((nz, 2, max(pairs - 1, 1))), DMA((nz, 2, max(pairs - 1, 1))),
        DMA((nz, 2)), DMA((nz, 2)),
    ]
    fits = size <= 54_000_000 and stages >= 1 and nz > 1 and nz * pairs > slots
    return fits, slots, [pltpu.VMEM(*v) for v in vmem] + sems


def moe_net(h, g_all, w_gate, w_up, w_down, nz, ne, fl, slots, scratch, cid):
    rows, wide = h.shape
    per_dev, width, _ = w_gate.shape
    return pl.pallas_call(
        functools.partial(moe_net_kernel, nz, ne, per_dev, slots),
        out_shape=[
            jax.ShapeDtypeStruct((nz * ne, rows, wide), BF),
            jax.ShapeDtypeStruct((ne, nz, rows, width), BF),
            jax.ShapeDtypeStruct((rows, wide), F32),
            jax.ShapeDtypeStruct((width, 2 * per_dev * fl), BF),
            jax.ShapeDtypeStruct((per_dev * fl, width), F32),
        ],
        in_specs=[VMEM, ANY, ANY, ANY, ANY],
        out_specs=[ANY, ANY, VMEM, ANY, ANY],
        scratch_shapes=scratch,
        compiler_params=pltpu.CompilerParams(
            collective_id=cid, has_side_effects=True, vmem_limit_bytes=66_500_000
        ),
        name="moe_net",
    )(h, g_all.reshape(nz * ne, rows, width), w_gate, w_up, w_down)


def body(inputs, segments, routes, w_qkv, w_out, w_router, gains, w_gate, w_up, w_down, cotangent):
    z = lax.axis_index("dp")
    e = lax.axis_index("expert")
    nz = lax.axis_size("dp")
    ne = lax.axis_size("expert")
    count, width = inputs.shape
    num_seqs, length = segments.shape
    heads = width // HD // ne
    hw = heads * HD
    expert_count = w_router.shape[1]
    per_dev = w_gate.shape[0]
    hidden = w_gate.shape[2]
    fl = hidden // nz
    both = ("dp", "expert")

    pad = -(expert_count + 4) % 16
    small = jnp.concatenate(
        [w_router.T, gains.T, jnp.zeros((pad, gains.shape[0]), BF)], axis=0
    )
    seg8 = jnp.broadcast_to(segments[:, None, :], (num_seqs, 8, length)).reshape(-1, length)
    in_all, wq, wo, small, seg_all, cot = start_gather(
        inputs, w_qkv.transpose(1, 0, 2), w_out, small, seg8, cotangent, nz, ne, hw, 0
    )
    small = small.transpose(1, 0, 2).reshape(-1, width)
    router_t = small[:expert_count]
    gain_mat = small[expert_count : expert_count + 4].astype(F32)
    my_gains = lax.dynamic_slice_in_dim(gain_mat, e * hw, hw, axis=1)
    seg_all = seg_all.reshape(ne * num_seqs, 8, length)

    g_all = lax.all_gather(cot, both, axis=0, tiled=True)
    inputs_f = inputs.astype(F32)
    scale_one = rms_scale(inputs_f)
    tables = rope_lanes(length)
    *saved, x1_part = attn_fwd(in_all, wq, wo, gain_mat, my_gains, seg_all, tables, 9)
    (x1_sum,) = scatter_tokens(x1_part, nz, ne, False, 1)
    x1 = inputs_f + x1_sum

    a2 = rms_scale(x1)
    h2 = (x1 * a2 * gain_mat[3]).astype(BF)
    probs = jax.nn.softmax(dot(h2, router_t, NT), axis=-1)
    picks = jnp.sum(
        (routes[:, :, None] == jnp.arange(expert_count, dtype=jnp.int32)).astype(F32), axis=1
    )
    gates = picks * probs

    split = 64
    high = gates.astype(BF)
    low = (gates - high.astype(F32)).astype(BF)
    blank = jnp.zeros((count, split - expert_count), BF)
    h2_wide = jnp.concatenate([h2, high, blank, low, blank], axis=1)
    wide = width + 2 * split
    fits, slots, scratch = moe_net_scratch(nz, ne, per_dev, count, width, wide, fl)
    if fits:
        _, mix, gh_sum, dwin, dwd = moe_net(
            h2_wide, g_all, w_gate, w_up, w_down, nz, ne, fl, slots, scratch, 2
        )
        mix = mix.reshape(-1, width)
    else:
        h2_all = gather_tokens(h2_wide, nz, ne, True, 2).reshape(-1, wide)
        wg = lax.dynamic_slice_in_dim(w_gate, z * fl, fl, axis=2)
        wu = lax.dynamic_slice_in_dim(w_up, z * fl, fl, axis=2)
        wd = lax.dynamic_slice_in_dim(w_down, z * fl, fl, axis=1).reshape(per_dev * fl, width)
        w_in = jnp.concatenate([*wg, *wu], axis=1)
        mix, gh, dwin, dwd = moe(
            h2_all, g_all, w_in, wd, per_dev, nz, ne, count, min(4, ne)
        )
        gh_sum, mix = scatter_tokens(
            gh.reshape(nz * ne, count, wide), nz, ne, True, 3, after=mix.reshape(-1, width)
        )
    grad_from_experts = gh_sum[:, :width]
    grad_gates = (
        gh_sum[:, width : width + expert_count]
        + gh_sum[:, width + split : width + split + expert_count]
    )

    mix = lax.psum_scatter(mix, "expert", scatter_dimension=0, tiled=True)
    mix = lax.psum_scatter(mix, "dp", scatter_dimension=0, tiled=True)
    output = (x1 + mix.astype(F32)).astype(BF)

    dwin = lax.all_to_all(
        dwin.reshape(nz, width // nz, 2 * per_dev * fl),
        "dp", split_axis=0, concat_axis=0, tiled=True,
    )
    grad_w_gate, grad_w_up = lay_experts(dwin, per_dev, fl)
    grad_w_down = dwd.reshape(per_dev, fl, width)

    grad_top = cotangent.astype(F32)
    grad_probs = picks * grad_gates
    glog = (probs * (grad_probs - jnp.sum(probs * grad_probs, axis=-1, keepdims=True))).astype(BF)
    local_router = dot(glog, h2, TN)
    gh2 = grad_from_experts + dot(glog, router_t, NN)
    grad_ffn, gain_ffn = rms_backward(x1, a2, gain_mat[3], gh2)
    gx1 = grad_top + grad_ffn
    gab = gx1.astype(BF)

    gab_all = gather_tokens(gab, nz, ne, False, 4)
    gh1_part, parts, gain_qk = attn_bwd(gab_all, wq, wo, my_gains, seg_all, tables, saved, 10)
    mine = lax.psum_scatter(parts, "dp", scatter_dimension=0, tiled=True)
    (gh1,) = scatter_tokens(gh1_part, nz, ne, False, 5)
    grad_front, gain_attn = rms_backward(inputs_f, scale_one, gain_mat[0], gh1)
    grad_inputs = (gx1 + grad_front).astype(BF)

    wide = gather_tokens(mine, nz, ne, False, 6)
    grad_w_qkv, grad_w_out = lay_mixer(wide, 4, hw)
    grad_w_qkv = grad_w_qkv.transpose(1, 0, 2)

    place = lambda part: lax.dynamic_update_slice_in_dim(
        jnp.zeros((1, width), F32), part[None], e * hw, axis=1
    )
    tiny = jnp.concatenate(
        [
            local_router, gain_attn[None], place(gain_qk[0]), place(gain_qk[1]), gain_ffn[None],
            jnp.zeros((-(expert_count + 4) % 8, width), F32),
        ],
        axis=0,
    )
    tiny = reduce_columns(tiny, nz, ne, 7)
    grad_w_router = tiny[:expert_count].T
    grad_gains = tiny[expert_count : expert_count + 4].T
    return (
        output,
        grad_inputs,
        grad_w_qkv,
        grad_w_out,
        grad_w_router,
        grad_gains,
        grad_w_gate,
        grad_w_up,
        grad_w_down,
    )


def solution(mesh):
    tokens = P(("dp", "expert"), None)
    rows = P("dp", None)
    rows3 = P("dp", None, None)
    owned = P("expert", None, None)
    return jax.shard_map(
        body,
        mesh=mesh,
        in_specs=(tokens, tokens, tokens, rows3, rows, rows, rows, owned, owned, owned, tokens),
        out_specs=(tokens, tokens, rows3, rows, rows, rows)
        + (P("expert", "dp", None),) * 3,
        check_vma=False,
    )
```

```python
import functools

import jax
import jax.numpy as jnp
from jax import lax
from jax.experimental import pallas as pl
from jax.experimental.pallas import tpu as pltpu
from jax.sharding import PartitionSpec as P


HD = 128
EPS = 1e-05
ROPE_BASE = 10000.0
MASKED = -1e30
BF = jnp.bfloat16
F32 = jnp.float32


def dot(a, b, dims):
    return lax.dot_general(a, b, (dims, ((), ())), preferred_element_type=F32)


NN = ((1,), (0,))
NT = ((1,), (1,))
TN = ((0,), (0,))


def rms_scale(values):
    return lax.rsqrt(jnp.mean(values * values, axis=-1, keepdims=True) + EPS)


def rms_backward(values, inv_rms, gain_col, grad_out):
    normed = values * inv_rms
    grad_gain = jnp.sum(grad_out * normed, axis=0)
    scaled = grad_out * gain_col
    grad_values = inv_rms * (scaled - normed * jnp.mean(scaled * normed, axis=-1, keepdims=True))
    return (grad_values, grad_gain)


MESH = pl.DeviceIdType.MESH
ANY = pl.BlockSpec(memory_space=pl.ANY)
VMEM = pl.BlockSpec(memory_space=pltpu.VMEM)
DMA = pltpu.SemaphoreType.DMA


def flip(index, bit):
    return index + bit * (1 - 2 * ((index // bit) % 2))


def flips(index, bits):
    out = [index]
    for bit in bits:
        out = out + [flip(i, bit) for i in out]
    return out


def bit_orders(ne):
    bits = [1 << b for b in range(ne.bit_length() - 1)]
    return [bits[:1] + bits[1:], bits[:1] + bits[1:][::-1]]


def nearest(z, r, nz):
    low = jnp.minimum(z, nz - 1 - z)
    near = z - (r + 1) // 2 if r % 2 else z + r // 2
    far = jnp.where(2 * z < nz, z + (r - low), z - (r - low))
    return jnp.where(r <= 2 * low, near, far)


def remote(src, dst, send, recv, peer):
    return pltpu.make_async_remote_copy(
        src_ref=src, dst_ref=dst, send_sem=send, recv_sem=recv, device_id=peer, device_id_type=MESH
    )


def for_others(nz, ne, z, e, act):
    def step(i, carry):
        flat = lax.rem(z * ne + e + i, nz * ne)
        act(flat // ne, lax.rem(flat, ne), flat)
        return carry

    lax.fori_loop(1, nz * ne, step, 0)


def meet_all(nz, ne, z, e):
    sem = pltpu.get_barrier_semaphore()

    def greet(zz, ee, flat):
        pl.semaphore_signal(sem, inc=1, device_id=(zz, ee), device_id_type=MESH)

    for_others(nz, ne, z, e, greet)
    pl.semaphore_wait(sem, nz * ne - 1)


def meet_column_and_plane(nz, ne, z, e, spread):
    sem = pltpu.get_barrier_semaphore()
    peers = [(z, flip(e, 1 << b)) for b in range(ne.bit_length() - 1)]
    if spread:
        peers += [(lax.rem(z + r, nz), e) for r in range(1, nz)]
    for peer in peers:
        pl.semaphore_signal(sem, inc=1, device_id=peer, device_id_type=MESH)
    pl.semaphore_wait(sem, len(peers))


class PlaneGather:
    def __init__(self, nz, ne, z, e, spread, x_ref, out_ref, zsend, zrecv, send, recv, local):
        self.nz, self.ne, self.z, self.e, self.spread = nz, ne, z, e, spread
        self.x, self.out = x_ref, out_ref
        self.zsend, self.zrecv, self.send, self.recv = zsend, zrecv, send, recv
        self.rounds = nz if spread else 1
        self.half = x_ref.shape[0] // 2
        self.orders = [o[1:] + o[:1] for o in bit_orders(ne)]
        self.planes = [z if spread else 0] + [nearest(z, r, nz) for r in range(1, self.rounds)]
        self.pending, self.arrivals = [], {}
        own = self.slot(0, e)
        keep = pltpu.make_async_copy(x_ref, out_ref.at[own], local)
        keep.start()
        self.pending.append(keep.wait)

    @staticmethod
    def scratch(nz, ne, spread):
        rounds = nz if spread else 1
        return [DMA((nz,)), DMA((nz,)), DMA((rounds, 2, ne - 1)), DMA((rounds, 2, ne - 1)), DMA]

    def slot(self, r, ee):
        return self.planes[r] * self.ne + ee

    def spread_own(self):
        for r in range(1, self.rounds):
            to = self.planes[r]
            copy = remote(
                self.x, self.out.at[self.slot(0, self.e)],
                self.zsend.at[r], self.zrecv.at[self.z], (to, self.e),
            )
            copy.start()
            self.pending.append(copy.wait_send)

    def forward(self, r, s, stage, subset):
        order = self.orders[s]
        rows = pl.ds(s * self.half, self.half)
        peer_e = flip(self.e, order[stage])
        n = (1 << stage) - 1 + subset
        block = self.slot(r, flips(self.e, order[:stage])[subset])
        dst = self.out.at[block, rows]
        src = self.x.at[rows] if r == 0 and subset == 0 else dst
        sems = self.send.at[r, s, n], self.recv.at[r, s, n]
        copy = remote(src, dst, *sems, (self.z, peer_e))
        copy.start()
        self.pending.append(copy.wait_send)
        got = self.out.at[self.slot(r, flips(peer_e, order[:stage])[subset]), rows]
        self.arrivals[(r, s, stage, subset)] = remote(got, got, *sems, (self.z, peer_e)).wait_recv

    def start_round(self, r):
        if r > 0:
            here = self.out.at[self.slot(r, self.e)]
            remote(
                here, here, self.zsend.at[r], self.zrecv.at[self.planes[r]], (self.planes[r], self.e)
            ).wait_recv()
        for stage in range(len(self.orders[0])):
            for s in range(2):
                self.forward(r, s, stage, 0)

    def finish_round(self, r):
        stages = len(self.orders[0])
        for stage in range(stages):
            for subset in range(1 << stage):
                for s in range(2):
                    self.arrivals.pop((r, s, stage, subset))()
                    for later in range(stage + 1, stages):
                        self.forward(r, s, later, subset + (1 << stage))

    def finish(self):
        for wait in self.pending:
            wait()


def gather_kernel(nz, ne, spread, x_ref, out_ref, *sems):
    z, e = lax.axis_index("dp"), lax.axis_index("expert")
    meet_column_and_plane(nz, ne, z, e, spread)
    net = PlaneGather(nz, ne, z, e, spread, x_ref, out_ref, *sems)
    net.spread_own()
    net.start_round(0)
    for r in range(1, net.rounds):
        net.start_round(r)
        net.finish_round(r - 1)
    net.finish_round(net.rounds - 1)
    net.finish()


def gather_tokens(x, nz, ne, spread, cid):
    rounds = nz if spread else 1
    return pl.pallas_call(
        functools.partial(gather_kernel, nz, ne, spread),
        out_shape=jax.ShapeDtypeStruct((rounds * ne, *x.shape), x.dtype),
        in_specs=[VMEM],
        out_specs=ANY,
        scratch_shapes=PlaneGather.scratch(nz, ne, spread),
        compiler_params=pltpu.CompilerParams(collective_id=cid, has_side_effects=True),
        name="gather_tokens",
    )(x)


def add_rows(dst, src, tile=16):
    def step(i, carry):
        rows = pl.ds(pl.multiple_of(i * tile, tile), tile)
        dst[rows, :] = (dst[rows, :].astype(F32) + src[rows, :].astype(F32)).astype(dst.dtype)
        return carry

    lax.fori_loop(0, dst.shape[0] // tile, step, 0)


def scatter_kernel(nz, ne, spread, x_ref, *refs):
    out_ref, acc, got, zgot, loads, send, recv, zsend, zrecv = refs[-9:]
    z, e = lax.axis_index("dp"), lax.axis_index("expert")
    meet_column_and_plane(nz, ne, z, e, spread)
    rounds = nz if spread else 1
    stages = ne.bit_length() - 1
    half = out_ref.shape[0] // 2
    orders = bit_orders(ne)
    pending, arrivals, zwait = [], {}, {}
    ranks = list(range(1, rounds)) + [0]
    first = [0] * (stages + 1)
    for j in range(stages):
        first[j + 1] = first[j] + (ne >> (j + 1))

    def plane_of(r):
        return lax.rem(z + r, nz) * ne if spread else 0

    def push(r, s, j):
        order = orders[s]
        peer = (z, flip(e, order[j]))
        rest = ne >> (j + 1)
        for i in range(rest):
            n = first[j] + i
            if j == 0:
                block = flips(peer[1], order[:0:-1])[i]
                src = x_ref.at[plane_of(r) + block, pl.ds(s * half, half)]
            else:
                src = acc.at[r, s, rest + i]
            copy = remote(src, got.at[r, s, n], send.at[r, s, n], recv.at[r, s, n], peer)
            copy.start()
            pending.append(copy.wait_send)
            arrivals.setdefault((r, s, j), []).append((copy.wait_recv, i, n))

    for r in ranks:
        for s in range(2):
            push(r, s, 0)
            for i, block in enumerate(flips(e, orders[s][:0:-1])):
                copy = pltpu.make_async_copy(
                    x_ref.at[plane_of(r) + block, pl.ds(s * half, half)],
                    acc.at[r, s, i],
                    loads.at[r, s, i],
                )
                copy.start()
                arrivals.setdefault((r, s, -1), []).append(copy.wait)
    for t in range(rounds + stages):
        for place, r in enumerate(ranks):
            j = t - place
            if not 0 <= j < stages:
                continue
            for s in range(2):
                if j == 0:
                    for wait in arrivals.pop((r, s, -1)):
                        wait()
                for wait, i, n in arrivals.pop((r, s, j)):
                    wait()
                    add_rows(acc.at[r, s, i], got.at[r, s, n])
                if j + 1 < stages:
                    push(r, s, j + 1)
                elif r > 0:
                    copy = remote(
                        acc.at[r, s, 0], zgot.at[r, s], zsend.at[r, s], zrecv.at[r, s],
                        (lax.rem(z + r, nz), e),
                    )
                    copy.start()
                    pending.append(copy.wait_send)
                    zwait[(r, s)] = copy.wait_recv
    for s in range(2):
        for r in range(1, rounds):
            zwait[(r, s)]()

        def step(i, carry):
            rows = pl.ds(pl.multiple_of(i * 16, 16), 16)
            total = acc[0, s, 0, rows, :].astype(F32)
            for r in range(1, rounds):
                total = total + zgot[r, s, rows, :].astype(F32)
            out_ref[pl.ds(pl.multiple_of(s * half + i * 16, 16), 16), :] = total.astype(out_ref.dtype)
            return carry

        lax.fori_loop(0, half // 16, step, 0)
    for wait in pending:
        wait()


def scatter_tokens(parts, nz, ne, spread, cid, after=None):
    rounds = nz if spread else 1
    _, count, width = parts.shape
    half = count // 2
    held = (2 * rounds * (ne // 2 + ne - 1) + 2 * nz) * half * width * 2
    if held > 56_000_000:
        cut = width // 256 * 128
        left = scatter_tokens(parts[..., :cut], nz, ne, spread, cid, after)
        right = scatter_tokens(parts[..., cut:], nz, ne, spread, cid + 16)
        return [jnp.concatenate([left[0], right[0]], axis=1), *left[1:]]
    more = [] if after is None else [after]
    return pl.pallas_call(
        functools.partial(scatter_kernel, nz, ne, spread),
        out_shape=[jax.ShapeDtypeStruct(m.shape, m.dtype) for m in more]
        + [jax.ShapeDtypeStruct((count, width), F32)],
        in_specs=[ANY] * (1 + len(more)),
        out_specs=[ANY] * len(more) + [VMEM],
        scratch_shapes=[
            pltpu.VMEM((rounds, 2, ne // 2, half, width), BF),
            pltpu.VMEM((rounds, 2, ne - 1, half, width), BF),
            pltpu.VMEM((nz, 2, half, width), BF),
            DMA((rounds, 2, ne // 2)),
            DMA((rounds, 2, ne - 1)),
            DMA((rounds, 2, ne - 1)),
            DMA((nz, 2)),
            DMA((nz, 2)),
        ],
        input_output_aliases={1: 0} if more else {},
        compiler_params=pltpu.CompilerParams(
            collective_id=cid, has_side_effects=True, vmem_limit_bytes=64_000_000
        ),
        name="scatter_tokens",
    )(parts, *more)[::-1]


def start_kernel(
    nz, ne, x_ref, wqkv_ref, wout_ref, small_ref, seg_ref, _,
    out_ref, wq_ref, wo_ref, small_out, seg_out, _2,
    wbuf, pbuf, zsend, zrecv, send, recv, local,
    up_send, up_recv, dn_send, dn_recv, wload, wkeep, pload, psend, precv, pkeep,
    small_send, small_recv, seg_send, seg_recv,
):
    z, e = lax.axis_index("dp"), lax.axis_index("expert")
    kinds, depth, hw = wbuf.shape
    per = ne // nz
    loads = [
        pltpu.make_async_copy(wqkv_ref.at[j, :, pl.ds(e * hw, hw)], wbuf.at[j], wload.at[j])
        for j in range(kinds)
    ]
    for copy in loads:
        copy.start()
    pieces = [
        pltpu.make_async_copy(
            wout_ref.at[pl.ds(i * hw, hw), pl.ds(e * hw, hw)], pbuf.at[i], pload.at[i]
        )
        for i in range(per)
    ]
    for copy in pieces:
        copy.start()
    meet_all(nz, ne, z, e)

    def rows_of(zz):
        return pl.ds(pl.multiple_of(zz * depth, depth), depth)

    def hop(j, zz, dist, up):
        send, recv = (up_send, up_recv) if up else (dn_send, dn_recv)
        here = wq_ref.at[j, rows_of(zz)]
        src = wbuf.at[j] if dist == 1 else here
        to = z + 1 if up else z - 1
        return remote(src, here, send.at[dist, j], recv.at[dist, j], (to, e))

    keeps = []
    for j in range(kinds):
        loads[j].wait()

        @pl.when(z + 1 < nz)
        def _():
            hop(j, z, 1, True).start()

        @pl.when(z > 0)
        def _():
            hop(j, z, 1, False).start()

        keep = pltpu.make_async_copy(wbuf.at[j], wq_ref.at[j, rows_of(z)], wkeep.at[j])
        keep.start()
        keeps.append(keep)

    def wait_all(ref, send, recv, count):
        most = ref.at[pl.ds(0, count)]
        both = remote(most, most, send, recv, (z, flip(e, 1)))
        both.wait_send()
        both.wait_recv()

    small_out[z] = small_ref[...]
    for r in range(1, nz):
        remote(
            small_ref, small_out.at[z], small_send, small_recv, (lax.rem(z + r, nz), e)
        ).start()
    seg_out[e] = seg_ref[...]
    for r in range(1, ne):
        remote(seg_ref, seg_out.at[e], seg_send, seg_recv, (z, lax.rem(e + r, ne))).start()
    net = PlaneGather(nz, ne, z, e, False, x_ref, out_ref, zsend, zrecv, send, recv, local)
    net.start_round(0)

    columns = pl.ds(e * hw, hw)
    for i in range(per):
        pieces[i].wait()
    for r in range(nz):
        for i in range(per):
            to = (lax.rem(z + r, nz), z * per + i)
            give = remote(pbuf.at[i], wo_ref.at[:, columns], psend.at[r, i], precv, to)
            if r > 0:
                give.start()
            else:
                own = pltpu.make_async_copy(pbuf.at[i], wo_ref.at[:, columns], pkeep)

                @pl.when(to[1] == e)
                def _():
                    own.start()

                @pl.when(to[1] != e)
                def _():
                    give.start()
    net.finish_round(0)
    for dist in range(1, nz):
        for j in range(kinds):

            @pl.when(z - dist >= 0)
            def _():
                got = wq_ref.at[j, rows_of(z - dist)]
                remote(got, got, up_send.at[dist, j], up_recv.at[dist, j], (z, e)).wait_recv()

                @pl.when(z + 1 < nz)
                def _():
                    if dist + 1 < nz:
                        hop(j, z - dist, dist + 1, True).start()

            @pl.when(z + dist < nz)
            def _():
                got = wq_ref.at[j, rows_of(z + dist)]
                remote(got, got, dn_send.at[dist, j], dn_recv.at[dist, j], (z, e)).wait_recv()

                @pl.when(z > 0)
                def _():
                    if dist + 1 < nz:
                        hop(j, z + dist, dist + 1, False).start()

    net.finish()
    for keep in keeps:
        keep.wait()
    for dist in range(1, nz):
        for j in range(kinds):

            @pl.when((z - dist + 1 >= 0) & (z + 1 < nz))
            def _():
                hop(j, z - dist + 1, dist, True).wait_send()

            @pl.when((z + dist - 1 < nz) & (z > 0))
            def _():
                hop(j, z + dist - 1, dist, False).wait_send()

    for r in range(nz):
        for i in range(per):
            to = (lax.rem(z + r, nz), z * per + i)
            give = remote(pbuf.at[i], wo_ref.at[:, columns], psend.at[r, i], precv, to)
            if r > 0:
                give.wait_send()
            else:
                own = pltpu.make_async_copy(pbuf.at[i], wo_ref.at[:, columns], pkeep)

                @pl.when(to[1] == e)
                def _():
                    own.wait()

                @pl.when(to[1] != e)
                def _():
                    give.wait_send()

    def wait_pieces(count):
        most = wo_ref.at[:, pl.ds(0, count * hw)]
        remote(most, most, psend.at[0, 0], precv, (z, e)).wait_recv()

    @pl.when(z == e // per)
    def _():
        wait_pieces(ne - 1)

    @pl.when(z != e // per)
    def _():
        wait_pieces(ne)

    wait_all(small_out, small_send, small_recv, nz - 1)
    wait_all(seg_out, seg_send, seg_recv, ne - 1)


def start_gather(x, w_qkv, w_out, small, seg, after, nz, ne, hw, cid):
    kinds, depth, width = w_qkv.shape
    per = ne // nz
    return pl.pallas_call(
        functools.partial(start_kernel, nz, ne),
        out_shape=[
            jax.ShapeDtypeStruct((ne, *x.shape), x.dtype),
            jax.ShapeDtypeStruct((kinds, nz * depth, hw), BF),
            jax.ShapeDtypeStruct((hw, width), BF),
            jax.ShapeDtypeStruct((nz, *small.shape), small.dtype),
            jax.ShapeDtypeStruct((ne, *seg.shape), seg.dtype),
            jax.ShapeDtypeStruct(after.shape, after.dtype),
        ],
        in_specs=[VMEM, ANY, ANY, VMEM, VMEM, ANY],
        out_specs=[ANY, ANY, ANY, VMEM, VMEM, ANY],
        input_output_aliases={5: 5},
        scratch_shapes=[
            pltpu.VMEM((kinds, depth, hw), BF),
            pltpu.VMEM((per, hw, hw), BF),
            *PlaneGather.scratch(nz, ne, False),
            DMA((nz, kinds)), DMA((nz, kinds)), DMA((nz, kinds)), DMA((nz, kinds)),
            DMA((kinds,)), DMA((kinds,)), DMA((per,)), DMA((nz, per)), DMA, DMA,
            DMA, DMA, DMA, DMA,
        ],
        compiler_params=pltpu.CompilerParams(collective_id=cid, has_side_effects=True),
        name="start_gather",
    )(x, w_qkv, w_out, small, seg, after)


def rope_lanes(length):
    half = HD // 2
    freqs = jnp.exp(-jnp.log(ROPE_BASE) * (2.0 * jnp.arange(half, dtype=F32) / HD))
    angles = jnp.arange(length, dtype=F32)[:, None] * freqs[None, :]
    cos, sin = jnp.cos(angles), jnp.sin(angles)
    return jnp.concatenate([cos, cos], axis=1), jnp.concatenate([-sin, sin], axis=1)


def turn(x, cos, sin):
    return x * cos + pltpu.roll(x, HD // 2, 1) * sin


def meet_plane(ne, z, e):
    sem = pltpu.get_barrier_semaphore()
    for r in range(1, ne):
        pl.semaphore_signal(
            sem, inc=1, device_id=(z, lax.rem(e + r, ne)), device_id_type=MESH
        )
    pl.semaphore_wait(sem, ne - 1)


def plane_totals(ne, z, e, mine, theirs, send, recv):
    copies = []
    for r in range(1, ne):
        to = (z, lax.rem(e + r, ne))
        copy = remote(mine, theirs.at[r], send.at[r], recv.at[r], to)
        copy.start()
        copies.append(copy)
    total = mine[...]
    for r, copy in enumerate(copies):
        copy.wait_recv()
        total = total + theirs[r + 1]
    for copy in copies:
        copy.wait_send()
    return total


def store_columns(sums, first, columns):
    rows = columns[0].shape[0]
    lanes = lax.broadcasted_iota(jnp.int32, (rows, 128), 1)
    wide = jnp.zeros((rows, 128), F32)
    for j, column in enumerate(columns):
        wide = jnp.where(lanes == j, column, wide)
    sums[:, pl.ds(first, rows)] = wide.T[:8]


def as_columns(total, out):
    rows = total.shape[1]
    for first in range(0, rows, 128):
        chunk = total[:, first : first + 128]
        out[first : first + 128, :] = jnp.concatenate([chunk] * 16, axis=0).T


def allowed_pairs(seg_ref, n):
    length = seg_ref.shape[2]
    keys = jnp.broadcast_to(seg_ref[n, :1].astype(F32), (length, length))
    i = lax.broadcasted_iota(jnp.int32, (length, length), 0)
    j = lax.broadcasted_iota(jnp.int32, (length, length), 1)
    return (i >= j) & (keys == keys.T)


def attend(rq, rk, allowed):
    scores = jnp.where(allowed, dot(rq, rk, NT) * HD ** (-0.5), MASKED)
    top = jnp.max(scores, axis=-1, keepdims=True)
    lse = top + jnp.log(jnp.sum(jnp.exp(scores - top), axis=-1, keepdims=True))
    return jnp.exp(scores - lse)


def attn_fwd_kernel(
    ne, x_ref, wq_ref, wo_ref, gain_ref, mine_ref, seg_ref, cos_ref, sin_ref,
    h1_ref, q_ref, k_ref, rq_ref, rk_ref, v_ref, o_ref, scale_ref, x1_ref,
    sums, theirs, send, recv,
):
    z, e = lax.axis_index("dp"), lax.axis_index("expert")
    width = x_ref.shape[2]
    count, hw = q_ref.shape
    length = seg_ref.shape[2]
    rows_dev = x_ref.shape[1]
    tile = min(512, count)
    meet_plane(ne, z, e)

    def normed(b, carry):
        x = x_ref[b].astype(F32)
        h1 = x * rms_scale(x) * gain_ref[:1]
        h1_ref[pl.ds(pl.multiple_of(b * rows_dev, rows_dev), rows_dev), :] = h1.astype(BF)
        return carry

    lax.fori_loop(0, ne, normed, 0)
    for first in range(0, count, tile):
        rows = slice(first, first + tile)
        h1 = h1_ref[rows, :]
        q, k = dot(h1, wq_ref[0], NN), dot(h1, wq_ref[1], NN)
        q_ref[rows, :] = q
        k_ref[rows, :] = k
        v_ref[rows, :] = dot(h1, wq_ref[2], NN).astype(BF)
        store_columns(
            sums, first, [jnp.sum(t * t, axis=-1, keepdims=True) for t in (q, k)]
        )
    total = plane_totals(ne, z, e, sums, theirs, send, recv)
    as_columns(lax.rsqrt(total / width + EPS), scale_ref)
    cos, sin = cos_ref[...], sin_ref[...]

    def sequence(n, carry):
        rows = pl.ds(pl.multiple_of(n * length, length), length)
        allowed = allowed_pairs(seg_ref, n)
        aq, ak = scale_ref[rows, 0:1], scale_ref[rows, 1:2]
        for c in range(0, hw, HD):
            cols = slice(c, c + HD)
            rq = turn(q_ref[rows, cols] * aq * mine_ref[1:2, cols], cos, sin).astype(BF)
            rk = turn(k_ref[rows, cols] * ak * mine_ref[2:3, cols], cos, sin).astype(BF)
            rq_ref[rows, cols] = rq
            rk_ref[rows, cols] = rk
            probs = attend(rq, rk, allowed).astype(BF)
            o_ref[rows, cols] = dot(probs, v_ref[rows, cols], NN).astype(BF)
        return carry

    lax.fori_loop(0, count // length, sequence, 0)
    for first in range(0, count, tile):
        x1 = dot(o_ref[first : first + tile, :], wo_ref[...], NN).astype(BF)
        blocks = tile // rows_dev
        x1_ref[first // rows_dev : first // rows_dev + blocks] = x1.reshape(
            blocks, rows_dev, width
        )


def attn_fwd(in_all, wq, wo, gain_mat, my_gains, seg, tables, cid):
    ne, rows_dev, width = in_all.shape
    count, hw = ne * rows_dev, wo.shape[0]
    return pl.pallas_call(
        functools.partial(attn_fwd_kernel, ne),
        out_shape=[
            jax.ShapeDtypeStruct((count, width), BF),
            jax.ShapeDtypeStruct((count, hw), F32),
            jax.ShapeDtypeStruct((count, hw), F32),
            jax.ShapeDtypeStruct((count, hw), BF),
            jax.ShapeDtypeStruct((count, hw), BF),
            jax.ShapeDtypeStruct((count, hw), BF),
            jax.ShapeDtypeStruct((count, hw), BF),
            jax.ShapeDtypeStruct((count, 128), F32),
            jax.ShapeDtypeStruct((ne, rows_dev, width), BF),
        ],
        in_specs=[VMEM] * 8,
        out_specs=[VMEM] * 9,
        scratch_shapes=[
            pltpu.VMEM((8, count), F32), pltpu.VMEM((ne, 8, count), F32), DMA((ne,)), DMA((ne,)),
        ],
        compiler_params=pltpu.CompilerParams(
            collective_id=cid, has_side_effects=True, vmem_limit_bytes=60_000_000
        ),
        name="attn_fwd",
    )(in_all, wq, wo, gain_mat, my_gains, seg, *tables)


def attn_bwd_kernel(
    ne, gab_ref, wq_ref, wo_ref, mine_ref, seg_ref, cos_ref, sin_ref,
    h1_ref, q_ref, k_ref, rq_ref, rk_ref, v_ref, o_ref, scale_ref,
    gh1_ref, parts_ref, gain_ref,
    pout, go_ref, gqn_ref, gkn_ref, gp_ref, sums, theirs, means, send, recv, psend, precv,
):
    z, e = lax.axis_index("dp"), lax.axis_index("expert")
    count, hw = q_ref.shape
    width = gab_ref.shape[2]
    rows_dev = gab_ref.shape[1]
    length = seg_ref.shape[2]
    tile = min(512, count)
    blocks = tile // rows_dev
    meet_plane(ne, z, e)

    gab = lambda first: gab_ref[first // rows_dev : first // rows_dev + blocks].reshape(tile, width)
    part = dot(o_ref[:tile, :], gab(0), TN)
    for first in range(tile, count, tile):
        part = part + dot(o_ref[first : first + tile, :], gab(first), TN)
    pout[...] = part.astype(BF)
    for first in range(0, count, tile):
        go_ref[first : first + tile, :] = dot(gab(first), wo_ref[...], NT).astype(BF)
    my_rows = pl.ds(pl.multiple_of(e * hw, hw), hw)
    last = pl.ds(3 * hw, hw)
    gives = []
    for r in range(1, ne):
        to = lax.rem(e + r, ne)
        give = remote(
            pout.at[:, pl.ds(pl.multiple_of(to * hw, hw), hw)], parts_ref.at[my_rows, last],
            psend.at[r], precv.at[r], (z, to),
        )
        give.start()
        gives.append(give)
    parts_ref[my_rows, last] = pout[:, my_rows]

    cos, sin = cos_ref[...], -sin_ref[...]
    gain_ref[...] = jnp.zeros_like(gain_ref)

    def sequence(n, carry):
        start = pl.multiple_of(n * length, length)
        rows = pl.ds(start, length)
        allowed = allowed_pairs(seg_ref, n)
        aq, ak = scale_ref[rows, 0:1], scale_ref[rows, 1:2]
        sum_q = jnp.zeros((length, 1), F32)
        sum_k = jnp.zeros((length, 1), F32)
        for c in range(0, hw, HD):
            cols = slice(c, c + HD)
            rq, rk, go = rq_ref[rows, cols], rk_ref[rows, cols], go_ref[rows, cols]
            probs = attend(rq, rk, allowed)
            gv = dot(probs.astype(BF), go, TN).astype(BF)
            gp_ref[rows, slice(2 * hw + c, 2 * hw + c + HD)] = gv
            grad = dot(go, v_ref[rows, cols], NT)
            delta = jnp.sum(probs * grad, axis=-1, keepdims=True)
            gs = (probs * (grad - delta) * HD ** (-0.5)).astype(BF)
            gqn = turn(dot(gs, rk, NN), cos, sin)
            gkn = turn(dot(gs, rq, TN), cos, sin)
            gqn_ref[rows, cols] = gqn
            gkn_ref[rows, cols] = gkn
            tq = gqn * (q_ref[rows, cols] * aq)
            tk = gkn * (k_ref[rows, cols] * ak)
            gain_ref[0:1, cols] += jnp.sum(tq, axis=0, keepdims=True)
            gain_ref[1:2, cols] += jnp.sum(tk, axis=0, keepdims=True)
            sum_q = sum_q + jnp.sum(tq * mine_ref[1:2, cols], axis=-1, keepdims=True)
            sum_k = sum_k + jnp.sum(tk * mine_ref[2:3, cols], axis=-1, keepdims=True)
        store_columns(sums, start, [sum_q, sum_k])
        return carry

    lax.fori_loop(0, count // length, sequence, 0)
    total = plane_totals(ne, z, e, sums, theirs, send, recv)
    as_columns(total / width, means)
    for first in range(0, count, tile):
        rows = slice(first, first + tile)
        aq, ak = scale_ref[rows, 0:1], scale_ref[rows, 1:2]
        mq, mk = means[rows, 0:1], means[rows, 1:2]
        gq = aq * (gqn_ref[rows, :] * mine_ref[1:2] - q_ref[rows, :] * aq * mq)
        gk = ak * (gkn_ref[rows, :] * mine_ref[2:3] - k_ref[rows, :] * ak * mk)
        gp_ref[rows, :hw] = gq.astype(BF)
        gp_ref[rows, hw : 2 * hw] = gk.astype(BF)
    for first in range(0, width, tile):
        rows = slice(first, first + tile)
        parts_ref[rows, : 3 * hw] = dot(h1_ref[:, rows], gp_ref[...], TN).astype(BF)
    for first in range(0, count, tile):
        rows = slice(first, first + tile)
        gh1 = dot(gp_ref[rows, :hw], wq_ref[0], NT)
        for j in range(1, 3):
            gh1 = gh1 + dot(gp_ref[rows, j * hw : (j + 1) * hw], wq_ref[j], NT)
        gh1_ref[first // rows_dev : first // rows_dev + blocks] = gh1.astype(BF).reshape(
            blocks, rows_dev, width
        )
    for give in gives:
        give.wait_send()
        give.wait_recv()


def attn_bwd(gab, wq, wo, my_gains, seg, tables, saved, cid):
    ne, rows_dev, width = gab.shape
    count, hw = ne * rows_dev, wo.shape[0]
    return pl.pallas_call(
        functools.partial(attn_bwd_kernel, ne),
        out_shape=[
            jax.ShapeDtypeStruct((ne, rows_dev, width), BF),
            jax.ShapeDtypeStruct((width, 4 * hw), BF),
            jax.ShapeDtypeStruct((8, hw), F32),
        ],
        in_specs=[VMEM] * 15,
        out_specs=[VMEM] * 3,
        scratch_shapes=[
            pltpu.VMEM((hw, width), BF),
            pltpu.VMEM((count, hw), BF),
            pltpu.VMEM((count, hw), F32),
            pltpu.VMEM((count, hw), F32),
            pltpu.VMEM((count, 3 * hw), BF),
            pltpu.VMEM((8, count), F32),
            pltpu.VMEM((ne, 8, count), F32),
            pltpu.VMEM((count, 128), F32),
            DMA((ne,)), DMA((ne,)), DMA((ne,)), DMA((ne,)),
        ],
        compiler_params=pltpu.CompilerParams(
            collective_id=cid, has_side_effects=True, vmem_limit_bytes=64_000_000
        ),
        name="attn_bwd",
    )(gab, wq, wo, my_gains, seg, *tables, *saved)


class PlaneScatter:
    def __init__(self, ne, z, e, x_ref, acc, got, loads, send, recv):
        self.ne, self.z, self.e = ne, z, e
        self.x, self.acc, self.got = x_ref, acc, got
        self.loads, self.send, self.recv = loads, send, recv
        self.half = acc.shape[2]
        self.stages = ne.bit_length() - 1
        self.orders = bit_orders(ne)
        self.first = [0]
        for j in range(self.stages):
            self.first.append(self.first[j] + (ne >> (j + 1)))
        self.pending, self.arrivals = [], {}

    def push(self, s, j):
        order = self.orders[s]
        peer_e = flip(self.e, order[j])
        rest = self.ne >> (j + 1)
        for i in range(rest):
            n = self.first[j] + i
            if j == 0:
                block = flips(peer_e, order[:0:-1])[i]
                src = self.x.at[block, pl.ds(s * self.half, self.half)]
            else:
                src = self.acc.at[s, rest + i]
            copy = remote(
                src, self.got.at[s, n], self.send.at[s, n], self.recv.at[s, n], (self.z, peer_e)
            )
            copy.start()
            self.pending.append(copy.wait_send)
            self.arrivals.setdefault((s, j), []).append((copy.wait_recv, i, n))

    def start(self):
        for s in range(2):
            self.push(s, 0)
            for i, block in enumerate(flips(self.e, self.orders[s][:0:-1])):
                copy = pltpu.make_async_copy(
                    self.x.at[block, pl.ds(s * self.half, self.half)],
                    self.acc.at[s, i],
                    self.loads.at[s, i],
                )
                copy.start()
                self.arrivals.setdefault((s, -1), []).append(copy.wait)

    def stage(self, j):
        for s in range(2):
            if j == 0:
                for wait in self.arrivals.pop((s, -1)):
                    wait()
            for wait, i, n in self.arrivals.pop((s, j)):
                wait()
                add_rows(self.acc.at[s, i], self.got.at[s, n])
            if j + 1 < self.stages:
                self.push(s, j + 1)

    def finish(self):
        for wait in self.pending:
            wait()


def tail_kernel(
    nz, ne, kinds, gain_row, parts_ref, gh1_ref, x_ref, gx1_ref, gain_ref, tiny_ref,
    grad_ref, qkv_ref, out_ref, small_ref,
    work, below, above, wide, stage, acc, got, gsum, tbuf, tgot, total, far,
    wload, usend, urecv, dsend, drecv, zsend, zrecv, gsend, grecv, glocal,
    hload, hsend, hrecv, flush, send1, recv1, send2, recv2,
):
    z, e = lax.axis_index("dp"), lax.axis_index("expert")
    per = ne // nz
    chunks, rows = work.shape[1], work.shape[2]
    hw = work.shape[3] // kinds
    width = x_ref.shape[1]
    loads = [
        pltpu.make_async_copy(
            parts_ref.at[pl.ds((t * chunks + c) * rows, rows)], work.at[t, c], wload.at[t, c]
        )
        for c in range(chunks)
        for t in range(nz)
    ]
    for copy in loads:
        copy.start()
    meet_all(nz, ne, z, e)
    mine = PlaneScatter(ne, z, e, gh1_ref, acc, got, hload, hsend, hrecv)
    mine.start()
    for copy in loads:
        copy.wait()

    def rise(t, c):
        return remote(
            work.at[t, c], below.at[t, c], usend.at[t, c], urecv.at[t, c], (z + 1, e)
        )

    def sink(t, c):
        return remote(
            work.at[t, c], above.at[t, c], dsend.at[t, c], drecv.at[t, c], (z - 1, e)
        )

    for c in range(chunks):
        for t in range(nz - 1, 0, -1):

            @pl.when(z == 0)
            def _():
                rise(t, c).start()

        for t in range(nz - 1):

            @pl.when(z == nz - 1)
            def _():
                sink(t, c).start()

    def arrive(t, c, buffer, recv):
        remote(buffer.at[t, c], buffer.at[t, c], usend.at[0, 0], recv.at[t, c], (z, e)).wait_recv()
        add_rows(work.at[t, c], buffer.at[t, c])

    def line(c):
        for far_off in range(nz - 1):
            up, down = nz - 1 - far_off, far_off

            @pl.when((z < up) & (z > 0))
            def _():
                arrive(up, c, below, urecv)
                rise(up, c).start()

            @pl.when((z > down) & (z < nz - 1))
            def _():
                arrive(down, c, above, drecv)
                sink(down, c).start()

        @pl.when(z > 0)
        def _():
            arrive(z, c, below, urecv)

        @pl.when(z < nz - 1)
        def _():
            arrive(z, c, above, drecv)

    def spread(c):
        net = PlaneGather(
            nz, ne, z, e, False, work.at[z, c], wide.at[c], zsend, zrecv,
            gsend.at[c], grecv.at[c], glocal.at[c],
        )
        net.start_round(0)
        return net

    def outs(c):
        p = c % 2
        span = pl.ds(c * rows, rows)
        return [
            pltpu.make_async_copy(
                stage.at[p, j], qkv_ref.at[j, span] if j < kinds - 1 else out_ref.at[span],
                flush.at[p, j],
            )
            for j in range(kinds)
        ]

    def lay(c, net):
        net.finish_round(0)
        net.finish()
        p = c % 2
        if c >= 2:
            for copy in outs(c - 2):
                copy.wait()

        def column(n, carry):
            cols = pl.ds(pl.multiple_of(n * hw, hw), hw)
            for j in range(kinds):
                stage[p, j, :, cols] = wide[c, n, :, j * hw : (j + 1) * hw].astype(F32)
            return carry

        lax.fori_loop(0, ne, column, 0)
        for copy in outs(c):
            copy.start()

    for j in range(mine.stages):
        mine.stage(j)
    line(0)
    nets = {0: spread(0)}

    half = acc.shape[2]
    gsum[...] = jnp.zeros_like(gsum)
    for s in range(2):

        def front(n, carry):
            here = pl.ds(pl.multiple_of(n * 16, 16), 16)
            span = pl.ds(pl.multiple_of(s * half + n * 16, 16), 16)
            grad = acc[s, 0, here, :].astype(F32)
            x = x_ref[span, :].astype(F32)
            scale = rms_scale(x)
            normed = x * scale
            gsum[...] += grad * normed
            scaled = grad * gain_ref[:1]
            inner = jnp.mean(scaled * normed, axis=-1, keepdims=True)
            grad_ref[span, :] = (gx1_ref[span, :] + scale * (scaled - normed * inner)).astype(BF)
            return carry

        lax.fori_loop(0, half // 16, front, 0)
    tbuf[...] = tiny_ref[...]
    tbuf[gain_row : gain_row + 1, :] = jnp.sum(gsum[...], axis=0, keepdims=True)

    cw = width // ne
    block = lambda ee: pl.ds(pl.multiple_of(ee * cw, cw), cw)
    first = []
    for r in range(1, ne):
        to = lax.rem(e + r, ne)
        copy = remote(tbuf.at[:, block(to)], tgot.at[r], send1.at[r], recv1.at[r], (z, to))
        copy.start()
        first.append(copy)
    if chunks > 1:
        line(1)
        nets[1] = spread(1)
    sums = tbuf[:, block(e)]
    for r, copy in enumerate(first):
        copy.wait_recv()
        sums = sums + tgot[r + 1]
    total[...] = sums
    home, place = e // per, lax.rem(e, per)

    def give(r):
        to = lax.rem(e + r, ne)
        return remote(total, far.at[z, place], send2.at[r], recv2, (home, to))

    for r in range(ne):
        if r > 0:
            give(r).start()
        else:

            @pl.when(home != z)
            def _():
                give(0).start()

            @pl.when(home == z)
            def _():
                far[z, place] = total[...]

    lay(0, nets.pop(0))
    for c in range(2, chunks):
        line(c)
        nets[c] = spread(c)
        lay(c - 1, nets.pop(c - 1))
    if chunks > 1:
        lay(chunks - 1, nets.pop(chunks - 1))
    for copy in first:
        copy.wait_send()

    def arrived(count):
        flat = tgot.at[pl.ds(0, count)]
        remote(flat, flat, send2.at[0], recv2, (z, e)).wait_recv()

    for r in range(ne):
        if r > 0:
            give(r).wait_send()
        else:

            @pl.when(home != z)
            def _():
                give(0).wait_send()
                arrived(nz * per)

            @pl.when(home == z)
            def _():
                arrived(nz * per - 1)

    for i in range(per):
        small_ref[i] = sum(far[k, i] for k in range(nz))
    mine.finish()
    for c in range(chunks):
        for t in range(nz):

            @pl.when(z < t)
            def _():
                rise(t, c).wait_send()

            @pl.when(z > t)
            def _():
                sink(t, c).wait_send()

    for c in range(max(chunks - 2, 0), chunks):
        for copy in outs(c):
            copy.wait()


def tail(parts, gh1_part, x, gx1, gain_mat, tiny, gain_row, nz, ne, hw, cid):
    width, total_cols = parts.shape
    kinds = total_cols // hw
    count = x.shape[0]
    depth = width // nz
    rows = min(128, depth)
    chunks = depth // rows
    small_rows, cw = tiny.shape[0], width // ne
    per = ne // nz
    block = (nz, chunks, rows, total_cols)
    out = pl.pallas_call(
        functools.partial(tail_kernel, nz, ne, kinds, gain_row),
        out_shape=[
            jax.ShapeDtypeStruct((count, width), BF),
            jax.ShapeDtypeStruct((kinds - 1, depth, width), F32),
            jax.ShapeDtypeStruct((depth, width), F32),
            jax.ShapeDtypeStruct((per, small_rows, cw), F32),
        ],
        in_specs=[ANY, ANY, VMEM, VMEM, VMEM, VMEM],
        out_specs=[VMEM, ANY, ANY, VMEM],
        scratch_shapes=[
            pltpu.VMEM(block, BF), pltpu.VMEM(block, BF), pltpu.VMEM(block, BF),
            pltpu.VMEM((chunks, ne, rows, total_cols), BF),
            pltpu.VMEM((2, kinds, rows, width), F32),
            pltpu.VMEM((2, ne // 2, count // 2, width), BF),
            pltpu.VMEM((2, ne - 1, count // 2, width), BF),
            pltpu.VMEM((16, width), F32),
            pltpu.VMEM((small_rows, width), F32),
            pltpu.VMEM((max(ne, nz * per), small_rows, cw), F32),
            pltpu.VMEM((small_rows, cw), F32),
            pltpu.VMEM((nz, per, small_rows, cw), F32),
            DMA((nz, chunks)),
            DMA((nz, chunks)), DMA((nz, chunks)), DMA((nz, chunks)), DMA((nz, chunks)),
            DMA((nz,)), DMA((nz,)),
            DMA((chunks, 1, 2, ne - 1)), DMA((chunks, 1, 2, ne - 1)), DMA((chunks,)),
            DMA((2, ne // 2)), DMA((2, ne - 1)), DMA((2, ne - 1)),
            DMA((2, kinds)),
            DMA((ne,)), DMA((ne,)), DMA((ne,)), DMA,
        ],
        compiler_params=pltpu.CompilerParams(
            collective_id=cid, has_side_effects=True, vmem_limit_bytes=64_000_000
        ),
        name="tail",
    )(parts, gh1_part, x, gx1, gain_mat, tiny)
    *out, small = out
    return *out, small.transpose(1, 0, 2).reshape(small_rows, per * cw)


def lay_experts_kernel(per_dev, fl, x_ref, gate_ref, up_ref):
    for i in range(per_dev):
        gate_ref[i] = x_ref[0, :, i * fl : (i + 1) * fl].astype(F32)
        up_ref[i] = x_ref[0, :, (per_dev + i) * fl : (per_dev + i + 1) * fl].astype(F32)


def lay_experts(wide, per_dev, fl):
    nz, rows, _ = wide.shape
    out = jax.ShapeDtypeStruct((per_dev, rows, nz * fl), F32)
    spec = pl.BlockSpec((per_dev, rows, fl), lambda i: (0, 0, i))
    return pl.pallas_call(
        functools.partial(lay_experts_kernel, per_dev, fl),
        grid=(nz,),
        in_specs=[pl.BlockSpec((1, rows, 2 * per_dev * fl), lambda i: (i, 0, 0))],
        out_specs=[spec, spec],
        out_shape=[out, out],
        name="lay_experts",
    )(wide)


def moe_kernel(
    fl, h_ref, g_ref, win_ref, wd_ref,
    mix_ref, gh_ref, dwin_ref, dwd_ref, acc_in, acc_d,
):
    step = pl.program_id(0)
    tile, width = g_ref.shape
    per_dev = wd_ref.shape[0] // fl
    e = lax.axis_index("expert")
    h = h_ref[:, :width]
    g = g_ref[...]
    extra = h_ref[:, width:].astype(F32)
    pre = dot(h, win_ref[...], NN)
    graw = dot(g, wd_ref[...], NT)
    scaled_act, grad_gate, grad_up = [], [], []
    lanes = lax.broadcasted_iota(jnp.int32, (tile, 128), 1)
    gg = jnp.zeros((tile, 128), F32)
    split = 64
    for i in range(per_dev):
        u = pre[:, i * fl : (i + 1) * fl]
        w = pre[:, (per_dev + i) * fl : (per_dev + 1 + i) * fl]
        gr = graw[:, i * fl : (i + 1) * fl]
        mine = e * per_dev + i
        picked = (lanes == mine) | (lanes == mine + split)
        gate = jnp.sum(jnp.where(picked, extra, 0.0), axis=-1, keepdims=True)
        sig = 1.0 / (1.0 + jnp.exp(-u))
        silu = u * sig
        act = silu * w
        total = jnp.sum(act.astype(BF).astype(F32) * gr, axis=-1, keepdims=True)
        rounded = total.astype(BF).astype(F32)
        gg = jnp.where(lanes == mine, rounded, gg)
        gg = jnp.where(lanes == mine + split, total - rounded, gg)
        scaled_act.append((gate * act).astype(BF))
        gact = gate * gr
        grad_gate.append((gact * w * (sig * (1.0 + u * (1.0 - sig)))).astype(BF))
        grad_up.append((gact * silu).astype(BF))
    a = jnp.concatenate(scaled_act, axis=1)
    gin = jnp.concatenate(grad_gate + grad_up, axis=1)
    blocks, rows = mix_ref.shape[0], mix_ref.shape[2]
    mix_ref[...] = dot(a, wd_ref[...], NN).astype(BF).reshape(blocks, 1, rows, width)
    gh_ref[:, :width] = dot(gin, win_ref[...], NT).astype(BF)
    gh_ref[:, width:] = gg.astype(BF)

    @pl.when(step == 0)
    def _():
        acc_in[...] = jnp.zeros_like(acc_in)
        acc_d[...] = jnp.zeros_like(acc_d)

    acc_in[...] += dot(h, gin, TN)
    acc_d[...] += dot(a, g, TN)

    @pl.when(step == pl.num_programs(0) - 1)
    def _():
        dwin_ref[...] = acc_in[...].astype(BF)
        dwd_ref[...] = acc_d[...]


def moe(h_all, g_all, w_in, wd, per_dev, nz, ne, rows_dev, blocks):
    count, width = g_all.shape
    wide = h_all.shape[1]
    hid4 = w_in.shape[1]
    hid2 = wd.shape[0]
    fl = hid2 // per_dev
    tile = blocks * rows_dev
    turns = ne // blocks
    rows = lambda n: pl.BlockSpec((tile, n), lambda i: (i, 0))
    whole = lambda s: pl.BlockSpec(s, lambda i: (0, 0), pipeline_mode=pl.Buffered(1))
    return pl.pallas_call(
        functools.partial(moe_kernel, fl),
        grid=(count // tile,),
        in_specs=[
            rows(wide), rows(width),
            whole(w_in.shape), whole(wd.shape),
        ],
        out_specs=[
            pl.BlockSpec((blocks, 1, rows_dev, width), lambda i: (i % turns, i // turns, 0, 0)),
            rows(wide),
            whole((width, hid4)), whole((hid2, width)),
        ],
        out_shape=[
            jax.ShapeDtypeStruct((ne, nz, rows_dev, width), BF),
            jax.ShapeDtypeStruct((count, wide), BF),
            jax.ShapeDtypeStruct((width, hid4), BF),
            jax.ShapeDtypeStruct((hid2, width), F32),
        ],
        scratch_shapes=[pltpu.VMEM((width, hid4), F32), pltpu.VMEM((hid2, width), F32)],
        compiler_params=pltpu.CompilerParams(vmem_limit_bytes=66_000_000),
        cost_estimate=pl.CostEstimate(
            flops=2 * count * width * hid2 * 9,
            bytes_accessed=8 * count * width + 24 * hid4 * width,
            transcendentals=count * hid2,
        ),
        name="moe",
    )(h_all, g_all, w_in, wd)


def moe_net_kernel(
    nz, ne, per_dev, slots, h_ref, g_ref, wg_ref, wu_ref, wd_ref,
    hall_ref, mix_ref, gh_ref, dwin_ref, dwd_ref,
    win, wd, acc_in, acc_d, htile, gtile, mixbuf, qbuf, cgot, acc, got, zgot, dbuf,
    wload, tload, mixsem, keep, flush, zsend, zrecv, send, recv,
    csend, crecv, credit, rsend, rrecv, ysend, yrecv,
):
    z, e = lax.axis_index("dp"), lax.axis_index("expert")
    rows, width = g_ref.shape[1], g_ref.shape[2]
    half = rows // 2
    fl = wd.shape[0] // per_dev
    upper = [2 << b for b in range(ne.bit_length() - 2)]
    stages = len(upper)
    pairs = ne // 2
    steps = nz * pairs
    gather_orders = [upper + [1], upper[::-1] + [1]]
    sum_orders = [[1] + upper, [1] + upper[::-1]]
    at = [e]
    for bit in [1] + upper:
        at = at + [flip(i, bit) for i in at]
    partner = (z, at[1])

    def plane(r):
        low = jnp.minimum(z, nz - 1 - z)
        near = jnp.where(lax.rem(r, 2) == 1, z - (r + 1) // 2, z + r // 2)
        far = jnp.where(2 * z < nz, z + (r - low), z - (r - low))
        return jnp.where(r <= 2 * low, near, far)

    planes = [z] + [nearest(z, r, nz) for r in range(1, nz)]

    def part(s):
        return pl.ds(s * half, half)

    def subset_mask(order, subset):
        return sum(bit for b, bit in enumerate(order) if subset >> b & 1)

    def pass_on(r, s, stage, subset, own=False):
        order = gather_orders[s]
        dst = hall_ref.at[plane(r) * ne + at[subset_mask(order, subset)], part(s)]
        n = (1 << stage) - 1 + subset
        src = h_ref.at[part(s)] if own else dst
        return remote(src, dst, send.at[r, s, n], recv.at[r, s, n], (z, at[order[stage]]))

    def take(r, s, stage, subset):
        order = gather_orders[s]
        mask = subset_mask(order, subset) | order[stage]
        n = (1 << stage) - 1 + subset
        here = hall_ref.at[plane(r) * ne + at[mask], part(s)]
        remote(here, here, send.at[r, s, n], recv.at[r, s, n], partner).wait_recv()
        for later in range(stage + 1, stages + 1):
            pass_on(r, s, later, subset + (1 << stage)).start()

    def start_round(r):
        if r > 0:
            here = hall_ref.at[planes[r] * ne + e]
            remote(here, here, zsend.at[r], zrecv.at[planes[r]], partner).wait_recv()
        for stage in range(stages + 1):
            for s in range(2):
                pass_on(r, s, stage, 0, own=r == 0).start()

    def take_pair(r, i):
        if i == 1:
            for stage in range(stages):
                for s in range(2):
                    take(r, s, stage, 0)
        mask = 2 * i
        for s in range(2):
            order = gather_orders[s]
            places = [b for b in range(stages) if order[b] & mask]
            if len(places) > 1:
                take(r, s, places[-1], sum(1 << b for b in places[:-1]))
        for s in range(2):
            order = gather_orders[s]
            take(r, s, stages, sum(1 << b for b in range(stages) if order[b] & mask))

    def blocks_of(k):
        r, i = k // pairs, lax.rem(k, pairs)
        home = plane(r)
        lane = e
        for b, bit in enumerate(upper):
            lane = lane + lax.rem(i // (1 << b), 2) * (at[bit] - e)
        return home, lane, lane + (at[1] - e)

    def loads(k):
        home, one, two = blocks_of(k)
        p = lax.rem(k, 2)
        out = []
        for j, lane in enumerate((one, two)):
            to = pl.ds(j * rows, rows)
            block = home * ne + lane
            out.append(pltpu.make_async_copy(hall_ref.at[block], htile.at[p, to], tload.at[p, 2 * j]))
            out.append(
                pltpu.make_async_copy(g_ref.at[block], gtile.at[p, to], tload.at[p, 2 * j + 1])
            )
        return out

    def mix_out(k):
        home, one, two = blocks_of(k)
        p = lax.rem(k, 2)
        return [
            pltpu.make_async_copy(
                mixbuf.at[p, pl.ds(j * rows, rows)], mix_ref.at[lane, home], mixsem.at[p, j]
            )
            for j, lane in enumerate((one, two))
        ]

    def to_partner(k):
        return remote(
            qbuf.at[lax.rem(k, 2)], cgot.at[lax.rem(k, slots)],
            csend.at[lax.rem(k, 2)], crecv.at[lax.rem(k, slots)], partner,
        )

    def place_of(t, keep_index):
        return (1 << stages) - (1 << (stages - t + 1)) + keep_index

    def push(r, s, t, keep_index):
        order = sum_orders[s]
        mask = order[t] | subset_mask(order[t + 1 :], keep_index)
        n = place_of(t, keep_index)
        return remote(
            acc.at[r, mask // 2, part(s)], got.at[r, s, n],
            rsend.at[r, s, n], rrecv.at[r, s, n], (z, at[order[t]]),
        )

    def merge(k):
        slot = lax.rem(k, slots)
        remote(cgot.at[slot], cgot.at[slot], csend.at[0], crecv.at[slot], partner).wait_recv()
        r, i = k // pairs, lax.rem(k, pairs)
        add_rows(acc.at[r, i], cgot.at[slot])

        @pl.when(k + slots < steps)
        def _():
            pl.semaphore_signal(credit, inc=1, device_id=partner, device_id_type=MESH)

        for j in range(1, pairs):

            @pl.when(i == j)
            def _():
                for s in range(2):
                    order = sum_orders[s]
                    if order[1] & (2 * j):
                        rest = [b for b, bit in enumerate(order[2:]) if bit & (2 * j)]
                        push(r, s, 1, sum(1 << b for b in rest)).start()

    def home_copy(r, s):
        return remote(
            acc.at[r, 0, part(s)], zgot.at[z, part(s)], ysend.at[r, s], yrecv.at[z, s],
            (plane(r), e),
        )

    def settle(r, t):
        for s in range(2):
            order = sum_orders[s]
            for index in range(1 << (stages - t)):
                copy = push(r, s, t, index)
                copy.wait_recv()
                mask = subset_mask(order[t + 1 :], index)
                add_rows(acc.at[r, mask // 2, part(s)], got.at[r, s, place_of(t, index)])
            if t < stages:
                for index in range(1 << (stages - t - 1)):
                    push(r, s, t + 1, index).start()
            else:

                @pl.when(r > 0)
                def _():
                    home_copy(r, s).start()

    weights = []
    for i in range(per_dev):
        cols = pl.ds(z * fl, fl)
        weights += [
            (wg_ref.at[i, :, cols], win.at[:, pl.ds(i * fl, fl)]),
            (wu_ref.at[i, :, cols], win.at[:, pl.ds((per_dev + i) * fl, fl)]),
            (wd_ref.at[i, cols, :], wd.at[pl.ds(i * fl, fl), :]),
        ]
    weights = [
        pltpu.make_async_copy(src, dst, wload.at[j]) for j, (src, dst) in enumerate(weights)
    ]
    for copy in weights:
        copy.start()
    meet_column_and_plane(nz, ne, z, e, True)
    own = pltpu.make_async_copy(h_ref, hall_ref.at[z * ne + e], keep)
    own.start()
    for r in range(1, nz):
        remote(
            h_ref, hall_ref.at[z * ne + e], zsend.at[r], zrecv.at[z], (planes[r], e)
        ).start()
    start_round(0)
    acc_in[...] = jnp.zeros_like(acc_in)
    acc_d[...] = jnp.zeros_like(acc_d)
    take_pair(0, 0)
    own.wait()
    for copy in loads(0):
        copy.start()
    for copy in weights:
        copy.wait()

    tile = 2 * rows
    lanes = lax.broadcasted_iota(jnp.int32, (tile, 128), 1)
    split = 64

    def step(k, carry):
        p = lax.rem(k, 2)
        r, i = k // pairs, lax.rem(k, pairs)
        for copy in loads(k):
            copy.wait()
        pre = dot(htile[p, :, :width], win[...], NN)
        graw = dot(gtile[p], wd[...], NT)
        extra = htile[p, :, width:].astype(F32)
        scaled_act, grad_gate, grad_up = [], [], []
        gg = jnp.zeros((tile, 128), F32)
        for j in range(per_dev):
            u = pre[:, j * fl : (j + 1) * fl]
            w = pre[:, (per_dev + j) * fl : (per_dev + 1 + j) * fl]
            gr = graw[:, j * fl : (j + 1) * fl]
            mine = e * per_dev + j
            picked = (lanes == mine) | (lanes == mine + split)
            gate = jnp.sum(jnp.where(picked, extra, 0.0), axis=-1, keepdims=True)
            sig = 1.0 / (1.0 + jnp.exp(-u))
            silu = u * sig
            act = silu * w
            total = jnp.sum(act.astype(BF).astype(F32) * gr, axis=-1, keepdims=True)
            rounded = total.astype(BF).astype(F32)
            gg = jnp.where(lanes == mine, rounded, gg)
            gg = jnp.where(lanes == mine + split, total - rounded, gg)
            scaled_act.append((gate * act).astype(BF))
            gact = gate * gr
            grad_gate.append((gact * w * (sig * (1.0 + u * (1.0 - sig)))).astype(BF))
            grad_up.append((gact * silu).astype(BF))
        a = jnp.concatenate(scaled_act, axis=1)
        gin = jnp.concatenate(grad_gate + grad_up, axis=1)

        for r1 in range(1, nz):

            @pl.when(k == (r1 - 1) * (pairs - 1) + 1)
            def _():
                start_round(r1)

        @pl.when(k + 1 < steps)
        def _():
            ahead = k + 1
            for j in range(pairs):

                @pl.when(lax.rem(ahead, pairs) == j)
                def _():
                    take_pair(ahead // pairs, j)

            for copy in loads(ahead):
                copy.start()

        @pl.when(k >= 2)
        def _():
            for copy in mix_out(k - 2):
                copy.wait()
            to_partner(k - 2).wait_send()

        mixbuf[p] = dot(a, wd[...], NN).astype(BF)
        for copy in mix_out(k):
            copy.start()
        back = dot(gin, win[...], NT).astype(BF)
        gg = gg.astype(BF)
        acc[r, i, :, :width] = back[:rows]
        acc[r, i, :, width:] = gg[:rows]
        qbuf[p, :, :width] = back[rows:]
        qbuf[p, :, width:] = gg[rows:]
        acc_in[...] += dot(htile[p, :, :width], gin, TN)
        acc_d[...] += dot(a, gtile[p], TN)

        @pl.when(k >= slots)
        def _():
            pl.semaphore_wait(credit, 1)

        to_partner(k).start()

        @pl.when(k >= 1)
        def _():
            merge(k - 1)

        for t in range(1, stages + 1):
            late = k - pairs - 2 * t

            @pl.when((late >= 0) & (lax.rem(late + pairs, pairs) == 0))
            def _():
                settle(late // pairs, t)

        return carry

    lax.fori_loop(0, steps, step, 0)
    merge(steps - 1)
    final = pltpu.make_async_copy(acc_d, dwd_ref, flush.at[0])
    final.start()
    left = sorted(
        (r * pairs + pairs + 2 * t, r, t)
        for r in range(nz)
        for t in range(1, stages + 1)
        if r * pairs + pairs + 2 * t >= steps
    )
    chunk = dbuf.shape[1]

    def flush_chunk(c):
        return pltpu.make_async_copy(
            dbuf.at[c % 2], dwin_ref.at[pl.ds(c * chunk, chunk)], flush.at[1 + c % 2]
        )

    chunks = acc_in.shape[0] // chunk
    for c in range(chunks):
        if c >= 2:
            flush_chunk(c - 2).wait()
        dbuf[c % 2] = acc_in[pl.ds(c * chunk, chunk), :].astype(BF)
        flush_chunk(c).start()
    for _, r, t in left:
        settle(jnp.int32(r), t)
    for s in range(2):
        for r in range(1, nz):
            here = zgot.at[planes[r], part(s)]
            remote(here, here, ysend.at[r, s], yrecv.at[planes[r], s], partner).wait_recv()

        def total_rows(n, carry):
            span = pl.ds(pl.multiple_of(s * half + n * 16, 16), 16)
            total = acc[0, 0, span, :].astype(F32)
            for r in range(1, nz):
                total = total + zgot[planes[r], span, :].astype(F32)
            gh_ref[span, :] = total
            return carry

        lax.fori_loop(0, half // 16, total_rows, 0)
    final.wait()
    for c in range(max(chunks - 2, 0), chunks):
        flush_chunk(c).wait()
    for k in range(max(steps - 2, 0), steps):
        for copy in mix_out(jnp.int32(k)):
            copy.wait()
        to_partner(jnp.int32(k)).wait_send()
    for r in range(nz):
        if r > 0:
            remote(
                h_ref, hall_ref.at[z * ne + e], zsend.at[r], zrecv.at[z], (planes[r], e)
            ).wait_send()
        for s in range(2):
            for stage in range(stages + 1):
                for subset in range(1 << stage):
                    pass_on(r, s, stage, subset, own=r == 0 and subset == 0).wait_send()
            for t in range(1, stages + 1):
                for index in range(1 << (stages - t)):
                    push(r, s, t, index).wait_send()
            if r > 0:
                home_copy(jnp.int32(r), s).wait_send()


def moe_net_scratch(nz, ne, per_dev, rows, width, wide, fl):
    pairs = ne // 2
    slots = 4
    stages = ne.bit_length() - 2
    vmem = [
        ((width, 2 * per_dev * fl), BF),
        ((per_dev * fl, width), BF),
        ((width, 2 * per_dev * fl), F32),
        ((per_dev * fl, width), F32),
        ((2, 2 * rows, wide), BF),
        ((2, 2 * rows, width), BF),
        ((2, 2 * rows, width), BF),
        ((2, rows, wide), BF),
        ((slots, rows, wide), BF),
        ((nz, pairs, rows, wide), BF),
        ((nz, 2, max(pairs - 1, 1), rows // 2, wide), BF),
        ((nz, rows, wide), BF),
        ((2, width // 8, 2 * per_dev * fl), BF),
    ]
    size = sum(functools.reduce(lambda a, b: a * b, s) * (2 if d == BF else 4) for s, d in vmem)
    sems = [
        DMA((3 * per_dev,)), DMA((2, 4)), DMA((2, 2)), DMA, DMA((3,)),
        DMA((nz,)), DMA((nz,)), DMA((nz, 2, ne - 1)), DMA((nz, 2, ne - 1)),
        DMA((2,)), DMA((slots,)), pltpu.SemaphoreType.REGULAR,
        DMA((nz, 2, max(pairs - 1, 1))), DMA((nz, 2, max(pairs - 1, 1))),
        DMA((nz, 2)), DMA((nz, 2)),
    ]
    fits = size <= 54_000_000 and stages >= 1 and nz > 1 and nz * pairs > slots
    return fits, slots, [pltpu.VMEM(*v) for v in vmem] + sems


def moe_net(h, g_all, w_gate, w_up, w_down, nz, ne, fl, slots, scratch, cid):
    rows, wide = h.shape
    per_dev, width, _ = w_gate.shape
    return pl.pallas_call(
        functools.partial(moe_net_kernel, nz, ne, per_dev, slots),
        out_shape=[
            jax.ShapeDtypeStruct((nz * ne, rows, wide), BF),
            jax.ShapeDtypeStruct((ne, nz, rows, width), BF),
            jax.ShapeDtypeStruct((rows, wide), F32),
            jax.ShapeDtypeStruct((width, 2 * per_dev * fl), BF),
            jax.ShapeDtypeStruct((per_dev * fl, width), F32),
        ],
        in_specs=[VMEM, ANY, ANY, ANY, ANY],
        out_specs=[ANY, ANY, VMEM, ANY, ANY],
        scratch_shapes=scratch,
        compiler_params=pltpu.CompilerParams(
            collective_id=cid, has_side_effects=True, vmem_limit_bytes=66_500_000
        ),
        name="moe_net",
    )(h, g_all.reshape(nz * ne, rows, width), w_gate, w_up, w_down)


def body(inputs, segments, routes, w_qkv, w_out, w_router, gains, w_gate, w_up, w_down, cotangent):
    z = lax.axis_index("dp")
    e = lax.axis_index("expert")
    nz = lax.axis_size("dp")
    ne = lax.axis_size("expert")
    count, width = inputs.shape
    num_seqs, length = segments.shape
    heads = width // HD // ne
    hw = heads * HD
    expert_count = w_router.shape[1]
    per_dev = w_gate.shape[0]
    hidden = w_gate.shape[2]
    fl = hidden // nz
    both = ("dp", "expert")

    pad = -(expert_count + 4) % 16
    small = jnp.concatenate(
        [w_router.T, gains.T, jnp.zeros((pad, gains.shape[0]), BF)], axis=0
    )
    seg8 = jnp.broadcast_to(segments[:, None, :], (num_seqs, 8, length)).reshape(-1, length)
    in_all, wq, wo, small, seg_all, cot = start_gather(
        inputs, w_qkv.transpose(1, 0, 2), w_out, small, seg8, cotangent, nz, ne, hw, 0
    )
    small = small.transpose(1, 0, 2).reshape(-1, width)
    router_t = small[:expert_count]
    gain_mat = small[expert_count : expert_count + 4].astype(F32)
    my_gains = lax.dynamic_slice_in_dim(gain_mat, e * hw, hw, axis=1)
    seg_all = seg_all.reshape(ne * num_seqs, 8, length)

    g_all = lax.all_gather(cot, both, axis=0, tiled=True)
    inputs_f = inputs.astype(F32)
    tables = rope_lanes(length)
    *saved, x1_part = attn_fwd(in_all, wq, wo, gain_mat, my_gains, seg_all, tables, 9)
    (x1_sum,) = scatter_tokens(x1_part, nz, ne, False, 1)
    x1 = inputs_f + x1_sum

    a2 = rms_scale(x1)
    h2 = (x1 * a2 * gain_mat[3]).astype(BF)
    probs = jax.nn.softmax(dot(h2, router_t, NT), axis=-1)
    picks = jnp.sum(
        (routes[:, :, None] == jnp.arange(expert_count, dtype=jnp.int32)).astype(F32), axis=1
    )
    gates = picks * probs

    split = 64
    high = gates.astype(BF)
    low = (gates - high.astype(F32)).astype(BF)
    blank = jnp.zeros((count, split - expert_count), BF)
    h2_wide = jnp.concatenate([h2, high, blank, low, blank], axis=1)
    wide = width + 2 * split
    fits, slots, scratch = moe_net_scratch(nz, ne, per_dev, count, width, wide, fl)
    if fits:
        _, mix, gh_sum, dwin, dwd = moe_net(
            h2_wide, g_all, w_gate, w_up, w_down, nz, ne, fl, slots, scratch, 2
        )
        mix = mix.reshape(-1, width)
    else:
        h2_all = gather_tokens(h2_wide, nz, ne, True, 2).reshape(-1, wide)
        wg = lax.dynamic_slice_in_dim(w_gate, z * fl, fl, axis=2)
        wu = lax.dynamic_slice_in_dim(w_up, z * fl, fl, axis=2)
        wd = lax.dynamic_slice_in_dim(w_down, z * fl, fl, axis=1).reshape(per_dev * fl, width)
        w_in = jnp.concatenate([*wg, *wu], axis=1)
        mix, gh, dwin, dwd = moe(
            h2_all, g_all, w_in, wd, per_dev, nz, ne, count, min(4, ne)
        )
        gh_sum, mix = scatter_tokens(
            gh.reshape(nz * ne, count, wide), nz, ne, True, 3, after=mix.reshape(-1, width)
        )
    grad_from_experts = gh_sum[:, :width]
    grad_gates = (
        gh_sum[:, width : width + expert_count]
        + gh_sum[:, width + split : width + split + expert_count]
    )

    mix = lax.psum_scatter(mix, "expert", scatter_dimension=0, tiled=True)
    mix = lax.psum_scatter(mix, "dp", scatter_dimension=0, tiled=True)
    output = (x1 + mix.astype(F32)).astype(BF)

    dwin = lax.all_to_all(
        dwin.reshape(nz, width // nz, 2 * per_dev * fl),
        "dp", split_axis=0, concat_axis=0, tiled=True,
    )
    grad_w_gate, grad_w_up = lay_experts(dwin, per_dev, fl)
    grad_w_down = dwd.reshape(per_dev, fl, width)

    grad_top = cotangent.astype(F32)
    grad_probs = picks * grad_gates
    glog = (probs * (grad_probs - jnp.sum(probs * grad_probs, axis=-1, keepdims=True))).astype(BF)
    local_router = dot(glog, h2, TN)
    gh2 = grad_from_experts + dot(glog, router_t, NN)
    grad_ffn, gain_ffn = rms_backward(x1, a2, gain_mat[3], gh2)
    gx1 = grad_top + grad_ffn
    gab = gx1.astype(BF)

    gab_all = gather_tokens(gab, nz, ne, False, 4)
    gh1_part, parts, gain_qk = attn_bwd(gab_all, wq, wo, my_gains, seg_all, tables, saved, 10)
    place = lambda part: lax.dynamic_update_slice_in_dim(
        jnp.zeros((1, width), F32), part[None], e * hw, axis=1
    )
    tiny = jnp.concatenate(
        [
            local_router, jnp.zeros((1, width), F32), place(gain_qk[0]), place(gain_qk[1]),
            gain_ffn[None], jnp.zeros((-(expert_count + 4) % 8, width), F32),
        ],
        axis=0,
    )
    grad_inputs, grad_w_qkv, grad_w_out, tiny = tail(
        parts, gh1_part, inputs, gx1, gain_mat, tiny, expert_count, nz, ne, hw, 5
    )
    grad_w_qkv = grad_w_qkv.transpose(1, 0, 2)
    grad_w_router = tiny[:expert_count].T
    grad_gains = tiny[expert_count : expert_count + 4].T
    return (
        output,
        grad_inputs,
        grad_w_qkv,
        grad_w_out,
        grad_w_router,
        grad_gains,
        grad_w_gate,
        grad_w_up,
        grad_w_down,
    )


def solution(mesh):
    tokens = P(("dp", "expert"), None)
    rows = P("dp", None)
    rows3 = P("dp", None, None)
    owned = P("expert", None, None)
    return jax.shard_map(
        body,
        mesh=mesh,
        in_specs=(tokens, tokens, tokens, rows3, rows, rows, rows, owned, owned, owned, tokens),
        out_specs=(tokens, tokens, rows3, rows, rows, rows)
        + (P("expert", "dp", None),) * 3,
        check_vma=False,
    )
```

```python
import functools

import jax
import jax.numpy as jnp
from jax import lax
from jax.experimental import pallas as pl
from jax.experimental.pallas import tpu as pltpu
from jax.sharding import PartitionSpec as P


HD = 128
EPS = 1e-05
ROPE_BASE = 10000.0
MASKED = -1e30
BF = jnp.bfloat16
F32 = jnp.float32


def dot(a, b, dims):
    return lax.dot_general(a, b, (dims, ((), ())), preferred_element_type=F32)


NN = ((1,), (0,))
NT = ((1,), (1,))
TN = ((0,), (0,))


def rms_scale(values):
    return lax.rsqrt(jnp.mean(values * values, axis=-1, keepdims=True) + EPS)


def rms_backward(values, inv_rms, gain_col, grad_out):
    normed = values * inv_rms
    grad_gain = jnp.sum(grad_out * normed, axis=0)
    scaled = grad_out * gain_col
    grad_values = inv_rms * (scaled - normed * jnp.mean(scaled * normed, axis=-1, keepdims=True))
    return (grad_values, grad_gain)


MESH = pl.DeviceIdType.MESH
ANY = pl.BlockSpec(memory_space=pl.ANY)
VMEM = pl.BlockSpec(memory_space=pltpu.VMEM)
DMA = pltpu.SemaphoreType.DMA


def flip(index, bit):
    return index + bit * (1 - 2 * ((index // bit) % 2))


def flips(index, bits):
    out = [index]
    for bit in bits:
        out = out + [flip(i, bit) for i in out]
    return out


def bit_orders(ne):
    bits = [1 << b for b in range(ne.bit_length() - 1)]
    return [bits[:1] + bits[1:], bits[:1] + bits[1:][::-1]]


def nearest(z, r, nz):
    low = jnp.minimum(z, nz - 1 - z)
    near = z - (r + 1) // 2 if r % 2 else z + r // 2
    far = jnp.where(2 * z < nz, z + (r - low), z - (r - low))
    return jnp.where(r <= 2 * low, near, far)


def remote(src, dst, send, recv, peer):
    return pltpu.make_async_remote_copy(
        src_ref=src, dst_ref=dst, send_sem=send, recv_sem=recv, device_id=peer, device_id_type=MESH
    )


def for_others(nz, ne, z, e, act):
    def step(i, carry):
        flat = lax.rem(z * ne + e + i, nz * ne)
        act(flat // ne, lax.rem(flat, ne), flat)
        return carry

    lax.fori_loop(1, nz * ne, step, 0)


def meet_all(nz, ne, z, e):
    sem = pltpu.get_barrier_semaphore()

    def greet(zz, ee, flat):
        pl.semaphore_signal(sem, inc=1, device_id=(zz, ee), device_id_type=MESH)

    for_others(nz, ne, z, e, greet)
    pl.semaphore_wait(sem, nz * ne - 1)


def meet_column_and_plane(nz, ne, z, e, spread):
    sem = pltpu.get_barrier_semaphore()
    peers = [(z, flip(e, 1 << b)) for b in range(ne.bit_length() - 1)]
    if spread:
        peers += [(lax.rem(z + r, nz), e) for r in range(1, nz)]
    for peer in peers:
        pl.semaphore_signal(sem, inc=1, device_id=peer, device_id_type=MESH)
    pl.semaphore_wait(sem, len(peers))


class PlaneGather:
    def __init__(self, nz, ne, z, e, spread, x_ref, out_ref, zsend, zrecv, send, recv, local):
        self.nz, self.ne, self.z, self.e, self.spread = nz, ne, z, e, spread
        self.x, self.out = x_ref, out_ref
        self.zsend, self.zrecv, self.send, self.recv = zsend, zrecv, send, recv
        self.rounds = nz if spread else 1
        self.half = x_ref.shape[0] // 2
        self.orders = [o[1:] + o[:1] for o in bit_orders(ne)]
        self.planes = [z if spread else 0] + [nearest(z, r, nz) for r in range(1, self.rounds)]
        self.pending, self.arrivals = [], {}
        own = self.slot(0, e)
        keep = pltpu.make_async_copy(x_ref, out_ref.at[own], local)
        keep.start()
        self.pending.append(keep.wait)

    @staticmethod
    def scratch(nz, ne, spread):
        rounds = nz if spread else 1
        return [DMA((nz,)), DMA((nz,)), DMA((rounds, 2, ne - 1)), DMA((rounds, 2, ne - 1)), DMA]

    def slot(self, r, ee):
        return self.planes[r] * self.ne + ee

    def spread_own(self):
        for r in range(1, self.rounds):
            to = self.planes[r]
            copy = remote(
                self.x, self.out.at[self.slot(0, self.e)],
                self.zsend.at[r], self.zrecv.at[self.z], (to, self.e),
            )
            copy.start()
            self.pending.append(copy.wait_send)

    def forward(self, r, s, stage, subset):
        order = self.orders[s]
        rows = pl.ds(s * self.half, self.half)
        peer_e = flip(self.e, order[stage])
        n = (1 << stage) - 1 + subset
        block = self.slot(r, flips(self.e, order[:stage])[subset])
        dst = self.out.at[block, rows]
        src = self.x.at[rows] if r == 0 and subset == 0 else dst
        sems = self.send.at[r, s, n], self.recv.at[r, s, n]
        copy = remote(src, dst, *sems, (self.z, peer_e))
        copy.start()
        self.pending.append(copy.wait_send)
        got = self.out.at[self.slot(r, flips(peer_e, order[:stage])[subset]), rows]
        self.arrivals[(r, s, stage, subset)] = remote(got, got, *sems, (self.z, peer_e)).wait_recv

    def start_round(self, r):
        if r > 0:
            here = self.out.at[self.slot(r, self.e)]
            remote(
                here, here, self.zsend.at[r], self.zrecv.at[self.planes[r]], (self.planes[r], self.e)
            ).wait_recv()
        for stage in range(len(self.orders[0])):
            for s in range(2):
                self.forward(r, s, stage, 0)

    def finish_round(self, r):
        stages = len(self.orders[0])
        for stage in range(stages):
            for subset in range(1 << stage):
                for s in range(2):
                    self.arrivals.pop((r, s, stage, subset))()
                    for later in range(stage + 1, stages):
                        self.forward(r, s, later, subset + (1 << stage))

    def finish(self):
        for wait in self.pending:
            wait()


def gather_kernel(nz, ne, spread, x_ref, out_ref, *sems):
    z, e = lax.axis_index("dp"), lax.axis_index("expert")
    meet_column_and_plane(nz, ne, z, e, spread)
    net = PlaneGather(nz, ne, z, e, spread, x_ref, out_ref, *sems)
    net.spread_own()
    net.start_round(0)
    for r in range(1, net.rounds):
        net.start_round(r)
        net.finish_round(r - 1)
    net.finish_round(net.rounds - 1)
    net.finish()


def gather_tokens(x, nz, ne, spread, cid):
    rounds = nz if spread else 1
    return pl.pallas_call(
        functools.partial(gather_kernel, nz, ne, spread),
        out_shape=jax.ShapeDtypeStruct((rounds * ne, *x.shape), x.dtype),
        in_specs=[VMEM],
        out_specs=ANY,
        scratch_shapes=PlaneGather.scratch(nz, ne, spread),
        compiler_params=pltpu.CompilerParams(collective_id=cid, has_side_effects=True),
        name="gather_tokens",
    )(x)


def add_rows(dst, src, tile=16):
    def step(i, carry):
        rows = pl.ds(pl.multiple_of(i * tile, tile), tile)
        dst[rows, :] = (dst[rows, :].astype(F32) + src[rows, :].astype(F32)).astype(dst.dtype)
        return carry

    lax.fori_loop(0, dst.shape[0] // tile, step, 0)


def scatter_kernel(nz, ne, spread, x_ref, *refs):
    out_ref, acc, got, zgot, loads, send, recv, zsend, zrecv = refs[-9:]
    z, e = lax.axis_index("dp"), lax.axis_index("expert")
    meet_column_and_plane(nz, ne, z, e, spread)
    rounds = nz if spread else 1
    stages = ne.bit_length() - 1
    half = out_ref.shape[0] // 2
    orders = bit_orders(ne)
    pending, arrivals, zwait = [], {}, {}
    ranks = list(range(1, rounds)) + [0]
    first = [0] * (stages + 1)
    for j in range(stages):
        first[j + 1] = first[j] + (ne >> (j + 1))

    def plane_of(r):
        return lax.rem(z + r, nz) * ne if spread else 0

    def push(r, s, j):
        order = orders[s]
        peer = (z, flip(e, order[j]))
        rest = ne >> (j + 1)
        for i in range(rest):
            n = first[j] + i
            if j == 0:
                block = flips(peer[1], order[:0:-1])[i]
                src = x_ref.at[plane_of(r) + block, pl.ds(s * half, half)]
            else:
                src = acc.at[r, s, rest + i]
            copy = remote(src, got.at[r, s, n], send.at[r, s, n], recv.at[r, s, n], peer)
            copy.start()
            pending.append(copy.wait_send)
            arrivals.setdefault((r, s, j), []).append((copy.wait_recv, i, n))

    for r in ranks:
        for s in range(2):
            push(r, s, 0)
            for i, block in enumerate(flips(e, orders[s][:0:-1])):
                copy = pltpu.make_async_copy(
                    x_ref.at[plane_of(r) + block, pl.ds(s * half, half)],
                    acc.at[r, s, i],
                    loads.at[r, s, i],
                )
                copy.start()
                arrivals.setdefault((r, s, -1), []).append(copy.wait)
    for t in range(rounds + stages):
        for place, r in enumerate(ranks):
            j = t - place
            if not 0 <= j < stages:
                continue
            for s in range(2):
                if j == 0:
                    for wait in arrivals.pop((r, s, -1)):
                        wait()
                for wait, i, n in arrivals.pop((r, s, j)):
                    wait()
                    add_rows(acc.at[r, s, i], got.at[r, s, n])
                if j + 1 < stages:
                    push(r, s, j + 1)
                elif r > 0:
                    copy = remote(
                        acc.at[r, s, 0], zgot.at[r, s], zsend.at[r, s], zrecv.at[r, s],
                        (lax.rem(z + r, nz), e),
                    )
                    copy.start()
                    pending.append(copy.wait_send)
                    zwait[(r, s)] = copy.wait_recv
    for s in range(2):
        for r in range(1, rounds):
            zwait[(r, s)]()

        def step(i, carry):
            rows = pl.ds(pl.multiple_of(i * 16, 16), 16)
            total = acc[0, s, 0, rows, :].astype(F32)
            for r in range(1, rounds):
                total = total + zgot[r, s, rows, :].astype(F32)
            out_ref[pl.ds(pl.multiple_of(s * half + i * 16, 16), 16), :] = total.astype(out_ref.dtype)
            return carry

        lax.fori_loop(0, half // 16, step, 0)
    for wait in pending:
        wait()


def scatter_tokens(parts, nz, ne, spread, cid, after=None):
    rounds = nz if spread else 1
    _, count, width = parts.shape
    half = count // 2
    held = (2 * rounds * (ne // 2 + ne - 1) + 2 * nz) * half * width * 2
    if held > 56_000_000:
        cut = width // 256 * 128
        left = scatter_tokens(parts[..., :cut], nz, ne, spread, cid, after)
        right = scatter_tokens(parts[..., cut:], nz, ne, spread, cid + 16)
        return [jnp.concatenate([left[0], right[0]], axis=1), *left[1:]]
    more = [] if after is None else [after]
    return pl.pallas_call(
        functools.partial(scatter_kernel, nz, ne, spread),
        out_shape=[jax.ShapeDtypeStruct(m.shape, m.dtype) for m in more]
        + [jax.ShapeDtypeStruct((count, width), F32)],
        in_specs=[ANY] * (1 + len(more)),
        out_specs=[ANY] * len(more) + [VMEM],
        scratch_shapes=[
            pltpu.VMEM((rounds, 2, ne // 2, half, width), BF),
            pltpu.VMEM((rounds, 2, ne - 1, half, width), BF),
            pltpu.VMEM((nz, 2, half, width), BF),
            DMA((rounds, 2, ne // 2)),
            DMA((rounds, 2, ne - 1)),
            DMA((rounds, 2, ne - 1)),
            DMA((nz, 2)),
            DMA((nz, 2)),
        ],
        input_output_aliases={1: 0} if more else {},
        compiler_params=pltpu.CompilerParams(
            collective_id=cid, has_side_effects=True, vmem_limit_bytes=64_000_000
        ),
        name="scatter_tokens",
    )(parts, *more)[::-1]


def start_kernel(
    nz, ne, x_ref, wqkv_ref, wout_ref, small_ref, seg_ref, _,
    out_ref, wq_ref, wo_ref, small_out, seg_out, _2,
    wbuf, pbuf, zsend, zrecv, send, recv, local,
    up_send, up_recv, dn_send, dn_recv, wload, wkeep, pload, psend, precv, pkeep,
    small_send, small_recv, seg_send, seg_recv,
):
    z, e = lax.axis_index("dp"), lax.axis_index("expert")
    kinds, depth, hw = wbuf.shape
    per = ne // nz
    loads = [
        pltpu.make_async_copy(wqkv_ref.at[j, :, pl.ds(e * hw, hw)], wbuf.at[j], wload.at[j])
        for j in range(kinds)
    ]
    for copy in loads:
        copy.start()
    pieces = [
        pltpu.make_async_copy(
            wout_ref.at[pl.ds(i * hw, hw), pl.ds(e * hw, hw)], pbuf.at[i], pload.at[i]
        )
        for i in range(per)
    ]
    for copy in pieces:
        copy.start()
    meet_all(nz, ne, z, e)

    def rows_of(zz):
        return pl.ds(pl.multiple_of(zz * depth, depth), depth)

    def hop(j, zz, dist, up):
        send, recv = (up_send, up_recv) if up else (dn_send, dn_recv)
        here = wq_ref.at[j, rows_of(zz)]
        src = wbuf.at[j] if dist == 1 else here
        to = z + 1 if up else z - 1
        return remote(src, here, send.at[dist, j], recv.at[dist, j], (to, e))

    keeps = []
    for j in range(kinds):
        loads[j].wait()

        @pl.when(z + 1 < nz)
        def _():
            hop(j, z, 1, True).start()

        @pl.when(z > 0)
        def _():
            hop(j, z, 1, False).start()

        keep = pltpu.make_async_copy(wbuf.at[j], wq_ref.at[j, rows_of(z)], wkeep.at[j])
        keep.start()
        keeps.append(keep)

    def wait_all(ref, send, recv, count):
        most = ref.at[pl.ds(0, count)]
        both = remote(most, most, send, recv, (z, flip(e, 1)))
        both.wait_send()
        both.wait_recv()

    small_out[z] = small_ref[...]
    for r in range(1, nz):
        remote(
            small_ref, small_out.at[z], small_send, small_recv, (lax.rem(z + r, nz), e)
        ).start()
    seg_out[e] = seg_ref[...]
    for r in range(1, ne):
        remote(seg_ref, seg_out.at[e], seg_send, seg_recv, (z, lax.rem(e + r, ne))).start()
    net = PlaneGather(nz, ne, z, e, False, x_ref, out_ref, zsend, zrecv, send, recv, local)
    net.start_round(0)

    columns = pl.ds(e * hw, hw)
    for i in range(per):
        pieces[i].wait()
    for r in range(nz):
        for i in range(per):
            to = (lax.rem(z + r, nz), z * per + i)
            give = remote(pbuf.at[i], wo_ref.at[:, columns], psend.at[r, i], precv, to)
            if r > 0:
                give.start()
            else:
                own = pltpu.make_async_copy(pbuf.at[i], wo_ref.at[:, columns], pkeep)

                @pl.when(to[1] == e)
                def _():
                    own.start()

                @pl.when(to[1] != e)
                def _():
                    give.start()
    net.finish_round(0)
    for dist in range(1, nz):
        for j in range(kinds):

            @pl.when(z - dist >= 0)
            def _():
                got = wq_ref.at[j, rows_of(z - dist)]
                remote(got, got, up_send.at[dist, j], up_recv.at[dist, j], (z, e)).wait_recv()

                @pl.when(z + 1 < nz)
                def _():
                    if dist + 1 < nz:
                        hop(j, z - dist, dist + 1, True).start()

            @pl.when(z + dist < nz)
            def _():
                got = wq_ref.at[j, rows_of(z + dist)]
                remote(got, got, dn_send.at[dist, j], dn_recv.at[dist, j], (z, e)).wait_recv()

                @pl.when(z > 0)
                def _():
                    if dist + 1 < nz:
                        hop(j, z + dist, dist + 1, False).start()

    net.finish()
    for keep in keeps:
        keep.wait()
    for dist in range(1, nz):
        for j in range(kinds):

            @pl.when((z - dist + 1 >= 0) & (z + 1 < nz))
            def _():
                hop(j, z - dist + 1, dist, True).wait_send()

            @pl.when((z + dist - 1 < nz) & (z > 0))
            def _():
                hop(j, z + dist - 1, dist, False).wait_send()

    for r in range(nz):
        for i in range(per):
            to = (lax.rem(z + r, nz), z * per + i)
            give = remote(pbuf.at[i], wo_ref.at[:, columns], psend.at[r, i], precv, to)
            if r > 0:
                give.wait_send()
            else:
                own = pltpu.make_async_copy(pbuf.at[i], wo_ref.at[:, columns], pkeep)

                @pl.when(to[1] == e)
                def _():
                    own.wait()

                @pl.when(to[1] != e)
                def _():
                    give.wait_send()

    def wait_pieces(count):
        most = wo_ref.at[:, pl.ds(0, count * hw)]
        remote(most, most, psend.at[0, 0], precv, (z, e)).wait_recv()

    @pl.when(z == e // per)
    def _():
        wait_pieces(ne - 1)

    @pl.when(z != e // per)
    def _():
        wait_pieces(ne)

    wait_all(small_out, small_send, small_recv, nz - 1)
    wait_all(seg_out, seg_send, seg_recv, ne - 1)


def start_gather(x, w_qkv, w_out, small, seg, after, nz, ne, hw, cid):
    kinds, depth, width = w_qkv.shape
    per = ne // nz
    return pl.pallas_call(
        functools.partial(start_kernel, nz, ne),
        out_shape=[
            jax.ShapeDtypeStruct((ne, *x.shape), x.dtype),
            jax.ShapeDtypeStruct((kinds, nz * depth, hw), BF),
            jax.ShapeDtypeStruct((hw, width), BF),
            jax.ShapeDtypeStruct((nz, *small.shape), small.dtype),
            jax.ShapeDtypeStruct((ne, *seg.shape), seg.dtype),
            jax.ShapeDtypeStruct(after.shape, after.dtype),
        ],
        in_specs=[VMEM, ANY, ANY, VMEM, VMEM, ANY],
        out_specs=[ANY, ANY, ANY, VMEM, VMEM, ANY],
        input_output_aliases={5: 5},
        scratch_shapes=[
            pltpu.VMEM((kinds, depth, hw), BF),
            pltpu.VMEM((per, hw, hw), BF),
            *PlaneGather.scratch(nz, ne, False),
            DMA((nz, kinds)), DMA((nz, kinds)), DMA((nz, kinds)), DMA((nz, kinds)),
            DMA((kinds,)), DMA((kinds,)), DMA((per,)), DMA((nz, per)), DMA, DMA,
            DMA, DMA, DMA, DMA,
        ],
        compiler_params=pltpu.CompilerParams(collective_id=cid, has_side_effects=True),
        name="start_gather",
    )(x, w_qkv, w_out, small, seg, after)


def rope_lanes(length):
    half = HD // 2
    freqs = jnp.exp(-jnp.log(ROPE_BASE) * (2.0 * jnp.arange(half, dtype=F32) / HD))
    angles = jnp.arange(length, dtype=F32)[:, None] * freqs[None, :]
    cos, sin = jnp.cos(angles), jnp.sin(angles)
    return jnp.concatenate([cos, cos], axis=1), jnp.concatenate([-sin, sin], axis=1)


def turn(x, cos, sin):
    return x * cos + pltpu.roll(x, HD // 2, 1) * sin


def meet_plane(ne, z, e):
    sem = pltpu.get_barrier_semaphore()
    for r in range(1, ne):
        pl.semaphore_signal(
            sem, inc=1, device_id=(z, lax.rem(e + r, ne)), device_id_type=MESH
        )
    pl.semaphore_wait(sem, ne - 1)


def plane_totals(ne, z, e, mine, theirs, send, recv):
    copies = []
    for r in range(1, ne):
        to = (z, lax.rem(e + r, ne))
        copy = remote(mine, theirs.at[r], send.at[r], recv.at[r], to)
        copy.start()
        copies.append(copy)
    total = mine[...]
    for r, copy in enumerate(copies):
        copy.wait_recv()
        total = total + theirs[r + 1]
    for copy in copies:
        copy.wait_send()
    return total


def store_columns(sums, first, columns):
    rows = columns[0].shape[0]
    lanes = lax.broadcasted_iota(jnp.int32, (rows, 128), 1)
    wide = jnp.zeros((rows, 128), F32)
    for j, column in enumerate(columns):
        wide = jnp.where(lanes == j, column, wide)
    sums[:, pl.ds(first, rows)] = wide.T[:8]


def as_columns(total, out):
    rows = total.shape[1]
    for first in range(0, rows, 128):
        chunk = total[:, first : first + 128]
        out[first : first + 128, :] = jnp.concatenate([chunk] * 16, axis=0).T


def allowed_pairs(seg_ref, n):
    length = seg_ref.shape[2]
    keys = jnp.broadcast_to(seg_ref[n, :1].astype(F32), (length, length))
    i = lax.broadcasted_iota(jnp.int32, (length, length), 0)
    j = lax.broadcasted_iota(jnp.int32, (length, length), 1)
    return (i >= j) & (keys == keys.T)


def attend(rq, rk, allowed):
    scores = jnp.where(allowed, dot(rq, rk, NT) * HD ** (-0.5), MASKED)
    top = jnp.max(scores, axis=-1, keepdims=True)
    lse = top + jnp.log(jnp.sum(jnp.exp(scores - top), axis=-1, keepdims=True))
    return jnp.exp(scores - lse)


def attn_fwd_kernel(
    ne, x_ref, wq_ref, wo_ref, gain_ref, mine_ref, seg_ref, cos_ref, sin_ref,
    h1_ref, q_ref, k_ref, rq_ref, rk_ref, v_ref, o_ref, scale_ref, x1_ref,
    sums, theirs, send, recv,
):
    z, e = lax.axis_index("dp"), lax.axis_index("expert")
    width = x_ref.shape[2]
    count, hw = q_ref.shape
    length = seg_ref.shape[2]
    rows_dev = x_ref.shape[1]
    tile = min(512, count)
    meet_plane(ne, z, e)

    def normed(b, carry):
        x = x_ref[b].astype(F32)
        h1 = x * rms_scale(x) * gain_ref[:1]
        h1_ref[pl.ds(pl.multiple_of(b * rows_dev, rows_dev), rows_dev), :] = h1.astype(BF)
        return carry

    lax.fori_loop(0, ne, normed, 0)
    for first in range(0, count, tile):
        rows = slice(first, first + tile)
        h1 = h1_ref[rows, :]
        q, k = dot(h1, wq_ref[0], NN), dot(h1, wq_ref[1], NN)
        q_ref[rows, :] = q
        k_ref[rows, :] = k
        v_ref[rows, :] = dot(h1, wq_ref[2], NN).astype(BF)
        store_columns(
            sums, first, [jnp.sum(t * t, axis=-1, keepdims=True) for t in (q, k)]
        )
    total = plane_totals(ne, z, e, sums, theirs, send, recv)
    as_columns(lax.rsqrt(total / width + EPS), scale_ref)
    cos, sin = cos_ref[...], sin_ref[...]

    def sequence(n, carry):
        rows = pl.ds(pl.multiple_of(n * length, length), length)
        allowed = allowed_pairs(seg_ref, n)
        aq, ak = scale_ref[rows, 0:1], scale_ref[rows, 1:2]
        for c in range(0, hw, HD):
            cols = slice(c, c + HD)
            rq = turn(q_ref[rows, cols] * aq * mine_ref[1:2, cols], cos, sin).astype(BF)
            rk = turn(k_ref[rows, cols] * ak * mine_ref[2:3, cols], cos, sin).astype(BF)
            rq_ref[rows, cols] = rq
            rk_ref[rows, cols] = rk
            probs = attend(rq, rk, allowed).astype(BF)
            o_ref[rows, cols] = dot(probs, v_ref[rows, cols], NN).astype(BF)
        return carry

    lax.fori_loop(0, count // length, sequence, 0)
    for first in range(0, count, tile):
        x1 = dot(o_ref[first : first + tile, :], wo_ref[...], NN).astype(BF)
        blocks = tile // rows_dev
        x1_ref[first // rows_dev : first // rows_dev + blocks] = x1.reshape(
            blocks, rows_dev, width
        )


def attn_fwd(in_all, wq, wo, gain_mat, my_gains, seg, tables, cid):
    ne, rows_dev, width = in_all.shape
    count, hw = ne * rows_dev, wo.shape[0]
    return pl.pallas_call(
        functools.partial(attn_fwd_kernel, ne),
        out_shape=[
            jax.ShapeDtypeStruct((count, width), BF),
            jax.ShapeDtypeStruct((count, hw), F32),
            jax.ShapeDtypeStruct((count, hw), F32),
            jax.ShapeDtypeStruct((count, hw), BF),
            jax.ShapeDtypeStruct((count, hw), BF),
            jax.ShapeDtypeStruct((count, hw), BF),
            jax.ShapeDtypeStruct((count, hw), BF),
            jax.ShapeDtypeStruct((count, 128), F32),
            jax.ShapeDtypeStruct((ne, rows_dev, width), BF),
        ],
        in_specs=[VMEM] * 8,
        out_specs=[VMEM] * 9,
        scratch_shapes=[
            pltpu.VMEM((8, count), F32), pltpu.VMEM((ne, 8, count), F32), DMA((ne,)), DMA((ne,)),
        ],
        compiler_params=pltpu.CompilerParams(
            collective_id=cid, has_side_effects=True, vmem_limit_bytes=60_000_000
        ),
        name="attn_fwd",
    )(in_all, wq, wo, gain_mat, my_gains, seg, *tables)


def attn_bwd_kernel(
    ne, gab_ref, wq_ref, wo_ref, mine_ref, seg_ref, cos_ref, sin_ref,
    h1_ref, q_ref, k_ref, rq_ref, rk_ref, v_ref, o_ref, scale_ref,
    gh1_ref, parts_ref, gain_ref,
    pout, go_ref, gqn_ref, gkn_ref, gp_ref, sums, theirs, means, send, recv, psend, precv,
):
    z, e = lax.axis_index("dp"), lax.axis_index("expert")
    count, hw = q_ref.shape
    width = gab_ref.shape[2]
    rows_dev = gab_ref.shape[1]
    length = seg_ref.shape[2]
    tile = min(512, count)
    blocks = tile // rows_dev
    meet_plane(ne, z, e)

    gab = lambda first: gab_ref[first // rows_dev : first // rows_dev + blocks].reshape(tile, width)
    part = dot(o_ref[:tile, :], gab(0), TN)
    for first in range(tile, count, tile):
        part = part + dot(o_ref[first : first + tile, :], gab(first), TN)
    pout[...] = part.astype(BF)
    for first in range(0, count, tile):
        go_ref[first : first + tile, :] = dot(gab(first), wo_ref[...], NT).astype(BF)
    my_rows = pl.ds(pl.multiple_of(e * hw, hw), hw)
    last = pl.ds(3 * hw, hw)
    gives = []
    for r in range(1, ne):
        to = lax.rem(e + r, ne)
        give = remote(
            pout.at[:, pl.ds(pl.multiple_of(to * hw, hw), hw)], parts_ref.at[my_rows, last],
            psend.at[r], precv.at[r], (z, to),
        )
        give.start()
        gives.append(give)
    parts_ref[my_rows, last] = pout[:, my_rows]

    cos, sin = cos_ref[...], -sin_ref[...]
    gain_ref[...] = jnp.zeros_like(gain_ref)

    def sequence(n, carry):
        start = pl.multiple_of(n * length, length)
        rows = pl.ds(start, length)
        allowed = allowed_pairs(seg_ref, n)
        aq, ak = scale_ref[rows, 0:1], scale_ref[rows, 1:2]
        sum_q = jnp.zeros((length, 1), F32)
        sum_k = jnp.zeros((length, 1), F32)
        for c in range(0, hw, HD):
            cols = slice(c, c + HD)
            rq, rk, go = rq_ref[rows, cols], rk_ref[rows, cols], go_ref[rows, cols]
            probs = attend(rq, rk, allowed)
            gv = dot(probs.astype(BF), go, TN).astype(BF)
            gp_ref[rows, slice(2 * hw + c, 2 * hw + c + HD)] = gv
            grad = dot(go, v_ref[rows, cols], NT)
            delta = jnp.sum(probs * grad, axis=-1, keepdims=True)
            gs = (probs * (grad - delta) * HD ** (-0.5)).astype(BF)
            gqn = turn(dot(gs, rk, NN), cos, sin)
            gkn = turn(dot(gs, rq, TN), cos, sin)
            gqn_ref[rows, cols] = gqn
            gkn_ref[rows, cols] = gkn
            tq = gqn * (q_ref[rows, cols] * aq)
            tk = gkn * (k_ref[rows, cols] * ak)
            gain_ref[0:1, cols] += jnp.sum(tq, axis=0, keepdims=True)
            gain_ref[1:2, cols] += jnp.sum(tk, axis=0, keepdims=True)
            sum_q = sum_q + jnp.sum(tq * mine_ref[1:2, cols], axis=-1, keepdims=True)
            sum_k = sum_k + jnp.sum(tk * mine_ref[2:3, cols], axis=-1, keepdims=True)
        store_columns(sums, start, [sum_q, sum_k])
        return carry

    lax.fori_loop(0, count // length, sequence, 0)
    total = plane_totals(ne, z, e, sums, theirs, send, recv)
    as_columns(total / width, means)
    for first in range(0, count, tile):
        rows = slice(first, first + tile)
        aq, ak = scale_ref[rows, 0:1], scale_ref[rows, 1:2]
        mq, mk = means[rows, 0:1], means[rows, 1:2]
        gq = aq * (gqn_ref[rows, :] * mine_ref[1:2] - q_ref[rows, :] * aq * mq)
        gk = ak * (gkn_ref[rows, :] * mine_ref[2:3] - k_ref[rows, :] * ak * mk)
        gp_ref[rows, :hw] = gq.astype(BF)
        gp_ref[rows, hw : 2 * hw] = gk.astype(BF)
    for first in range(0, width, tile):
        rows = slice(first, first + tile)
        parts_ref[rows, : 3 * hw] = dot(h1_ref[:, rows], gp_ref[...], TN).astype(BF)
    for first in range(0, count, tile):
        rows = slice(first, first + tile)
        gh1 = dot(gp_ref[rows, :hw], wq_ref[0], NT)
        for j in range(1, 3):
            gh1 = gh1 + dot(gp_ref[rows, j * hw : (j + 1) * hw], wq_ref[j], NT)
        gh1_ref[first // rows_dev : first // rows_dev + blocks] = gh1.astype(BF).reshape(
            blocks, rows_dev, width
        )
    for give in gives:
        give.wait_send()
        give.wait_recv()


def attn_bwd(gab, wq, wo, my_gains, seg, tables, saved, cid):
    ne, rows_dev, width = gab.shape
    count, hw = ne * rows_dev, wo.shape[0]
    return pl.pallas_call(
        functools.partial(attn_bwd_kernel, ne),
        out_shape=[
            jax.ShapeDtypeStruct((ne, rows_dev, width), BF),
            jax.ShapeDtypeStruct((width, 4 * hw), BF),
            jax.ShapeDtypeStruct((8, hw), F32),
        ],
        in_specs=[VMEM] * 15,
        out_specs=[VMEM] * 3,
        scratch_shapes=[
            pltpu.VMEM((hw, width), BF),
            pltpu.VMEM((count, hw), BF),
            pltpu.VMEM((count, hw), F32),
            pltpu.VMEM((count, hw), F32),
            pltpu.VMEM((count, 3 * hw), BF),
            pltpu.VMEM((8, count), F32),
            pltpu.VMEM((ne, 8, count), F32),
            pltpu.VMEM((count, 128), F32),
            DMA((ne,)), DMA((ne,)), DMA((ne,)), DMA((ne,)),
        ],
        compiler_params=pltpu.CompilerParams(
            collective_id=cid, has_side_effects=True, vmem_limit_bytes=64_000_000
        ),
        name="attn_bwd",
    )(gab, wq, wo, my_gains, seg, *tables, *saved)


class PlaneScatter:
    def __init__(self, ne, z, e, x_ref, acc, got, loads, send, recv):
        self.ne, self.z, self.e = ne, z, e
        self.x, self.acc, self.got = x_ref, acc, got
        self.loads, self.send, self.recv = loads, send, recv
        self.half = acc.shape[2]
        self.stages = ne.bit_length() - 1
        self.orders = bit_orders(ne)
        self.first = [0]
        for j in range(self.stages):
            self.first.append(self.first[j] + (ne >> (j + 1)))
        self.pending, self.arrivals = [], {}

    def push(self, s, j):
        order = self.orders[s]
        peer_e = flip(self.e, order[j])
        rest = self.ne >> (j + 1)
        for i in range(rest):
            n = self.first[j] + i
            if j == 0:
                block = flips(peer_e, order[:0:-1])[i]
                src = self.x.at[block, pl.ds(s * self.half, self.half)]
            else:
                src = self.acc.at[s, rest + i]
            copy = remote(
                src, self.got.at[s, n], self.send.at[s, n], self.recv.at[s, n], (self.z, peer_e)
            )
            copy.start()
            self.pending.append(copy.wait_send)
            self.arrivals.setdefault((s, j), []).append((copy.wait_recv, i, n))

    def start(self):
        for s in range(2):
            self.push(s, 0)
            for i, block in enumerate(flips(self.e, self.orders[s][:0:-1])):
                copy = pltpu.make_async_copy(
                    self.x.at[block, pl.ds(s * self.half, self.half)],
                    self.acc.at[s, i],
                    self.loads.at[s, i],
                )
                copy.start()
                self.arrivals.setdefault((s, -1), []).append(copy.wait)

    def stage(self, j):
        for s in range(2):
            if j == 0:
                for wait in self.arrivals.pop((s, -1)):
                    wait()
            for wait, i, n in self.arrivals.pop((s, j)):
                wait()
                add_rows(self.acc.at[s, i], self.got.at[s, n])
            if j + 1 < self.stages:
                self.push(s, j + 1)

    def finish(self):
        for wait in self.pending:
            wait()


def tail_kernel(
    nz, ne, kinds, gain_row, parts_ref, gh1_ref, x_ref, gx1_ref, gain_ref, tiny_ref,
    grad_ref, laid_ref, small_ref,
    work, below, above, wide, acc, got, gsum, tbuf, tgot, total, far,
    wload, usend, urecv, dsend, drecv, zsend, zrecv, gsend, grecv, glocal,
    hload, hsend, hrecv, flush, send1, recv1, send2, recv2,
):
    z, e = lax.axis_index("dp"), lax.axis_index("expert")
    per = ne // nz
    chunks, rows = work.shape[1], work.shape[2]
    hw = work.shape[3] // kinds
    width = x_ref.shape[1]
    loads = [
        pltpu.make_async_copy(
            parts_ref.at[pl.ds((t * chunks + c) * rows, rows)], work.at[t, c], wload.at[t, c]
        )
        for c in range(chunks)
        for t in range(nz)
    ]
    for copy in loads:
        copy.start()
    meet_all(nz, ne, z, e)
    mine = PlaneScatter(ne, z, e, gh1_ref, acc, got, hload, hsend, hrecv)
    mine.start()
    for copy in loads:
        copy.wait()

    def rise(t, c):
        return remote(
            work.at[t, c], below.at[t, c], usend.at[t, c], urecv.at[t, c], (z + 1, e)
        )

    def sink(t, c):
        return remote(
            work.at[t, c], above.at[t, c], dsend.at[t, c], drecv.at[t, c], (z - 1, e)
        )

    for c in range(chunks):
        for t in range(nz - 1, 0, -1):

            @pl.when(z == 0)
            def _():
                rise(t, c).start()

        for t in range(nz - 1):

            @pl.when(z == nz - 1)
            def _():
                sink(t, c).start()

    def arrive(t, c, buffer, recv):
        remote(buffer.at[t, c], buffer.at[t, c], usend.at[0, 0], recv.at[t, c], (z, e)).wait_recv()
        add_rows(work.at[t, c], buffer.at[t, c])

    def line(t):
        for p in range(nz):

            @pl.when(z == p)
            def _():
                c = t - (p - 1)
                if p > 0 and 0 <= c < chunks:
                    for target in range(nz - 1, p - 1, -1):
                        arrive(target, c, below, urecv)
                        if target > p:
                            rise(target, c).start()
                c = t - (nz - 2 - p)
                if p < nz - 1 and 0 <= c < chunks:
                    for target in range(p + 1):
                        arrive(target, c, above, drecv)
                        if target < p:
                            sink(target, c).start()

    def spread(c):
        net = PlaneGather(
            nz, ne, z, e, False, work.at[z, c], wide.at[c], zsend, zrecv,
            gsend.at[c], grecv.at[c], glocal.at[c],
        )
        net.start_round(0)
        return net

    def outs(c):
        span = pl.ds(c * rows, rows)
        copies = []
        for n in range(ne):
            for j in range(kinds):
                copies.append(
                    pltpu.make_async_copy(
                        wide.at[c, n, :, pl.ds(j * hw, hw)],
                        laid_ref.at[j, span, pl.ds(n * hw, hw)],
                        flush.at[c, n, j],
                    )
                )
        return copies

    def lay(c, net):
        net.finish_round(0)
        net.finish()
        for copy in outs(c):
            copy.start()

    mine.stage(0)
    line(0)
    for j in range(1, mine.stages):
        mine.stage(j)
    line(1)
    nets = {}

    def advance(t):
        c = t - max(nz - 2, 0)
        if 0 <= c < chunks:
            nets[c] = spread(c)
        if c - 1 in nets:
            lay(c - 1, nets.pop(c - 1))

    advance(0)
    advance(1)

    half = acc.shape[2]
    gsum[...] = jnp.zeros_like(gsum)
    for s in range(2):

        def front(n, carry):
            here = pl.ds(pl.multiple_of(n * 16, 16), 16)
            span = pl.ds(pl.multiple_of(s * half + n * 16, 16), 16)
            grad = acc[s, 0, here, :].astype(F32)
            x = x_ref[span, :].astype(F32)
            scale = rms_scale(x)
            normed = x * scale
            gsum[...] += grad * normed
            scaled = grad * gain_ref[:1]
            inner = jnp.mean(scaled * normed, axis=-1, keepdims=True)
            grad_ref[span, :] = (gx1_ref[span, :] + scale * (scaled - normed * inner)).astype(BF)
            return carry

        lax.fori_loop(0, half // 16, front, 0)
    tbuf[...] = tiny_ref[...]
    tbuf[gain_row : gain_row + 1, :] = jnp.sum(gsum[...], axis=0, keepdims=True)

    cw = width // ne
    block = lambda ee: pl.ds(pl.multiple_of(ee * cw, cw), cw)
    first = []
    for r in range(1, ne):
        to = lax.rem(e + r, ne)
        copy = remote(tbuf.at[:, block(to)], tgot.at[r], send1.at[r], recv1.at[r], (z, to))
        copy.start()
        first.append(copy)
    line(2)
    advance(2)
    sums = tbuf[:, block(e)]
    for r, copy in enumerate(first):
        copy.wait_recv()
        sums = sums + tgot[r + 1]
    total[...] = sums
    home, place = e // per, lax.rem(e, per)

    def give(r):
        to = lax.rem(e + r, ne)
        return remote(total, far.at[z, place], send2.at[r], recv2, (home, to))

    for r in range(ne):
        if r > 0:
            give(r).start()
        else:

            @pl.when(home != z)
            def _():
                give(0).start()

            @pl.when(home == z)
            def _():
                far[z, place] = total[...]

    for t in range(3, chunks + nz):
        line(t)
        advance(t)
    for copy in first:
        copy.wait_send()

    def arrived(count):
        flat = tgot.at[pl.ds(0, count)]
        remote(flat, flat, send2.at[0], recv2, (z, e)).wait_recv()

    for r in range(ne):
        if r > 0:
            give(r).wait_send()
        else:

            @pl.when(home != z)
            def _():
                give(0).wait_send()
                arrived(nz * per)

            @pl.when(home == z)
            def _():
                arrived(nz * per - 1)

    for i in range(per):
        small_ref[i] = sum(far[k, i] for k in range(nz))
    mine.finish()
    for c in range(chunks):
        for t in range(nz):

            @pl.when(z < t)
            def _():
                rise(t, c).wait_send()

            @pl.when(z > t)
            def _():
                sink(t, c).wait_send()

    for c in range(chunks):
        for copy in outs(c):
            copy.wait()


def tail(parts, gh1_part, x, gx1, gain_mat, tiny, gain_row, nz, ne, hw, cid):
    width, total_cols = parts.shape
    kinds = total_cols // hw
    count = x.shape[0]
    depth = width // nz
    rows = min(128, depth)
    chunks = depth // rows
    small_rows, cw = tiny.shape[0], width // ne
    per = ne // nz
    block = (nz, chunks, rows, total_cols)
    out = pl.pallas_call(
        functools.partial(tail_kernel, nz, ne, kinds, gain_row),
        out_shape=[
            jax.ShapeDtypeStruct((count, width), BF),
            jax.ShapeDtypeStruct((kinds, depth, width), BF),
            jax.ShapeDtypeStruct((per, small_rows, cw), F32),
        ],
        in_specs=[ANY, ANY, VMEM, VMEM, VMEM, VMEM],
        out_specs=[VMEM, ANY, VMEM],
        scratch_shapes=[
            pltpu.VMEM(block, BF), pltpu.VMEM(block, BF), pltpu.VMEM(block, BF),
            pltpu.VMEM((chunks, ne, rows, total_cols), BF),
            pltpu.VMEM((2, ne // 2, count // 2, width), BF),
            pltpu.VMEM((2, ne - 1, count // 2, width), BF),
            pltpu.VMEM((16, width), F32),
            pltpu.VMEM((small_rows, width), F32),
            pltpu.VMEM((max(ne, nz * per), small_rows, cw), F32),
            pltpu.VMEM((small_rows, cw), F32),
            pltpu.VMEM((nz, per, small_rows, cw), F32),
            DMA((nz, chunks)),
            DMA((nz, chunks)), DMA((nz, chunks)), DMA((nz, chunks)), DMA((nz, chunks)),
            DMA((nz,)), DMA((nz,)),
            DMA((chunks, 1, 2, ne - 1)), DMA((chunks, 1, 2, ne - 1)), DMA((chunks,)),
            DMA((2, ne // 2)), DMA((2, ne - 1)), DMA((2, ne - 1)),
            DMA((chunks, ne, kinds)),
            DMA((ne,)), DMA((ne,)), DMA((ne,)), DMA,
        ],
        compiler_params=pltpu.CompilerParams(
            collective_id=cid, has_side_effects=True, vmem_limit_bytes=64_000_000
        ),
        name="tail",
    )(parts, gh1_part, x, gx1, gain_mat, tiny)
    *out, small = out
    return *out, small.transpose(1, 0, 2).reshape(small_rows, per * cw)


def add_kernel(x_ref, y_ref, out_ref):
    out_ref[...] = (x_ref[...] + y_ref[...].astype(F32)).astype(out_ref.dtype)


def add_up(x, y):
    return pl.pallas_call(
        add_kernel, out_shape=jax.ShapeDtypeStruct(y.shape, y.dtype), name="add_up"
    )(x, y)


def lay_experts_kernel(per_dev, fl, x_ref, gate_ref, up_ref):
    for i in range(per_dev):
        gate_ref[i] = x_ref[0, :, i * fl : (i + 1) * fl].astype(F32)
        up_ref[i] = x_ref[0, :, (per_dev + i) * fl : (per_dev + i + 1) * fl].astype(F32)


def lay_experts(wide, per_dev, fl):
    nz, rows, _ = wide.shape
    out = jax.ShapeDtypeStruct((per_dev, rows, nz * fl), F32)
    spec = pl.BlockSpec((per_dev, rows, fl), lambda i: (0, 0, i))
    return pl.pallas_call(
        functools.partial(lay_experts_kernel, per_dev, fl),
        grid=(nz,),
        in_specs=[pl.BlockSpec((1, rows, 2 * per_dev * fl), lambda i: (i, 0, 0))],
        out_specs=[spec, spec],
        out_shape=[out, out],
        name="lay_experts",
    )(wide)


def moe_kernel(
    fl, h_ref, g_ref, win_ref, wd_ref,
    mix_ref, gh_ref, dwin_ref, dwd_ref, acc_in, acc_d,
):
    step = pl.program_id(0)
    tile, width = g_ref.shape
    per_dev = wd_ref.shape[0] // fl
    e = lax.axis_index("expert")
    h = h_ref[:, :width]
    g = g_ref[...]
    extra = h_ref[:, width:].astype(F32)
    pre = dot(h, win_ref[...], NN)
    graw = dot(g, wd_ref[...], NT)
    scaled_act, grad_gate, grad_up = [], [], []
    lanes = lax.broadcasted_iota(jnp.int32, (tile, 128), 1)
    gg = jnp.zeros((tile, 128), F32)
    split = 64
    for i in range(per_dev):
        u = pre[:, i * fl : (i + 1) * fl]
        w = pre[:, (per_dev + i) * fl : (per_dev + 1 + i) * fl]
        gr = graw[:, i * fl : (i + 1) * fl]
        mine = e * per_dev + i
        picked = (lanes == mine) | (lanes == mine + split)
        gate = jnp.sum(jnp.where(picked, extra, 0.0), axis=-1, keepdims=True)
        sig = 1.0 / (1.0 + jnp.exp(-u))
        silu = u * sig
        act = silu * w
        total = jnp.sum(act.astype(BF).astype(F32) * gr, axis=-1, keepdims=True)
        rounded = total.astype(BF).astype(F32)
        gg = jnp.where(lanes == mine, rounded, gg)
        gg = jnp.where(lanes == mine + split, total - rounded, gg)
        scaled_act.append((gate * act).astype(BF))
        gact = gate * gr
        grad_gate.append((gact * w * (sig * (1.0 + u * (1.0 - sig)))).astype(BF))
        grad_up.append((gact * silu).astype(BF))
    a = jnp.concatenate(scaled_act, axis=1)
    gin = jnp.concatenate(grad_gate + grad_up, axis=1)
    mix_ref[...] = dot(a, wd_ref[...], NN).astype(BF)
    gh_ref[:, :width] = dot(gin, win_ref[...], NT).astype(BF)
    gh_ref[:, width:] = gg.astype(BF)

    @pl.when(step == 0)
    def _():
        acc_in[...] = jnp.zeros_like(acc_in)
        acc_d[...] = jnp.zeros_like(acc_d)

    acc_in[...] += dot(h, gin, TN)
    acc_d[...] += dot(a, g, TN)

    @pl.when(step == pl.num_programs(0) - 1)
    def _():
        dwin_ref[...] = acc_in[...].astype(BF)
        dwd_ref[...] = acc_d[...]


def moe(h_all, g_all, w_in, wd, per_dev, rows_dev, blocks):
    count, width = g_all.shape
    wide = h_all.shape[1]
    hid4 = w_in.shape[1]
    hid2 = wd.shape[0]
    fl = hid2 // per_dev
    tile = blocks * rows_dev
    rows = lambda n: pl.BlockSpec((tile, n), lambda i: (i, 0))
    whole = lambda s: pl.BlockSpec(s, lambda i: (0, 0), pipeline_mode=pl.Buffered(1))
    return pl.pallas_call(
        functools.partial(moe_kernel, fl),
        grid=(count // tile,),
        in_specs=[
            rows(wide), rows(width),
            whole(w_in.shape), whole(wd.shape),
        ],
        out_specs=[
            rows(width),
            rows(wide),
            whole((width, hid4)), whole((hid2, width)),
        ],
        out_shape=[
            jax.ShapeDtypeStruct((count, width), BF),
            jax.ShapeDtypeStruct((count, wide), BF),
            jax.ShapeDtypeStruct((width, hid4), BF),
            jax.ShapeDtypeStruct((hid2, width), F32),
        ],
        scratch_shapes=[pltpu.VMEM((width, hid4), F32), pltpu.VMEM((hid2, width), F32)],
        compiler_params=pltpu.CompilerParams(vmem_limit_bytes=66_000_000),
        cost_estimate=pl.CostEstimate(
            flops=2 * count * width * hid2 * 9,
            bytes_accessed=8 * count * width + 24 * hid4 * width,
            transcendentals=count * hid2,
        ),
        name="moe",
    )(h_all, g_all, w_in, wd)


def moe_net_kernel(
    nz, ne, per_dev, slots, h_ref, g_ref, wg_ref, wu_ref, wd_ref,
    hall_ref, mix_ref, gh_ref, dwin_ref, dwd_ref,
    win, wd, acc_in, acc_d, htile, gtile, mixbuf, qbuf, cgot, acc, got, zgot, dbuf,
    wload, tload, mixsem, keep, flush, zsend, zrecv, send, recv,
    csend, crecv, credit, rsend, rrecv, ysend, yrecv,
):
    z, e = lax.axis_index("dp"), lax.axis_index("expert")
    rows, width = g_ref.shape[1], g_ref.shape[2]
    half = rows // 2
    fl = wd.shape[0] // per_dev
    upper = [2 << b for b in range(ne.bit_length() - 2)]
    stages = len(upper)
    pairs = ne // 2
    steps = nz * pairs
    gather_orders = [upper + [1], upper[::-1] + [1]]
    sum_orders = [[1] + upper, [1] + upper[::-1]]
    at = [e]
    for bit in [1] + upper:
        at = at + [flip(i, bit) for i in at]
    partner = (z, at[1])

    def plane(r):
        low = jnp.minimum(z, nz - 1 - z)
        near = jnp.where(lax.rem(r, 2) == 1, z - (r + 1) // 2, z + r // 2)
        far = jnp.where(2 * z < nz, z + (r - low), z - (r - low))
        return jnp.where(r <= 2 * low, near, far)

    planes = [z] + [nearest(z, r, nz) for r in range(1, nz)]

    def part(s):
        return pl.ds(s * half, half)

    def subset_mask(order, subset):
        return sum(bit for b, bit in enumerate(order) if subset >> b & 1)

    def pass_on(r, s, stage, subset, own=False):
        order = gather_orders[s]
        dst = hall_ref.at[plane(r) * ne + at[subset_mask(order, subset)], part(s)]
        n = (1 << stage) - 1 + subset
        src = h_ref.at[part(s)] if own else dst
        return remote(src, dst, send.at[r, s, n], recv.at[r, s, n], (z, at[order[stage]]))

    def take(r, s, stage, subset):
        order = gather_orders[s]
        mask = subset_mask(order, subset) | order[stage]
        n = (1 << stage) - 1 + subset
        here = hall_ref.at[plane(r) * ne + at[mask], part(s)]
        remote(here, here, send.at[r, s, n], recv.at[r, s, n], partner).wait_recv()
        for later in range(stage + 1, stages + 1):
            pass_on(r, s, later, subset + (1 << stage)).start()

    def start_round(r):
        if r > 0:
            here = hall_ref.at[planes[r] * ne + e]
            remote(here, here, zsend.at[r], zrecv.at[planes[r]], partner).wait_recv()
        for stage in range(stages + 1):
            for s in range(2):
                pass_on(r, s, stage, 0, own=r == 0).start()

    def take_pair(r, i):
        if i == 1:
            for stage in range(stages):
                for s in range(2):
                    take(r, s, stage, 0)
        mask = 2 * i
        for s in range(2):
            order = gather_orders[s]
            places = [b for b in range(stages) if order[b] & mask]
            if len(places) > 1:
                take(r, s, places[-1], sum(1 << b for b in places[:-1]))
        for s in range(2):
            order = gather_orders[s]
            take(r, s, stages, sum(1 << b for b in range(stages) if order[b] & mask))

    def blocks_of(k):
        r, i = k // pairs, lax.rem(k, pairs)
        home = plane(r)
        lane = e
        for b, bit in enumerate(upper):
            lane = lane + lax.rem(i // (1 << b), 2) * (at[bit] - e)
        return home, lane, lane + (at[1] - e)

    def loads(k):
        home, one, two = blocks_of(k)
        p = lax.rem(k, 2)
        out = []
        for j, lane in enumerate((one, two)):
            to = pl.ds(j * rows, rows)
            block = home * ne + lane
            out.append(pltpu.make_async_copy(hall_ref.at[block], htile.at[p, to], tload.at[p, 2 * j]))
            out.append(
                pltpu.make_async_copy(g_ref.at[block], gtile.at[p, to], tload.at[p, 2 * j + 1])
            )
        return out

    def mix_out(k):
        home, one, two = blocks_of(k)
        p = lax.rem(k, 2)
        return [
            pltpu.make_async_copy(
                mixbuf.at[p, pl.ds(j * rows, rows)], mix_ref.at[home * ne + lane], mixsem.at[p, j]
            )
            for j, lane in enumerate((one, two))
        ]

    def to_partner(k):
        return remote(
            qbuf.at[lax.rem(k, 2)], cgot.at[lax.rem(k, slots)],
            csend.at[lax.rem(k, 2)], crecv.at[lax.rem(k, slots)], partner,
        )

    def place_of(t, keep_index):
        return (1 << stages) - (1 << (stages - t + 1)) + keep_index

    def push(r, s, t, keep_index):
        order = sum_orders[s]
        mask = order[t] | subset_mask(order[t + 1 :], keep_index)
        n = place_of(t, keep_index)
        return remote(
            acc.at[r, mask // 2, part(s)], got.at[r, s, n],
            rsend.at[r, s, n], rrecv.at[r, s, n], (z, at[order[t]]),
        )

    def merge(k):
        slot = lax.rem(k, slots)
        remote(cgot.at[slot], cgot.at[slot], csend.at[0], crecv.at[slot], partner).wait_recv()
        r, i = k // pairs, lax.rem(k, pairs)
        add_rows(acc.at[r, i], cgot.at[slot])

        @pl.when(k + slots < steps)
        def _():
            pl.semaphore_signal(credit, inc=1, device_id=partner, device_id_type=MESH)

        for j in range(1, pairs):

            @pl.when(i == j)
            def _():
                for s in range(2):
                    order = sum_orders[s]
                    if order[1] & (2 * j):
                        rest = [b for b, bit in enumerate(order[2:]) if bit & (2 * j)]
                        push(r, s, 1, sum(1 << b for b in rest)).start()

    def home_copy(r, s):
        return remote(
            acc.at[r, 0, part(s)], zgot.at[z, part(s)], ysend.at[r, s], yrecv.at[z, s],
            (plane(r), e),
        )

    def settle(r, t):
        for s in range(2):
            order = sum_orders[s]
            for index in range(1 << (stages - t)):
                copy = push(r, s, t, index)
                copy.wait_recv()
                mask = subset_mask(order[t + 1 :], index)
                add_rows(acc.at[r, mask // 2, part(s)], got.at[r, s, place_of(t, index)])
            if t < stages:
                for index in range(1 << (stages - t - 1)):
                    push(r, s, t + 1, index).start()
            else:

                @pl.when(r > 0)
                def _():
                    home_copy(r, s).start()

    weights = []
    for i in range(per_dev):
        cols = pl.ds(z * fl, fl)
        weights += [
            (wg_ref.at[i, :, cols], win.at[:, pl.ds(i * fl, fl)]),
            (wu_ref.at[i, :, cols], win.at[:, pl.ds((per_dev + i) * fl, fl)]),
            (wd_ref.at[i, cols, :], wd.at[pl.ds(i * fl, fl), :]),
        ]
    weights = [
        pltpu.make_async_copy(src, dst, wload.at[j]) for j, (src, dst) in enumerate(weights)
    ]
    for copy in weights:
        copy.start()
    meet_column_and_plane(nz, ne, z, e, True)
    own = pltpu.make_async_copy(h_ref, hall_ref.at[z * ne + e], keep)
    own.start()
    for r in range(1, nz):
        remote(
            h_ref, hall_ref.at[z * ne + e], zsend.at[r], zrecv.at[z], (planes[r], e)
        ).start()
    start_round(0)
    acc_in[...] = jnp.zeros_like(acc_in)
    acc_d[...] = jnp.zeros_like(acc_d)
    take_pair(0, 0)
    own.wait()
    for copy in loads(0):
        copy.start()
    for copy in weights:
        copy.wait()

    tile = 2 * rows
    lanes = lax.broadcasted_iota(jnp.int32, (tile, 128), 1)
    split = 64

    def step(k, carry):
        p = lax.rem(k, 2)
        r, i = k // pairs, lax.rem(k, pairs)
        for copy in loads(k):
            copy.wait()
        pre = dot(htile[p, :, :width], win[...], NN)
        graw = dot(gtile[p], wd[...], NT)
        extra = htile[p, :, width:].astype(F32)
        scaled_act, grad_gate, grad_up = [], [], []
        gg = jnp.zeros((tile, 128), F32)
        for j in range(per_dev):
            u = pre[:, j * fl : (j + 1) * fl]
            w = pre[:, (per_dev + j) * fl : (per_dev + 1 + j) * fl]
            gr = graw[:, j * fl : (j + 1) * fl]
            mine = e * per_dev + j
            picked = (lanes == mine) | (lanes == mine + split)
            gate = jnp.sum(jnp.where(picked, extra, 0.0), axis=-1, keepdims=True)
            sig = 1.0 / (1.0 + jnp.exp(-u))
            silu = u * sig
            act = silu * w
            total = jnp.sum(act.astype(BF).astype(F32) * gr, axis=-1, keepdims=True)
            rounded = total.astype(BF).astype(F32)
            gg = jnp.where(lanes == mine, rounded, gg)
            gg = jnp.where(lanes == mine + split, total - rounded, gg)
            scaled_act.append((gate * act).astype(BF))
            gact = gate * gr
            grad_gate.append((gact * w * (sig * (1.0 + u * (1.0 - sig)))).astype(BF))
            grad_up.append((gact * silu).astype(BF))
        a = jnp.concatenate(scaled_act, axis=1)
        gin = jnp.concatenate(grad_gate + grad_up, axis=1)

        for r1 in range(1, nz):

            @pl.when(k == (r1 - 1) * (pairs - 1) + 1)
            def _():
                start_round(r1)

        @pl.when(k + 1 < steps)
        def _():
            ahead = k + 1
            for j in range(pairs):

                @pl.when(lax.rem(ahead, pairs) == j)
                def _():
                    take_pair(ahead // pairs, j)

            for copy in loads(ahead):
                copy.start()

        @pl.when(k >= 2)
        def _():
            for copy in mix_out(k - 2):
                copy.wait()
            to_partner(k - 2).wait_send()

        mixbuf[p] = dot(a, wd[...], NN).astype(BF)
        for copy in mix_out(k):
            copy.start()
        back = dot(gin, win[...], NT).astype(BF)
        gg = gg.astype(BF)
        acc[r, i, :, :width] = back[:rows]
        acc[r, i, :, width:] = gg[:rows]
        qbuf[p, :, :width] = back[rows:]
        qbuf[p, :, width:] = gg[rows:]
        acc_in[...] += dot(htile[p, :, :width], gin, TN)
        acc_d[...] += dot(a, gtile[p], TN)

        @pl.when(k >= slots)
        def _():
            pl.semaphore_wait(credit, 1)

        to_partner(k).start()

        @pl.when(k >= 1)
        def _():
            merge(k - 1)

        for t in range(1, stages + 1):
            late = k - pairs - 2 * t

            @pl.when((late >= 0) & (lax.rem(late + pairs, pairs) == 0))
            def _():
                settle(late // pairs, t)

        return carry

    lax.fori_loop(0, steps, step, 0)
    merge(steps - 1)
    final = pltpu.make_async_copy(acc_d, dwd_ref, flush.at[0])
    final.start()
    left = sorted(
        (r * pairs + pairs + 2 * t, r, t)
        for r in range(nz)
        for t in range(1, stages + 1)
        if r * pairs + pairs + 2 * t >= steps
    )
    chunk = dbuf.shape[1]

    def flush_chunk(c):
        return pltpu.make_async_copy(
            dbuf.at[c % 2], dwin_ref.at[pl.ds(c * chunk, chunk)], flush.at[1 + c % 2]
        )

    chunks = acc_in.shape[0] // chunk
    for c in range(chunks):
        if c >= 2:
            flush_chunk(c - 2).wait()
        dbuf[c % 2] = acc_in[pl.ds(c * chunk, chunk), :].astype(BF)
        flush_chunk(c).start()
    for _, r, t in left:
        settle(jnp.int32(r), t)
    for s in range(2):
        for r in range(1, nz):
            here = zgot.at[planes[r], part(s)]
            remote(here, here, ysend.at[r, s], yrecv.at[planes[r], s], partner).wait_recv()

        def total_rows(n, carry):
            span = pl.ds(pl.multiple_of(s * half + n * 16, 16), 16)
            total = acc[0, 0, span, :].astype(F32)
            for r in range(1, nz):
                total = total + zgot[planes[r], span, :].astype(F32)
            gh_ref[span, :] = total
            return carry

        lax.fori_loop(0, half // 16, total_rows, 0)
    final.wait()
    for c in range(max(chunks - 2, 0), chunks):
        flush_chunk(c).wait()
    for k in range(max(steps - 2, 0), steps):
        for copy in mix_out(jnp.int32(k)):
            copy.wait()
        to_partner(jnp.int32(k)).wait_send()
    for r in range(nz):
        if r > 0:
            remote(
                h_ref, hall_ref.at[z * ne + e], zsend.at[r], zrecv.at[z], (planes[r], e)
            ).wait_send()
        for s in range(2):
            for stage in range(stages + 1):
                for subset in range(1 << stage):
                    pass_on(r, s, stage, subset, own=r == 0 and subset == 0).wait_send()
            for t in range(1, stages + 1):
                for index in range(1 << (stages - t)):
                    push(r, s, t, index).wait_send()
            if r > 0:
                home_copy(jnp.int32(r), s).wait_send()


def moe_net_scratch(nz, ne, per_dev, rows, width, wide, fl):
    pairs = ne // 2
    slots = 4
    stages = ne.bit_length() - 2
    vmem = [
        ((width, 2 * per_dev * fl), BF),
        ((per_dev * fl, width), BF),
        ((width, 2 * per_dev * fl), F32),
        ((per_dev * fl, width), F32),
        ((2, 2 * rows, wide), BF),
        ((2, 2 * rows, width), BF),
        ((2, 2 * rows, width), BF),
        ((2, rows, wide), BF),
        ((slots, rows, wide), BF),
        ((nz, pairs, rows, wide), BF),
        ((nz, 2, max(pairs - 1, 1), rows // 2, wide), BF),
        ((nz, rows, wide), BF),
        ((2, width // 8, 2 * per_dev * fl), BF),
    ]
    size = sum(functools.reduce(lambda a, b: a * b, s) * (2 if d == BF else 4) for s, d in vmem)
    sems = [
        DMA((3 * per_dev,)), DMA((2, 4)), DMA((2, 2)), DMA, DMA((3,)),
        DMA((nz,)), DMA((nz,)), DMA((nz, 2, ne - 1)), DMA((nz, 2, ne - 1)),
        DMA((2,)), DMA((slots,)), pltpu.SemaphoreType.REGULAR,
        DMA((nz, 2, max(pairs - 1, 1))), DMA((nz, 2, max(pairs - 1, 1))),
        DMA((nz, 2)), DMA((nz, 2)),
    ]
    fits = size <= 54_000_000 and stages >= 1 and nz > 1 and nz * pairs > slots
    return fits, slots, [pltpu.VMEM(*v) for v in vmem] + sems


def moe_net(h, g_all, w_gate, w_up, w_down, nz, ne, fl, slots, scratch, cid):
    rows, wide = h.shape
    per_dev, width, _ = w_gate.shape
    return pl.pallas_call(
        functools.partial(moe_net_kernel, nz, ne, per_dev, slots),
        out_shape=[
            jax.ShapeDtypeStruct((nz * ne, rows, wide), BF),
            jax.ShapeDtypeStruct((nz * ne, rows, width), BF),
            jax.ShapeDtypeStruct((rows, wide), F32),
            jax.ShapeDtypeStruct((width, 2 * per_dev * fl), BF),
            jax.ShapeDtypeStruct((per_dev * fl, width), F32),
        ],
        in_specs=[VMEM, ANY, ANY, ANY, ANY],
        out_specs=[ANY, ANY, VMEM, ANY, ANY],
        scratch_shapes=scratch,
        compiler_params=pltpu.CompilerParams(
            collective_id=cid, has_side_effects=True, vmem_limit_bytes=66_500_000
        ),
        name="moe_net",
    )(h, g_all.reshape(nz * ne, rows, width), w_gate, w_up, w_down)


def body(inputs, segments, routes, w_qkv, w_out, w_router, gains, w_gate, w_up, w_down, cotangent):
    z = lax.axis_index("dp")
    e = lax.axis_index("expert")
    nz = lax.axis_size("dp")
    ne = lax.axis_size("expert")
    count, width = inputs.shape
    num_seqs, length = segments.shape
    heads = width // HD // ne
    hw = heads * HD
    expert_count = w_router.shape[1]
    per_dev = w_gate.shape[0]
    hidden = w_gate.shape[2]
    fl = hidden // nz
    both = ("dp", "expert")

    pad = -(expert_count + 4) % 16
    small = jnp.concatenate(
        [w_router.T, gains.T, jnp.zeros((pad, gains.shape[0]), BF)], axis=0
    )
    seg8 = jnp.broadcast_to(segments[:, None, :], (num_seqs, 8, length)).reshape(-1, length)
    in_all, wq, wo, small, seg_all, cot = start_gather(
        inputs, w_qkv.transpose(1, 0, 2), w_out, small, seg8, cotangent, nz, ne, hw, 0
    )
    small = small.transpose(1, 0, 2).reshape(-1, width)
    router_t = small[:expert_count]
    gain_mat = small[expert_count : expert_count + 4].astype(F32)
    my_gains = lax.dynamic_slice_in_dim(gain_mat, e * hw, hw, axis=1)
    seg_all = seg_all.reshape(ne * num_seqs, 8, length)

    g_all = lax.all_gather(cot, both, axis=0, tiled=True)
    inputs_f = inputs.astype(F32)
    tables = rope_lanes(length)
    *saved, x1_part = attn_fwd(in_all, wq, wo, gain_mat, my_gains, seg_all, tables, 9)
    (x1_sum,) = scatter_tokens(x1_part, nz, ne, False, 1)
    x1 = inputs_f + x1_sum

    a2 = rms_scale(x1)
    h2 = (x1 * a2 * gain_mat[3]).astype(BF)
    probs = jax.nn.softmax(dot(h2, router_t, NT), axis=-1)
    picks = jnp.sum(
        (routes[:, :, None] == jnp.arange(expert_count, dtype=jnp.int32)).astype(F32), axis=1
    )
    gates = picks * probs

    split = 64
    high = gates.astype(BF)
    low = (gates - high.astype(F32)).astype(BF)
    blank = jnp.zeros((count, split - expert_count), BF)
    h2_wide = jnp.concatenate([h2, high, blank, low, blank], axis=1)
    wide = width + 2 * split
    fits, slots, scratch = moe_net_scratch(nz, ne, per_dev, count, width, wide, fl)
    if fits:
        _, mix, gh_sum, dwin, dwd = moe_net(
            h2_wide, g_all, w_gate, w_up, w_down, nz, ne, fl, slots, scratch, 2
        )
        mix = mix.reshape(-1, width)
    else:
        h2_all = gather_tokens(h2_wide, nz, ne, True, 2).reshape(-1, wide)
        wg = lax.dynamic_slice_in_dim(w_gate, z * fl, fl, axis=2)
        wu = lax.dynamic_slice_in_dim(w_up, z * fl, fl, axis=2)
        wd = lax.dynamic_slice_in_dim(w_down, z * fl, fl, axis=1).reshape(per_dev * fl, width)
        w_in = jnp.concatenate([*wg, *wu], axis=1)
        mix, gh, dwin, dwd = moe(h2_all, g_all, w_in, wd, per_dev, count, min(4, ne))
        gh_sum, mix = scatter_tokens(
            gh.reshape(nz * ne, count, wide), nz, ne, True, 3, after=mix.reshape(-1, width)
        )
    grad_from_experts = gh_sum[:, :width]
    grad_gates = (
        gh_sum[:, width : width + expert_count]
        + gh_sum[:, width + split : width + split + expert_count]
    )

    mix = lax.psum_scatter(mix, both, scatter_dimension=0, tiled=True)
    output = add_up(x1, mix)

    dwin = lax.all_to_all(
        dwin.reshape(nz, width // nz, 2 * per_dev * fl),
        "dp", split_axis=0, concat_axis=0, tiled=True,
    )
    grad_w_gate, grad_w_up = lay_experts(dwin, per_dev, fl)
    grad_w_down = dwd.reshape(per_dev, fl, width)

    grad_top = cotangent.astype(F32)
    grad_probs = picks * grad_gates
    glog = (probs * (grad_probs - jnp.sum(probs * grad_probs, axis=-1, keepdims=True))).astype(BF)
    local_router = dot(glog, h2, TN)
    gh2 = grad_from_experts + dot(glog, router_t, NN)
    grad_ffn, gain_ffn = rms_backward(x1, a2, gain_mat[3], gh2)
    gx1 = grad_top + grad_ffn
    gab = gx1.astype(BF)

    gab_all = gather_tokens(gab, nz, ne, False, 4)
    gh1_part, parts, gain_qk = attn_bwd(
        gab_all, wq, wo, my_gains, seg_all, tables, saved, 10
    )
    place = lambda part: lax.dynamic_update_slice_in_dim(
        jnp.zeros((1, width), F32), part[None], e * hw, axis=1
    )
    tiny = jnp.concatenate(
        [
            local_router, jnp.zeros((1, width), F32), place(gain_qk[0]), place(gain_qk[1]),
            gain_ffn[None], jnp.zeros((-(expert_count + 4) % 8, width), F32),
        ],
        axis=0,
    )
    grad_inputs, laid, tiny = tail(
        parts, gh1_part, inputs, gx1, gain_mat, tiny, expert_count, nz, ne, hw, 5
    )
    laid = laid.astype(F32)
    grad_w_qkv, grad_w_out = laid[:-1].transpose(1, 0, 2), laid[-1]
    grad_w_router = tiny[:expert_count].T
    grad_gains = tiny[expert_count : expert_count + 4].T
    return (
        output,
        grad_inputs,
        grad_w_qkv,
        grad_w_out,
        grad_w_router,
        grad_gains,
        grad_w_gate,
        grad_w_up,
        grad_w_down,
    )


def solution(mesh):
    tokens = P(("dp", "expert"), None)
    rows = P("dp", None)
    rows3 = P("dp", None, None)
    owned = P("expert", None, None)
    return jax.shard_map(
        body,
        mesh=mesh,
        in_specs=(tokens, tokens, tokens, rows3, rows, rows, rows, owned, owned, owned, tokens),
        out_specs=(tokens, tokens, rows3, rows, rows, rows)
        + (P("expert", "dp", None),) * 3,
        check_vma=False,
    )
```

```python
import functools

import jax
import jax.numpy as jnp
from jax import lax
from jax.experimental import pallas as pl
from jax.experimental.pallas import tpu as pltpu
from jax.sharding import PartitionSpec as P


HD = 128
EPS = 1e-05
ROPE_BASE = 10000.0
MASKED = -1e30
BF = jnp.bfloat16
F32 = jnp.float32


def dot(a, b, dims):
    return lax.dot_general(a, b, (dims, ((), ())), preferred_element_type=F32)


NN = ((1,), (0,))
NT = ((1,), (1,))
TN = ((0,), (0,))


def rms_scale(values):
    return lax.rsqrt(jnp.mean(values * values, axis=-1, keepdims=True) + EPS)


def rms_backward(values, inv_rms, gain_col, grad_out):
    normed = values * inv_rms
    grad_gain = jnp.sum(grad_out * normed, axis=0)
    scaled = grad_out * gain_col
    grad_values = inv_rms * (scaled - normed * jnp.mean(scaled * normed, axis=-1, keepdims=True))
    return (grad_values, grad_gain)


MESH = pl.DeviceIdType.MESH
ANY = pl.BlockSpec(memory_space=pl.ANY)
VMEM = pl.BlockSpec(memory_space=pltpu.VMEM)
DMA = pltpu.SemaphoreType.DMA


def flip(index, bit):
    return index + bit * (1 - 2 * ((index // bit) % 2))


def flips(index, bits):
    out = [index]
    for bit in bits:
        out = out + [flip(i, bit) for i in out]
    return out


def bit_orders(ne):
    bits = [1 << b for b in range(ne.bit_length() - 1)]
    return [bits[:1] + bits[1:], bits[:1] + bits[1:][::-1]]


def nearest(z, r, nz):
    low = jnp.minimum(z, nz - 1 - z)
    near = z - (r + 1) // 2 if r % 2 else z + r // 2
    far = jnp.where(2 * z < nz, z + (r - low), z - (r - low))
    return jnp.where(r <= 2 * low, near, far)


def remote(src, dst, send, recv, peer):
    return pltpu.make_async_remote_copy(
        src_ref=src, dst_ref=dst, send_sem=send, recv_sem=recv, device_id=peer, device_id_type=MESH
    )


def for_others(nz, ne, z, e, act):
    def step(i, carry):
        flat = lax.rem(z * ne + e + i, nz * ne)
        act(flat // ne, lax.rem(flat, ne), flat)
        return carry

    lax.fori_loop(1, nz * ne, step, 0)


def meet_all(nz, ne, z, e):
    sem = pltpu.get_barrier_semaphore()

    def greet(zz, ee, flat):
        pl.semaphore_signal(sem, inc=1, device_id=(zz, ee), device_id_type=MESH)

    for_others(nz, ne, z, e, greet)
    pl.semaphore_wait(sem, nz * ne - 1)


def meet_column_and_plane(nz, ne, z, e, spread):
    sem = pltpu.get_barrier_semaphore()
    peers = [(z, flip(e, 1 << b)) for b in range(ne.bit_length() - 1)]
    if spread:
        peers += [(lax.rem(z + r, nz), e) for r in range(1, nz)]
    for peer in peers:
        pl.semaphore_signal(sem, inc=1, device_id=peer, device_id_type=MESH)
    pl.semaphore_wait(sem, len(peers))


class PlaneGather:
    def __init__(self, nz, ne, z, e, spread, x_ref, out_ref, zsend, zrecv, send, recv, local):
        self.nz, self.ne, self.z, self.e, self.spread = nz, ne, z, e, spread
        self.x, self.out = x_ref, out_ref
        self.zsend, self.zrecv, self.send, self.recv = zsend, zrecv, send, recv
        self.rounds = nz if spread else 1
        self.half = x_ref.shape[0] // 2
        self.orders = [o[1:] + o[:1] for o in bit_orders(ne)]
        self.planes = [z if spread else 0] + [nearest(z, r, nz) for r in range(1, self.rounds)]
        self.pending, self.arrivals = [], {}
        own = self.slot(0, e)
        keep = pltpu.make_async_copy(x_ref, out_ref.at[own], local)
        keep.start()
        self.pending.append(keep.wait)

    @staticmethod
    def scratch(nz, ne, spread):
        rounds = nz if spread else 1
        return [DMA((nz,)), DMA((nz,)), DMA((rounds, 2, ne - 1)), DMA((rounds, 2, ne - 1)), DMA]

    def slot(self, r, ee):
        return self.planes[r] * self.ne + ee

    def spread_own(self):
        for r in range(1, self.rounds):
            to = self.planes[r]
            copy = remote(
                self.x, self.out.at[self.slot(0, self.e)],
                self.zsend.at[r], self.zrecv.at[self.z], (to, self.e),
            )
            copy.start()
            self.pending.append(copy.wait_send)

    def forward(self, r, s, stage, subset):
        order = self.orders[s]
        rows = pl.ds(s * self.half, self.half)
        peer_e = flip(self.e, order[stage])
        n = (1 << stage) - 1 + subset
        block = self.slot(r, flips(self.e, order[:stage])[subset])
        dst = self.out.at[block, rows]
        src = self.x.at[rows] if r == 0 and subset == 0 else dst
        sems = self.send.at[r, s, n], self.recv.at[r, s, n]
        copy = remote(src, dst, *sems, (self.z, peer_e))
        copy.start()
        self.pending.append(copy.wait_send)
        got = self.out.at[self.slot(r, flips(peer_e, order[:stage])[subset]), rows]
        self.arrivals[(r, s, stage, subset)] = remote(got, got, *sems, (self.z, peer_e)).wait_recv

    def start_round(self, r):
        if r > 0:
            here = self.out.at[self.slot(r, self.e)]
            remote(
                here, here, self.zsend.at[r], self.zrecv.at[self.planes[r]], (self.planes[r], self.e)
            ).wait_recv()
        for stage in range(len(self.orders[0])):
            for s in range(2):
                self.forward(r, s, stage, 0)

    def finish_round(self, r):
        stages = len(self.orders[0])
        for stage in range(stages):
            for subset in range(1 << stage):
                for s in range(2):
                    self.arrivals.pop((r, s, stage, subset))()
                    for later in range(stage + 1, stages):
                        self.forward(r, s, later, subset + (1 << stage))

    def finish(self):
        for wait in self.pending:
            wait()


def gather_kernel(nz, ne, spread, x_ref, out_ref, *sems):
    z, e = lax.axis_index("dp"), lax.axis_index("expert")
    meet_column_and_plane(nz, ne, z, e, spread)
    net = PlaneGather(nz, ne, z, e, spread, x_ref, out_ref, *sems)
    net.spread_own()
    net.start_round(0)
    for r in range(1, net.rounds):
        net.start_round(r)
        net.finish_round(r - 1)
    net.finish_round(net.rounds - 1)
    net.finish()


def gather_tokens(x, nz, ne, spread, cid):
    rounds = nz if spread else 1
    return pl.pallas_call(
        functools.partial(gather_kernel, nz, ne, spread),
        out_shape=jax.ShapeDtypeStruct((rounds * ne, *x.shape), x.dtype),
        in_specs=[VMEM],
        out_specs=ANY,
        scratch_shapes=PlaneGather.scratch(nz, ne, spread),
        compiler_params=pltpu.CompilerParams(collective_id=cid, has_side_effects=True),
        name="gather_tokens",
    )(x)


def add_rows(dst, src, tile=16):
    def step(i, carry):
        rows = pl.ds(pl.multiple_of(i * tile, tile), tile)
        dst[rows, :] = (dst[rows, :].astype(F32) + src[rows, :].astype(F32)).astype(dst.dtype)
        return carry

    lax.fori_loop(0, dst.shape[0] // tile, step, 0)


class TokenScatter:
    def __init__(self, nz, ne, z, e, spread, x_ref, acc, got, zgot, loads, send, recv, zsend, zrecv):
        self.nz, self.ne, self.z, self.e, self.spread = nz, ne, z, e, spread
        self.x, self.acc, self.got, self.zgot = x_ref, acc, got, zgot
        self.loads, self.send, self.recv, self.zsend, self.zrecv = loads, send, recv, zsend, zrecv
        self.rounds = nz if spread else 1
        self.stages = ne.bit_length() - 1
        self.steps = self.rounds + self.stages - 1
        self.half = acc.shape[3]
        self.orders = bit_orders(ne)
        self.ranks = list(range(1, self.rounds)) + [0]
        self.first = [0]
        for j in range(self.stages):
            self.first.append(self.first[j] + (ne >> (j + 1)))
        self.pending, self.arrivals, self.zwait = [], {}, {}

    def block(self, r, ee):
        home = lax.rem(self.z + r, self.nz) * self.ne if self.spread else 0
        return home + ee

    def push(self, r, s, j):
        order = self.orders[s]
        peer_e = flip(self.e, order[j])
        rest = self.ne >> (j + 1)
        for i in range(rest):
            n = self.first[j] + i
            if j == 0:
                ee = flips(peer_e, order[:0:-1])[i]
                src = self.x.at[self.block(r, ee), pl.ds(s * self.half, self.half)]
            else:
                src = self.acc.at[r, s, rest + i]
            copy = remote(
                src, self.got.at[r, s, n], self.send.at[r, s, n], self.recv.at[r, s, n],
                (self.z, peer_e),
            )
            copy.start()
            self.pending.append(copy.wait_send)
            self.arrivals.setdefault((r, s, j), []).append((copy.wait_recv, i, n))

    def start(self):
        for r in self.ranks:
            for s in range(2):
                self.push(r, s, 0)
                for i, ee in enumerate(flips(self.e, self.orders[s][:0:-1])):
                    copy = pltpu.make_async_copy(
                        self.x.at[self.block(r, ee), pl.ds(s * self.half, self.half)],
                        self.acc.at[r, s, i],
                        self.loads.at[r, s, i],
                    )
                    copy.start()
                    self.arrivals.setdefault((r, s, -1), []).append(copy.wait)

    def step(self, t):
        for place, r in enumerate(self.ranks):
            j = t - place
            if not 0 <= j < self.stages:
                continue
            for s in range(2):
                if j == 0:
                    for wait in self.arrivals.pop((r, s, -1)):
                        wait()
                for wait, i, n in self.arrivals.pop((r, s, j)):
                    wait()
                    add_rows(self.acc.at[r, s, i], self.got.at[r, s, n])
                if j + 1 < self.stages:
                    self.push(r, s, j + 1)
                elif r > 0:
                    copy = remote(
                        self.acc.at[r, s, 0], self.zgot.at[r, s],
                        self.zsend.at[r, s], self.zrecv.at[r, s],
                        (lax.rem(self.z + r, self.nz), self.e),
                    )
                    copy.start()
                    self.pending.append(copy.wait_send)
                    self.zwait[(r, s)] = copy.wait_recv

    def arrive(self):
        for wait in self.zwait.values():
            wait()

    def rows(self, s, here):
        total = self.acc[0, s, 0, here, :].astype(F32)
        for r in range(1, self.rounds):
            total = total + self.zgot[r, s, here, :].astype(F32)
        return total

    def finish(self):
        for wait in self.pending:
            wait()

    @staticmethod
    def scratch(nz, ne, spread, count, width):
        rounds = nz if spread else 1
        half = count // 2
        return [
            pltpu.VMEM((rounds, 2, ne // 2, half, width), BF),
            pltpu.VMEM((rounds, 2, ne - 1, half, width), BF),
            pltpu.VMEM((nz if spread else 1, 2, half, width), BF),
            DMA((rounds, 2, ne // 2)),
            DMA((rounds, 2, ne - 1)),
            DMA((rounds, 2, ne - 1)),
            DMA((nz, 2)),
            DMA((nz, 2)),
        ]


def over_rows(half, act, tile=16):
    for s in range(2):

        def step(n, carry):
            here = pl.ds(pl.multiple_of(n * tile, tile), tile)
            span = pl.ds(pl.multiple_of(s * half + n * tile, tile), tile)
            act(s, here, span)
            return carry

        lax.fori_loop(0, half // tile, step, 0)


def scatter_kernel(nz, ne, spread, x_ref, *refs):
    out_ref, *rest = refs[-9:]
    z, e = lax.axis_index("dp"), lax.axis_index("expert")
    meet_column_and_plane(nz, ne, z, e, spread)
    net = TokenScatter(nz, ne, z, e, spread, x_ref, *rest)
    net.start()
    for t in range(net.steps):
        net.step(t)
    net.arrive()

    def write(s, here, span):
        out_ref[span, :] = net.rows(s, here)

    over_rows(net.half, write)
    net.finish()


def scatter_tokens(parts, nz, ne, spread, cid, after=None):
    rounds = nz if spread else 1
    _, count, width = parts.shape
    half = count // 2
    held = (2 * rounds * (ne // 2 + ne - 1) + 2 * nz) * half * width * 2
    if held > 56_000_000:
        cut = width // 256 * 128
        left = scatter_tokens(parts[..., :cut], nz, ne, spread, cid, after)
        right = scatter_tokens(parts[..., cut:], nz, ne, spread, cid + 16)
        return [jnp.concatenate([left[0], right[0]], axis=1), *left[1:]]
    more = [] if after is None else [after]
    return pl.pallas_call(
        functools.partial(scatter_kernel, nz, ne, spread),
        out_shape=[jax.ShapeDtypeStruct(m.shape, m.dtype) for m in more]
        + [jax.ShapeDtypeStruct((count, width), F32)],
        in_specs=[ANY] * (1 + len(more)),
        out_specs=[ANY] * len(more) + [VMEM],
        scratch_shapes=TokenScatter.scratch(nz, ne, spread, count, width),
        input_output_aliases={1: 0} if more else {},
        compiler_params=pltpu.CompilerParams(
            collective_id=cid, has_side_effects=True, vmem_limit_bytes=64_000_000
        ),
        name="scatter_tokens",
    )(parts, *more)[::-1]


def start_kernel(
    nz, ne, x_ref, wqkv_ref, wout_ref, small_ref, seg_ref, cot_ref,
    out_ref, wq_ref, wo_ref, small_out, seg_out, cot_out,
    wbuf, pbuf, zsend, zrecv, send, recv, local, czsend, czrecv, csend, crecv, clocal,
    up_send, up_recv, dn_send, dn_recv, wload, wkeep, pload, psend, precv, pkeep,
    small_send, small_recv, seg_send, seg_recv,
):
    z, e = lax.axis_index("dp"), lax.axis_index("expert")
    kinds, depth, hw = wbuf.shape
    per = ne // nz
    loads = [
        pltpu.make_async_copy(wqkv_ref.at[j, :, pl.ds(e * hw, hw)], wbuf.at[j], wload.at[j])
        for j in range(kinds)
    ]
    for copy in loads:
        copy.start()
    pieces = [
        pltpu.make_async_copy(
            wout_ref.at[pl.ds(i * hw, hw), pl.ds(e * hw, hw)], pbuf.at[i], pload.at[i]
        )
        for i in range(per)
    ]
    for copy in pieces:
        copy.start()
    meet_all(nz, ne, z, e)
    cot = PlaneGather(
        nz, ne, z, e, True, cot_ref, cot_out, czsend, czrecv, csend, crecv, clocal
    )
    cot.spread_own()

    def rows_of(zz):
        return pl.ds(pl.multiple_of(zz * depth, depth), depth)

    def hop(j, zz, dist, up):
        send, recv = (up_send, up_recv) if up else (dn_send, dn_recv)
        here = wq_ref.at[j, rows_of(zz)]
        src = wbuf.at[j] if dist == 1 else here
        to = z + 1 if up else z - 1
        return remote(src, here, send.at[dist, j], recv.at[dist, j], (to, e))

    keeps = []
    for j in range(kinds):
        loads[j].wait()

        @pl.when(z + 1 < nz)
        def _():
            hop(j, z, 1, True).start()

        @pl.when(z > 0)
        def _():
            hop(j, z, 1, False).start()

        keep = pltpu.make_async_copy(wbuf.at[j], wq_ref.at[j, rows_of(z)], wkeep.at[j])
        keep.start()
        keeps.append(keep)

    def wait_all(ref, send, recv, count):
        most = ref.at[pl.ds(0, count)]
        both = remote(most, most, send, recv, (z, flip(e, 1)))
        both.wait_send()
        both.wait_recv()

    small_out[z] = small_ref[...]
    for r in range(1, nz):
        remote(
            small_ref, small_out.at[z], small_send, small_recv, (lax.rem(z + r, nz), e)
        ).start()
    seg_out[e] = seg_ref[...]
    for r in range(1, ne):
        remote(seg_ref, seg_out.at[e], seg_send, seg_recv, (z, lax.rem(e + r, ne))).start()
    net = PlaneGather(nz, ne, z, e, False, x_ref, out_ref, zsend, zrecv, send, recv, local)
    net.start_round(0)

    columns = pl.ds(e * hw, hw)
    for i in range(per):
        pieces[i].wait()
    for r in range(nz):
        for i in range(per):
            to = (lax.rem(z + r, nz), z * per + i)
            give = remote(pbuf.at[i], wo_ref.at[:, columns], psend.at[r, i], precv, to)
            if r > 0:
                give.start()
            else:
                own = pltpu.make_async_copy(pbuf.at[i], wo_ref.at[:, columns], pkeep)

                @pl.when(to[1] == e)
                def _():
                    own.start()

                @pl.when(to[1] != e)
                def _():
                    give.start()
    net.finish_round(0)
    cot.start_round(0)
    for dist in range(1, nz):
        cot.start_round(dist)
        cot.finish_round(dist - 1)
        for j in range(kinds):

            @pl.when(z - dist >= 0)
            def _():
                got = wq_ref.at[j, rows_of(z - dist)]
                remote(got, got, up_send.at[dist, j], up_recv.at[dist, j], (z, e)).wait_recv()

                @pl.when(z + 1 < nz)
                def _():
                    if dist + 1 < nz:
                        hop(j, z - dist, dist + 1, True).start()

            @pl.when(z + dist < nz)
            def _():
                got = wq_ref.at[j, rows_of(z + dist)]
                remote(got, got, dn_send.at[dist, j], dn_recv.at[dist, j], (z, e)).wait_recv()

                @pl.when(z > 0)
                def _():
                    if dist + 1 < nz:
                        hop(j, z + dist, dist + 1, False).start()

    cot.finish_round(nz - 1)
    cot.finish()
    net.finish()
    for keep in keeps:
        keep.wait()
    for dist in range(1, nz):
        for j in range(kinds):

            @pl.when((z - dist + 1 >= 0) & (z + 1 < nz))
            def _():
                hop(j, z - dist + 1, dist, True).wait_send()

            @pl.when((z + dist - 1 < nz) & (z > 0))
            def _():
                hop(j, z + dist - 1, dist, False).wait_send()

    for r in range(nz):
        for i in range(per):
            to = (lax.rem(z + r, nz), z * per + i)
            give = remote(pbuf.at[i], wo_ref.at[:, columns], psend.at[r, i], precv, to)
            if r > 0:
                give.wait_send()
            else:
                own = pltpu.make_async_copy(pbuf.at[i], wo_ref.at[:, columns], pkeep)

                @pl.when(to[1] == e)
                def _():
                    own.wait()

                @pl.when(to[1] != e)
                def _():
                    give.wait_send()

    def wait_pieces(count):
        most = wo_ref.at[:, pl.ds(0, count * hw)]
        remote(most, most, psend.at[0, 0], precv, (z, e)).wait_recv()

    @pl.when(z == e // per)
    def _():
        wait_pieces(ne - 1)

    @pl.when(z != e // per)
    def _():
        wait_pieces(ne)

    wait_all(small_out, small_send, small_recv, nz - 1)
    wait_all(seg_out, seg_send, seg_recv, ne - 1)


def start_gather(x, w_qkv, w_out, small, seg, cot, nz, ne, hw, cid):
    kinds, depth, width = w_qkv.shape
    per = ne // nz
    return pl.pallas_call(
        functools.partial(start_kernel, nz, ne),
        out_shape=[
            jax.ShapeDtypeStruct((ne, *x.shape), x.dtype),
            jax.ShapeDtypeStruct((kinds, nz * depth, hw), BF),
            jax.ShapeDtypeStruct((hw, width), BF),
            jax.ShapeDtypeStruct((nz, *small.shape), small.dtype),
            jax.ShapeDtypeStruct((ne, *seg.shape), seg.dtype),
            jax.ShapeDtypeStruct((nz * ne, *cot.shape), cot.dtype),
        ],
        in_specs=[VMEM, ANY, ANY, VMEM, VMEM, VMEM],
        out_specs=[ANY, ANY, ANY, VMEM, VMEM, ANY],
        scratch_shapes=[
            pltpu.VMEM((kinds, depth, hw), BF),
            pltpu.VMEM((per, hw, hw), BF),
            *PlaneGather.scratch(nz, ne, False),
            *PlaneGather.scratch(nz, ne, True),
            DMA((nz, kinds)), DMA((nz, kinds)), DMA((nz, kinds)), DMA((nz, kinds)),
            DMA((kinds,)), DMA((kinds,)), DMA((per,)), DMA((nz, per)), DMA, DMA,
            DMA, DMA, DMA, DMA,
        ],
        compiler_params=pltpu.CompilerParams(collective_id=cid, has_side_effects=True),
        name="start_gather",
    )(x, w_qkv, w_out, small, seg, cot)


def rope_lanes(length):
    half = HD // 2
    freqs = jnp.exp(-jnp.log(ROPE_BASE) * (2.0 * jnp.arange(half, dtype=F32) / HD))
    angles = jnp.arange(length, dtype=F32)[:, None] * freqs[None, :]
    cos, sin = jnp.cos(angles), jnp.sin(angles)
    return jnp.concatenate([cos, cos], axis=1), jnp.concatenate([-sin, sin], axis=1)


def turn(x, cos, sin):
    return x * cos + pltpu.roll(x, HD // 2, 1) * sin


def meet_plane(ne, z, e):
    sem = pltpu.get_barrier_semaphore()
    for r in range(1, ne):
        pl.semaphore_signal(
            sem, inc=1, device_id=(z, lax.rem(e + r, ne)), device_id_type=MESH
        )
    pl.semaphore_wait(sem, ne - 1)


def plane_totals(ne, z, e, mine, theirs, send, recv):
    copies = []
    for r in range(1, ne):
        to = (z, lax.rem(e + r, ne))
        copy = remote(mine, theirs.at[r], send.at[r], recv.at[r], to)
        copy.start()
        copies.append(copy)
    total = mine[...]
    for r, copy in enumerate(copies):
        copy.wait_recv()
        total = total + theirs[r + 1]
    for copy in copies:
        copy.wait_send()
    return total


def store_columns(sums, first, columns):
    rows = columns[0].shape[0]
    lanes = lax.broadcasted_iota(jnp.int32, (rows, 128), 1)
    wide = jnp.zeros((rows, 128), F32)
    for j, column in enumerate(columns):
        wide = jnp.where(lanes == j, column, wide)
    sums[:, pl.ds(first, rows)] = wide.T[:8]


def as_columns(total, out):
    rows = total.shape[1]
    for first in range(0, rows, 128):
        chunk = total[:, first : first + 128]
        out[first : first + 128, :] = jnp.concatenate([chunk] * 16, axis=0).T


def allowed_pairs(seg_ref, n):
    length = seg_ref.shape[2]
    keys = jnp.broadcast_to(seg_ref[n, :1].astype(F32), (length, length))
    i = lax.broadcasted_iota(jnp.int32, (length, length), 0)
    j = lax.broadcasted_iota(jnp.int32, (length, length), 1)
    return (i >= j) & (keys == keys.T)


def attend(rq, rk, allowed):
    scores = jnp.where(allowed, dot(rq, rk, NT) * HD ** (-0.5), MASKED)
    top = jnp.max(scores, axis=-1, keepdims=True)
    lse = top + jnp.log(jnp.sum(jnp.exp(scores - top), axis=-1, keepdims=True))
    return jnp.exp(scores - lse)


def attn_fwd_kernel(
    ne, x_ref, wq_ref, wo_ref, gain_ref, mine_ref, seg_ref, cos_ref, sin_ref,
    h1_ref, q_ref, k_ref, rq_ref, rk_ref, v_ref, o_ref, scale_ref, x1_ref,
    sums, theirs, send, recv,
):
    z, e = lax.axis_index("dp"), lax.axis_index("expert")
    width = x_ref.shape[2]
    count, hw = q_ref.shape
    length = seg_ref.shape[2]
    rows_dev = x_ref.shape[1]
    tile = min(512, count)
    meet_plane(ne, z, e)

    def normed(b, carry):
        x = x_ref[b].astype(F32)
        h1 = x * rms_scale(x) * gain_ref[:1]
        h1_ref[pl.ds(pl.multiple_of(b * rows_dev, rows_dev), rows_dev), :] = h1.astype(BF)
        return carry

    lax.fori_loop(0, ne, normed, 0)
    for first in range(0, count, tile):
        rows = slice(first, first + tile)
        h1 = h1_ref[rows, :]
        q, k = dot(h1, wq_ref[0], NN), dot(h1, wq_ref[1], NN)
        q_ref[rows, :] = q
        k_ref[rows, :] = k
        v_ref[rows, :] = dot(h1, wq_ref[2], NN).astype(BF)
        store_columns(
            sums, first, [jnp.sum(t * t, axis=-1, keepdims=True) for t in (q, k)]
        )
    total = plane_totals(ne, z, e, sums, theirs, send, recv)
    as_columns(lax.rsqrt(total / width + EPS), scale_ref)
    cos, sin = cos_ref[...], sin_ref[...]

    def sequence(n, carry):
        rows = pl.ds(pl.multiple_of(n * length, length), length)
        allowed = allowed_pairs(seg_ref, n)
        aq, ak = scale_ref[rows, 0:1], scale_ref[rows, 1:2]
        for c in range(0, hw, HD):
            cols = slice(c, c + HD)
            rq = turn(q_ref[rows, cols] * aq * mine_ref[1:2, cols], cos, sin).astype(BF)
            rk = turn(k_ref[rows, cols] * ak * mine_ref[2:3, cols], cos, sin).astype(BF)
            rq_ref[rows, cols] = rq
            rk_ref[rows, cols] = rk
            probs = attend(rq, rk, allowed).astype(BF)
            o_ref[rows, cols] = dot(probs, v_ref[rows, cols], NN).astype(BF)
        return carry

    lax.fori_loop(0, count // length, sequence, 0)
    for first in range(0, count, tile):
        x1 = dot(o_ref[first : first + tile, :], wo_ref[...], NN).astype(BF)
        blocks = tile // rows_dev
        x1_ref[first // rows_dev : first // rows_dev + blocks] = x1.reshape(
            blocks, rows_dev, width
        )


def attn_fwd(in_all, wq, wo, gain_mat, my_gains, seg, tables, cid):
    ne, rows_dev, width = in_all.shape
    count, hw = ne * rows_dev, wo.shape[0]
    return pl.pallas_call(
        functools.partial(attn_fwd_kernel, ne),
        out_shape=[
            jax.ShapeDtypeStruct((count, width), BF),
            jax.ShapeDtypeStruct((count, hw), F32),
            jax.ShapeDtypeStruct((count, hw), F32),
            jax.ShapeDtypeStruct((count, hw), BF),
            jax.ShapeDtypeStruct((count, hw), BF),
            jax.ShapeDtypeStruct((count, hw), BF),
            jax.ShapeDtypeStruct((count, hw), BF),
            jax.ShapeDtypeStruct((count, 128), F32),
            jax.ShapeDtypeStruct((ne, rows_dev, width), BF),
        ],
        in_specs=[VMEM] * 8,
        out_specs=[VMEM] * 9,
        scratch_shapes=[
            pltpu.VMEM((8, count), F32), pltpu.VMEM((ne, 8, count), F32), DMA((ne,)), DMA((ne,)),
        ],
        compiler_params=pltpu.CompilerParams(
            collective_id=cid, has_side_effects=True, vmem_limit_bytes=60_000_000
        ),
        name="attn_fwd",
    )(in_all, wq, wo, gain_mat, my_gains, seg, *tables)


def attn_bwd_kernel(
    ne, gab_ref, wq_ref, wo_ref, mine_ref, seg_ref, cos_ref, sin_ref,
    h1_ref, q_ref, k_ref, rq_ref, rk_ref, v_ref, o_ref, scale_ref,
    gh1_ref, parts_ref, gain_ref,
    pout, go_ref, gqn_ref, gkn_ref, gp_ref, sums, theirs, means, send, recv, psend, precv,
):
    z, e = lax.axis_index("dp"), lax.axis_index("expert")
    count, hw = q_ref.shape
    width = gab_ref.shape[2]
    rows_dev = gab_ref.shape[1]
    length = seg_ref.shape[2]
    tile = min(512, count)
    blocks = tile // rows_dev
    meet_plane(ne, z, e)

    gab = lambda first: gab_ref[first // rows_dev : first // rows_dev + blocks].reshape(tile, width)
    part = dot(o_ref[:tile, :], gab(0), TN)
    for first in range(tile, count, tile):
        part = part + dot(o_ref[first : first + tile, :], gab(first), TN)
    pout[...] = part.astype(BF)
    for first in range(0, count, tile):
        go_ref[first : first + tile, :] = dot(gab(first), wo_ref[...], NT).astype(BF)
    my_rows = pl.ds(pl.multiple_of(e * hw, hw), hw)
    last = pl.ds(3 * hw, hw)
    gives = []
    for r in range(1, ne):
        to = lax.rem(e + r, ne)
        give = remote(
            pout.at[:, pl.ds(pl.multiple_of(to * hw, hw), hw)], parts_ref.at[my_rows, last],
            psend.at[r], precv.at[r], (z, to),
        )
        give.start()
        gives.append(give)
    parts_ref[my_rows, last] = pout[:, my_rows]

    cos, sin = cos_ref[...], -sin_ref[...]
    gain_ref[...] = jnp.zeros_like(gain_ref)

    def sequence(n, carry):
        start = pl.multiple_of(n * length, length)
        rows = pl.ds(start, length)
        allowed = allowed_pairs(seg_ref, n)
        aq, ak = scale_ref[rows, 0:1], scale_ref[rows, 1:2]
        sum_q = jnp.zeros((length, 1), F32)
        sum_k = jnp.zeros((length, 1), F32)
        for c in range(0, hw, HD):
            cols = slice(c, c + HD)
            rq, rk, go = rq_ref[rows, cols], rk_ref[rows, cols], go_ref[rows, cols]
            probs = attend(rq, rk, allowed)
            gv = dot(probs.astype(BF), go, TN).astype(BF)
            gp_ref[rows, slice(2 * hw + c, 2 * hw + c + HD)] = gv
            grad = dot(go, v_ref[rows, cols], NT)
            delta = jnp.sum(probs * grad, axis=-1, keepdims=True)
            gs = (probs * (grad - delta) * HD ** (-0.5)).astype(BF)
            gqn = turn(dot(gs, rk, NN), cos, sin)
            gkn = turn(dot(gs, rq, TN), cos, sin)
            gqn_ref[rows, cols] = gqn
            gkn_ref[rows, cols] = gkn
            tq = gqn * (q_ref[rows, cols] * aq)
            tk = gkn * (k_ref[rows, cols] * ak)
            gain_ref[0:1, cols] += jnp.sum(tq, axis=0, keepdims=True)
            gain_ref[1:2, cols] += jnp.sum(tk, axis=0, keepdims=True)
            sum_q = sum_q + jnp.sum(tq * mine_ref[1:2, cols], axis=-1, keepdims=True)
            sum_k = sum_k + jnp.sum(tk * mine_ref[2:3, cols], axis=-1, keepdims=True)
        store_columns(sums, start, [sum_q, sum_k])
        return carry

    lax.fori_loop(0, count // length, sequence, 0)
    total = plane_totals(ne, z, e, sums, theirs, send, recv)
    as_columns(total / width, means)
    for first in range(0, count, tile):
        rows = slice(first, first + tile)
        aq, ak = scale_ref[rows, 0:1], scale_ref[rows, 1:2]
        mq, mk = means[rows, 0:1], means[rows, 1:2]
        gq = aq * (gqn_ref[rows, :] * mine_ref[1:2] - q_ref[rows, :] * aq * mq)
        gk = ak * (gkn_ref[rows, :] * mine_ref[2:3] - k_ref[rows, :] * ak * mk)
        gp_ref[rows, :hw] = gq.astype(BF)
        gp_ref[rows, hw : 2 * hw] = gk.astype(BF)
    for first in range(0, width, tile):
        rows = slice(first, first + tile)
        parts_ref[rows, : 3 * hw] = dot(h1_ref[:, rows], gp_ref[...], TN).astype(BF)
    for first in range(0, count, tile):
        rows = slice(first, first + tile)
        gh1 = dot(gp_ref[rows, :hw], wq_ref[0], NT)
        for j in range(1, 3):
            gh1 = gh1 + dot(gp_ref[rows, j * hw : (j + 1) * hw], wq_ref[j], NT)
        gh1_ref[first // rows_dev : first // rows_dev + blocks] = gh1.astype(BF).reshape(
            blocks, rows_dev, width
        )
    for give in gives:
        give.wait_send()
        give.wait_recv()


def attn_bwd(gab, wq, wo, my_gains, seg, tables, saved, cid):
    ne, rows_dev, width = gab.shape
    count, hw = ne * rows_dev, wo.shape[0]
    return pl.pallas_call(
        functools.partial(attn_bwd_kernel, ne),
        out_shape=[
            jax.ShapeDtypeStruct((ne, rows_dev, width), BF),
            jax.ShapeDtypeStruct((width, 4 * hw), BF),
            jax.ShapeDtypeStruct((8, hw), F32),
        ],
        in_specs=[VMEM] * 15,
        out_specs=[VMEM] * 3,
        scratch_shapes=[
            pltpu.VMEM((hw, width), BF),
            pltpu.VMEM((count, hw), BF),
            pltpu.VMEM((count, hw), F32),
            pltpu.VMEM((count, hw), F32),
            pltpu.VMEM((count, 3 * hw), BF),
            pltpu.VMEM((8, count), F32),
            pltpu.VMEM((ne, 8, count), F32),
            pltpu.VMEM((count, 128), F32),
            DMA((ne,)), DMA((ne,)), DMA((ne,)), DMA((ne,)),
        ],
        compiler_params=pltpu.CompilerParams(
            collective_id=cid, has_side_effects=True, vmem_limit_bytes=64_000_000
        ),
        name="attn_bwd",
    )(gab, wq, wo, my_gains, seg, *tables, *saved)


def tail_kernel(
    nz, ne, kinds, gain_row, with_mix, parts_ref, gh1_ref, mix_ref, x_ref, x1_ref, gx1_ref,
    gain_ref, tiny_ref, grad_ref, laid_ref, small_ref, out_ref,
    work, below, above, wide, gsum, tbuf, tgot, total, far,
    wload, usend, urecv, dsend, drecv, zsend, zrecv, gsend, grecv, glocal,
    flush, send1, recv1, send2, recv2, *nets_scratch,
):
    z, e = lax.axis_index("dp"), lax.axis_index("expert")
    per = ne // nz
    chunks, rows = work.shape[1], work.shape[2]
    hw = work.shape[3] // kinds
    width = x_ref.shape[1]
    loads = [
        pltpu.make_async_copy(
            parts_ref.at[pl.ds((t * chunks + c) * rows, rows)], work.at[t, c], wload.at[t, c]
        )
        for c in range(chunks)
        for t in range(nz)
    ]
    for copy in loads:
        copy.start()
    meet_all(nz, ne, z, e)
    mine = TokenScatter(nz, ne, z, e, False, gh1_ref, *nets_scratch[:8])
    mine.start()
    if with_mix:
        mix = TokenScatter(nz, ne, z, e, True, mix_ref, *nets_scratch[8:])
        mix.start()
    for copy in loads:
        copy.wait()

    def rise(t, c):
        return remote(
            work.at[t, c], below.at[t, c], usend.at[t, c], urecv.at[t, c], (z + 1, e)
        )

    def sink(t, c):
        return remote(
            work.at[t, c], above.at[t, c], dsend.at[t, c], drecv.at[t, c], (z - 1, e)
        )

    for c in range(chunks):
        for t in range(nz - 1, 0, -1):

            @pl.when(z == 0)
            def _():
                rise(t, c).start()

        for t in range(nz - 1):

            @pl.when(z == nz - 1)
            def _():
                sink(t, c).start()

    def arrive(t, c, buffer, recv):
        remote(buffer.at[t, c], buffer.at[t, c], usend.at[0, 0], recv.at[t, c], (z, e)).wait_recv()
        add_rows(work.at[t, c], buffer.at[t, c])

    def line(t):
        for p in range(nz):

            @pl.when(z == p)
            def _():
                c = t - (p - 1)
                if p > 0 and 0 <= c < chunks:
                    for target in range(nz - 1, p - 1, -1):
                        arrive(target, c, below, urecv)
                        if target > p:
                            rise(target, c).start()
                c = t - (nz - 2 - p)
                if p < nz - 1 and 0 <= c < chunks:
                    for target in range(p + 1):
                        arrive(target, c, above, drecv)
                        if target < p:
                            sink(target, c).start()

    def spread(c):
        net = PlaneGather(
            nz, ne, z, e, False, work.at[z, c], wide.at[c], zsend, zrecv,
            gsend.at[c], grecv.at[c], glocal.at[c],
        )
        net.start_round(0)
        return net

    def outs(c):
        span = pl.ds(c * rows, rows)
        copies = []
        for n in range(ne):
            for j in range(kinds):
                copies.append(
                    pltpu.make_async_copy(
                        wide.at[c, n, :, pl.ds(j * hw, hw)],
                        laid_ref.at[j, span, pl.ds(n * hw, hw)],
                        flush.at[c, n, j],
                    )
                )
        return copies

    def lay(c, net):
        net.finish_round(0)
        net.finish()
        for copy in outs(c):
            copy.start()

    def mix_step(t):
        if with_mix and t < mix.steps:
            mix.step(t)

    mine.step(0)
    mix_step(0)
    line(0)
    for j in range(1, mine.stages):
        mine.step(j)
    mix_step(1)
    line(1)
    nets = {}

    def advance(t):
        c = t - max(nz - 2, 0)
        if 0 <= c < chunks:
            nets[c] = spread(c)
        if c - 1 in nets:
            lay(c - 1, nets.pop(c - 1))

    advance(0)
    advance(1)

    gsum[...] = jnp.zeros_like(gsum)

    def front(s, here, span):
        grad = mine.rows(s, here)
        x = x_ref[span, :].astype(F32)
        scale = rms_scale(x)
        normed = x * scale
        gsum[...] += grad * normed
        scaled = grad * gain_ref[:1]
        inner = jnp.mean(scaled * normed, axis=-1, keepdims=True)
        grad_ref[span, :] = (gx1_ref[span, :] + scale * (scaled - normed * inner)).astype(BF)

    over_rows(mine.half, front)
    tbuf[...] = tiny_ref[...]
    tbuf[gain_row : gain_row + 1, :] = jnp.sum(gsum[...], axis=0, keepdims=True)

    cw = width // ne
    block = lambda ee: pl.ds(pl.multiple_of(ee * cw, cw), cw)
    first = []
    for r in range(1, ne):
        to = lax.rem(e + r, ne)
        copy = remote(tbuf.at[:, block(to)], tgot.at[r], send1.at[r], recv1.at[r], (z, to))
        copy.start()
        first.append(copy)
    mix_step(2)
    line(2)
    advance(2)
    sums = tbuf[:, block(e)]
    for r, copy in enumerate(first):
        copy.wait_recv()
        sums = sums + tgot[r + 1]
    total[...] = sums
    home, place = e // per, lax.rem(e, per)

    def give(r):
        to = lax.rem(e + r, ne)
        return remote(total, far.at[z, place], send2.at[r], recv2, (home, to))

    for r in range(ne):
        if r > 0:
            give(r).start()
        else:

            @pl.when(home != z)
            def _():
                give(0).start()

            @pl.when(home == z)
            def _():
                far[z, place] = total[...]

    for t in range(3, max(chunks + nz, mix.steps if with_mix else 0)):
        mix_step(t)
        line(t)
        advance(t)
    if with_mix:
        mix.arrive()

        def finish_output(s, here, span):
            out_ref[span, :] = (x1_ref[span, :] + mix.rows(s, here)).astype(BF)

        over_rows(mix.half, finish_output)
        mix.finish()
    else:
        out_ref[...] = jnp.zeros_like(out_ref)
    for copy in first:
        copy.wait_send()

    def arrived(count):
        flat = tgot.at[pl.ds(0, count)]
        remote(flat, flat, send2.at[0], recv2, (z, e)).wait_recv()

    for r in range(ne):
        if r > 0:
            give(r).wait_send()
        else:

            @pl.when(home != z)
            def _():
                give(0).wait_send()
                arrived(nz * per)

            @pl.when(home == z)
            def _():
                arrived(nz * per - 1)

    for i in range(per):
        small_ref[i] = sum(far[k, i] for k in range(nz))
    mine.finish()
    for c in range(chunks):
        for t in range(nz):

            @pl.when(z < t)
            def _():
                rise(t, c).wait_send()

            @pl.when(z > t)
            def _():
                sink(t, c).wait_send()

    for c in range(chunks):
        for copy in outs(c):
            copy.wait()


def tail(parts, gh1_part, mix, x, x1, gx1, gain_mat, tiny, gain_row, nz, ne, hw, cid):
    width, total_cols = parts.shape
    kinds = total_cols // hw
    count = x.shape[0]
    depth = width // nz
    rows = min(128, depth)
    chunks = depth // rows
    small_rows, cw = tiny.shape[0], width // ne
    per = ne // nz
    block = (nz, chunks, rows, total_cols)
    with_mix = mix is not None
    scratch = TokenScatter.scratch(nz, ne, False, count, width)
    if with_mix:
        scratch += TokenScatter.scratch(nz, ne, True, count, width)
    grad, laid, small, output = pl.pallas_call(
        functools.partial(tail_kernel, nz, ne, kinds, gain_row, with_mix),
        out_shape=[
            jax.ShapeDtypeStruct((count, width), BF),
            jax.ShapeDtypeStruct((kinds, depth, width), BF),
            jax.ShapeDtypeStruct((per, small_rows, cw), F32),
            jax.ShapeDtypeStruct((count, width), BF),
        ],
        in_specs=[ANY, ANY, ANY, VMEM, VMEM, VMEM, VMEM, VMEM],
        out_specs=[VMEM, ANY, VMEM, VMEM],
        scratch_shapes=[
            pltpu.VMEM(block, BF), pltpu.VMEM(block, BF), pltpu.VMEM(block, BF),
            pltpu.VMEM((chunks, ne, rows, total_cols), BF),
            pltpu.VMEM((16, width), F32),
            pltpu.VMEM((small_rows, width), F32),
            pltpu.VMEM((max(ne, nz * per), small_rows, cw), F32),
            pltpu.VMEM((small_rows, cw), F32),
            pltpu.VMEM((nz, per, small_rows, cw), F32),
            DMA((nz, chunks)),
            DMA((nz, chunks)), DMA((nz, chunks)), DMA((nz, chunks)), DMA((nz, chunks)),
            DMA((nz,)), DMA((nz,)),
            DMA((chunks, 1, 2, ne - 1)), DMA((chunks, 1, 2, ne - 1)), DMA((chunks,)),
            DMA((chunks, ne, kinds)),
            DMA((ne,)), DMA((ne,)), DMA((ne,)), DMA,
            *scratch,
        ],
        compiler_params=pltpu.CompilerParams(
            collective_id=cid, has_side_effects=True, vmem_limit_bytes=66_000_000
        ),
        name="tail",
    )(parts, gh1_part, mix if with_mix else gh1_part, x, x1, gx1, gain_mat, tiny)
    small = small.transpose(1, 0, 2).reshape(small_rows, per * cw)
    return grad, laid, small, output


def add_kernel(x_ref, y_ref, out_ref):
    out_ref[...] = (x_ref[...] + y_ref[...].astype(F32)).astype(out_ref.dtype)


def add_up(x, y):
    return pl.pallas_call(
        add_kernel, out_shape=jax.ShapeDtypeStruct(y.shape, y.dtype), name="add_up"
    )(x, y)


def lay_experts_kernel(per_dev, fl, x_ref, gate_ref, up_ref):
    for i in range(per_dev):
        gate_ref[i] = x_ref[0, :, i * fl : (i + 1) * fl].astype(F32)
        up_ref[i] = x_ref[0, :, (per_dev + i) * fl : (per_dev + i + 1) * fl].astype(F32)


def lay_experts(wide, per_dev, fl):
    nz, rows, _ = wide.shape
    out = jax.ShapeDtypeStruct((per_dev, rows, nz * fl), F32)
    spec = pl.BlockSpec((per_dev, rows, fl), lambda i: (0, 0, i))
    return pl.pallas_call(
        functools.partial(lay_experts_kernel, per_dev, fl),
        grid=(nz,),
        in_specs=[pl.BlockSpec((1, rows, 2 * per_dev * fl), lambda i: (i, 0, 0))],
        out_specs=[spec, spec],
        out_shape=[out, out],
        name="lay_experts",
    )(wide)


def moe_kernel(
    fl, h_ref, g_ref, win_ref, wd_ref,
    mix_ref, gh_ref, dwin_ref, dwd_ref, acc_in, acc_d,
):
    step = pl.program_id(0)
    tile, width = g_ref.shape
    per_dev = wd_ref.shape[0] // fl
    e = lax.axis_index("expert")
    h = h_ref[:, :width]
    g = g_ref[...]
    extra = h_ref[:, width:].astype(F32)
    pre = dot(h, win_ref[...], NN)
    graw = dot(g, wd_ref[...], NT)
    scaled_act, grad_gate, grad_up = [], [], []
    lanes = lax.broadcasted_iota(jnp.int32, (tile, 128), 1)
    gg = jnp.zeros((tile, 128), F32)
    split = 64
    for i in range(per_dev):
        u = pre[:, i * fl : (i + 1) * fl]
        w = pre[:, (per_dev + i) * fl : (per_dev + 1 + i) * fl]
        gr = graw[:, i * fl : (i + 1) * fl]
        mine = e * per_dev + i
        picked = (lanes == mine) | (lanes == mine + split)
        gate = jnp.sum(jnp.where(picked, extra, 0.0), axis=-1, keepdims=True)
        sig = 1.0 / (1.0 + jnp.exp(-u))
        silu = u * sig
        act = silu * w
        total = jnp.sum(act.astype(BF).astype(F32) * gr, axis=-1, keepdims=True)
        rounded = total.astype(BF).astype(F32)
        gg = jnp.where(lanes == mine, rounded, gg)
        gg = jnp.where(lanes == mine + split, total - rounded, gg)
        scaled_act.append((gate * act).astype(BF))
        gact = gate * gr
        grad_gate.append((gact * w * (sig * (1.0 + u * (1.0 - sig)))).astype(BF))
        grad_up.append((gact * silu).astype(BF))
    a = jnp.concatenate(scaled_act, axis=1)
    gin = jnp.concatenate(grad_gate + grad_up, axis=1)
    mix_ref[...] = dot(a, wd_ref[...], NN).astype(BF)
    gh_ref[:, :width] = dot(gin, win_ref[...], NT).astype(BF)
    gh_ref[:, width:] = gg.astype(BF)

    @pl.when(step == 0)
    def _():
        acc_in[...] = jnp.zeros_like(acc_in)
        acc_d[...] = jnp.zeros_like(acc_d)

    acc_in[...] += dot(h, gin, TN)
    acc_d[...] += dot(a, g, TN)

    @pl.when(step == pl.num_programs(0) - 1)
    def _():
        dwin_ref[...] = acc_in[...].astype(BF)
        dwd_ref[...] = acc_d[...]


def moe(h_all, g_all, w_in, wd, per_dev, rows_dev, blocks):
    count, width = g_all.shape
    wide = h_all.shape[1]
    hid4 = w_in.shape[1]
    hid2 = wd.shape[0]
    fl = hid2 // per_dev
    tile = blocks * rows_dev
    rows = lambda n: pl.BlockSpec((tile, n), lambda i: (i, 0))
    whole = lambda s: pl.BlockSpec(s, lambda i: (0, 0), pipeline_mode=pl.Buffered(1))
    return pl.pallas_call(
        functools.partial(moe_kernel, fl),
        grid=(count // tile,),
        in_specs=[
            rows(wide), rows(width),
            whole(w_in.shape), whole(wd.shape),
        ],
        out_specs=[
            rows(width),
            rows(wide),
            whole((width, hid4)), whole((hid2, width)),
        ],
        out_shape=[
            jax.ShapeDtypeStruct((count, width), BF),
            jax.ShapeDtypeStruct((count, wide), BF),
            jax.ShapeDtypeStruct((width, hid4), BF),
            jax.ShapeDtypeStruct((hid2, width), F32),
        ],
        scratch_shapes=[pltpu.VMEM((width, hid4), F32), pltpu.VMEM((hid2, width), F32)],
        compiler_params=pltpu.CompilerParams(vmem_limit_bytes=66_000_000),
        cost_estimate=pl.CostEstimate(
            flops=2 * count * width * hid2 * 9,
            bytes_accessed=8 * count * width + 24 * hid4 * width,
            transcendentals=count * hid2,
        ),
        name="moe",
    )(h_all, g_all, w_in, wd)


def moe_net_kernel(
    nz, ne, per_dev, slots, h_ref, g_ref, wg_ref, wu_ref, wd_ref,
    hall_ref, mix_ref, gh_ref, dwin_ref, dwd_ref,
    win, wd, acc_in, acc_d, htile, gtile, mixbuf, qbuf, cgot, acc, got, zgot, dbuf,
    wload, tload, mixsem, keep, flush, zsend, zrecv, send, recv,
    csend, crecv, credit, rsend, rrecv, ysend, yrecv,
):
    z, e = lax.axis_index("dp"), lax.axis_index("expert")
    rows, width = g_ref.shape[1], g_ref.shape[2]
    half = rows // 2
    fl = wd.shape[0] // per_dev
    upper = [2 << b for b in range(ne.bit_length() - 2)]
    stages = len(upper)
    pairs = ne // 2
    steps = nz * pairs
    gather_orders = [upper + [1], upper[::-1] + [1]]
    sum_orders = [[1] + upper, [1] + upper[::-1]]
    at = [e]
    for bit in [1] + upper:
        at = at + [flip(i, bit) for i in at]
    partner = (z, at[1])

    def plane(r):
        low = jnp.minimum(z, nz - 1 - z)
        near = jnp.where(lax.rem(r, 2) == 1, z - (r + 1) // 2, z + r // 2)
        far = jnp.where(2 * z < nz, z + (r - low), z - (r - low))
        return jnp.where(r <= 2 * low, near, far)

    planes = [z] + [nearest(z, r, nz) for r in range(1, nz)]

    def part(s):
        return pl.ds(s * half, half)

    def subset_mask(order, subset):
        return sum(bit for b, bit in enumerate(order) if subset >> b & 1)

    def pass_on(r, s, stage, subset, own=False):
        order = gather_orders[s]
        dst = hall_ref.at[plane(r) * ne + at[subset_mask(order, subset)], part(s)]
        n = (1 << stage) - 1 + subset
        src = h_ref.at[part(s)] if own else dst
        return remote(src, dst, send.at[r, s, n], recv.at[r, s, n], (z, at[order[stage]]))

    def take(r, s, stage, subset):
        order = gather_orders[s]
        mask = subset_mask(order, subset) | order[stage]
        n = (1 << stage) - 1 + subset
        here = hall_ref.at[plane(r) * ne + at[mask], part(s)]
        remote(here, here, send.at[r, s, n], recv.at[r, s, n], partner).wait_recv()
        for later in range(stage + 1, stages + 1):
            pass_on(r, s, later, subset + (1 << stage)).start()

    def start_round(r):
        if r > 0:
            here = hall_ref.at[planes[r] * ne + e]
            remote(here, here, zsend.at[r], zrecv.at[planes[r]], partner).wait_recv()
        for stage in range(stages + 1):
            for s in range(2):
                pass_on(r, s, stage, 0, own=r == 0).start()

    def take_pair(r, i):
        if i == 1:
            for stage in range(stages):
                for s in range(2):
                    take(r, s, stage, 0)
        mask = 2 * i
        for s in range(2):
            order = gather_orders[s]
            places = [b for b in range(stages) if order[b] & mask]
            if len(places) > 1:
                take(r, s, places[-1], sum(1 << b for b in places[:-1]))
        for s in range(2):
            order = gather_orders[s]
            take(r, s, stages, sum(1 << b for b in range(stages) if order[b] & mask))

    def blocks_of(k):
        r, i = k // pairs, lax.rem(k, pairs)
        home = plane(r)
        lane = e
        for b, bit in enumerate(upper):
            lane = lane + lax.rem(i // (1 << b), 2) * (at[bit] - e)
        return home, lane, lane + (at[1] - e)

    def loads(k):
        home, one, two = blocks_of(k)
        p = lax.rem(k, 2)
        out = []
        for j, lane in enumerate((one, two)):
            to = pl.ds(j * rows, rows)
            block = home * ne + lane
            out.append(pltpu.make_async_copy(hall_ref.at[block], htile.at[p, to], tload.at[p, 2 * j]))
            out.append(
                pltpu.make_async_copy(g_ref.at[block], gtile.at[p, to], tload.at[p, 2 * j + 1])
            )
        return out

    def mix_out(k):
        home, one, two = blocks_of(k)
        p = lax.rem(k, 2)
        return [
            pltpu.make_async_copy(
                mixbuf.at[p, pl.ds(j * rows, rows)], mix_ref.at[home * ne + lane], mixsem.at[p, j]
            )
            for j, lane in enumerate((one, two))
        ]

    def to_partner(k):
        return remote(
            qbuf.at[lax.rem(k, 2)], cgot.at[lax.rem(k, slots)],
            csend.at[lax.rem(k, 2)], crecv.at[lax.rem(k, slots)], partner,
        )

    def place_of(t, keep_index):
        return (1 << stages) - (1 << (stages - t + 1)) + keep_index

    def push(r, s, t, keep_index):
        order = sum_orders[s]
        mask = order[t] | subset_mask(order[t + 1 :], keep_index)
        n = place_of(t, keep_index)
        return remote(
            acc.at[r, mask // 2, part(s)], got.at[r, s, n],
            rsend.at[r, s, n], rrecv.at[r, s, n], (z, at[order[t]]),
        )

    def merge(k):
        slot = lax.rem(k, slots)
        remote(cgot.at[slot], cgot.at[slot], csend.at[0], crecv.at[slot], partner).wait_recv()
        r, i = k // pairs, lax.rem(k, pairs)
        add_rows(acc.at[r, i], cgot.at[slot])

        @pl.when(k + slots < steps)
        def _():
            pl.semaphore_signal(credit, inc=1, device_id=partner, device_id_type=MESH)

        for j in range(1, pairs):

            @pl.when(i == j)
            def _():
                for s in range(2):
                    order = sum_orders[s]
                    if order[1] & (2 * j):
                        rest = [b for b, bit in enumerate(order[2:]) if bit & (2 * j)]
                        push(r, s, 1, sum(1 << b for b in rest)).start()

    def home_copy(r, s):
        return remote(
            acc.at[r, 0, part(s)], zgot.at[z, part(s)], ysend.at[r, s], yrecv.at[z, s],
            (plane(r), e),
        )

    def settle(r, t):
        for s in range(2):
            order = sum_orders[s]
            for index in range(1 << (stages - t)):
                copy = push(r, s, t, index)
                copy.wait_recv()
                mask = subset_mask(order[t + 1 :], index)
                add_rows(acc.at[r, mask // 2, part(s)], got.at[r, s, place_of(t, index)])
            if t < stages:
                for index in range(1 << (stages - t - 1)):
                    push(r, s, t + 1, index).start()
            else:

                @pl.when(r > 0)
                def _():
                    home_copy(r, s).start()

    weights = []
    for i in range(per_dev):
        cols = pl.ds(z * fl, fl)
        weights += [
            (wg_ref.at[i, :, cols], win.at[:, pl.ds(i * fl, fl)]),
            (wu_ref.at[i, :, cols], win.at[:, pl.ds((per_dev + i) * fl, fl)]),
            (wd_ref.at[i, cols, :], wd.at[pl.ds(i * fl, fl), :]),
        ]
    weights = [
        pltpu.make_async_copy(src, dst, wload.at[j]) for j, (src, dst) in enumerate(weights)
    ]
    for copy in weights:
        copy.start()
    meet_column_and_plane(nz, ne, z, e, True)
    own = pltpu.make_async_copy(h_ref, hall_ref.at[z * ne + e], keep)
    own.start()
    for r in range(1, nz):
        remote(
            h_ref, hall_ref.at[z * ne + e], zsend.at[r], zrecv.at[z], (planes[r], e)
        ).start()
    start_round(0)
    acc_in[...] = jnp.zeros_like(acc_in)
    acc_d[...] = jnp.zeros_like(acc_d)
    take_pair(0, 0)
    own.wait()
    for copy in loads(0):
        copy.start()
    for copy in weights:
        copy.wait()

    tile = 2 * rows
    lanes = lax.broadcasted_iota(jnp.int32, (tile, 128), 1)
    split = 64

    def step(k, carry):
        p = lax.rem(k, 2)
        r, i = k // pairs, lax.rem(k, pairs)
        for copy in loads(k):
            copy.wait()
        pre = dot(htile[p, :, :width], win[...], NN)
        graw = dot(gtile[p], wd[...], NT)
        extra = htile[p, :, width:].astype(F32)
        scaled_act, grad_gate, grad_up = [], [], []
        gg = jnp.zeros((tile, 128), F32)
        for j in range(per_dev):
            u = pre[:, j * fl : (j + 1) * fl]
            w = pre[:, (per_dev + j) * fl : (per_dev + 1 + j) * fl]
            gr = graw[:, j * fl : (j + 1) * fl]
            mine = e * per_dev + j
            picked = (lanes == mine) | (lanes == mine + split)
            gate = jnp.sum(jnp.where(picked, extra, 0.0), axis=-1, keepdims=True)
            sig = 1.0 / (1.0 + jnp.exp(-u))
            silu = u * sig
            act = silu * w
            total = jnp.sum(act.astype(BF).astype(F32) * gr, axis=-1, keepdims=True)
            rounded = total.astype(BF).astype(F32)
            gg = jnp.where(lanes == mine, rounded, gg)
            gg = jnp.where(lanes == mine + split, total - rounded, gg)
            scaled_act.append((gate * act).astype(BF))
            gact = gate * gr
            grad_gate.append((gact * w * (sig * (1.0 + u * (1.0 - sig)))).astype(BF))
            grad_up.append((gact * silu).astype(BF))
        a = jnp.concatenate(scaled_act, axis=1)
        gin = jnp.concatenate(grad_gate + grad_up, axis=1)

        for r1 in range(1, nz):

            @pl.when(k == (r1 - 1) * (pairs - 1) + 1)
            def _():
                start_round(r1)

        @pl.when(k + 1 < steps)
        def _():
            ahead = k + 1
            for j in range(pairs):

                @pl.when(lax.rem(ahead, pairs) == j)
                def _():
                    take_pair(ahead // pairs, j)

            for copy in loads(ahead):
                copy.start()

        @pl.when(k >= 2)
        def _():
            for copy in mix_out(k - 2):
                copy.wait()
            to_partner(k - 2).wait_send()

        mixbuf[p] = dot(a, wd[...], NN).astype(BF)
        for copy in mix_out(k):
            copy.start()
        back = dot(gin, win[...], NT).astype(BF)
        gg = gg.astype(BF)
        acc[r, i, :, :width] = back[:rows]
        acc[r, i, :, width:] = gg[:rows]
        qbuf[p, :, :width] = back[rows:]
        qbuf[p, :, width:] = gg[rows:]
        acc_in[...] += dot(htile[p, :, :width], gin, TN)
        acc_d[...] += dot(a, gtile[p], TN)

        @pl.when(k >= slots)
        def _():
            pl.semaphore_wait(credit, 1)

        to_partner(k).start()

        @pl.when(k >= 1)
        def _():
            merge(k - 1)

        for t in range(1, stages + 1):
            late = k - pairs - 2 * t

            @pl.when((late >= 0) & (lax.rem(late + pairs, pairs) == 0))
            def _():
                settle(late // pairs, t)

        return carry

    lax.fori_loop(0, steps, step, 0)
    merge(steps - 1)
    final = pltpu.make_async_copy(acc_d, dwd_ref, flush.at[0])
    final.start()
    left = sorted(
        (r * pairs + pairs + 2 * t, r, t)
        for r in range(nz)
        for t in range(1, stages + 1)
        if r * pairs + pairs + 2 * t >= steps
    )
    chunk = dbuf.shape[1]

    def flush_chunk(c):
        return pltpu.make_async_copy(
            dbuf.at[c % 2], dwin_ref.at[pl.ds(c * chunk, chunk)], flush.at[1 + c % 2]
        )

    chunks = acc_in.shape[0] // chunk
    for c in range(chunks):
        if c >= 2:
            flush_chunk(c - 2).wait()
        dbuf[c % 2] = acc_in[pl.ds(c * chunk, chunk), :].astype(BF)
        flush_chunk(c).start()
    for _, r, t in left:
        settle(jnp.int32(r), t)
    for s in range(2):
        for r in range(1, nz):
            here = zgot.at[planes[r], part(s)]
            remote(here, here, ysend.at[r, s], yrecv.at[planes[r], s], partner).wait_recv()

        def total_rows(n, carry):
            span = pl.ds(pl.multiple_of(s * half + n * 16, 16), 16)
            total = acc[0, 0, span, :].astype(F32)
            for r in range(1, nz):
                total = total + zgot[planes[r], span, :].astype(F32)
            gh_ref[span, :] = total
            return carry

        lax.fori_loop(0, half // 16, total_rows, 0)
    final.wait()
    for c in range(max(chunks - 2, 0), chunks):
        flush_chunk(c).wait()
    for k in range(max(steps - 2, 0), steps):
        for copy in mix_out(jnp.int32(k)):
            copy.wait()
        to_partner(jnp.int32(k)).wait_send()
    for r in range(nz):
        if r > 0:
            remote(
                h_ref, hall_ref.at[z * ne + e], zsend.at[r], zrecv.at[z], (planes[r], e)
            ).wait_send()
        for s in range(2):
            for stage in range(stages + 1):
                for subset in range(1 << stage):
                    pass_on(r, s, stage, subset, own=r == 0 and subset == 0).wait_send()
            for t in range(1, stages + 1):
                for index in range(1 << (stages - t)):
                    push(r, s, t, index).wait_send()
            if r > 0:
                home_copy(jnp.int32(r), s).wait_send()


def moe_net_scratch(nz, ne, per_dev, rows, width, wide, fl):
    pairs = ne // 2
    slots = 4
    stages = ne.bit_length() - 2
    vmem = [
        ((width, 2 * per_dev * fl), BF),
        ((per_dev * fl, width), BF),
        ((width, 2 * per_dev * fl), F32),
        ((per_dev * fl, width), F32),
        ((2, 2 * rows, wide), BF),
        ((2, 2 * rows, width), BF),
        ((2, 2 * rows, width), BF),
        ((2, rows, wide), BF),
        ((slots, rows, wide), BF),
        ((nz, pairs, rows, wide), BF),
        ((nz, 2, max(pairs - 1, 1), rows // 2, wide), BF),
        ((nz, rows, wide), BF),
        ((2, width // 8, 2 * per_dev * fl), BF),
    ]
    size = sum(functools.reduce(lambda a, b: a * b, s) * (2 if d == BF else 4) for s, d in vmem)
    sems = [
        DMA((3 * per_dev,)), DMA((2, 4)), DMA((2, 2)), DMA, DMA((3,)),
        DMA((nz,)), DMA((nz,)), DMA((nz, 2, ne - 1)), DMA((nz, 2, ne - 1)),
        DMA((2,)), DMA((slots,)), pltpu.SemaphoreType.REGULAR,
        DMA((nz, 2, max(pairs - 1, 1))), DMA((nz, 2, max(pairs - 1, 1))),
        DMA((nz, 2)), DMA((nz, 2)),
    ]
    fits = size <= 54_000_000 and stages >= 1 and nz > 1 and nz * pairs > slots
    return fits, slots, [pltpu.VMEM(*v) for v in vmem] + sems


def moe_net(h, g_all, w_gate, w_up, w_down, nz, ne, fl, slots, scratch, cid):
    rows, wide = h.shape
    per_dev, width, _ = w_gate.shape
    return pl.pallas_call(
        functools.partial(moe_net_kernel, nz, ne, per_dev, slots),
        out_shape=[
            jax.ShapeDtypeStruct((nz * ne, rows, wide), BF),
            jax.ShapeDtypeStruct((nz * ne, rows, width), BF),
            jax.ShapeDtypeStruct((rows, wide), F32),
            jax.ShapeDtypeStruct((width, 2 * per_dev * fl), BF),
            jax.ShapeDtypeStruct((per_dev * fl, width), F32),
        ],
        in_specs=[VMEM, ANY, ANY, ANY, ANY],
        out_specs=[ANY, ANY, VMEM, ANY, ANY],
        scratch_shapes=scratch,
        compiler_params=pltpu.CompilerParams(
            collective_id=cid, has_side_effects=True, vmem_limit_bytes=66_500_000
        ),
        name="moe_net",
    )(h, g_all.reshape(nz * ne, rows, width), w_gate, w_up, w_down)


def body(inputs, segments, routes, w_qkv, w_out, w_router, gains, w_gate, w_up, w_down, cotangent):
    z = lax.axis_index("dp")
    e = lax.axis_index("expert")
    nz = lax.axis_size("dp")
    ne = lax.axis_size("expert")
    count, width = inputs.shape
    num_seqs, length = segments.shape
    heads = width // HD // ne
    hw = heads * HD
    expert_count = w_router.shape[1]
    per_dev = w_gate.shape[0]
    hidden = w_gate.shape[2]
    fl = hidden // nz
    both = ("dp", "expert")

    pad = -(expert_count + 4) % 16
    small = jnp.concatenate(
        [w_router.T, gains.T, jnp.zeros((pad, gains.shape[0]), BF)], axis=0
    )
    seg8 = jnp.broadcast_to(segments[:, None, :], (num_seqs, 8, length)).reshape(-1, length)
    in_all, wq, wo, small, seg_all, g_all = start_gather(
        inputs, w_qkv.transpose(1, 0, 2), w_out, small, seg8, cotangent, nz, ne, hw, 0
    )
    small = small.transpose(1, 0, 2).reshape(-1, width)
    router_t = small[:expert_count]
    gain_mat = small[expert_count : expert_count + 4].astype(F32)
    my_gains = lax.dynamic_slice_in_dim(gain_mat, e * hw, hw, axis=1)
    seg_all = seg_all.reshape(ne * num_seqs, 8, length)

    g_all = g_all.reshape(-1, width)
    inputs_f = inputs.astype(F32)
    tables = rope_lanes(length)
    *saved, x1_part = attn_fwd(in_all, wq, wo, gain_mat, my_gains, seg_all, tables, 9)
    (x1_sum,) = scatter_tokens(x1_part, nz, ne, False, 1)
    x1 = inputs_f + x1_sum

    a2 = rms_scale(x1)
    h2 = (x1 * a2 * gain_mat[3]).astype(BF)
    probs = jax.nn.softmax(dot(h2, router_t, NT), axis=-1)
    picks = jnp.sum(
        (routes[:, :, None] == jnp.arange(expert_count, dtype=jnp.int32)).astype(F32), axis=1
    )
    gates = picks * probs

    split = 64
    high = gates.astype(BF)
    low = (gates - high.astype(F32)).astype(BF)
    blank = jnp.zeros((count, split - expert_count), BF)
    h2_wide = jnp.concatenate([h2, high, blank, low, blank], axis=1)
    wide = width + 2 * split
    fits, slots, scratch = moe_net_scratch(nz, ne, per_dev, count, width, wide, fl)
    if fits:
        _, mix, gh_sum, dwin, dwd = moe_net(
            h2_wide, g_all, w_gate, w_up, w_down, nz, ne, fl, slots, scratch, 2
        )
        mix = mix.reshape(-1, width)
    else:
        h2_all = gather_tokens(h2_wide, nz, ne, True, 2).reshape(-1, wide)
        wg = lax.dynamic_slice_in_dim(w_gate, z * fl, fl, axis=2)
        wu = lax.dynamic_slice_in_dim(w_up, z * fl, fl, axis=2)
        wd = lax.dynamic_slice_in_dim(w_down, z * fl, fl, axis=1).reshape(per_dev * fl, width)
        w_in = jnp.concatenate([*wg, *wu], axis=1)
        mix, gh, dwin, dwd = moe(h2_all, g_all, w_in, wd, per_dev, count, min(4, ne))
        gh_sum, mix = scatter_tokens(
            gh.reshape(nz * ne, count, wide), nz, ne, True, 3, after=mix.reshape(-1, width)
        )
    grad_from_experts = gh_sum[:, :width]
    grad_gates = (
        gh_sum[:, width : width + expert_count]
        + gh_sum[:, width + split : width + split + expert_count]
    )

    dwin = lax.all_to_all(
        dwin.reshape(nz, width // nz, 2 * per_dev * fl),
        "dp", split_axis=0, concat_axis=0, tiled=True,
    )
    grad_w_gate, grad_w_up = lay_experts(dwin, per_dev, fl)
    grad_w_down = dwd.reshape(per_dev, fl, width)

    grad_top = cotangent.astype(F32)
    grad_probs = picks * grad_gates
    glog = (probs * (grad_probs - jnp.sum(probs * grad_probs, axis=-1, keepdims=True))).astype(BF)
    local_router = dot(glog, h2, TN)
    gh2 = grad_from_experts + dot(glog, router_t, NN)
    grad_ffn, gain_ffn = rms_backward(x1, a2, gain_mat[3], gh2)
    gx1 = grad_top + grad_ffn
    gab = gx1.astype(BF)

    gab_all = gather_tokens(gab, nz, ne, False, 4)
    gh1_part, parts, gain_qk = attn_bwd(
        gab_all, wq, wo, my_gains, seg_all, tables, saved, 10
    )
    place = lambda part: lax.dynamic_update_slice_in_dim(
        jnp.zeros((1, width), F32), part[None], e * hw, axis=1
    )
    tiny = jnp.concatenate(
        [
            local_router, jnp.zeros((1, width), F32), place(gain_qk[0]), place(gain_qk[1]),
            gain_ffn[None], jnp.zeros((-(expert_count + 4) % 8, width), F32),
        ],
        axis=0,
    )
    grad_inputs, laid, tiny, output = tail(
        parts, gh1_part, mix.reshape(-1, count, width) if fits else None, inputs, x1, gx1,
        gain_mat, tiny, expert_count, nz, ne, hw, 5,
    )
    if not fits:
        mix = lax.psum_scatter(mix, both, scatter_dimension=0, tiled=True)
        output = add_up(x1, mix)
    grad_w_qkv = laid[:-1].astype(F32).transpose(1, 0, 2)
    grad_w_out = laid[-1].astype(F32)
    grad_w_router = tiny[:expert_count].T
    grad_gains = tiny[expert_count : expert_count + 4].T
    return (
        output,
        grad_inputs,
        grad_w_qkv,
        grad_w_out,
        grad_w_router,
        grad_gains,
        grad_w_gate,
        grad_w_up,
        grad_w_down,
    )


def solution(mesh):
    tokens = P(("dp", "expert"), None)
    rows = P("dp", None)
    rows3 = P("dp", None, None)
    owned = P("expert", None, None)
    return jax.shard_map(
        body,
        mesh=mesh,
        in_specs=(tokens, tokens, tokens, rows3, rows, rows, rows, owned, owned, owned, tokens),
        out_specs=(tokens, tokens, rows3, rows, rows, rows)
        + (P("expert", "dp", None),) * 3,
        check_vma=False,
    )
```

```python
import functools

import jax
import jax.numpy as jnp
from jax import lax
from jax.experimental import pallas as pl
from jax.experimental.pallas import tpu as pltpu
from jax.sharding import PartitionSpec as P


HD = 128
EPS = 1e-05
ROPE_BASE = 10000.0
MASKED = -1e30
BF = jnp.bfloat16
F32 = jnp.float32


def dot(a, b, dims):
    return lax.dot_general(a, b, (dims, ((), ())), preferred_element_type=F32)


NN = ((1,), (0,))
NT = ((1,), (1,))
TN = ((0,), (0,))


def rms_scale(values):
    return lax.rsqrt(jnp.mean(values * values, axis=-1, keepdims=True) + EPS)


def rms_backward(values, inv_rms, gain_col, grad_out):
    normed = values * inv_rms
    grad_gain = jnp.sum(grad_out * normed, axis=0)
    scaled = grad_out * gain_col
    grad_values = inv_rms * (scaled - normed * jnp.mean(scaled * normed, axis=-1, keepdims=True))
    return (grad_values, grad_gain)


MESH = pl.DeviceIdType.MESH
ANY = pl.BlockSpec(memory_space=pl.ANY)
VMEM = pl.BlockSpec(memory_space=pltpu.VMEM)
DMA = pltpu.SemaphoreType.DMA


def flip(index, bit):
    return index + bit * (1 - 2 * ((index // bit) % 2))


def flips(index, bits):
    out = [index]
    for bit in bits:
        out = out + [flip(i, bit) for i in out]
    return out


def bit_orders(ne):
    bits = [1 << b for b in range(ne.bit_length() - 1)]
    return [bits[:1] + bits[1:], bits[:1] + bits[1:][::-1]]


def nearest(z, r, nz):
    low = jnp.minimum(z, nz - 1 - z)
    near = z - (r + 1) // 2 if r % 2 else z + r // 2
    far = jnp.where(2 * z < nz, z + (r - low), z - (r - low))
    return jnp.where(r <= 2 * low, near, far)


def remote(src, dst, send, recv, peer):
    return pltpu.make_async_remote_copy(
        src_ref=src, dst_ref=dst, send_sem=send, recv_sem=recv, device_id=peer, device_id_type=MESH
    )


def for_others(nz, ne, z, e, act):
    def step(i, carry):
        flat = lax.rem(z * ne + e + i, nz * ne)
        act(flat // ne, lax.rem(flat, ne), flat)
        return carry

    lax.fori_loop(1, nz * ne, step, 0)


def meet_all(nz, ne, z, e):
    sem = pltpu.get_barrier_semaphore()

    def greet(zz, ee, flat):
        pl.semaphore_signal(sem, inc=1, device_id=(zz, ee), device_id_type=MESH)

    for_others(nz, ne, z, e, greet)
    pl.semaphore_wait(sem, nz * ne - 1)


def meet_column_and_plane(nz, ne, z, e, spread):
    sem = pltpu.get_barrier_semaphore()
    peers = [(z, flip(e, 1 << b)) for b in range(ne.bit_length() - 1)]
    if spread:
        peers += [(lax.rem(z + r, nz), e) for r in range(1, nz)]
    for peer in peers:
        pl.semaphore_signal(sem, inc=1, device_id=peer, device_id_type=MESH)
    pl.semaphore_wait(sem, len(peers))


class PlaneGather:
    def __init__(self, nz, ne, z, e, spread, x_ref, out_ref, zsend, zrecv, send, recv, local):
        self.nz, self.ne, self.z, self.e, self.spread = nz, ne, z, e, spread
        self.x, self.out = x_ref, out_ref
        self.zsend, self.zrecv, self.send, self.recv = zsend, zrecv, send, recv
        self.rounds = nz if spread else 1
        self.half = x_ref.shape[0] // 2
        self.orders = [o[1:] + o[:1] for o in bit_orders(ne)]
        self.planes = [z if spread else 0] + [nearest(z, r, nz) for r in range(1, self.rounds)]
        self.pending, self.arrivals = [], {}
        own = self.slot(0, e)
        keep = pltpu.make_async_copy(x_ref, out_ref.at[own], local)
        keep.start()
        self.pending.append(keep.wait)

    @staticmethod
    def scratch(nz, ne, spread):
        rounds = nz if spread else 1
        return [DMA((nz,)), DMA((nz,)), DMA((rounds, 2, ne - 1)), DMA((rounds, 2, ne - 1)), DMA]

    def slot(self, r, ee):
        return self.planes[r] * self.ne + ee

    def spread_own(self):
        for r in range(1, self.rounds):
            to = self.planes[r]
            copy = remote(
                self.x, self.out.at[self.slot(0, self.e)],
                self.zsend.at[r], self.zrecv.at[self.z], (to, self.e),
            )
            copy.start()
            self.pending.append(copy.wait_send)

    def forward(self, r, s, stage, subset):
        order = self.orders[s]
        rows = pl.ds(s * self.half, self.half)
        peer_e = flip(self.e, order[stage])
        n = (1 << stage) - 1 + subset
        block = self.slot(r, flips(self.e, order[:stage])[subset])
        dst = self.out.at[block, rows]
        src = self.x.at[rows] if r == 0 and subset == 0 else dst
        sems = self.send.at[r, s, n], self.recv.at[r, s, n]
        copy = remote(src, dst, *sems, (self.z, peer_e))
        copy.start()
        self.pending.append(copy.wait_send)
        got = self.out.at[self.slot(r, flips(peer_e, order[:stage])[subset]), rows]
        self.arrivals[(r, s, stage, subset)] = remote(got, got, *sems, (self.z, peer_e)).wait_recv

    def start_round(self, r):
        if r > 0:
            here = self.out.at[self.slot(r, self.e)]
            remote(
                here, here, self.zsend.at[r], self.zrecv.at[self.planes[r]], (self.planes[r], self.e)
            ).wait_recv()
        for stage in range(len(self.orders[0])):
            for s in range(2):
                self.forward(r, s, stage, 0)

    def finish_round(self, r):
        stages = len(self.orders[0])
        for stage in range(stages):
            for subset in range(1 << stage):
                for s in range(2):
                    self.arrivals.pop((r, s, stage, subset))()
                    for later in range(stage + 1, stages):
                        self.forward(r, s, later, subset + (1 << stage))

    def finish(self):
        for wait in self.pending:
            wait()


def gather_kernel(nz, ne, spread, x_ref, out_ref, *sems):
    z, e = lax.axis_index("dp"), lax.axis_index("expert")
    meet_column_and_plane(nz, ne, z, e, spread)
    net = PlaneGather(nz, ne, z, e, spread, x_ref, out_ref, *sems)
    net.spread_own()
    net.start_round(0)
    for r in range(1, net.rounds):
        net.start_round(r)
        net.finish_round(r - 1)
    net.finish_round(net.rounds - 1)
    net.finish()


def gather_tokens(x, nz, ne, spread, cid):
    rounds = nz if spread else 1
    return pl.pallas_call(
        functools.partial(gather_kernel, nz, ne, spread),
        out_shape=jax.ShapeDtypeStruct((rounds * ne, *x.shape), x.dtype),
        in_specs=[VMEM],
        out_specs=ANY,
        scratch_shapes=PlaneGather.scratch(nz, ne, spread),
        compiler_params=pltpu.CompilerParams(collective_id=cid, has_side_effects=True),
        name="gather_tokens",
    )(x)


def add_rows(dst, src, tile=16):
    def step(i, carry):
        rows = pl.ds(pl.multiple_of(i * tile, tile), tile)
        dst[rows, :] = dst[rows, :] + src[rows, :]
        return carry

    lax.fori_loop(0, dst.shape[0] // tile, step, 0)


class TokenScatter:
    def __init__(self, nz, ne, z, e, ranks, x_ref, acc, got, zgot, loads, send, recv, zsend, zrecv):
        self.nz, self.ne, self.z, self.e = nz, ne, z, e
        self.x, self.acc, self.got, self.zgot = x_ref, acc, got, zgot
        self.loads, self.send, self.recv, self.zsend, self.zrecv = loads, send, recv, zsend, zrecv
        self.ranks = ranks
        self.stages = ne.bit_length() - 1
        self.steps = len(ranks) + self.stages - 1
        self.half = acc.shape[3]
        self.orders = bit_orders(ne)
        self.first = [0]
        for j in range(self.stages):
            self.first.append(self.first[j] + (ne >> (j + 1)))
        self.pending, self.arrivals, self.zwait = [], {}, []

    def block(self, r, ee):
        if self.ranks[r] is None:
            return ee
        return lax.rem(self.z + self.ranks[r], self.nz) * self.ne + ee

    def push(self, r, s, j):
        order = self.orders[s]
        peer_e = flip(self.e, order[j])
        rest = self.ne >> (j + 1)
        for i in range(rest):
            n = self.first[j] + i
            if j == 0:
                ee = flips(peer_e, order[:0:-1])[i]
                src = self.x.at[self.block(r, ee), pl.ds(s * self.half, self.half)]
            else:
                src = self.acc.at[r, s, rest + i]
            copy = remote(
                src, self.got.at[r, s, n], self.send.at[r, s, n], self.recv.at[r, s, n],
                (self.z, peer_e),
            )
            copy.start()
            self.pending.append(copy.wait_send)
            self.arrivals.setdefault((r, s, j), []).append((copy.wait_recv, i, n))

    def start(self):
        for r in range(len(self.ranks)):
            for s in range(2):
                self.push(r, s, 0)
                for i, ee in enumerate(flips(self.e, self.orders[s][:0:-1])):
                    copy = pltpu.make_async_copy(
                        self.x.at[self.block(r, ee), pl.ds(s * self.half, self.half)],
                        self.acc.at[r, s, i],
                        self.loads.at[r, s, i],
                    )
                    copy.start()
                    self.arrivals.setdefault((r, s, -1), []).append(copy.wait)

    def step(self, t):
        for r, rank in enumerate(self.ranks):
            j = t - r
            if not 0 <= j < self.stages:
                continue
            for s in range(2):
                if j == 0:
                    for wait in self.arrivals.pop((r, s, -1)):
                        wait()
                for wait, i, n in self.arrivals.pop((r, s, j)):
                    wait()
                    add_rows(self.acc.at[r, s, i], self.got.at[r, s, n])
                if j + 1 < self.stages:
                    self.push(r, s, j + 1)
                elif rank:
                    copy = remote(
                        self.acc.at[r, s, 0], self.zgot.at[r, s],
                        self.zsend.at[r, s], self.zrecv.at[r, s],
                        (lax.rem(self.z + rank, self.nz), self.e),
                    )
                    copy.start()
                    self.pending.append(copy.wait_send)
                    self.zwait.append(copy.wait_recv)

    def arrive(self):
        for wait in self.zwait:
            wait()

    def rows(self, s, here):
        parts = [
            self.zgot[r, s, here, :] if rank else self.acc[r, s, 0, here, :]
            for r, rank in enumerate(self.ranks)
        ]
        return sum(part.astype(F32) for part in parts)

    def finish(self):
        for wait in self.pending:
            wait()

    @staticmethod
    def scratch(ne, ranks, count, width):
        rounds = len(ranks)
        half = count // 2
        return [
            pltpu.VMEM((rounds, 2, ne // 2, half, width), BF),
            pltpu.VMEM((rounds, 2, ne - 1, half, width), BF),
            pltpu.VMEM((rounds, 2, half, width), BF),
            DMA((rounds, 2, ne // 2)),
            DMA((rounds, 2, ne - 1)),
            DMA((rounds, 2, ne - 1)),
            DMA((rounds, 2)),
            DMA((rounds, 2)),
        ]


def split_ranks(nz):
    ranks = scatter_ranks(nz, True)
    return ranks[: nz // 2], ranks[nz // 2 :]


def scatter_ranks(nz, spread):
    return [*range(1, nz), 0] if spread else [None]


def over_rows(half, act, tile=16):
    for s in range(2):

        def step(n, carry):
            here = pl.ds(pl.multiple_of(n * tile, tile), tile)
            span = pl.ds(pl.multiple_of(s * half + n * tile, tile), tile)
            act(s, here, span)
            return carry

        lax.fori_loop(0, half // tile, step, 0)


def scatter_kernel(nz, ne, spread, x_ref, *refs):
    out_ref, *rest = refs[-9:]
    z, e = lax.axis_index("dp"), lax.axis_index("expert")
    meet_column_and_plane(nz, ne, z, e, spread)
    net = TokenScatter(nz, ne, z, e, scatter_ranks(nz, spread), x_ref, *rest)
    net.start()
    for t in range(net.steps):
        net.step(t)
    net.arrive()

    def write(s, here, span):
        out_ref[span, :] = net.rows(s, here)

    over_rows(net.half, write)
    net.finish()


def scatter_tokens(parts, nz, ne, spread, cid, after=None):
    rounds = nz if spread else 1
    _, count, width = parts.shape
    half = count // 2
    held = (2 * rounds * (ne // 2 + ne - 1) + 2 * nz) * half * width * 2
    if held > 56_000_000:
        cut = width // 256 * 128
        left = scatter_tokens(parts[..., :cut], nz, ne, spread, cid, after)
        right = scatter_tokens(parts[..., cut:], nz, ne, spread, cid + 16)
        return [jnp.concatenate([left[0], right[0]], axis=1), *left[1:]]
    more = [] if after is None else [after]
    return pl.pallas_call(
        functools.partial(scatter_kernel, nz, ne, spread),
        out_shape=[jax.ShapeDtypeStruct(m.shape, m.dtype) for m in more]
        + [jax.ShapeDtypeStruct((count, width), F32)],
        in_specs=[ANY] * (1 + len(more)),
        out_specs=[ANY] * len(more) + [VMEM],
        scratch_shapes=TokenScatter.scratch(ne, scatter_ranks(nz, spread), count, width),
        input_output_aliases={1: 0} if more else {},
        compiler_params=pltpu.CompilerParams(
            collective_id=cid, has_side_effects=True, vmem_limit_bytes=64_000_000
        ),
        name="scatter_tokens",
    )(parts, *more)[::-1]


def start_kernel(
    nz, ne, x_ref, wqkv_ref, wout_ref, small_ref, seg_ref, cot_ref,
    out_ref, wq_ref, wo_ref, small_out, seg_out, cot_out,
    wbuf, pbuf, zsend, zrecv, send, recv, local, czsend, czrecv, csend, crecv, clocal,
    up_send, up_recv, dn_send, dn_recv, wload, wkeep, pload, psend, precv, pkeep,
    small_send, small_recv, seg_send, seg_recv,
):
    z, e = lax.axis_index("dp"), lax.axis_index("expert")
    kinds, depth, hw = wbuf.shape
    per = ne // nz
    loads = [
        pltpu.make_async_copy(wqkv_ref.at[j, :, pl.ds(e * hw, hw)], wbuf.at[j], wload.at[j])
        for j in range(kinds)
    ]
    for copy in loads:
        copy.start()
    pieces = [
        pltpu.make_async_copy(
            wout_ref.at[pl.ds(i * hw, hw), pl.ds(e * hw, hw)], pbuf.at[i], pload.at[i]
        )
        for i in range(per)
    ]
    for copy in pieces:
        copy.start()
    meet_all(nz, ne, z, e)
    cot = PlaneGather(
        nz, ne, z, e, True, cot_ref, cot_out, czsend, czrecv, csend, crecv, clocal
    )
    cot.spread_own()

    def rows_of(zz):
        return pl.ds(pl.multiple_of(zz * depth, depth), depth)

    def hop(j, zz, dist, up):
        send, recv = (up_send, up_recv) if up else (dn_send, dn_recv)
        here = wq_ref.at[j, rows_of(zz)]
        src = wbuf.at[j] if dist == 1 else here
        to = z + 1 if up else z - 1
        return remote(src, here, send.at[dist, j], recv.at[dist, j], (to, e))

    keeps = []
    for j in range(kinds):
        loads[j].wait()

        @pl.when(z + 1 < nz)
        def _():
            hop(j, z, 1, True).start()

        @pl.when(z > 0)
        def _():
            hop(j, z, 1, False).start()

        keep = pltpu.make_async_copy(wbuf.at[j], wq_ref.at[j, rows_of(z)], wkeep.at[j])
        keep.start()
        keeps.append(keep)

    def wait_all(ref, send, recv, count):
        most = ref.at[pl.ds(0, count)]
        both = remote(most, most, send, recv, (z, flip(e, 1)))
        both.wait_send()
        both.wait_recv()

    small_out[z] = small_ref[...]
    for r in range(1, nz):
        remote(
            small_ref, small_out.at[z], small_send, small_recv, (lax.rem(z + r, nz), e)
        ).start()
    seg_out[e] = seg_ref[...]
    for r in range(1, ne):
        remote(seg_ref, seg_out.at[e], seg_send, seg_recv, (z, lax.rem(e + r, ne))).start()
    net = PlaneGather(nz, ne, z, e, False, x_ref, out_ref, zsend, zrecv, send, recv, local)
    net.start_round(0)
    cot.start_round(0)

    columns = pl.ds(e * hw, hw)
    for i in range(per):
        pieces[i].wait()
    for r in range(nz):
        for i in range(per):
            to = (lax.rem(z + r, nz), z * per + i)
            give = remote(pbuf.at[i], wo_ref.at[:, columns], psend.at[r, i], precv, to)
            if r > 0:
                give.start()
            else:
                own = pltpu.make_async_copy(pbuf.at[i], wo_ref.at[:, columns], pkeep)

                @pl.when(to[1] == e)
                def _():
                    own.start()

                @pl.when(to[1] != e)
                def _():
                    give.start()
    net.finish_round(0)
    for r in range(1, nz):
        cot.start_round(r)
        if r + 1 < nz:
            cot.finish_round(r - 1)
    left = list(range(max(nz - 2, 0), nz))
    for dist in range(1, nz):
        for j in range(kinds):

            @pl.when(z - dist >= 0)
            def _():
                got = wq_ref.at[j, rows_of(z - dist)]
                remote(got, got, up_send.at[dist, j], up_recv.at[dist, j], (z, e)).wait_recv()

                @pl.when(z + 1 < nz)
                def _():
                    if dist + 1 < nz:
                        hop(j, z - dist, dist + 1, True).start()

            @pl.when(z + dist < nz)
            def _():
                got = wq_ref.at[j, rows_of(z + dist)]
                remote(got, got, dn_send.at[dist, j], dn_recv.at[dist, j], (z, e)).wait_recv()

                @pl.when(z > 0)
                def _():
                    if dist + 1 < nz:
                        hop(j, z + dist, dist + 1, False).start()

        if left:
            cot.finish_round(left.pop(0))
    for r in left:
        cot.finish_round(r)
    cot.finish()
    net.finish()
    for keep in keeps:
        keep.wait()
    for dist in range(1, nz):
        for j in range(kinds):

            @pl.when((z - dist + 1 >= 0) & (z + 1 < nz))
            def _():
                hop(j, z - dist + 1, dist, True).wait_send()

            @pl.when((z + dist - 1 < nz) & (z > 0))
            def _():
                hop(j, z + dist - 1, dist, False).wait_send()

    for r in range(nz):
        for i in range(per):
            to = (lax.rem(z + r, nz), z * per + i)
            give = remote(pbuf.at[i], wo_ref.at[:, columns], psend.at[r, i], precv, to)
            if r > 0:
                give.wait_send()
            else:
                own = pltpu.make_async_copy(pbuf.at[i], wo_ref.at[:, columns], pkeep)

                @pl.when(to[1] == e)
                def _():
                    own.wait()

                @pl.when(to[1] != e)
                def _():
                    give.wait_send()

    def wait_pieces(count):
        most = wo_ref.at[:, pl.ds(0, count * hw)]
        remote(most, most, psend.at[0, 0], precv, (z, e)).wait_recv()

    @pl.when(z == e // per)
    def _():
        wait_pieces(ne - 1)

    @pl.when(z != e // per)
    def _():
        wait_pieces(ne)

    wait_all(small_out, small_send, small_recv, nz - 1)
    wait_all(seg_out, seg_send, seg_recv, ne - 1)


def start_gather(x, w_qkv, w_out, small, seg, cot, nz, ne, hw, cid):
    kinds, depth, width = w_qkv.shape
    per = ne // nz
    return pl.pallas_call(
        functools.partial(start_kernel, nz, ne),
        out_shape=[
            jax.ShapeDtypeStruct((ne, *x.shape), x.dtype),
            jax.ShapeDtypeStruct((kinds, nz * depth, hw), BF),
            jax.ShapeDtypeStruct((hw, width), BF),
            jax.ShapeDtypeStruct((nz, *small.shape), small.dtype),
            jax.ShapeDtypeStruct((ne, *seg.shape), seg.dtype),
            jax.ShapeDtypeStruct((nz * ne, *cot.shape), cot.dtype),
        ],
        in_specs=[VMEM, ANY, ANY, VMEM, VMEM, VMEM],
        out_specs=[ANY, ANY, ANY, VMEM, VMEM, ANY],
        scratch_shapes=[
            pltpu.VMEM((kinds, depth, hw), BF),
            pltpu.VMEM((per, hw, hw), BF),
            *PlaneGather.scratch(nz, ne, False),
            *PlaneGather.scratch(nz, ne, True),
            DMA((nz, kinds)), DMA((nz, kinds)), DMA((nz, kinds)), DMA((nz, kinds)),
            DMA((kinds,)), DMA((kinds,)), DMA((per,)), DMA((nz, per)), DMA, DMA,
            DMA, DMA, DMA, DMA,
        ],
        compiler_params=pltpu.CompilerParams(collective_id=cid, has_side_effects=True),
        name="start_gather",
    )(x, w_qkv, w_out, small, seg, cot)


def rope_lanes(length):
    half = HD // 2
    freqs = jnp.exp(-jnp.log(ROPE_BASE) * (2.0 * jnp.arange(half, dtype=F32) / HD))
    angles = jnp.arange(length, dtype=F32)[:, None] * freqs[None, :]
    cos, sin = jnp.cos(angles), jnp.sin(angles)
    return jnp.concatenate([cos, cos], axis=1), jnp.concatenate([-sin, sin], axis=1)


def turn(x, cos, sin):
    return x * cos + pltpu.roll(x, HD // 2, 1) * sin


def meet_plane(ne, z, e):
    sem = pltpu.get_barrier_semaphore()
    for r in range(1, ne):
        pl.semaphore_signal(
            sem, inc=1, device_id=(z, lax.rem(e + r, ne)), device_id_type=MESH
        )
    pl.semaphore_wait(sem, ne - 1)


def plane_totals(ne, z, e, mine, theirs, send, recv):
    copies = []
    for r in range(1, ne):
        to = (z, lax.rem(e + r, ne))
        copy = remote(mine, theirs.at[r], send.at[r], recv.at[r], to)
        copy.start()
        copies.append(copy)
    total = mine[...]
    for r, copy in enumerate(copies):
        copy.wait_recv()
        total = total + theirs[r + 1]
    for copy in copies:
        copy.wait_send()
    return total


def store_columns(sums, first, columns):
    rows = columns[0].shape[0]
    lanes = lax.broadcasted_iota(jnp.int32, (rows, 128), 1)
    wide = jnp.zeros((rows, 128), F32)
    for j, column in enumerate(columns):
        wide = jnp.where(lanes == j, column, wide)
    sums[:, pl.ds(first, rows)] = wide.T[:8]


def as_columns(total, out):
    rows = total.shape[1]
    for first in range(0, rows, 128):
        chunk = total[:, first : first + 128]
        out[first : first + 128, :] = jnp.concatenate([chunk] * 16, axis=0).T


def allowed_pairs(seg_ref, n):
    length = seg_ref.shape[2]
    keys = jnp.broadcast_to(seg_ref[n, :1].astype(F32), (length, length))
    i = lax.broadcasted_iota(jnp.int32, (length, length), 0)
    j = lax.broadcasted_iota(jnp.int32, (length, length), 1)
    return (i >= j) & (keys == keys.T)


def attend(rq, rk, allowed):
    scores = jnp.where(allowed, dot(rq, rk, NT) * HD ** (-0.5), MASKED)
    top = jnp.max(scores, axis=-1, keepdims=True)
    lse = top + jnp.log(jnp.sum(jnp.exp(scores - top), axis=-1, keepdims=True))
    return jnp.exp(scores - lse)


def attn_fwd_kernel(
    ne, x_ref, wq_ref, wo_ref, gain_ref, mine_ref, seg_ref, cos_ref, sin_ref,
    h1_ref, q_ref, k_ref, rq_ref, rk_ref, v_ref, o_ref, scale_ref, x1_ref,
    sums, theirs, send, recv,
):
    z, e = lax.axis_index("dp"), lax.axis_index("expert")
    width = x_ref.shape[2]
    count, hw = q_ref.shape
    length = seg_ref.shape[2]
    rows_dev = x_ref.shape[1]
    tile = min(512, count)
    meet_plane(ne, z, e)

    def normed(b, carry):
        x = x_ref[b].astype(F32)
        h1 = x * rms_scale(x) * gain_ref[:1]
        h1_ref[pl.ds(pl.multiple_of(b * rows_dev, rows_dev), rows_dev), :] = h1.astype(BF)
        return carry

    lax.fori_loop(0, ne, normed, 0)
    for first in range(0, count, tile):
        rows = slice(first, first + tile)
        h1 = h1_ref[rows, :]
        q, k = dot(h1, wq_ref[0], NN), dot(h1, wq_ref[1], NN)
        q_ref[rows, :] = q
        k_ref[rows, :] = k
        v_ref[rows, :] = dot(h1, wq_ref[2], NN).astype(BF)
        store_columns(
            sums, first, [jnp.sum(t * t, axis=-1, keepdims=True) for t in (q, k)]
        )
    total = plane_totals(ne, z, e, sums, theirs, send, recv)
    as_columns(lax.rsqrt(total / width + EPS), scale_ref)
    cos, sin = cos_ref[...], sin_ref[...]

    def sequence(n, carry):
        rows = pl.ds(pl.multiple_of(n * length, length), length)
        allowed = allowed_pairs(seg_ref, n)
        aq, ak = scale_ref[rows, 0:1], scale_ref[rows, 1:2]
        for c in range(0, hw, HD):
            cols = slice(c, c + HD)
            rq = turn(q_ref[rows, cols] * aq * mine_ref[1:2, cols], cos, sin).astype(BF)
            rk = turn(k_ref[rows, cols] * ak * mine_ref[2:3, cols], cos, sin).astype(BF)
            rq_ref[rows, cols] = rq
            rk_ref[rows, cols] = rk
            probs = attend(rq, rk, allowed).astype(BF)
            o_ref[rows, cols] = dot(probs, v_ref[rows, cols], NN).astype(BF)
        return carry

    lax.fori_loop(0, count // length, sequence, 0)
    for first in range(0, count, tile):
        x1 = dot(o_ref[first : first + tile, :], wo_ref[...], NN).astype(BF)
        blocks = tile // rows_dev
        x1_ref[first // rows_dev : first // rows_dev + blocks] = x1.reshape(
            blocks, rows_dev, width
        )


def attn_fwd(in_all, wq, wo, gain_mat, my_gains, seg, tables, cid):
    ne, rows_dev, width = in_all.shape
    count, hw = ne * rows_dev, wo.shape[0]
    return pl.pallas_call(
        functools.partial(attn_fwd_kernel, ne),
        out_shape=[
            jax.ShapeDtypeStruct((count, width), BF),
            jax.ShapeDtypeStruct((count, hw), F32),
            jax.ShapeDtypeStruct((count, hw), F32),
            jax.ShapeDtypeStruct((count, hw), BF),
            jax.ShapeDtypeStruct((count, hw), BF),
            jax.ShapeDtypeStruct((count, hw), BF),
            jax.ShapeDtypeStruct((count, hw), BF),
            jax.ShapeDtypeStruct((count, 128), F32),
            jax.ShapeDtypeStruct((ne, rows_dev, width), BF),
        ],
        in_specs=[VMEM] * 8,
        out_specs=[VMEM] * 9,
        scratch_shapes=[
            pltpu.VMEM((8, count), F32), pltpu.VMEM((ne, 8, count), F32), DMA((ne,)), DMA((ne,)),
        ],
        compiler_params=pltpu.CompilerParams(
            collective_id=cid, has_side_effects=True, vmem_limit_bytes=60_000_000
        ),
        name="attn_fwd",
    )(in_all, wq, wo, gain_mat, my_gains, seg, *tables)


def attn_bwd_kernel(
    nz, ne, with_mix, gab_ref, wq_ref, wo_ref, mine_ref, seg_ref, cos_ref, sin_ref,
    h1_ref, q_ref, k_ref, rq_ref, rk_ref, v_ref, o_ref, scale_ref, x1_ref, mix_ref,
    gh1_ref, parts_ref, gain_ref, x1m_ref,
    pout, go_ref, gqn_ref, gkn_ref, gp_ref, sums, theirs, means, send, recv, psend, precv,
    *mix_scratch,
):
    z, e = lax.axis_index("dp"), lax.axis_index("expert")
    count, hw = q_ref.shape
    width = gab_ref.shape[2]
    rows_dev = gab_ref.shape[1]
    length = seg_ref.shape[2]
    tile = min(512, count)
    blocks = tile // rows_dev
    if with_mix:
        meet_all(nz, ne, z, e)
        mix = TokenScatter(nz, ne, z, e, split_ranks(nz)[0], mix_ref, *mix_scratch)
        mix.start()
    else:
        meet_plane(ne, z, e)

    def mix_step(t):
        if with_mix and t < mix.steps:
            mix.step(t)

    gab = lambda first: gab_ref[first // rows_dev : first // rows_dev + blocks].reshape(tile, width)
    part = dot(o_ref[:tile, :], gab(0), TN)
    for first in range(tile, count, tile):
        part = part + dot(o_ref[first : first + tile, :], gab(first), TN)
    pout[...] = part.astype(BF)
    for first in range(0, count, tile):
        go_ref[first : first + tile, :] = dot(gab(first), wo_ref[...], NT).astype(BF)
    my_rows = pl.ds(pl.multiple_of(e * hw, hw), hw)
    last = pl.ds(3 * hw, hw)
    gives = []
    for r in range(1, ne):
        to = lax.rem(e + r, ne)
        give = remote(
            pout.at[:, pl.ds(pl.multiple_of(to * hw, hw), hw)], parts_ref.at[my_rows, last],
            psend.at[r], precv.at[r], (z, to),
        )
        give.start()
        gives.append(give)
    parts_ref[my_rows, last] = pout[:, my_rows]
    mix_step(0)

    cos, sin = cos_ref[...], -sin_ref[...]
    gain_ref[...] = jnp.zeros_like(gain_ref)

    def sequence(n, carry):
        start = pl.multiple_of(n * length, length)
        rows = pl.ds(start, length)
        allowed = allowed_pairs(seg_ref, n)
        aq, ak = scale_ref[rows, 0:1], scale_ref[rows, 1:2]
        sum_q = jnp.zeros((length, 1), F32)
        sum_k = jnp.zeros((length, 1), F32)
        for c in range(0, hw, HD):
            cols = slice(c, c + HD)
            rq, rk, go = rq_ref[rows, cols], rk_ref[rows, cols], go_ref[rows, cols]
            probs = attend(rq, rk, allowed)
            gv = dot(probs.astype(BF), go, TN).astype(BF)
            gp_ref[rows, slice(2 * hw + c, 2 * hw + c + HD)] = gv
            grad = dot(go, v_ref[rows, cols], NT)
            delta = jnp.sum(probs * grad, axis=-1, keepdims=True)
            gs = (probs * (grad - delta) * HD ** (-0.5)).astype(BF)
            gqn = turn(dot(gs, rk, NN), cos, sin)
            gkn = turn(dot(gs, rq, TN), cos, sin)
            gqn_ref[rows, cols] = gqn
            gkn_ref[rows, cols] = gkn
            tq = gqn * (q_ref[rows, cols] * aq)
            tk = gkn * (k_ref[rows, cols] * ak)
            gain_ref[0:1, cols] += jnp.sum(tq, axis=0, keepdims=True)
            gain_ref[1:2, cols] += jnp.sum(tk, axis=0, keepdims=True)
            sum_q = sum_q + jnp.sum(tq * mine_ref[1:2, cols], axis=-1, keepdims=True)
            sum_k = sum_k + jnp.sum(tk * mine_ref[2:3, cols], axis=-1, keepdims=True)
        store_columns(sums, start, [sum_q, sum_k])
        return carry

    seqs = count // length
    lax.fori_loop(0, seqs // 2, sequence, 0)
    mix_step(1)
    lax.fori_loop(seqs // 2, seqs, sequence, 0)
    mix_step(2)
    total = plane_totals(ne, z, e, sums, theirs, send, recv)
    mix_step(3)
    as_columns(total / width, means)
    for first in range(0, count, tile):
        rows = slice(first, first + tile)
        aq, ak = scale_ref[rows, 0:1], scale_ref[rows, 1:2]
        mq, mk = means[rows, 0:1], means[rows, 1:2]
        gq = aq * (gqn_ref[rows, :] * mine_ref[1:2] - q_ref[rows, :] * aq * mq)
        gk = ak * (gkn_ref[rows, :] * mine_ref[2:3] - k_ref[rows, :] * ak * mk)
        gp_ref[rows, :hw] = gq.astype(BF)
        gp_ref[rows, hw : 2 * hw] = gk.astype(BF)
    for first in range(0, width, tile):
        rows = slice(first, first + tile)
        parts_ref[rows, : 3 * hw] = dot(h1_ref[:, rows], gp_ref[...], TN).astype(BF)
    for first in range(0, count, tile):
        rows = slice(first, first + tile)
        gh1 = dot(gp_ref[rows, :hw], wq_ref[0], NT)
        for j in range(1, 3):
            gh1 = gh1 + dot(gp_ref[rows, j * hw : (j + 1) * hw], wq_ref[j], NT)
        gh1_ref[first // rows_dev : first // rows_dev + blocks] = gh1.astype(BF).reshape(
            blocks, rows_dev, width
        )
    for give in gives:
        give.wait_send()
        give.wait_recv()
    if with_mix:
        for t in range(4, mix.steps):
            mix_step(t)
        mix.arrive()

        def add_part(s, here, span):
            x1m_ref[span, :] = x1_ref[span, :] + mix.rows(s, here)

        over_rows(mix.half, add_part)
        mix.finish()
    else:
        x1m_ref[...] = x1_ref[...]


def attn_bwd(gab, wq, wo, my_gains, seg, tables, saved, x1, mix, nz, cid):
    ne, rows_dev, width = gab.shape
    count, hw = ne * rows_dev, wo.shape[0]
    return pl.pallas_call(
        functools.partial(attn_bwd_kernel, nz, ne, mix is not None),
        out_shape=[
            jax.ShapeDtypeStruct((ne, rows_dev, width), BF),
            jax.ShapeDtypeStruct((width, 4 * hw), BF),
            jax.ShapeDtypeStruct((8, hw), F32),
            jax.ShapeDtypeStruct((rows_dev, width), F32),
        ],
        in_specs=[VMEM] * 16 + [ANY],
        out_specs=[VMEM] * 4,
        scratch_shapes=[
            pltpu.VMEM((hw, width), BF),
            pltpu.VMEM((count, hw), BF),
            pltpu.VMEM((count, hw), F32),
            pltpu.VMEM((count, hw), F32),
            pltpu.VMEM((count, 3 * hw), BF),
            pltpu.VMEM((8, count), F32),
            pltpu.VMEM((ne, 8, count), F32),
            pltpu.VMEM((count, 128), F32),
            DMA((ne,)), DMA((ne,)), DMA((ne,)), DMA((ne,)),
        ]
        + (
            []
            if mix is None
            else TokenScatter.scratch(ne, split_ranks(nz)[0], rows_dev, width)
        ),
        compiler_params=pltpu.CompilerParams(
            collective_id=cid, has_side_effects=True, vmem_limit_bytes=64_000_000
        ),
        name="attn_bwd",
    )(gab, wq, wo, my_gains, seg, *tables, *saved, x1, gab if mix is None else mix)


def tail_kernel(
    nz, ne, kinds, gain_row, with_mix, parts_ref, gh1_ref, mix_ref, x_ref, x1_ref, gx1_ref,
    gain_ref, tiny_ref, grad_ref, laid_ref, small_ref, out_ref,
    work, below, above, wide, gsum, tbuf, tgot, total, far,
    wload, usend, urecv, dsend, drecv, zsend, zrecv, gsend, grecv, glocal,
    flush, send1, recv1, send2, recv2, *nets_scratch,
):
    z, e = lax.axis_index("dp"), lax.axis_index("expert")
    per = ne // nz
    chunks, rows = work.shape[1], work.shape[2]
    hw = work.shape[3] // kinds
    width = x_ref.shape[1]
    loads = [
        pltpu.make_async_copy(
            parts_ref.at[pl.ds((t * chunks + c) * rows, rows)], work.at[t, c], wload.at[t, c]
        )
        for c in range(chunks)
        for t in range(nz)
    ]
    for copy in loads:
        copy.start()
    meet_all(nz, ne, z, e)
    mine = TokenScatter(nz, ne, z, e, [None], gh1_ref, *nets_scratch[:8])
    mine.start()
    if with_mix:
        mix = TokenScatter(nz, ne, z, e, split_ranks(nz)[1], mix_ref, *nets_scratch[8:])
        mix.start()
    for copy in loads:
        copy.wait()

    def rise(t, c):
        return remote(
            work.at[t, c], below.at[t, c], usend.at[t, c], urecv.at[t, c], (z + 1, e)
        )

    def sink(t, c):
        return remote(
            work.at[t, c], above.at[t, c], dsend.at[t, c], drecv.at[t, c], (z - 1, e)
        )

    for c in range(chunks):
        for t in range(nz - 1, 0, -1):

            @pl.when(z == 0)
            def _():
                rise(t, c).start()

        for t in range(nz - 1):

            @pl.when(z == nz - 1)
            def _():
                sink(t, c).start()

    def arrive(t, c, buffer, recv):
        remote(buffer.at[t, c], buffer.at[t, c], usend.at[0, 0], recv.at[t, c], (z, e)).wait_recv()
        add_rows(work.at[t, c], buffer.at[t, c])

    def line(t):
        for p in range(nz):

            @pl.when(z == p)
            def _():
                c = t - (p - 1)
                if p > 0 and 0 <= c < chunks:
                    for target in range(nz - 1, p - 1, -1):
                        arrive(target, c, below, urecv)
                        if target > p:
                            rise(target, c).start()
                c = t - (nz - 2 - p)
                if p < nz - 1 and 0 <= c < chunks:
                    for target in range(p + 1):
                        arrive(target, c, above, drecv)
                        if target < p:
                            sink(target, c).start()

    def spread(c):
        net = PlaneGather(
            nz, ne, z, e, False, work.at[z, c], wide.at[c], zsend, zrecv,
            gsend.at[c], grecv.at[c], glocal.at[c],
        )
        net.start_round(0)
        return net

    def outs(c):
        span = pl.ds(c * rows, rows)
        copies = []
        for n in range(ne):
            for j in range(kinds):
                copies.append(
                    pltpu.make_async_copy(
                        wide.at[c, n, :, pl.ds(j * hw, hw)],
                        laid_ref.at[j, span, pl.ds(n * hw, hw)],
                        flush.at[c, n, j],
                    )
                )
        return copies

    def lay(c, net):
        net.finish_round(0)
        net.finish()
        for copy in outs(c):
            copy.start()

    def mix_step(t):
        if with_mix and t < mix.steps:
            mix.step(t)

    mine.step(0)
    mix_step(0)
    line(0)
    for j in range(1, mine.stages):
        mine.step(j)
    mix_step(1)
    line(1)
    nets = {}

    def advance(t):
        c = t - max(nz - 2, 0)
        if 0 <= c < chunks:
            nets[c] = spread(c)
        if c - 1 in nets:
            lay(c - 1, nets.pop(c - 1))

    advance(0)
    advance(1)

    gsum[...] = jnp.zeros_like(gsum)

    def front(s, here, span):
        grad = mine.rows(s, here)
        x = x_ref[span, :].astype(F32)
        scale = rms_scale(x)
        normed = x * scale
        gsum[...] += grad * normed
        scaled = grad * gain_ref[:1]
        inner = jnp.mean(scaled * normed, axis=-1, keepdims=True)
        grad_ref[span, :] = (gx1_ref[span, :] + scale * (scaled - normed * inner)).astype(BF)

    over_rows(mine.half, front)
    tbuf[...] = tiny_ref[...]
    tbuf[gain_row : gain_row + 1, :] = jnp.sum(gsum[...], axis=0, keepdims=True)

    cw = width // ne
    block = lambda ee: pl.ds(pl.multiple_of(ee * cw, cw), cw)
    first = []
    for r in range(1, ne):
        to = lax.rem(e + r, ne)
        copy = remote(tbuf.at[:, block(to)], tgot.at[r], send1.at[r], recv1.at[r], (z, to))
        copy.start()
        first.append(copy)
    mix_step(2)
    line(2)
    advance(2)
    sums = tbuf[:, block(e)]
    for r, copy in enumerate(first):
        copy.wait_recv()
        sums = sums + tgot[r + 1]
    total[...] = sums
    home, place = e // per, lax.rem(e, per)

    def give(r):
        to = lax.rem(e + r, ne)
        return remote(total, far.at[z, place], send2.at[r], recv2, (home, to))

    for r in range(ne):
        if r > 0:
            give(r).start()
        else:

            @pl.when(home != z)
            def _():
                give(0).start()

            @pl.when(home == z)
            def _():
                far[z, place] = total[...]

    for t in range(3, max(chunks + nz, mix.steps if with_mix else 0)):
        mix_step(t)
        line(t)
        advance(t)
    if with_mix:
        mix.arrive()

        def finish_output(s, here, span):
            out_ref[span, :] = (x1_ref[span, :] + mix.rows(s, here)).astype(BF)

        over_rows(mix.half, finish_output)
        mix.finish()
    else:
        out_ref[...] = jnp.zeros_like(out_ref)
    for copy in first:
        copy.wait_send()

    def arrived(count):
        flat = tgot.at[pl.ds(0, count)]
        remote(flat, flat, send2.at[0], recv2, (z, e)).wait_recv()

    for r in range(ne):
        if r > 0:
            give(r).wait_send()
        else:

            @pl.when(home != z)
            def _():
                give(0).wait_send()
                arrived(nz * per)

            @pl.when(home == z)
            def _():
                arrived(nz * per - 1)

    for i in range(per):
        small_ref[i] = sum(far[k, i] for k in range(nz))
    mine.finish()
    for c in range(chunks):
        for t in range(nz):

            @pl.when(z < t)
            def _():
                rise(t, c).wait_send()

            @pl.when(z > t)
            def _():
                sink(t, c).wait_send()

    for c in range(chunks):
        for copy in outs(c):
            copy.wait()


def tail(parts, gh1_part, mix, x, x1, gx1, gain_mat, tiny, gain_row, nz, ne, hw, cid):
    width, total_cols = parts.shape
    kinds = total_cols // hw
    count = x.shape[0]
    depth = width // nz
    rows = min(128, depth)
    chunks = depth // rows
    small_rows, cw = tiny.shape[0], width // ne
    per = ne // nz
    block = (nz, chunks, rows, total_cols)
    with_mix = mix is not None
    scratch = TokenScatter.scratch(ne, [None], count, width)
    if with_mix:
        scratch += TokenScatter.scratch(ne, split_ranks(nz)[1], count, width)
    grad, laid, small, output = pl.pallas_call(
        functools.partial(tail_kernel, nz, ne, kinds, gain_row, with_mix),
        out_shape=[
            jax.ShapeDtypeStruct((count, width), BF),
            jax.ShapeDtypeStruct((kinds, depth, width), BF),
            jax.ShapeDtypeStruct((per, small_rows, cw), F32),
            jax.ShapeDtypeStruct((count, width), BF),
        ],
        in_specs=[ANY, ANY, ANY, VMEM, VMEM, VMEM, VMEM, VMEM],
        out_specs=[VMEM, ANY, VMEM, VMEM],
        scratch_shapes=[
            pltpu.VMEM(block, BF), pltpu.VMEM(block, BF), pltpu.VMEM(block, BF),
            pltpu.VMEM((chunks, ne, rows, total_cols), BF),
            pltpu.VMEM((16, width), F32),
            pltpu.VMEM((small_rows, width), F32),
            pltpu.VMEM((max(ne, nz * per), small_rows, cw), F32),
            pltpu.VMEM((small_rows, cw), F32),
            pltpu.VMEM((nz, per, small_rows, cw), F32),
            DMA((nz, chunks)),
            DMA((nz, chunks)), DMA((nz, chunks)), DMA((nz, chunks)), DMA((nz, chunks)),
            DMA((nz,)), DMA((nz,)),
            DMA((chunks, 1, 2, ne - 1)), DMA((chunks, 1, 2, ne - 1)), DMA((chunks,)),
            DMA((chunks, ne, kinds)),
            DMA((ne,)), DMA((ne,)), DMA((ne,)), DMA,
            *scratch,
        ],
        compiler_params=pltpu.CompilerParams(
            collective_id=cid, has_side_effects=True, vmem_limit_bytes=66_000_000
        ),
        name="tail",
    )(parts, gh1_part, mix if with_mix else gh1_part, x, x1, gx1, gain_mat, tiny)
    small = small.transpose(1, 0, 2).reshape(small_rows, per * cw)
    return grad, laid, small, output


def add_kernel(x_ref, y_ref, out_ref):
    out_ref[...] = (x_ref[...] + y_ref[...].astype(F32)).astype(out_ref.dtype)


def add_up(x, y):
    return pl.pallas_call(
        add_kernel, out_shape=jax.ShapeDtypeStruct(y.shape, y.dtype), name="add_up"
    )(x, y)


def lay_experts_kernel(per_dev, fl, x_ref, gate_ref, up_ref):
    for i in range(per_dev):
        gate_ref[i] = x_ref[0, :, i * fl : (i + 1) * fl].astype(F32)
        up_ref[i] = x_ref[0, :, (per_dev + i) * fl : (per_dev + i + 1) * fl].astype(F32)


def lay_experts(wide, per_dev, fl):
    nz, rows, _ = wide.shape
    out = jax.ShapeDtypeStruct((per_dev, rows, nz * fl), F32)
    spec = pl.BlockSpec((per_dev, rows, fl), lambda i: (0, 0, i))
    return pl.pallas_call(
        functools.partial(lay_experts_kernel, per_dev, fl),
        grid=(nz,),
        in_specs=[pl.BlockSpec((1, rows, 2 * per_dev * fl), lambda i: (i, 0, 0))],
        out_specs=[spec, spec],
        out_shape=[out, out],
        name="lay_experts",
    )(wide)


def moe_kernel(
    fl, h_ref, g_ref, win_ref, wd_ref,
    mix_ref, gh_ref, dwin_ref, dwd_ref, acc_in, acc_d,
):
    step = pl.program_id(0)
    tile, width = g_ref.shape
    per_dev = wd_ref.shape[0] // fl
    e = lax.axis_index("expert")
    h = h_ref[:, :width]
    g = g_ref[...]
    extra = h_ref[:, width:].astype(F32)
    pre = dot(h, win_ref[...], NN)
    graw = dot(g, wd_ref[...], NT)
    scaled_act, grad_gate, grad_up = [], [], []
    lanes = lax.broadcasted_iota(jnp.int32, (tile, 128), 1)
    gg = jnp.zeros((tile, 128), F32)
    split = 64
    for i in range(per_dev):
        u = pre[:, i * fl : (i + 1) * fl]
        w = pre[:, (per_dev + i) * fl : (per_dev + 1 + i) * fl]
        gr = graw[:, i * fl : (i + 1) * fl]
        mine = e * per_dev + i
        picked = (lanes == mine) | (lanes == mine + split)
        gate = jnp.sum(jnp.where(picked, extra, 0.0), axis=-1, keepdims=True)
        sig = 1.0 / (1.0 + jnp.exp(-u))
        silu = u * sig
        act = silu * w
        total = jnp.sum(act.astype(BF).astype(F32) * gr, axis=-1, keepdims=True)
        rounded = total.astype(BF).astype(F32)
        gg = jnp.where(lanes == mine, rounded, gg)
        gg = jnp.where(lanes == mine + split, total - rounded, gg)
        scaled_act.append((gate * act).astype(BF))
        gact = gate * gr
        grad_gate.append((gact * w * (sig * (1.0 + u * (1.0 - sig)))).astype(BF))
        grad_up.append((gact * silu).astype(BF))
    a = jnp.concatenate(scaled_act, axis=1)
    gin = jnp.concatenate(grad_gate + grad_up, axis=1)
    mix_ref[...] = dot(a, wd_ref[...], NN).astype(BF)
    gh_ref[:, :width] = dot(gin, win_ref[...], NT).astype(BF)
    gh_ref[:, width:] = gg.astype(BF)

    @pl.when(step == 0)
    def _():
        acc_in[...] = jnp.zeros_like(acc_in)
        acc_d[...] = jnp.zeros_like(acc_d)

    acc_in[...] += dot(h, gin, TN)
    acc_d[...] += dot(a, g, TN)

    @pl.when(step == pl.num_programs(0) - 1)
    def _():
        dwin_ref[...] = acc_in[...].astype(BF)
        dwd_ref[...] = acc_d[...]


def moe(h_all, g_all, w_in, wd, per_dev, rows_dev, blocks):
    count, width = g_all.shape
    wide = h_all.shape[1]
    hid4 = w_in.shape[1]
    hid2 = wd.shape[0]
    fl = hid2 // per_dev
    tile = blocks * rows_dev
    rows = lambda n: pl.BlockSpec((tile, n), lambda i: (i, 0))
    whole = lambda s: pl.BlockSpec(s, lambda i: (0, 0), pipeline_mode=pl.Buffered(1))
    return pl.pallas_call(
        functools.partial(moe_kernel, fl),
        grid=(count // tile,),
        in_specs=[
            rows(wide), rows(width),
            whole(w_in.shape), whole(wd.shape),
        ],
        out_specs=[
            rows(width),
            rows(wide),
            whole((width, hid4)), whole((hid2, width)),
        ],
        out_shape=[
            jax.ShapeDtypeStruct((count, width), BF),
            jax.ShapeDtypeStruct((count, wide), BF),
            jax.ShapeDtypeStruct((width, hid4), BF),
            jax.ShapeDtypeStruct((hid2, width), F32),
        ],
        scratch_shapes=[pltpu.VMEM((width, hid4), F32), pltpu.VMEM((hid2, width), F32)],
        compiler_params=pltpu.CompilerParams(vmem_limit_bytes=66_000_000),
        cost_estimate=pl.CostEstimate(
            flops=2 * count * width * hid2 * 9,
            bytes_accessed=8 * count * width + 24 * hid4 * width,
            transcendentals=count * hid2,
        ),
        name="moe",
    )(h_all, g_all, w_in, wd)


def moe_net_kernel(
    nz, ne, per_dev, slots, h_ref, g_ref, wg_ref, wu_ref, wd_ref,
    hall_ref, mix_ref, gh_ref, dwin_ref, dwd_ref,
    win, wd, acc_in, acc_d, htile, gtile, mixbuf, qbuf, cgot, acc, got, zgot, dbuf,
    wload, tload, mixsem, keep, flush, zsend, zrecv, send, recv,
    csend, crecv, credit, rsend, rrecv, ysend, yrecv,
):
    z, e = lax.axis_index("dp"), lax.axis_index("expert")
    rows, width = g_ref.shape[1], g_ref.shape[2]
    half = rows // 2
    fl = wd.shape[0] // per_dev
    upper = [2 << b for b in range(ne.bit_length() - 2)]
    stages = len(upper)
    pairs = ne // 2
    steps = nz * pairs
    gather_orders = [upper + [1], upper[::-1] + [1]]
    sum_orders = [[1] + upper, [1] + upper[::-1]]
    at = [e]
    for bit in [1] + upper:
        at = at + [flip(i, bit) for i in at]
    partner = (z, at[1])

    def plane(r):
        low = jnp.minimum(z, nz - 1 - z)
        near = jnp.where(lax.rem(r, 2) == 1, z - (r + 1) // 2, z + r // 2)
        far = jnp.where(2 * z < nz, z + (r - low), z - (r - low))
        return jnp.where(r <= 2 * low, near, far)

    planes = [z] + [nearest(z, r, nz) for r in range(1, nz)]

    def part(s):
        return pl.ds(s * half, half)

    def subset_mask(order, subset):
        return sum(bit for b, bit in enumerate(order) if subset >> b & 1)

    def subset_index(order, mask):
        return sum(1 << b for b, bit in enumerate(order) if bit & mask)

    def pass_on(r, s, stage, subset, own=False):
        order = gather_orders[s]
        dst = hall_ref.at[plane(r) * ne + at[subset_mask(order, subset)], part(s)]
        n = (1 << stage) - 1 + subset
        src = h_ref.at[part(s)] if own else dst
        return remote(src, dst, send.at[r, s, n], recv.at[r, s, n], (z, at[order[stage]]))

    def take(r, s, stage, subset):
        order = gather_orders[s]
        mask = subset_mask(order, subset) | order[stage]
        n = (1 << stage) - 1 + subset
        here = hall_ref.at[plane(r) * ne + at[mask], part(s)]
        remote(here, here, send.at[r, s, n], recv.at[r, s, n], partner).wait_recv()
        for later in range(stage + 1, stages + 1):
            pass_on(r, s, later, subset + (1 << stage)).start()

    def start_round(r):
        if r > 0:
            here = hall_ref.at[planes[r] * ne + e]
            remote(here, here, zsend.at[r], zrecv.at[planes[r]], partner).wait_recv()
        for stage in range(stages + 1):
            for s in range(2):
                pass_on(r, s, stage, 0, own=r == 0).start()

    def take_pair(r, i):
        if i == 1:
            for stage in range(stages):
                for s in range(2):
                    take(r, s, stage, 0)
        mask = 2 * i
        for s in range(2):
            order = gather_orders[s]
            places = [b for b in range(stages) if order[b] & mask]
            if len(places) > 1:
                take(r, s, places[-1], sum(1 << b for b in places[:-1]))
        for s in range(2):
            order = gather_orders[s]
            take(r, s, stages, sum(1 << b for b in range(stages) if order[b] & mask))

    def blocks_of(k):
        r, i = k // pairs, lax.rem(k, pairs)
        home = plane(r)
        lane = e
        for b, bit in enumerate(upper):
            lane = lane + lax.rem(i // (1 << b), 2) * (at[bit] - e)
        return home, lane, lane + (at[1] - e)

    def loads(k):
        home, one, two = blocks_of(k)
        p = lax.rem(k, 2)
        out = []
        for j, lane in enumerate((one, two)):
            to = pl.ds(j * rows, rows)
            block = home * ne + lane
            out.append(pltpu.make_async_copy(hall_ref.at[block], htile.at[p, to], tload.at[p, 2 * j]))
            out.append(
                pltpu.make_async_copy(g_ref.at[block], gtile.at[p, to], tload.at[p, 2 * j + 1])
            )
        return out

    def mix_out(k):
        home, one, two = blocks_of(k)
        p = lax.rem(k, 2)
        return [
            pltpu.make_async_copy(
                mixbuf.at[p, pl.ds(j * rows, rows)], mix_ref.at[home * ne + lane], mixsem.at[p, j]
            )
            for j, lane in enumerate((one, two))
        ]

    def to_partner(k):
        return remote(
            qbuf.at[lax.rem(k, 2)], cgot.at[lax.rem(k, slots)],
            csend.at[lax.rem(k, 2)], crecv.at[lax.rem(k, slots)], partner,
        )

    def place_of(t, keep_index):
        return (1 << stages) - (1 << (stages - t + 1)) + keep_index

    def push(r, s, t, keep_index):
        order = sum_orders[s]
        mask = order[t] | subset_mask(order[t + 1 :], keep_index)
        n = place_of(t, keep_index)
        return remote(
            acc.at[r, mask // 2, part(s)], got.at[r, s, n],
            rsend.at[r, s, n], rrecv.at[r, s, n], (z, at[order[t]]),
        )

    def merge(k):
        slot = lax.rem(k, slots)
        remote(cgot.at[slot], cgot.at[slot], csend.at[0], crecv.at[slot], partner).wait_recv()
        r, i = k // pairs, lax.rem(k, pairs)
        add_rows(acc.at[r, i], cgot.at[slot])

        @pl.when(k + slots < steps)
        def _():
            pl.semaphore_signal(credit, inc=1, device_id=partner, device_id_type=MESH)

        for j in range(1, pairs):

            @pl.when(i == j)
            def _():
                for s in range(2):
                    order = sum_orders[s]
                    if order[1] & (2 * j):
                        rest = [b for b, bit in enumerate(order[2:]) if bit & (2 * j)]
                        push(r, s, 1, sum(1 << b for b in rest)).start()

    def home_copy(r, s):
        return remote(
            acc.at[r, 0, part(s)], zgot.at[z, part(s)], ysend.at[r, s], yrecv.at[z, s],
            (plane(r), e),
        )

    def settle(r, t):
        for s in range(2):
            order = sum_orders[s]
            count = 1 << (stages - t)
            for index in range(count - 1, -1, -1):
                push(r, s, t, index).wait_recv()
                mask = subset_mask(order[t + 1 :], index)
                add_rows(acc.at[r, mask // 2, part(s)], got.at[r, s, place_of(t, index)])
                if 2 * index >= count:
                    keep = subset_index(order[t + 2 :], mask)
                    push(r, s, t + 1, keep).start()
            if t == stages:

                @pl.when(r > 0)
                def _():
                    home_copy(r, s).start()

    weights = []
    for i in range(per_dev):
        cols = pl.ds(z * fl, fl)
        weights += [
            (wg_ref.at[i, :, cols], win.at[:, pl.ds(i * fl, fl)]),
            (wu_ref.at[i, :, cols], win.at[:, pl.ds((per_dev + i) * fl, fl)]),
            (wd_ref.at[i, cols, :], wd.at[pl.ds(i * fl, fl), :]),
        ]
    weights = [
        pltpu.make_async_copy(src, dst, wload.at[j]) for j, (src, dst) in enumerate(weights)
    ]
    for copy in weights:
        copy.start()
    meet_column_and_plane(nz, ne, z, e, True)
    own = pltpu.make_async_copy(h_ref, hall_ref.at[z * ne + e], keep)
    own.start()
    for r in range(1, nz):
        remote(
            h_ref, hall_ref.at[z * ne + e], zsend.at[r], zrecv.at[z], (planes[r], e)
        ).start()
    start_round(0)
    acc_in[...] = jnp.zeros_like(acc_in)
    acc_d[...] = jnp.zeros_like(acc_d)
    take_pair(0, 0)
    own.wait()
    for copy in loads(0):
        copy.start()
    for copy in weights:
        copy.wait()

    tile = 2 * rows
    lanes = lax.broadcasted_iota(jnp.int32, (tile, 128), 1)
    split = 64

    def step(k, carry):
        p = lax.rem(k, 2)
        r, i = k // pairs, lax.rem(k, pairs)
        for copy in loads(k):
            copy.wait()
        pre = dot(htile[p, :, :width], win[...], NN)
        graw = dot(gtile[p], wd[...], NT)
        extra = htile[p, :, width:].astype(F32)
        scaled_act, grad_gate, grad_up = [], [], []
        gg = jnp.zeros((tile, 128), F32)
        for j in range(per_dev):
            u = pre[:, j * fl : (j + 1) * fl]
            w = pre[:, (per_dev + j) * fl : (per_dev + 1 + j) * fl]
            gr = graw[:, j * fl : (j + 1) * fl]
            mine = e * per_dev + j
            picked = (lanes == mine) | (lanes == mine + split)
            gate = jnp.sum(jnp.where(picked, extra, 0.0), axis=-1, keepdims=True)
            sig = 1.0 / (1.0 + jnp.exp(-u))
            silu = u * sig
            act = silu * w
            total = jnp.sum(act.astype(BF).astype(F32) * gr, axis=-1, keepdims=True)
            rounded = total.astype(BF).astype(F32)
            gg = jnp.where(lanes == mine, rounded, gg)
            gg = jnp.where(lanes == mine + split, total - rounded, gg)
            scaled_act.append((gate * act).astype(BF))
            gact = gate * gr
            grad_gate.append((gact * w * (sig * (1.0 + u * (1.0 - sig)))).astype(BF))
            grad_up.append((gact * silu).astype(BF))
        a = jnp.concatenate(scaled_act, axis=1)
        gin = jnp.concatenate(grad_gate + grad_up, axis=1)

        for r1 in range(1, nz):

            @pl.when(k == (r1 - 1) * (pairs - 1) + 1)
            def _():
                start_round(r1)

        @pl.when(k + 1 < steps)
        def _():
            ahead = k + 1
            for j in range(pairs):

                @pl.when(lax.rem(ahead, pairs) == j)
                def _():
                    take_pair(ahead // pairs, j)

            for copy in loads(ahead):
                copy.start()

        @pl.when(k >= 2)
        def _():
            for copy in mix_out(k - 2):
                copy.wait()
            to_partner(k - 2).wait_send()

        mixbuf[p] = dot(a, wd[...], NN).astype(BF)
        for copy in mix_out(k):
            copy.start()
        back = dot(gin, win[...], NT).astype(BF)
        gg = gg.astype(BF)
        acc[r, i, :, :width] = back[:rows]
        acc[r, i, :, width:] = gg[:rows]
        qbuf[p, :, :width] = back[rows:]
        qbuf[p, :, width:] = gg[rows:]
        acc_in[...] += dot(htile[p, :, :width], gin, TN)
        acc_d[...] += dot(a, gtile[p], TN)

        @pl.when(k >= slots)
        def _():
            pl.semaphore_wait(credit, 1)

        to_partner(k).start()

        @pl.when(k >= 1)
        def _():
            merge(k - 1)

        for t in range(1, stages + 1):
            late = k - pairs - 2 * t

            @pl.when((late >= 0) & (lax.rem(late + pairs, pairs) == 0))
            def _():
                settle(late // pairs, t)

        return carry

    lax.fori_loop(0, steps, step, 0)
    merge(steps - 1)
    final = pltpu.make_async_copy(acc_d, dwd_ref, flush.at[0])
    final.start()
    left = sorted(
        (r * pairs + pairs + 2 * t, r, t)
        for r in range(nz)
        for t in range(1, stages + 1)
        if r * pairs + pairs + 2 * t >= steps
    )
    chunk = dbuf.shape[1]

    def flush_chunk(c):
        return pltpu.make_async_copy(
            dbuf.at[c % 2], dwin_ref.at[pl.ds(c * chunk, chunk)], flush.at[1 + c % 2]
        )

    chunks = acc_in.shape[0] // chunk
    for c in range(chunks):
        if c >= 2:
            flush_chunk(c - 2).wait()
        dbuf[c % 2] = acc_in[pl.ds(c * chunk, chunk), :].astype(BF)
        flush_chunk(c).start()
    for _, r, t in left:
        settle(jnp.int32(r), t)
    for s in range(2):
        for r in range(1, nz):
            here = zgot.at[planes[r], part(s)]
            remote(here, here, ysend.at[r, s], yrecv.at[planes[r], s], partner).wait_recv()

        def total_rows(n, carry):
            span = pl.ds(pl.multiple_of(s * half + n * 16, 16), 16)
            total = acc[0, 0, span, :].astype(F32)
            for r in range(1, nz):
                total = total + zgot[planes[r], span, :].astype(F32)
            gh_ref[span, :] = total
            return carry

        lax.fori_loop(0, half // 16, total_rows, 0)
    final.wait()
    for c in range(max(chunks - 2, 0), chunks):
        flush_chunk(c).wait()
    for k in range(max(steps - 2, 0), steps):
        for copy in mix_out(jnp.int32(k)):
            copy.wait()
        to_partner(jnp.int32(k)).wait_send()
    for r in range(nz):
        if r > 0:
            remote(
                h_ref, hall_ref.at[z * ne + e], zsend.at[r], zrecv.at[z], (planes[r], e)
            ).wait_send()
        for s in range(2):
            for stage in range(stages + 1):
                for subset in range(1 << stage):
                    pass_on(r, s, stage, subset, own=r == 0 and subset == 0).wait_send()
            for t in range(1, stages + 1):
                for index in range(1 << (stages - t)):
                    push(r, s, t, index).wait_send()
            if r > 0:
                home_copy(jnp.int32(r), s).wait_send()


def moe_net_scratch(nz, ne, per_dev, rows, width, wide, fl):
    pairs = ne // 2
    slots = 4
    stages = ne.bit_length() - 2
    vmem = [
        ((width, 2 * per_dev * fl), BF),
        ((per_dev * fl, width), BF),
        ((width, 2 * per_dev * fl), F32),
        ((per_dev * fl, width), F32),
        ((2, 2 * rows, wide), BF),
        ((2, 2 * rows, width), BF),
        ((2, 2 * rows, width), BF),
        ((2, rows, wide), BF),
        ((slots, rows, wide), BF),
        ((nz, pairs, rows, wide), BF),
        ((nz, 2, max(pairs - 1, 1), rows // 2, wide), BF),
        ((nz, rows, wide), BF),
        ((2, width // 8, 2 * per_dev * fl), BF),
    ]
    size = sum(functools.reduce(lambda a, b: a * b, s) * (2 if d == BF else 4) for s, d in vmem)
    sems = [
        DMA((3 * per_dev,)), DMA((2, 4)), DMA((2, 2)), DMA, DMA((3,)),
        DMA((nz,)), DMA((nz,)), DMA((nz, 2, ne - 1)), DMA((nz, 2, ne - 1)),
        DMA((2,)), DMA((slots,)), pltpu.SemaphoreType.REGULAR,
        DMA((nz, 2, max(pairs - 1, 1))), DMA((nz, 2, max(pairs - 1, 1))),
        DMA((nz, 2)), DMA((nz, 2)),
    ]
    fits = size <= 54_000_000 and stages >= 1 and nz > 1 and nz * pairs > slots
    return fits, slots, [pltpu.VMEM(*v) for v in vmem] + sems


def moe_net(h, g_all, w_gate, w_up, w_down, nz, ne, fl, slots, scratch, cid):
    rows, wide = h.shape
    per_dev, width, _ = w_gate.shape
    return pl.pallas_call(
        functools.partial(moe_net_kernel, nz, ne, per_dev, slots),
        out_shape=[
            jax.ShapeDtypeStruct((nz * ne, rows, wide), BF),
            jax.ShapeDtypeStruct((nz * ne, rows, width), BF),
            jax.ShapeDtypeStruct((rows, wide), F32),
            jax.ShapeDtypeStruct((width, 2 * per_dev * fl), BF),
            jax.ShapeDtypeStruct((per_dev * fl, width), F32),
        ],
        in_specs=[VMEM, ANY, ANY, ANY, ANY],
        out_specs=[ANY, ANY, VMEM, ANY, ANY],
        scratch_shapes=scratch,
        compiler_params=pltpu.CompilerParams(
            collective_id=cid, has_side_effects=True, vmem_limit_bytes=66_500_000
        ),
        name="moe_net",
    )(h, g_all.reshape(nz * ne, rows, width), w_gate, w_up, w_down)


def body(inputs, segments, routes, w_qkv, w_out, w_router, gains, w_gate, w_up, w_down, cotangent):
    z = lax.axis_index("dp")
    e = lax.axis_index("expert")
    nz = lax.axis_size("dp")
    ne = lax.axis_size("expert")
    count, width = inputs.shape
    num_seqs, length = segments.shape
    heads = width // HD // ne
    hw = heads * HD
    expert_count = w_router.shape[1]
    per_dev = w_gate.shape[0]
    hidden = w_gate.shape[2]
    fl = hidden // nz
    both = ("dp", "expert")

    pad = -(expert_count + 4) % 16
    small = jnp.concatenate(
        [w_router.T, gains.T, jnp.zeros((pad, gains.shape[0]), BF)], axis=0
    )
    seg8 = jnp.broadcast_to(segments[:, None, :], (num_seqs, 8, length)).reshape(-1, length)
    in_all, wq, wo, small, seg_all, g_all = start_gather(
        inputs, w_qkv.transpose(1, 0, 2), w_out, small, seg8, cotangent, nz, ne, hw, 0
    )
    small = small.transpose(1, 0, 2).reshape(-1, width)
    router_t = small[:expert_count]
    gain_mat = small[expert_count : expert_count + 4].astype(F32)
    my_gains = lax.dynamic_slice_in_dim(gain_mat, e * hw, hw, axis=1)
    seg_all = seg_all.reshape(ne * num_seqs, 8, length)

    g_all = g_all.reshape(-1, width)
    inputs_f = inputs.astype(F32)
    tables = rope_lanes(length)
    *saved, x1_part = attn_fwd(in_all, wq, wo, gain_mat, my_gains, seg_all, tables, 9)
    (x1_sum,) = scatter_tokens(x1_part, nz, ne, False, 1)
    x1 = inputs_f + x1_sum

    a2 = rms_scale(x1)
    h2 = (x1 * a2 * gain_mat[3]).astype(BF)
    probs = jax.nn.softmax(dot(h2, router_t, NT), axis=-1)
    picks = jnp.sum(
        (routes[:, :, None] == jnp.arange(expert_count, dtype=jnp.int32)).astype(F32), axis=1
    )
    gates = picks * probs

    split = 64
    high = gates.astype(BF)
    low = (gates - high.astype(F32)).astype(BF)
    blank = jnp.zeros((count, split - expert_count), BF)
    h2_wide = jnp.concatenate([h2, high, blank, low, blank], axis=1)
    wide = width + 2 * split
    fits, slots, scratch = moe_net_scratch(nz, ne, per_dev, count, width, wide, fl)
    if fits:
        _, mix, gh_sum, dwin, dwd = moe_net(
            h2_wide, g_all, w_gate, w_up, w_down, nz, ne, fl, slots, scratch, 2
        )
        mix = mix.reshape(-1, width)
    else:
        h2_all = gather_tokens(h2_wide, nz, ne, True, 2).reshape(-1, wide)
        wg = lax.dynamic_slice_in_dim(w_gate, z * fl, fl, axis=2)
        wu = lax.dynamic_slice_in_dim(w_up, z * fl, fl, axis=2)
        wd = lax.dynamic_slice_in_dim(w_down, z * fl, fl, axis=1).reshape(per_dev * fl, width)
        w_in = jnp.concatenate([*wg, *wu], axis=1)
        mix, gh, dwin, dwd = moe(h2_all, g_all, w_in, wd, per_dev, count, min(4, ne))
        gh_sum, mix = scatter_tokens(
            gh.reshape(nz * ne, count, wide), nz, ne, True, 3, after=mix.reshape(-1, width)
        )
    grad_from_experts = gh_sum[:, :width]
    grad_gates = (
        gh_sum[:, width : width + expert_count]
        + gh_sum[:, width + split : width + split + expert_count]
    )

    dwin = lax.all_to_all(
        dwin.reshape(nz, width // nz, 2 * per_dev * fl),
        "dp", split_axis=0, concat_axis=0, tiled=True,
    )
    grad_w_gate, grad_w_up = lay_experts(dwin, per_dev, fl)
    grad_w_down = dwd.reshape(per_dev, fl, width)

    grad_top = cotangent.astype(F32)
    grad_probs = picks * grad_gates
    glog = (probs * (grad_probs - jnp.sum(probs * grad_probs, axis=-1, keepdims=True))).astype(BF)
    local_router = dot(glog, h2, TN)
    gh2 = grad_from_experts + dot(glog, router_t, NN)
    grad_ffn, gain_ffn = rms_backward(x1, a2, gain_mat[3], gh2)
    gx1 = grad_top + grad_ffn
    gab = gx1.astype(BF)

    gab_all = gather_tokens(gab, nz, ne, False, 4)
    gh1_part, parts, gain_qk, x1_mix = attn_bwd(
        gab_all, wq, wo, my_gains, seg_all, tables, saved, x1,
        mix.reshape(-1, count, width) if fits else None, nz, 10,
    )
    place = lambda part: lax.dynamic_update_slice_in_dim(
        jnp.zeros((1, width), F32), part[None], e * hw, axis=1
    )
    tiny = jnp.concatenate(
        [
            local_router, jnp.zeros((1, width), F32), place(gain_qk[0]), place(gain_qk[1]),
            gain_ffn[None], jnp.zeros((-(expert_count + 4) % 8, width), F32),
        ],
        axis=0,
    )
    grad_inputs, laid, tiny, output = tail(
        parts, gh1_part, mix.reshape(-1, count, width) if fits else None, inputs, x1_mix, gx1,
        gain_mat, tiny, expert_count, nz, ne, hw, 5,
    )
    if not fits:
        mix = lax.psum_scatter(mix, both, scatter_dimension=0, tiled=True)
        output = add_up(x1, mix)
    grad_w_qkv = laid[:-1].astype(F32).transpose(1, 0, 2)
    grad_w_out = laid[-1].astype(F32)
    grad_w_router = tiny[:expert_count].T
    grad_gains = tiny[expert_count : expert_count + 4].T
    return (
        output,
        grad_inputs,
        grad_w_qkv,
        grad_w_out,
        grad_w_router,
        grad_gains,
        grad_w_gate,
        grad_w_up,
        grad_w_down,
    )


def solution(mesh):
    tokens = P(("dp", "expert"), None)
    rows = P("dp", None)
    rows3 = P("dp", None, None)
    owned = P("expert", None, None)
    return jax.shard_map(
        body,
        mesh=mesh,
        in_specs=(tokens, tokens, tokens, rows3, rows, rows, rows, owned, owned, owned, tokens),
        out_specs=(tokens, tokens, rows3, rows, rows, rows)
        + (P("expert", "dp", None),) * 3,
        check_vma=False,
    )
```

```python
import functools

import jax
import jax.numpy as jnp
from jax import lax
from jax.experimental import pallas as pl
from jax.experimental.pallas import tpu as pltpu
from jax.sharding import PartitionSpec as P


HD = 128
EPS = 1e-05
ROPE_BASE = 10000.0
MASKED = -1e30
BF = jnp.bfloat16
F32 = jnp.float32


def dot(a, b, dims):
    return lax.dot_general(a, b, (dims, ((), ())), preferred_element_type=F32)


NN = ((1,), (0,))
NT = ((1,), (1,))
TN = ((0,), (0,))


def rms_scale(values):
    return lax.rsqrt(jnp.mean(values * values, axis=-1, keepdims=True) + EPS)


def rms_backward(values, inv_rms, gain_col, grad_out):
    normed = values * inv_rms
    grad_gain = jnp.sum(grad_out * normed, axis=0)
    scaled = grad_out * gain_col
    grad_values = inv_rms * (scaled - normed * jnp.mean(scaled * normed, axis=-1, keepdims=True))
    return (grad_values, grad_gain)


MESH = pl.DeviceIdType.MESH
ANY = pl.BlockSpec(memory_space=pl.ANY)
VMEM = pl.BlockSpec(memory_space=pltpu.VMEM)
DMA = pltpu.SemaphoreType.DMA


def flip(index, bit):
    return index + bit * (1 - 2 * ((index // bit) % 2))


def flips(index, bits):
    out = [index]
    for bit in bits:
        out = out + [flip(i, bit) for i in out]
    return out


def bit_orders(ne):
    bits = [1 << b for b in range(ne.bit_length() - 1)]
    return [bits[:1] + bits[1:], bits[:1] + bits[1:][::-1]]


def nearest(z, r, nz):
    low = jnp.minimum(z, nz - 1 - z)
    near = z - (r + 1) // 2 if r % 2 else z + r // 2
    far = jnp.where(2 * z < nz, z + (r - low), z - (r - low))
    return jnp.where(r <= 2 * low, near, far)


def remote(src, dst, send, recv, peer):
    return pltpu.make_async_remote_copy(
        src_ref=src, dst_ref=dst, send_sem=send, recv_sem=recv, device_id=peer, device_id_type=MESH
    )


def for_others(nz, ne, z, e, act):
    def step(i, carry):
        flat = lax.rem(z * ne + e + i, nz * ne)
        act(flat // ne, lax.rem(flat, ne), flat)
        return carry

    lax.fori_loop(1, nz * ne, step, 0)


def meet_all(nz, ne, z, e):
    sem = pltpu.get_barrier_semaphore()

    def greet(zz, ee, flat):
        pl.semaphore_signal(sem, inc=1, device_id=(zz, ee), device_id_type=MESH)

    for_others(nz, ne, z, e, greet)
    pl.semaphore_wait(sem, nz * ne - 1)


def meet_column_and_plane(nz, ne, z, e, spread):
    sem = pltpu.get_barrier_semaphore()
    peers = [(z, flip(e, 1 << b)) for b in range(ne.bit_length() - 1)]
    if spread:
        peers += [(lax.rem(z + r, nz), e) for r in range(1, nz)]
    for peer in peers:
        pl.semaphore_signal(sem, inc=1, device_id=peer, device_id_type=MESH)
    pl.semaphore_wait(sem, len(peers))


class PlaneGather:
    def __init__(self, nz, ne, z, e, spread, x_ref, out_ref, zsend, zrecv, send, recv, local):
        self.nz, self.ne, self.z, self.e, self.spread = nz, ne, z, e, spread
        self.x, self.out = x_ref, out_ref
        self.zsend, self.zrecv, self.send, self.recv = zsend, zrecv, send, recv
        self.rounds = nz if spread else 1
        self.half = x_ref.shape[0] // 2
        self.orders = [o[1:] + o[:1] for o in bit_orders(ne)]
        self.planes = [z if spread else 0] + [nearest(z, r, nz) for r in range(1, self.rounds)]
        self.pending, self.arrivals = [], {}
        own = self.slot(0, e)
        keep = pltpu.make_async_copy(x_ref, out_ref.at[own], local)
        keep.start()
        self.pending.append(keep.wait)

    @staticmethod
    def scratch(nz, ne, spread):
        rounds = nz if spread else 1
        return [DMA((nz,)), DMA((nz,)), DMA((rounds, 2, ne - 1)), DMA((rounds, 2, ne - 1)), DMA]

    def slot(self, r, ee):
        return self.planes[r] * self.ne + ee

    def spread_own(self):
        for r in range(1, self.rounds):
            to = self.planes[r]
            copy = remote(
                self.x, self.out.at[self.slot(0, self.e)],
                self.zsend.at[r], self.zrecv.at[self.z], (to, self.e),
            )
            copy.start()
            self.pending.append(copy.wait_send)

    def forward(self, r, s, stage, subset):
        order = self.orders[s]
        rows = pl.ds(s * self.half, self.half)
        peer_e = flip(self.e, order[stage])
        n = (1 << stage) - 1 + subset
        block = self.slot(r, flips(self.e, order[:stage])[subset])
        dst = self.out.at[block, rows]
        src = self.x.at[rows] if r == 0 and subset == 0 else dst
        sems = self.send.at[r, s, n], self.recv.at[r, s, n]
        copy = remote(src, dst, *sems, (self.z, peer_e))
        copy.start()
        self.pending.append(copy.wait_send)
        got = self.out.at[self.slot(r, flips(peer_e, order[:stage])[subset]), rows]
        self.arrivals[(r, s, stage, subset)] = remote(got, got, *sems, (self.z, peer_e)).wait_recv

    def start_round(self, r):
        if r > 0:
            here = self.out.at[self.slot(r, self.e)]
            remote(
                here, here, self.zsend.at[r], self.zrecv.at[self.planes[r]], (self.planes[r], self.e)
            ).wait_recv()
        for stage in range(len(self.orders[0])):
            for s in range(2):
                self.forward(r, s, stage, 0)

    def finish_round(self, r):
        stages = len(self.orders[0])
        for stage in range(stages):
            for subset in range(1 << stage):
                for s in range(2):
                    self.arrivals.pop((r, s, stage, subset))()
                    for later in range(stage + 1, stages):
                        self.forward(r, s, later, subset + (1 << stage))

    def finish(self):
        for wait in self.pending:
            wait()


def gather_kernel(nz, ne, spread, x_ref, out_ref, *sems):
    z, e = lax.axis_index("dp"), lax.axis_index("expert")
    meet_column_and_plane(nz, ne, z, e, spread)
    net = PlaneGather(nz, ne, z, e, spread, x_ref, out_ref, *sems)
    net.spread_own()
    net.start_round(0)
    net.finish_round(0)
    for r in range(1, net.rounds):
        net.start_round(r)
        net.finish_round(r)
    net.finish()


def gather_tokens(x, nz, ne, spread, cid):
    rounds = nz if spread else 1
    return pl.pallas_call(
        functools.partial(gather_kernel, nz, ne, spread),
        out_shape=jax.ShapeDtypeStruct((rounds * ne, *x.shape), x.dtype),
        in_specs=[VMEM],
        out_specs=ANY,
        scratch_shapes=PlaneGather.scratch(nz, ne, spread),
        compiler_params=pltpu.CompilerParams(collective_id=cid, has_side_effects=True),
        name="gather_tokens",
    )(x)


def add_rows(dst, src, tile=16):
    def step(i, carry):
        rows = pl.ds(pl.multiple_of(i * tile, tile), tile)
        dst[rows, :] = dst[rows, :] + src[rows, :]
        return carry

    lax.fori_loop(0, dst.shape[0] // tile, step, 0)


class TokenScatter:
    def __init__(self, nz, ne, z, e, ranks, x_ref, acc, got, zgot, loads, send, recv, zsend, zrecv):
        self.nz, self.ne, self.z, self.e = nz, ne, z, e
        self.x, self.acc, self.got, self.zgot = x_ref, acc, got, zgot
        self.loads, self.send, self.recv, self.zsend, self.zrecv = loads, send, recv, zsend, zrecv
        self.ranks = ranks
        self.stages = ne.bit_length() - 1
        self.steps = len(ranks) + self.stages - 1
        self.half = acc.shape[3]
        self.orders = bit_orders(ne)
        self.first = [0]
        for j in range(self.stages):
            self.first.append(self.first[j] + (ne >> (j + 1)))
        self.pending, self.arrivals, self.zwait = [], {}, []

    def block(self, r, ee):
        if self.ranks[r] is None:
            return ee
        return lax.rem(self.z + self.ranks[r], self.nz) * self.ne + ee

    def push(self, r, s, j):
        order = self.orders[s]
        peer_e = flip(self.e, order[j])
        rest = self.ne >> (j + 1)
        for i in range(rest):
            n = self.first[j] + i
            if j == 0:
                ee = flips(peer_e, order[:0:-1])[i]
                src = self.x.at[self.block(r, ee), pl.ds(s * self.half, self.half)]
            else:
                src = self.acc.at[r, s, rest + i]
            copy = remote(
                src, self.got.at[r, s, n], self.send.at[r, s, n], self.recv.at[r, s, n],
                (self.z, peer_e),
            )
            copy.start()
            self.pending.append(copy.wait_send)
            self.arrivals.setdefault((r, s, j), []).append((copy.wait_recv, i, n))

    def start(self):
        for r in range(len(self.ranks)):
            for s in range(2):
                self.push(r, s, 0)
                for i, ee in enumerate(flips(self.e, self.orders[s][:0:-1])):
                    copy = pltpu.make_async_copy(
                        self.x.at[self.block(r, ee), pl.ds(s * self.half, self.half)],
                        self.acc.at[r, s, i],
                        self.loads.at[r, s, i],
                    )
                    copy.start()
                    self.arrivals.setdefault((r, s, -1), []).append(copy.wait)

    def step(self, t):
        for r, rank in enumerate(self.ranks):
            j = t - r
            if not 0 <= j < self.stages:
                continue
            for s in range(2):
                if j == 0:
                    for wait in self.arrivals.pop((r, s, -1)):
                        wait()
                for wait, i, n in self.arrivals.pop((r, s, j)):
                    wait()
                    add_rows(self.acc.at[r, s, i], self.got.at[r, s, n])
                if j + 1 < self.stages:
                    self.push(r, s, j + 1)
                elif rank:
                    copy = remote(
                        self.acc.at[r, s, 0], self.zgot.at[r, s],
                        self.zsend.at[r, s], self.zrecv.at[r, s],
                        (lax.rem(self.z + rank, self.nz), self.e),
                    )
                    copy.start()
                    self.pending.append(copy.wait_send)
                    self.zwait.append(copy.wait_recv)

    def arrive(self):
        for wait in self.zwait:
            wait()

    def rows(self, s, here):
        parts = [
            self.zgot[r, s, here, :] if rank else self.acc[r, s, 0, here, :]
            for r, rank in enumerate(self.ranks)
        ]
        return sum(part.astype(F32) for part in parts)

    def finish(self):
        for wait in self.pending:
            wait()

    @staticmethod
    def scratch(ne, ranks, count, width):
        rounds = len(ranks)
        half = count // 2
        return [
            pltpu.VMEM((rounds, 2, ne // 2, half, width), BF),
            pltpu.VMEM((rounds, 2, ne - 1, half, width), BF),
            pltpu.VMEM((rounds, 2, half, width), BF),
            DMA((rounds, 2, ne // 2)),
            DMA((rounds, 2, ne - 1)),
            DMA((rounds, 2, ne - 1)),
            DMA((rounds, 2)),
            DMA((rounds, 2)),
        ]


def split_ranks(nz):
    return [], scatter_ranks(nz, True)


def scatter_ranks(nz, spread):
    return [*range(1, nz), 0] if spread else [None]


def over_rows(half, act, tile=16):
    for s in range(2):

        def step(n, carry):
            here = pl.ds(pl.multiple_of(n * tile, tile), tile)
            span = pl.ds(pl.multiple_of(s * half + n * tile, tile), tile)
            act(s, here, span)
            return carry

        lax.fori_loop(0, half // tile, step, 0)


def scatter_kernel(nz, ne, spread, x_ref, *refs):
    out_ref, *rest = refs[-9:]
    z, e = lax.axis_index("dp"), lax.axis_index("expert")
    meet_column_and_plane(nz, ne, z, e, spread)
    net = TokenScatter(nz, ne, z, e, scatter_ranks(nz, spread), x_ref, *rest)
    net.start()
    for t in range(net.steps):
        net.step(t)
    net.arrive()

    def write(s, here, span):
        out_ref[span, :] = net.rows(s, here)

    over_rows(net.half, write)
    net.finish()


def scatter_tokens(parts, nz, ne, spread, cid, after=None):
    rounds = nz if spread else 1
    _, count, width = parts.shape
    half = count // 2
    held = (2 * rounds * (ne // 2 + ne - 1) + 2 * nz) * half * width * 2
    if held > 56_000_000:
        cut = width // 256 * 128
        left = scatter_tokens(parts[..., :cut], nz, ne, spread, cid, after)
        right = scatter_tokens(parts[..., cut:], nz, ne, spread, cid + 16)
        return [jnp.concatenate([left[0], right[0]], axis=1), *left[1:]]
    more = [] if after is None else [after]
    return pl.pallas_call(
        functools.partial(scatter_kernel, nz, ne, spread),
        out_shape=[jax.ShapeDtypeStruct(m.shape, m.dtype) for m in more]
        + [jax.ShapeDtypeStruct((count, width), F32)],
        in_specs=[ANY] * (1 + len(more)),
        out_specs=[ANY] * len(more) + [VMEM],
        scratch_shapes=TokenScatter.scratch(ne, scatter_ranks(nz, spread), count, width),
        input_output_aliases={1: 0} if more else {},
        compiler_params=pltpu.CompilerParams(
            collective_id=cid, has_side_effects=True, vmem_limit_bytes=64_000_000
        ),
        name="scatter_tokens",
    )(parts, *more)[::-1]


def start_kernel(
    nz, ne, x_ref, wqkv_ref, wout_ref, small_ref, seg_ref, cot_ref,
    out_ref, wq_ref, wo_ref, small_out, seg_out, cot_out,
    wbuf, pbuf, zsend, zrecv, send, recv, local, czsend, czrecv, csend, crecv, clocal,
    up_send, up_recv, dn_send, dn_recv, wload, wkeep, pload, psend, precv, pkeep,
    small_send, small_recv, seg_send, seg_recv,
):
    z, e = lax.axis_index("dp"), lax.axis_index("expert")
    kinds, depth, hw = wbuf.shape
    per = ne // nz
    loads = [
        pltpu.make_async_copy(wqkv_ref.at[j, :, pl.ds(e * hw, hw)], wbuf.at[j], wload.at[j])
        for j in range(kinds)
    ]
    for copy in loads:
        copy.start()
    pieces = [
        pltpu.make_async_copy(
            wout_ref.at[pl.ds(i * hw, hw), pl.ds(e * hw, hw)], pbuf.at[i], pload.at[i]
        )
        for i in range(per)
    ]
    for copy in pieces:
        copy.start()
    meet_all(nz, ne, z, e)
    cot = PlaneGather(
        nz, ne, z, e, True, cot_ref, cot_out, czsend, czrecv, csend, crecv, clocal
    )
    cot.spread_own()

    def rows_of(zz):
        return pl.ds(pl.multiple_of(zz * depth, depth), depth)

    def hop(j, zz, dist, up):
        send, recv = (up_send, up_recv) if up else (dn_send, dn_recv)
        here = wq_ref.at[j, rows_of(zz)]
        src = wbuf.at[j] if dist == 1 else here
        to = z + 1 if up else z - 1
        return remote(src, here, send.at[dist, j], recv.at[dist, j], (to, e))

    keeps = []
    for j in range(kinds):
        loads[j].wait()

        @pl.when(z + 1 < nz)
        def _():
            hop(j, z, 1, True).start()

        @pl.when(z > 0)
        def _():
            hop(j, z, 1, False).start()

        keep = pltpu.make_async_copy(wbuf.at[j], wq_ref.at[j, rows_of(z)], wkeep.at[j])
        keep.start()
        keeps.append(keep)

    def wait_all(ref, send, recv, count):
        most = ref.at[pl.ds(0, count)]
        both = remote(most, most, send, recv, (z, flip(e, 1)))
        both.wait_send()
        both.wait_recv()

    small_out[z] = small_ref[...]
    for r in range(1, nz):
        remote(
            small_ref, small_out.at[z], small_send, small_recv, (lax.rem(z + r, nz), e)
        ).start()
    seg_out[e] = seg_ref[...]
    for r in range(1, ne):
        remote(seg_ref, seg_out.at[e], seg_send, seg_recv, (z, lax.rem(e + r, ne))).start()
    net = PlaneGather(nz, ne, z, e, False, x_ref, out_ref, zsend, zrecv, send, recv, local)
    net.start_round(0)
    cot.start_round(0)

    columns = pl.ds(e * hw, hw)
    for i in range(per):
        pieces[i].wait()
    for r in range(nz):
        for i in range(per):
            to = (lax.rem(z + r, nz), z * per + i)
            give = remote(pbuf.at[i], wo_ref.at[:, columns], psend.at[r, i], precv, to)
            if r > 0:
                give.start()
            else:
                own = pltpu.make_async_copy(pbuf.at[i], wo_ref.at[:, columns], pkeep)

                @pl.when(to[1] == e)
                def _():
                    own.start()

                @pl.when(to[1] != e)
                def _():
                    give.start()
    net.finish_round(0)
    for dist in range(1, nz):
        cot.start_round(dist)
        cot.finish_round(dist - 1)
        for j in range(kinds):

            @pl.when(z - dist >= 0)
            def _():
                got = wq_ref.at[j, rows_of(z - dist)]
                remote(got, got, up_send.at[dist, j], up_recv.at[dist, j], (z, e)).wait_recv()

                @pl.when(z + 1 < nz)
                def _():
                    if dist + 1 < nz:
                        hop(j, z - dist, dist + 1, True).start()

            @pl.when(z + dist < nz)
            def _():
                got = wq_ref.at[j, rows_of(z + dist)]
                remote(got, got, dn_send.at[dist, j], dn_recv.at[dist, j], (z, e)).wait_recv()

                @pl.when(z > 0)
                def _():
                    if dist + 1 < nz:
                        hop(j, z + dist, dist + 1, False).start()

    cot.finish_round(nz - 1)
    cot.finish()
    net.finish()
    for keep in keeps:
        keep.wait()
    for dist in range(1, nz):
        for j in range(kinds):

            @pl.when((z - dist + 1 >= 0) & (z + 1 < nz))
            def _():
                hop(j, z - dist + 1, dist, True).wait_send()

            @pl.when((z + dist - 1 < nz) & (z > 0))
            def _():
                hop(j, z + dist - 1, dist, False).wait_send()

    for r in range(nz):
        for i in range(per):
            to = (lax.rem(z + r, nz), z * per + i)
            give = remote(pbuf.at[i], wo_ref.at[:, columns], psend.at[r, i], precv, to)
            if r > 0:
                give.wait_send()
            else:
                own = pltpu.make_async_copy(pbuf.at[i], wo_ref.at[:, columns], pkeep)

                @pl.when(to[1] == e)
                def _():
                    own.wait()

                @pl.when(to[1] != e)
                def _():
                    give.wait_send()

    def wait_pieces(count):
        most = wo_ref.at[:, pl.ds(0, count * hw)]
        remote(most, most, psend.at[0, 0], precv, (z, e)).wait_recv()

    @pl.when(z == e // per)
    def _():
        wait_pieces(ne - 1)

    @pl.when(z != e // per)
    def _():
        wait_pieces(ne)

    wait_all(small_out, small_send, small_recv, nz - 1)
    wait_all(seg_out, seg_send, seg_recv, ne - 1)


def start_gather(x, w_qkv, w_out, small, seg, cot, nz, ne, hw, cid):
    kinds, depth, width = w_qkv.shape
    per = ne // nz
    return pl.pallas_call(
        functools.partial(start_kernel, nz, ne),
        out_shape=[
            jax.ShapeDtypeStruct((ne, *x.shape), x.dtype),
            jax.ShapeDtypeStruct((kinds, nz * depth, hw), BF),
            jax.ShapeDtypeStruct((hw, width), BF),
            jax.ShapeDtypeStruct((nz, *small.shape), small.dtype),
            jax.ShapeDtypeStruct((ne, *seg.shape), seg.dtype),
            jax.ShapeDtypeStruct((nz * ne, *cot.shape), cot.dtype),
        ],
        in_specs=[VMEM, ANY, ANY, VMEM, VMEM, VMEM],
        out_specs=[ANY, ANY, ANY, VMEM, VMEM, ANY],
        scratch_shapes=[
            pltpu.VMEM((kinds, depth, hw), BF),
            pltpu.VMEM((per, hw, hw), BF),
            *PlaneGather.scratch(nz, ne, False),
            *PlaneGather.scratch(nz, ne, True),
            DMA((nz, kinds)), DMA((nz, kinds)), DMA((nz, kinds)), DMA((nz, kinds)),
            DMA((kinds,)), DMA((kinds,)), DMA((per,)), DMA((nz, per)), DMA, DMA,
            DMA, DMA, DMA, DMA,
        ],
        compiler_params=pltpu.CompilerParams(collective_id=cid, has_side_effects=True),
        name="start_gather",
    )(x, w_qkv, w_out, small, seg, cot)


def rope_lanes(length):
    half = HD // 2
    freqs = jnp.exp(-jnp.log(ROPE_BASE) * (2.0 * jnp.arange(half, dtype=F32) / HD))
    angles = jnp.arange(length, dtype=F32)[:, None] * freqs[None, :]
    cos, sin = jnp.cos(angles), jnp.sin(angles)
    return jnp.concatenate([cos, cos], axis=1), jnp.concatenate([-sin, sin], axis=1)


def turn(x, cos, sin):
    return x * cos + pltpu.roll(x, HD // 2, 1) * sin


def meet_plane(ne, z, e):
    sem = pltpu.get_barrier_semaphore()
    for r in range(1, ne):
        pl.semaphore_signal(
            sem, inc=1, device_id=(z, lax.rem(e + r, ne)), device_id_type=MESH
        )
    pl.semaphore_wait(sem, ne - 1)


def plane_totals(ne, z, e, mine, theirs, send, recv):
    copies = []
    for r in range(1, ne):
        to = (z, lax.rem(e + r, ne))
        copy = remote(mine, theirs.at[r], send.at[r], recv.at[r], to)
        copy.start()
        copies.append(copy)
    total = mine[...]
    for r, copy in enumerate(copies):
        copy.wait_recv()
        total = total + theirs[r + 1]
    for copy in copies:
        copy.wait_send()
    return total


def store_columns(sums, first, columns):
    rows = columns[0].shape[0]
    lanes = lax.broadcasted_iota(jnp.int32, (rows, 128), 1)
    wide = jnp.zeros((rows, 128), F32)
    for j, column in enumerate(columns):
        wide = jnp.where(lanes == j, column, wide)
    sums[:, pl.ds(first, rows)] = wide.T[:8]


def as_columns(total, out):
    rows = total.shape[1]
    for first in range(0, rows, 128):
        chunk = total[:, first : first + 128]
        out[first : first + 128, :] = jnp.concatenate([chunk] * 16, axis=0).T


def allowed_pairs(seg_ref, n):
    length = seg_ref.shape[2]
    keys = jnp.broadcast_to(seg_ref[n, :1].astype(F32), (length, length))
    i = lax.broadcasted_iota(jnp.int32, (length, length), 0)
    j = lax.broadcasted_iota(jnp.int32, (length, length), 1)
    return (i >= j) & (keys == keys.T)


def attend(rq, rk, allowed):
    scores = jnp.where(allowed, dot(rq, rk, NT) * HD ** (-0.5), MASKED)
    top = jnp.max(scores, axis=-1, keepdims=True)
    lse = top + jnp.log(jnp.sum(jnp.exp(scores - top), axis=-1, keepdims=True))
    return jnp.exp(scores - lse)


def attn_fwd_kernel(
    ne, x_ref, wq_ref, wo_ref, gain_ref, mine_ref, seg_ref, cos_ref, sin_ref,
    h1_ref, q_ref, k_ref, rq_ref, rk_ref, v_ref, o_ref, scale_ref, x1_ref,
    sums, theirs, send, recv,
):
    z, e = lax.axis_index("dp"), lax.axis_index("expert")
    width = x_ref.shape[2]
    count, hw = q_ref.shape
    length = seg_ref.shape[2]
    rows_dev = x_ref.shape[1]
    tile = min(512, count)
    meet_plane(ne, z, e)

    def normed(b, carry):
        x = x_ref[b].astype(F32)
        h1 = x * rms_scale(x) * gain_ref[:1]
        h1_ref[pl.ds(pl.multiple_of(b * rows_dev, rows_dev), rows_dev), :] = h1.astype(BF)
        return carry

    lax.fori_loop(0, ne, normed, 0)
    for first in range(0, count, tile):
        rows = slice(first, first + tile)
        h1 = h1_ref[rows, :]
        q, k = dot(h1, wq_ref[0], NN), dot(h1, wq_ref[1], NN)
        q_ref[rows, :] = q
        k_ref[rows, :] = k
        v_ref[rows, :] = dot(h1, wq_ref[2], NN).astype(BF)
        store_columns(
            sums, first, [jnp.sum(t * t, axis=-1, keepdims=True) for t in (q, k)]
        )
    total = plane_totals(ne, z, e, sums, theirs, send, recv)
    as_columns(lax.rsqrt(total / width + EPS), scale_ref)
    cos, sin = cos_ref[...], sin_ref[...]

    def sequence(n, carry):
        rows = pl.ds(pl.multiple_of(n * length, length), length)
        allowed = allowed_pairs(seg_ref, n)
        aq, ak = scale_ref[rows, 0:1], scale_ref[rows, 1:2]
        for c in range(0, hw, HD):
            cols = slice(c, c + HD)
            rq = turn(q_ref[rows, cols] * aq * mine_ref[1:2, cols], cos, sin).astype(BF)
            rk = turn(k_ref[rows, cols] * ak * mine_ref[2:3, cols], cos, sin).astype(BF)
            rq_ref[rows, cols] = rq
            rk_ref[rows, cols] = rk
            probs = attend(rq, rk, allowed).astype(BF)
            o_ref[rows, cols] = dot(probs, v_ref[rows, cols], NN).astype(BF)
        return carry

    lax.fori_loop(0, count // length, sequence, 0)
    for first in range(0, count, tile):
        x1 = dot(o_ref[first : first + tile, :], wo_ref[...], NN).astype(BF)
        blocks = tile // rows_dev
        x1_ref[first // rows_dev : first // rows_dev + blocks] = x1.reshape(
            blocks, rows_dev, width
        )


def attn_fwd(in_all, wq, wo, gain_mat, my_gains, seg, tables, cid):
    ne, rows_dev, width = in_all.shape
    count, hw = ne * rows_dev, wo.shape[0]
    return pl.pallas_call(
        functools.partial(attn_fwd_kernel, ne),
        out_shape=[
            jax.ShapeDtypeStruct((count, width), BF),
            jax.ShapeDtypeStruct((count, hw), F32),
            jax.ShapeDtypeStruct((count, hw), F32),
            jax.ShapeDtypeStruct((count, hw), BF),
            jax.ShapeDtypeStruct((count, hw), BF),
            jax.ShapeDtypeStruct((count, hw), BF),
            jax.ShapeDtypeStruct((count, hw), BF),
            jax.ShapeDtypeStruct((count, 128), F32),
            jax.ShapeDtypeStruct((ne, rows_dev, width), BF),
        ],
        in_specs=[VMEM] * 8,
        out_specs=[VMEM] * 9,
        scratch_shapes=[
            pltpu.VMEM((8, count), F32), pltpu.VMEM((ne, 8, count), F32), DMA((ne,)), DMA((ne,)),
        ],
        compiler_params=pltpu.CompilerParams(
            collective_id=cid, has_side_effects=True, vmem_limit_bytes=60_000_000
        ),
        name="attn_fwd",
    )(in_all, wq, wo, gain_mat, my_gains, seg, *tables)


def attn_bwd_kernel(
    nz, ne, with_mix, gab_ref, wq_ref, wo_ref, mine_ref, seg_ref, cos_ref, sin_ref,
    h1_ref, q_ref, k_ref, rq_ref, rk_ref, v_ref, o_ref, scale_ref, x1_ref, mix_ref,
    gh1_ref, parts_ref, gain_ref, x1m_ref,
    pout, go_ref, gqn_ref, gkn_ref, gp_ref, sums, theirs, means, send, recv, psend, precv,
    *mix_scratch,
):
    z, e = lax.axis_index("dp"), lax.axis_index("expert")
    count, hw = q_ref.shape
    width = gab_ref.shape[2]
    rows_dev = gab_ref.shape[1]
    length = seg_ref.shape[2]
    tile = min(512, count)
    blocks = tile // rows_dev
    if with_mix:
        meet_all(nz, ne, z, e)
        mix = TokenScatter(nz, ne, z, e, split_ranks(nz)[0], mix_ref, *mix_scratch)
        mix.start()
    else:
        meet_plane(ne, z, e)

    def mix_step(t):
        if with_mix and t < mix.steps:
            mix.step(t)

    gab = lambda first: gab_ref[first // rows_dev : first // rows_dev + blocks].reshape(tile, width)
    part = dot(o_ref[:tile, :], gab(0), TN)
    for first in range(tile, count, tile):
        part = part + dot(o_ref[first : first + tile, :], gab(first), TN)
    pout[...] = part.astype(BF)
    for first in range(0, count, tile):
        go_ref[first : first + tile, :] = dot(gab(first), wo_ref[...], NT).astype(BF)
    my_rows = pl.ds(pl.multiple_of(e * hw, hw), hw)
    last = pl.ds(3 * hw, hw)
    gives = []
    for r in range(1, ne):
        to = lax.rem(e + r, ne)
        give = remote(
            pout.at[:, pl.ds(pl.multiple_of(to * hw, hw), hw)], parts_ref.at[my_rows, last],
            psend.at[r], precv.at[r], (z, to),
        )
        give.start()
        gives.append(give)
    parts_ref[my_rows, last] = pout[:, my_rows]
    mix_step(0)

    cos, sin = cos_ref[...], -sin_ref[...]
    gain_ref[...] = jnp.zeros_like(gain_ref)

    def sequence(n, carry):
        start = pl.multiple_of(n * length, length)
        rows = pl.ds(start, length)
        allowed = allowed_pairs(seg_ref, n)
        aq, ak = scale_ref[rows, 0:1], scale_ref[rows, 1:2]
        sum_q = jnp.zeros((length, 1), F32)
        sum_k = jnp.zeros((length, 1), F32)
        for c in range(0, hw, HD):
            cols = slice(c, c + HD)
            rq, rk, go = rq_ref[rows, cols], rk_ref[rows, cols], go_ref[rows, cols]
            probs = attend(rq, rk, allowed)
            gv = dot(probs.astype(BF), go, TN).astype(BF)
            gp_ref[rows, slice(2 * hw + c, 2 * hw + c + HD)] = gv
            grad = dot(go, v_ref[rows, cols], NT)
            delta = jnp.sum(probs * grad, axis=-1, keepdims=True)
            gs = (probs * (grad - delta) * HD ** (-0.5)).astype(BF)
            gqn = turn(dot(gs, rk, NN), cos, sin)
            gkn = turn(dot(gs, rq, TN), cos, sin)
            gqn_ref[rows, cols] = gqn
            gkn_ref[rows, cols] = gkn
            tq = gqn * (q_ref[rows, cols] * aq)
            tk = gkn * (k_ref[rows, cols] * ak)
            gain_ref[0:1, cols] += jnp.sum(tq, axis=0, keepdims=True)
            gain_ref[1:2, cols] += jnp.sum(tk, axis=0, keepdims=True)
            sum_q = sum_q + jnp.sum(tq * mine_ref[1:2, cols], axis=-1, keepdims=True)
            sum_k = sum_k + jnp.sum(tk * mine_ref[2:3, cols], axis=-1, keepdims=True)
        store_columns(sums, start, [sum_q, sum_k])
        return carry

    seqs = count // length
    lax.fori_loop(0, seqs // 2, sequence, 0)
    mix_step(1)
    lax.fori_loop(seqs // 2, seqs, sequence, 0)
    mix_step(2)
    total = plane_totals(ne, z, e, sums, theirs, send, recv)
    mix_step(3)
    as_columns(total / width, means)
    for first in range(0, count, tile):
        rows = slice(first, first + tile)
        aq, ak = scale_ref[rows, 0:1], scale_ref[rows, 1:2]
        mq, mk = means[rows, 0:1], means[rows, 1:2]
        gq = aq * (gqn_ref[rows, :] * mine_ref[1:2] - q_ref[rows, :] * aq * mq)
        gk = ak * (gkn_ref[rows, :] * mine_ref[2:3] - k_ref[rows, :] * ak * mk)
        gp_ref[rows, :hw] = gq.astype(BF)
        gp_ref[rows, hw : 2 * hw] = gk.astype(BF)
    for first in range(0, width, tile):
        rows = slice(first, first + tile)
        parts_ref[rows, : 3 * hw] = dot(h1_ref[:, rows], gp_ref[...], TN).astype(BF)
    for first in range(0, count, tile):
        rows = slice(first, first + tile)
        gh1 = dot(gp_ref[rows, :hw], wq_ref[0], NT)
        for j in range(1, 3):
            gh1 = gh1 + dot(gp_ref[rows, j * hw : (j + 1) * hw], wq_ref[j], NT)
        gh1_ref[first // rows_dev : first // rows_dev + blocks] = gh1.astype(BF).reshape(
            blocks, rows_dev, width
        )
    for give in gives:
        give.wait_send()
        give.wait_recv()
    if with_mix:
        for t in range(4, mix.steps):
            mix_step(t)
        mix.arrive()

        def add_part(s, here, span):
            x1m_ref[span, :] = x1_ref[span, :] + mix.rows(s, here)

        over_rows(mix.half, add_part)
        mix.finish()
    else:
        x1m_ref[...] = x1_ref[...]


def attn_bwd(gab, wq, wo, my_gains, seg, tables, saved, x1, mix, nz, cid):
    ne, rows_dev, width = gab.shape
    count, hw = ne * rows_dev, wo.shape[0]
    return pl.pallas_call(
        functools.partial(attn_bwd_kernel, nz, ne, mix is not None),
        out_shape=[
            jax.ShapeDtypeStruct((ne, rows_dev, width), BF),
            jax.ShapeDtypeStruct((width, 4 * hw), BF),
            jax.ShapeDtypeStruct((8, hw), F32),
            jax.ShapeDtypeStruct((rows_dev, width), F32),
        ],
        in_specs=[VMEM] * 16 + [ANY],
        out_specs=[VMEM] * 4,
        scratch_shapes=[
            pltpu.VMEM((hw, width), BF),
            pltpu.VMEM((count, hw), BF),
            pltpu.VMEM((count, hw), F32),
            pltpu.VMEM((count, hw), F32),
            pltpu.VMEM((count, 3 * hw), BF),
            pltpu.VMEM((8, count), F32),
            pltpu.VMEM((ne, 8, count), F32),
            pltpu.VMEM((count, 128), F32),
            DMA((ne,)), DMA((ne,)), DMA((ne,)), DMA((ne,)),
        ]
        + (
            []
            if mix is None
            else TokenScatter.scratch(ne, split_ranks(nz)[0], rows_dev, width)
        ),
        compiler_params=pltpu.CompilerParams(
            collective_id=cid, has_side_effects=True, vmem_limit_bytes=64_000_000
        ),
        name="attn_bwd",
    )(gab, wq, wo, my_gains, seg, *tables, *saved, x1, gab if mix is None else mix)


def tail_kernel(
    nz, ne, kinds, gain_row, with_mix, parts_ref, gh1_ref, mix_ref, x_ref, x1_ref, gx1_ref,
    gain_ref, tiny_ref, grad_ref, laid_ref, small_ref, out_ref,
    work, below, above, wide, gsum, tbuf, tgot, total, far,
    wload, usend, urecv, dsend, drecv, zsend, zrecv, gsend, grecv, glocal,
    flush, send1, recv1, send2, recv2, *nets_scratch,
):
    z, e = lax.axis_index("dp"), lax.axis_index("expert")
    per = ne // nz
    chunks, rows = work.shape[1], work.shape[2]
    hw = work.shape[3] // kinds
    width = x_ref.shape[1]
    loads = [
        pltpu.make_async_copy(
            parts_ref.at[pl.ds((t * chunks + c) * rows, rows)], work.at[t, c], wload.at[t, c]
        )
        for c in range(chunks)
        for t in range(nz)
    ]
    for copy in loads:
        copy.start()
    meet_all(nz, ne, z, e)
    mine = TokenScatter(nz, ne, z, e, [None], gh1_ref, *nets_scratch[:8])
    mine.start()
    if with_mix:
        mix = TokenScatter(nz, ne, z, e, split_ranks(nz)[1], mix_ref, *nets_scratch[8:])
        mix.start()
    for copy in loads:
        copy.wait()

    def rise(t, c):
        return remote(
            work.at[t, c], below.at[t, c], usend.at[t, c], urecv.at[t, c], (z + 1, e)
        )

    def sink(t, c):
        return remote(
            work.at[t, c], above.at[t, c], dsend.at[t, c], drecv.at[t, c], (z - 1, e)
        )

    for c in range(chunks):
        for t in range(nz - 1, 0, -1):

            @pl.when(z == 0)
            def _():
                rise(t, c).start()

        for t in range(nz - 1):

            @pl.when(z == nz - 1)
            def _():
                sink(t, c).start()

    def arrive(t, c, buffer, recv):
        remote(buffer.at[t, c], buffer.at[t, c], usend.at[0, 0], recv.at[t, c], (z, e)).wait_recv()
        add_rows(work.at[t, c], buffer.at[t, c])

    def line(t):
        for p in range(nz):

            @pl.when(z == p)
            def _():
                c = t - (p - 1)
                if p > 0 and 0 <= c < chunks:
                    for target in range(nz - 1, p - 1, -1):
                        arrive(target, c, below, urecv)
                        if target > p:
                            rise(target, c).start()
                c = t - (nz - 2 - p)
                if p < nz - 1 and 0 <= c < chunks:
                    for target in range(p + 1):
                        arrive(target, c, above, drecv)
                        if target < p:
                            sink(target, c).start()

    def spread(c):
        net = PlaneGather(
            nz, ne, z, e, False, work.at[z, c], wide.at[c], zsend, zrecv,
            gsend.at[c], grecv.at[c], glocal.at[c],
        )
        net.start_round(0)
        return net

    def outs(c):
        span = pl.ds(c * rows, rows)
        copies = []
        for n in range(ne):
            for j in range(kinds):
                copies.append(
                    pltpu.make_async_copy(
                        wide.at[c, n, :, pl.ds(j * hw, hw)],
                        laid_ref.at[j, span, pl.ds(n * hw, hw)],
                        flush.at[c, n, j],
                    )
                )
        return copies

    def lay(c, net):
        net.finish_round(0)
        net.finish()
        for copy in outs(c):
            copy.start()

    def mix_step(t):
        if with_mix and t < mix.steps:
            mix.step(t)

    mine.step(0)
    mix_step(0)
    line(0)
    for j in range(1, mine.stages):
        mine.step(j)
    mix_step(1)
    line(1)
    nets = {}

    def advance(t):
        c = t - max(nz - 2, 0)
        if 0 <= c < chunks:
            nets[c] = spread(c)
        if c - 1 in nets:
            lay(c - 1, nets.pop(c - 1))

    advance(0)
    advance(1)

    gsum[...] = jnp.zeros_like(gsum)

    def front(s, here, span):
        grad = mine.rows(s, here)
        x = x_ref[span, :].astype(F32)
        scale = rms_scale(x)
        normed = x * scale
        gsum[...] += grad * normed
        scaled = grad * gain_ref[:1]
        inner = jnp.mean(scaled * normed, axis=-1, keepdims=True)
        grad_ref[span, :] = (gx1_ref[span, :] + scale * (scaled - normed * inner)).astype(BF)

    over_rows(mine.half, front)
    tbuf[...] = tiny_ref[...]
    tbuf[gain_row : gain_row + 1, :] = jnp.sum(gsum[...], axis=0, keepdims=True)

    cw = width // ne
    block = lambda ee: pl.ds(pl.multiple_of(ee * cw, cw), cw)
    first = []
    for r in range(1, ne):
        to = lax.rem(e + r, ne)
        copy = remote(tbuf.at[:, block(to)], tgot.at[r], send1.at[r], recv1.at[r], (z, to))
        copy.start()
        first.append(copy)
    mix_step(2)
    line(2)
    advance(2)
    sums = tbuf[:, block(e)]
    for r, copy in enumerate(first):
        copy.wait_recv()
        sums = sums + tgot[r + 1]
    total[...] = sums
    home, place = e // per, lax.rem(e, per)

    def give(r):
        to = lax.rem(e + r, ne)
        return remote(total, far.at[z, place], send2.at[r], recv2, (home, to))

    for r in range(ne):
        if r > 0:
            give(r).start()
        else:

            @pl.when(home != z)
            def _():
                give(0).start()

            @pl.when(home == z)
            def _():
                far[z, place] = total[...]

    for t in range(3, max(chunks + nz, mix.steps if with_mix else 0)):
        mix_step(t)
        line(t)
        advance(t)
    if with_mix:
        mix.arrive()

        def finish_output(s, here, span):
            out_ref[span, :] = (x1_ref[span, :] + mix.rows(s, here)).astype(BF)

        over_rows(mix.half, finish_output)
        mix.finish()
    else:
        out_ref[...] = jnp.zeros_like(out_ref)
    for copy in first:
        copy.wait_send()

    def arrived(count):
        flat = tgot.at[pl.ds(0, count)]
        remote(flat, flat, send2.at[0], recv2, (z, e)).wait_recv()

    for r in range(ne):
        if r > 0:
            give(r).wait_send()
        else:

            @pl.when(home != z)
            def _():
                give(0).wait_send()
                arrived(nz * per)

            @pl.when(home == z)
            def _():
                arrived(nz * per - 1)

    for i in range(per):
        small_ref[i] = sum(far[k, i] for k in range(nz))
    mine.finish()
    for c in range(chunks):
        for t in range(nz):

            @pl.when(z < t)
            def _():
                rise(t, c).wait_send()

            @pl.when(z > t)
            def _():
                sink(t, c).wait_send()

    for c in range(chunks):
        for copy in outs(c):
            copy.wait()


def tail(parts, gh1_part, mix, x, x1, gx1, gain_mat, tiny, gain_row, nz, ne, hw, cid):
    width, total_cols = parts.shape
    kinds = total_cols // hw
    count = x.shape[0]
    depth = width // nz
    rows = min(128, depth)
    chunks = depth // rows
    small_rows, cw = tiny.shape[0], width // ne
    per = ne // nz
    block = (nz, chunks, rows, total_cols)
    with_mix = mix is not None
    scratch = TokenScatter.scratch(ne, [None], count, width)
    if with_mix:
        scratch += TokenScatter.scratch(ne, split_ranks(nz)[1], count, width)
    grad, laid, small, output = pl.pallas_call(
        functools.partial(tail_kernel, nz, ne, kinds, gain_row, with_mix),
        out_shape=[
            jax.ShapeDtypeStruct((count, width), BF),
            jax.ShapeDtypeStruct((kinds, depth, width), BF),
            jax.ShapeDtypeStruct((per, small_rows, cw), F32),
            jax.ShapeDtypeStruct((count, width), BF),
        ],
        in_specs=[ANY, ANY, ANY, VMEM, VMEM, VMEM, VMEM, VMEM],
        out_specs=[VMEM, ANY, VMEM, VMEM],
        scratch_shapes=[
            pltpu.VMEM(block, BF), pltpu.VMEM(block, BF), pltpu.VMEM(block, BF),
            pltpu.VMEM((chunks, ne, rows, total_cols), BF),
            pltpu.VMEM((16, width), F32),
            pltpu.VMEM((small_rows, width), F32),
            pltpu.VMEM((max(ne, nz * per), small_rows, cw), F32),
            pltpu.VMEM((small_rows, cw), F32),
            pltpu.VMEM((nz, per, small_rows, cw), F32),
            DMA((nz, chunks)),
            DMA((nz, chunks)), DMA((nz, chunks)), DMA((nz, chunks)), DMA((nz, chunks)),
            DMA((nz,)), DMA((nz,)),
            DMA((chunks, 1, 2, ne - 1)), DMA((chunks, 1, 2, ne - 1)), DMA((chunks,)),
            DMA((chunks, ne, kinds)),
            DMA((ne,)), DMA((ne,)), DMA((ne,)), DMA,
            *scratch,
        ],
        compiler_params=pltpu.CompilerParams(
            collective_id=cid, has_side_effects=True, vmem_limit_bytes=66_000_000
        ),
        name="tail",
    )(parts, gh1_part, mix if with_mix else gh1_part, x, x1, gx1, gain_mat, tiny)
    small = small.transpose(1, 0, 2).reshape(small_rows, per * cw)
    return grad, laid, small, output


def add_kernel(x_ref, y_ref, out_ref):
    out_ref[...] = (x_ref[...] + y_ref[...].astype(F32)).astype(out_ref.dtype)


def add_up(x, y):
    return pl.pallas_call(
        add_kernel, out_shape=jax.ShapeDtypeStruct(y.shape, y.dtype), name="add_up"
    )(x, y)


def lay_experts_kernel(per_dev, fl, x_ref, gate_ref, up_ref):
    for i in range(per_dev):
        gate_ref[i] = x_ref[0, :, i * fl : (i + 1) * fl].astype(F32)
        up_ref[i] = x_ref[0, :, (per_dev + i) * fl : (per_dev + i + 1) * fl].astype(F32)


def lay_experts(wide, per_dev, fl):
    nz, rows, _ = wide.shape
    out = jax.ShapeDtypeStruct((per_dev, rows, nz * fl), F32)
    spec = pl.BlockSpec((per_dev, rows, fl), lambda i: (0, 0, i))
    return pl.pallas_call(
        functools.partial(lay_experts_kernel, per_dev, fl),
        grid=(nz,),
        in_specs=[pl.BlockSpec((1, rows, 2 * per_dev * fl), lambda i: (i, 0, 0))],
        out_specs=[spec, spec],
        out_shape=[out, out],
        name="lay_experts",
    )(wide)


def moe_kernel(
    fl, h_ref, g_ref, win_ref, wd_ref,
    mix_ref, gh_ref, dwin_ref, dwd_ref, acc_in, acc_d,
):
    step = pl.program_id(0)
    tile, width = g_ref.shape
    per_dev = wd_ref.shape[0] // fl
    e = lax.axis_index("expert")
    h = h_ref[:, :width]
    g = g_ref[...]
    extra = h_ref[:, width:].astype(F32)
    pre = dot(h, win_ref[...], NN)
    graw = dot(g, wd_ref[...], NT)
    scaled_act, grad_gate, grad_up = [], [], []
    lanes = lax.broadcasted_iota(jnp.int32, (tile, 128), 1)
    gg = jnp.zeros((tile, 128), F32)
    split = 64
    for i in range(per_dev):
        u = pre[:, i * fl : (i + 1) * fl]
        w = pre[:, (per_dev + i) * fl : (per_dev + 1 + i) * fl]
        gr = graw[:, i * fl : (i + 1) * fl]
        mine = e * per_dev + i
        picked = (lanes == mine) | (lanes == mine + split)
        gate = jnp.sum(jnp.where(picked, extra, 0.0), axis=-1, keepdims=True)
        sig = 1.0 / (1.0 + jnp.exp(-u))
        silu = u * sig
        act = silu * w
        total = jnp.sum(act.astype(BF).astype(F32) * gr, axis=-1, keepdims=True)
        rounded = total.astype(BF).astype(F32)
        gg = jnp.where(lanes == mine, rounded, gg)
        gg = jnp.where(lanes == mine + split, total - rounded, gg)
        scaled_act.append((gate * act).astype(BF))
        gact = gate * gr
        grad_gate.append((gact * w * (sig * (1.0 + u * (1.0 - sig)))).astype(BF))
        grad_up.append((gact * silu).astype(BF))
    a = jnp.concatenate(scaled_act, axis=1)
    gin = jnp.concatenate(grad_gate + grad_up, axis=1)
    mix_ref[...] = dot(a, wd_ref[...], NN).astype(BF)
    gh_ref[:, :width] = dot(gin, win_ref[...], NT).astype(BF)
    gh_ref[:, width:] = gg.astype(BF)

    @pl.when(step == 0)
    def _():
        acc_in[...] = jnp.zeros_like(acc_in)
        acc_d[...] = jnp.zeros_like(acc_d)

    acc_in[...] += dot(h, gin, TN)
    acc_d[...] += dot(a, g, TN)

    @pl.when(step == pl.num_programs(0) - 1)
    def _():
        dwin_ref[...] = acc_in[...].astype(BF)
        dwd_ref[...] = acc_d[...]


def moe(h_all, g_all, w_in, wd, per_dev, rows_dev, blocks):
    count, width = g_all.shape
    wide = h_all.shape[1]
    hid4 = w_in.shape[1]
    hid2 = wd.shape[0]
    fl = hid2 // per_dev
    tile = blocks * rows_dev
    rows = lambda n: pl.BlockSpec((tile, n), lambda i: (i, 0))
    whole = lambda s: pl.BlockSpec(s, lambda i: (0, 0), pipeline_mode=pl.Buffered(1))
    return pl.pallas_call(
        functools.partial(moe_kernel, fl),
        grid=(count // tile,),
        in_specs=[
            rows(wide), rows(width),
            whole(w_in.shape), whole(wd.shape),
        ],
        out_specs=[
            rows(width),
            rows(wide),
            whole((width, hid4)), whole((hid2, width)),
        ],
        out_shape=[
            jax.ShapeDtypeStruct((count, width), BF),
            jax.ShapeDtypeStruct((count, wide), BF),
            jax.ShapeDtypeStruct((width, hid4), BF),
            jax.ShapeDtypeStruct((hid2, width), F32),
        ],
        scratch_shapes=[pltpu.VMEM((width, hid4), F32), pltpu.VMEM((hid2, width), F32)],
        compiler_params=pltpu.CompilerParams(vmem_limit_bytes=66_000_000),
        cost_estimate=pl.CostEstimate(
            flops=2 * count * width * hid2 * 9,
            bytes_accessed=8 * count * width + 24 * hid4 * width,
            transcendentals=count * hid2,
        ),
        name="moe",
    )(h_all, g_all, w_in, wd)


def moe_net_kernel(
    nz, ne, per_dev, slots, h_ref, g_ref, wg_ref, wu_ref, wd_ref,
    hall_ref, mix_ref, gh_ref, dwin_ref, dwd_ref,
    win, wd, acc_in, acc_d, htile, gtile, mixbuf, qbuf, cgot, acc, got, zgot, dbuf,
    wload, tload, mixsem, keep, flush, zsend, zrecv, send, recv,
    csend, crecv, credit, rsend, rrecv, ysend, yrecv,
):
    z, e = lax.axis_index("dp"), lax.axis_index("expert")
    rows, width = g_ref.shape[1], g_ref.shape[2]
    half = rows // 2
    fl = wd.shape[0] // per_dev
    upper = [2 << b for b in range(ne.bit_length() - 2)]
    stages = len(upper)
    pairs = ne // 2
    steps = nz * pairs
    gather_orders = [upper + [1], upper[::-1] + [1]]
    sum_orders = [[1] + upper, [1] + upper[::-1]]
    at = [e]
    for bit in [1] + upper:
        at = at + [flip(i, bit) for i in at]
    partner = (z, at[1])

    def plane(r):
        low = jnp.minimum(z, nz - 1 - z)
        near = jnp.where(lax.rem(r, 2) == 1, z - (r + 1) // 2, z + r // 2)
        far = jnp.where(2 * z < nz, z + (r - low), z - (r - low))
        return jnp.where(r <= 2 * low, near, far)

    planes = [z] + [nearest(z, r, nz) for r in range(1, nz)]

    def part(s):
        return pl.ds(s * half, half)

    def subset_mask(order, subset):
        return sum(bit for b, bit in enumerate(order) if subset >> b & 1)

    def subset_index(order, mask):
        return sum(1 << b for b, bit in enumerate(order) if bit & mask)

    def pass_on(r, s, stage, subset, own=False):
        order = gather_orders[s]
        dst = hall_ref.at[plane(r) * ne + at[subset_mask(order, subset)], part(s)]
        n = (1 << stage) - 1 + subset
        src = h_ref.at[part(s)] if own else dst
        return remote(src, dst, send.at[r, s, n], recv.at[r, s, n], (z, at[order[stage]]))

    def take(r, s, stage, subset):
        order = gather_orders[s]
        mask = subset_mask(order, subset) | order[stage]
        n = (1 << stage) - 1 + subset
        here = hall_ref.at[plane(r) * ne + at[mask], part(s)]
        remote(here, here, send.at[r, s, n], recv.at[r, s, n], partner).wait_recv()
        for later in range(stage + 1, stages + 1):
            pass_on(r, s, later, subset + (1 << stage)).start()

    def start_round(r):
        if r > 0:
            here = hall_ref.at[planes[r] * ne + e]
            remote(here, here, zsend.at[r], zrecv.at[planes[r]], partner).wait_recv()
        for stage in range(stages + 1):
            for s in range(2):
                pass_on(r, s, stage, 0, own=r == 0).start()

    def take_pair(r, i):
        if i == 1:
            for stage in range(stages):
                for s in range(2):
                    take(r, s, stage, 0)
        mask = 2 * i
        for s in range(2):
            order = gather_orders[s]
            places = [b for b in range(stages) if order[b] & mask]
            if len(places) > 1:
                take(r, s, places[-1], sum(1 << b for b in places[:-1]))
        for s in range(2):
            order = gather_orders[s]
            take(r, s, stages, sum(1 << b for b in range(stages) if order[b] & mask))

    def blocks_of(k):
        r, i = k // pairs, lax.rem(k, pairs)
        home = plane(r)
        lane = e
        for b, bit in enumerate(upper):
            lane = lane + lax.rem(i // (1 << b), 2) * (at[bit] - e)
        return home, lane, lane + (at[1] - e)

    def loads(k):
        home, one, two = blocks_of(k)
        p = lax.rem(k, 2)
        out = []
        for j, lane in enumerate((one, two)):
            to = pl.ds(j * rows, rows)
            block = home * ne + lane
            out.append(pltpu.make_async_copy(hall_ref.at[block], htile.at[p, to], tload.at[p, 2 * j]))
            out.append(
                pltpu.make_async_copy(g_ref.at[block], gtile.at[p, to], tload.at[p, 2 * j + 1])
            )
        return out

    def mix_out(k):
        home, one, two = blocks_of(k)
        p = lax.rem(k, 2)
        return [
            pltpu.make_async_copy(
                mixbuf.at[p, pl.ds(j * rows, rows)], mix_ref.at[home * ne + lane], mixsem.at[p, j]
            )
            for j, lane in enumerate((one, two))
        ]

    def to_partner(k):
        return remote(
            qbuf.at[lax.rem(k, 2)], cgot.at[lax.rem(k, slots)],
            csend.at[lax.rem(k, 2)], crecv.at[lax.rem(k, slots)], partner,
        )

    def place_of(t, keep_index):
        return (1 << stages) - (1 << (stages - t + 1)) + keep_index

    def push(r, s, t, keep_index):
        order = sum_orders[s]
        mask = order[t] | subset_mask(order[t + 1 :], keep_index)
        n = place_of(t, keep_index)
        return remote(
            acc.at[r, mask // 2, part(s)], got.at[r, s, n],
            rsend.at[r, s, n], rrecv.at[r, s, n], (z, at[order[t]]),
        )

    def merge(k):
        slot = lax.rem(k, slots)
        remote(cgot.at[slot], cgot.at[slot], csend.at[0], crecv.at[slot], partner).wait_recv()
        r, i = k // pairs, lax.rem(k, pairs)
        add_rows(acc.at[r, i], cgot.at[slot])

        @pl.when(k + slots < steps)
        def _():
            pl.semaphore_signal(credit, inc=1, device_id=partner, device_id_type=MESH)

        for j in range(1, pairs):

            @pl.when(i == j)
            def _():
                for s in range(2):
                    order = sum_orders[s]
                    if order[1] & (2 * j):
                        rest = [b for b, bit in enumerate(order[2:]) if bit & (2 * j)]
                        push(r, s, 1, sum(1 << b for b in rest)).start()

    def home_copy(r, s):
        return remote(
            acc.at[r, 0, part(s)], zgot.at[z, part(s)], ysend.at[r, s], yrecv.at[z, s],
            (plane(r), e),
        )

    def settle(r, t):
        for s in range(2):
            order = sum_orders[s]
            count = 1 << (stages - t)
            for index in range(count - 1, -1, -1):
                push(r, s, t, index).wait_recv()
                mask = subset_mask(order[t + 1 :], index)
                add_rows(acc.at[r, mask // 2, part(s)], got.at[r, s, place_of(t, index)])
                if 2 * index >= count:
                    keep = subset_index(order[t + 2 :], mask)
                    push(r, s, t + 1, keep).start()
            if t == stages:

                @pl.when(r > 0)
                def _():
                    home_copy(r, s).start()

    weights = []
    for i in range(per_dev):
        cols = pl.ds(z * fl, fl)
        weights += [
            (wg_ref.at[i, :, cols], win.at[:, pl.ds(i * fl, fl)]),
            (wu_ref.at[i, :, cols], win.at[:, pl.ds((per_dev + i) * fl, fl)]),
            (wd_ref.at[i, cols, :], wd.at[pl.ds(i * fl, fl), :]),
        ]
    weights = [
        pltpu.make_async_copy(src, dst, wload.at[j]) for j, (src, dst) in enumerate(weights)
    ]
    for copy in weights:
        copy.start()
    meet_column_and_plane(nz, ne, z, e, True)
    own = pltpu.make_async_copy(h_ref, hall_ref.at[z * ne + e], keep)
    own.start()
    for r in range(1, nz):
        remote(
            h_ref, hall_ref.at[z * ne + e], zsend.at[r], zrecv.at[z], (planes[r], e)
        ).start()
    start_round(0)
    acc_in[...] = jnp.zeros_like(acc_in)
    acc_d[...] = jnp.zeros_like(acc_d)
    take_pair(0, 0)
    own.wait()
    for copy in loads(0):
        copy.start()
    for copy in weights:
        copy.wait()

    tile = 2 * rows
    lanes = lax.broadcasted_iota(jnp.int32, (tile, 128), 1)
    split = 64

    def step(k, carry):
        p = lax.rem(k, 2)
        r, i = k // pairs, lax.rem(k, pairs)
        for copy in loads(k):
            copy.wait()
        pre = dot(htile[p, :, :width], win[...], NN)
        graw = dot(gtile[p], wd[...], NT)
        extra = htile[p, :, width:].astype(F32)
        scaled_act, grad_gate, grad_up = [], [], []
        gg = jnp.zeros((tile, 128), F32)
        for j in range(per_dev):
            u = pre[:, j * fl : (j + 1) * fl]
            w = pre[:, (per_dev + j) * fl : (per_dev + 1 + j) * fl]
            gr = graw[:, j * fl : (j + 1) * fl]
            mine = e * per_dev + j
            picked = (lanes == mine) | (lanes == mine + split)
            gate = jnp.sum(jnp.where(picked, extra, 0.0), axis=-1, keepdims=True)
            sig = 1.0 / (1.0 + jnp.exp(-u))
            silu = u * sig
            act = silu * w
            total = jnp.sum(act.astype(BF).astype(F32) * gr, axis=-1, keepdims=True)
            rounded = total.astype(BF).astype(F32)
            gg = jnp.where(lanes == mine, rounded, gg)
            gg = jnp.where(lanes == mine + split, total - rounded, gg)
            scaled_act.append((gate * act).astype(BF))
            gact = gate * gr
            grad_gate.append((gact * w * (sig * (1.0 + u * (1.0 - sig)))).astype(BF))
            grad_up.append((gact * silu).astype(BF))
        a = jnp.concatenate(scaled_act, axis=1)
        gin = jnp.concatenate(grad_gate + grad_up, axis=1)

        for r1 in range(1, nz):

            @pl.when(k == (r1 - 1) * pairs + 2)
            def _():
                start_round(r1)

        @pl.when(k + 1 < steps)
        def _():
            ahead = k + 1
            for j in range(pairs):

                @pl.when(lax.rem(ahead, pairs) == j)
                def _():
                    take_pair(ahead // pairs, j)

            for copy in loads(ahead):
                copy.start()

        @pl.when(k >= 2)
        def _():
            for copy in mix_out(k - 2):
                copy.wait()
            to_partner(k - 2).wait_send()

        mixbuf[p] = dot(a, wd[...], NN).astype(BF)
        for copy in mix_out(k):
            copy.start()
        back = dot(gin, win[...], NT).astype(BF)
        gg = gg.astype(BF)
        acc[r, i, :, :width] = back[:rows]
        acc[r, i, :, width:] = gg[:rows]
        qbuf[p, :, :width] = back[rows:]
        qbuf[p, :, width:] = gg[rows:]
        acc_in[...] += dot(htile[p, :, :width], gin, TN)
        acc_d[...] += dot(a, gtile[p], TN)

        @pl.when(k >= slots)
        def _():
            pl.semaphore_wait(credit, 1)

        to_partner(k).start()

        @pl.when(k >= 1)
        def _():
            merge(k - 1)

        for t in range(1, stages + 1):
            late = k - pairs - 2 * t

            @pl.when((late >= 0) & (lax.rem(late + pairs, pairs) == 0))
            def _():
                settle(late // pairs, t)

        return carry

    lax.fori_loop(0, steps, step, 0)
    merge(steps - 1)
    final = pltpu.make_async_copy(acc_d, dwd_ref, flush.at[0])
    final.start()
    left = sorted(
        (r * pairs + pairs + 2 * t, r, t)
        for r in range(nz)
        for t in range(1, stages + 1)
        if r * pairs + pairs + 2 * t >= steps
    )
    chunk = dbuf.shape[1]

    def flush_chunk(c):
        return pltpu.make_async_copy(
            dbuf.at[c % 2], dwin_ref.at[pl.ds(c * chunk, chunk)], flush.at[1 + c % 2]
        )

    chunks = acc_in.shape[0] // chunk
    for c in range(chunks):
        if c >= 2:
            flush_chunk(c - 2).wait()
        dbuf[c % 2] = acc_in[pl.ds(c * chunk, chunk), :].astype(BF)
        flush_chunk(c).start()
    for _, r, t in left:
        settle(jnp.int32(r), t)
    for s in range(2):
        for r in range(1, nz):
            here = zgot.at[planes[r], part(s)]
            remote(here, here, ysend.at[r, s], yrecv.at[planes[r], s], partner).wait_recv()

        def total_rows(n, carry):
            span = pl.ds(pl.multiple_of(s * half + n * 16, 16), 16)
            total = acc[0, 0, span, :].astype(F32)
            for r in range(1, nz):
                total = total + zgot[planes[r], span, :].astype(F32)
            gh_ref[span, :] = total
            return carry

        lax.fori_loop(0, half // 16, total_rows, 0)
    final.wait()
    for c in range(max(chunks - 2, 0), chunks):
        flush_chunk(c).wait()
    for k in range(max(steps - 2, 0), steps):
        for copy in mix_out(jnp.int32(k)):
            copy.wait()
        to_partner(jnp.int32(k)).wait_send()
    for r in range(nz):
        if r > 0:
            remote(
                h_ref, hall_ref.at[z * ne + e], zsend.at[r], zrecv.at[z], (planes[r], e)
            ).wait_send()
        for s in range(2):
            for stage in range(stages + 1):
                for subset in range(1 << stage):
                    pass_on(r, s, stage, subset, own=r == 0 and subset == 0).wait_send()
            for t in range(1, stages + 1):
                for index in range(1 << (stages - t)):
                    push(r, s, t, index).wait_send()
            if r > 0:
                home_copy(jnp.int32(r), s).wait_send()


def moe_net_scratch(nz, ne, per_dev, rows, width, wide, fl):
    pairs = ne // 2
    slots = 4
    stages = ne.bit_length() - 2
    vmem = [
        ((width, 2 * per_dev * fl), BF),
        ((per_dev * fl, width), BF),
        ((width, 2 * per_dev * fl), F32),
        ((per_dev * fl, width), F32),
        ((2, 2 * rows, wide), BF),
        ((2, 2 * rows, width), BF),
        ((2, 2 * rows, width), BF),
        ((2, rows, wide), BF),
        ((slots, rows, wide), BF),
        ((nz, pairs, rows, wide), BF),
        ((nz, 2, max(pairs - 1, 1), rows // 2, wide), BF),
        ((nz, rows, wide), BF),
        ((2, width // 8, 2 * per_dev * fl), BF),
    ]
    size = sum(functools.reduce(lambda a, b: a * b, s) * (2 if d == BF else 4) for s, d in vmem)
    sems = [
        DMA((3 * per_dev,)), DMA((2, 4)), DMA((2, 2)), DMA, DMA((3,)),
        DMA((nz,)), DMA((nz,)), DMA((nz, 2, ne - 1)), DMA((nz, 2, ne - 1)),
        DMA((2,)), DMA((slots,)), pltpu.SemaphoreType.REGULAR,
        DMA((nz, 2, max(pairs - 1, 1))), DMA((nz, 2, max(pairs - 1, 1))),
        DMA((nz, 2)), DMA((nz, 2)),
    ]
    fits = size <= 54_000_000 and stages >= 1 and nz > 1 and nz * pairs > slots
    return fits, slots, [pltpu.VMEM(*v) for v in vmem] + sems


def moe_net(h, g_all, w_gate, w_up, w_down, nz, ne, fl, slots, scratch, cid):
    rows, wide = h.shape
    per_dev, width, _ = w_gate.shape
    return pl.pallas_call(
        functools.partial(moe_net_kernel, nz, ne, per_dev, slots),
        out_shape=[
            jax.ShapeDtypeStruct((nz * ne, rows, wide), BF),
            jax.ShapeDtypeStruct((nz * ne, rows, width), BF),
            jax.ShapeDtypeStruct((rows, wide), F32),
            jax.ShapeDtypeStruct((width, 2 * per_dev * fl), BF),
            jax.ShapeDtypeStruct((per_dev * fl, width), F32),
        ],
        in_specs=[VMEM, ANY, ANY, ANY, ANY],
        out_specs=[ANY, ANY, VMEM, ANY, ANY],
        scratch_shapes=scratch,
        compiler_params=pltpu.CompilerParams(
            collective_id=cid, has_side_effects=True, vmem_limit_bytes=66_500_000
        ),
        name="moe_net",
    )(h, g_all.reshape(nz * ne, rows, width), w_gate, w_up, w_down)


def body(inputs, segments, routes, w_qkv, w_out, w_router, gains, w_gate, w_up, w_down, cotangent):
    z = lax.axis_index("dp")
    e = lax.axis_index("expert")
    nz = lax.axis_size("dp")
    ne = lax.axis_size("expert")
    count, width = inputs.shape
    num_seqs, length = segments.shape
    heads = width // HD // ne
    hw = heads * HD
    expert_count = w_router.shape[1]
    per_dev = w_gate.shape[0]
    hidden = w_gate.shape[2]
    fl = hidden // nz
    both = ("dp", "expert")

    pad = -(expert_count + 4) % 16
    small = jnp.concatenate(
        [w_router.T, gains.T, jnp.zeros((pad, gains.shape[0]), BF)], axis=0
    )
    seg8 = jnp.broadcast_to(segments[:, None, :], (num_seqs, 8, length)).reshape(-1, length)
    in_all, wq, wo, small, seg_all, g_all = start_gather(
        inputs, w_qkv.transpose(1, 0, 2), w_out, small, seg8, cotangent, nz, ne, hw, 0
    )
    small = small.transpose(1, 0, 2).reshape(-1, width)
    router_t = small[:expert_count]
    gain_mat = small[expert_count : expert_count + 4].astype(F32)
    my_gains = lax.dynamic_slice_in_dim(gain_mat, e * hw, hw, axis=1)
    seg_all = seg_all.reshape(ne * num_seqs, 8, length)

    g_all = g_all.reshape(-1, width)
    inputs_f = inputs.astype(F32)
    tables = rope_lanes(length)
    *saved, x1_part = attn_fwd(in_all, wq, wo, gain_mat, my_gains, seg_all, tables, 9)
    (x1_sum,) = scatter_tokens(x1_part, nz, ne, False, 1)
    x1 = inputs_f + x1_sum

    a2 = rms_scale(x1)
    h2 = (x1 * a2 * gain_mat[3]).astype(BF)
    probs = jax.nn.softmax(dot(h2, router_t, NT), axis=-1)
    picks = jnp.sum(
        (routes[:, :, None] == jnp.arange(expert_count, dtype=jnp.int32)).astype(F32), axis=1
    )
    gates = picks * probs

    split = 64
    high = gates.astype(BF)
    low = (gates - high.astype(F32)).astype(BF)
    blank = jnp.zeros((count, split - expert_count), BF)
    h2_wide = jnp.concatenate([h2, high, blank, low, blank], axis=1)
    wide = width + 2 * split
    fits, slots, scratch = moe_net_scratch(nz, ne, per_dev, count, width, wide, fl)
    if fits:
        _, mix, gh_sum, dwin, dwd = moe_net(
            h2_wide, g_all, w_gate, w_up, w_down, nz, ne, fl, slots, scratch, 2
        )
        mix = mix.reshape(-1, width)
    else:
        h2_all = gather_tokens(h2_wide, nz, ne, True, 2).reshape(-1, wide)
        wg = lax.dynamic_slice_in_dim(w_gate, z * fl, fl, axis=2)
        wu = lax.dynamic_slice_in_dim(w_up, z * fl, fl, axis=2)
        wd = lax.dynamic_slice_in_dim(w_down, z * fl, fl, axis=1).reshape(per_dev * fl, width)
        w_in = jnp.concatenate([*wg, *wu], axis=1)
        mix, gh, dwin, dwd = moe(h2_all, g_all, w_in, wd, per_dev, count, min(4, ne))
        gh_sum, mix = scatter_tokens(
            gh.reshape(nz * ne, count, wide), nz, ne, True, 3, after=mix.reshape(-1, width)
        )
    grad_from_experts = gh_sum[:, :width]
    grad_gates = (
        gh_sum[:, width : width + expert_count]
        + gh_sum[:, width + split : width + split + expert_count]
    )

    dwin = lax.all_to_all(
        dwin.reshape(nz, width // nz, 2 * per_dev * fl),
        "dp", split_axis=0, concat_axis=0, tiled=True,
    )
    grad_w_gate, grad_w_up = lay_experts(dwin, per_dev, fl)
    grad_w_down = dwd.reshape(per_dev, fl, width)

    grad_top = cotangent.astype(F32)
    grad_probs = picks * grad_gates
    glog = (probs * (grad_probs - jnp.sum(probs * grad_probs, axis=-1, keepdims=True))).astype(BF)
    local_router = dot(glog, h2, TN)
    gh2 = grad_from_experts + dot(glog, router_t, NN)
    grad_ffn, gain_ffn = rms_backward(x1, a2, gain_mat[3], gh2)
    gx1 = grad_top + grad_ffn
    gab = gx1.astype(BF)

    gab_all = gather_tokens(gab, nz, ne, False, 4)
    gh1_part, parts, gain_qk, x1_mix = attn_bwd(
        gab_all, wq, wo, my_gains, seg_all, tables, saved, x1,
        mix.reshape(-1, count, width) if fits and split_ranks(nz)[0] else None, nz, 10,
    )
    place = lambda part: lax.dynamic_update_slice_in_dim(
        jnp.zeros((1, width), F32), part[None], e * hw, axis=1
    )
    tiny = jnp.concatenate(
        [
            local_router, jnp.zeros((1, width), F32), place(gain_qk[0]), place(gain_qk[1]),
            gain_ffn[None], jnp.zeros((-(expert_count + 4) % 8, width), F32),
        ],
        axis=0,
    )
    grad_inputs, laid, tiny, output = tail(
        parts, gh1_part, mix.reshape(-1, count, width) if fits else None, inputs, x1_mix, gx1,
        gain_mat, tiny, expert_count, nz, ne, hw, 5,
    )
    if not fits:
        mix = lax.psum_scatter(mix, both, scatter_dimension=0, tiled=True)
        output = add_up(x1, mix)
    grad_w_qkv = laid[:-1].astype(F32).transpose(1, 0, 2)
    grad_w_out = laid[-1].astype(F32)
    grad_w_router = tiny[:expert_count].T
    grad_gains = tiny[expert_count : expert_count + 4].T
    return (
        output,
        grad_inputs,
        grad_w_qkv,
        grad_w_out,
        grad_w_router,
        grad_gains,
        grad_w_gate,
        grad_w_up,
        grad_w_down,
    )


def solution(mesh):
    tokens = P(("dp", "expert"), None)
    rows = P("dp", None)
    rows3 = P("dp", None, None)
    owned = P("expert", None, None)
    return jax.shard_map(
        body,
        mesh=mesh,
        in_specs=(tokens, tokens, tokens, rows3, rows, rows, rows, owned, owned, owned, tokens),
        out_specs=(tokens, tokens, rows3, rows, rows, rows)
        + (P("expert", "dp", None),) * 3,
        check_vma=False,
    )
```
